32 devices in a mesh: ctx: 4 (over x, core), seq: 2 (over y), tp: 4 (over z).
Axes of the slice: x: 2, y: 2, z: 4, core: 2. Of those that a mesh axis runs over, the one named last changes fastest.
Arguments:
- tokens: bfloat16 [2, 2048, 2048], P('seq', 'ctx'), may hold values from -8 to 8
- out_grad: bfloat16 [2, 2048, 2048], P('seq', 'ctx'), may hold values from -6 to 6
- group_order: int32 [2, 8], P('seq'), may hold values from 0 to 7, each once within a row
- w_query: bfloat16 [2048, 2048], P(None, 'tp'), may hold values from -5 to 5
- w_key: bfloat16 [2048, 2048], P(None, 'tp'), may hold values from -5 to 5
- w_value: bfloat16 [2048, 2048], P(None, 'tp'), may hold values from -0.125 to 0.125
- query_gain: float32 [16, 128], P('tp'), may hold values from 0.5 to 2
- key_gain: float32 [16, 128], P('tp'), may hold values from 0.5 to 2
- w_output: bfloat16 [2048, 2048], P('tp'), may hold values from -0.125 to 0.125
- attn_gain: float32 [2048], replicated, may hold values from 0.5 to 1.5
- w_gate: bfloat16 [2048, 8192], P(None, 'tp'), may hold values from -0.125 to 0.125
- w_up: bfloat16 [2048, 8192], P(None, 'tp'), may hold values from -0.125 to 0.125
- w_down: bfloat16 [8192, 2048], P('tp'), may hold values from -0.0625 to 0.0625
- mlp_gain: float32 [2048], replicated, may hold values from 0.5 to 1.5
Outputs:
- block_out: float32 [2, 2048, 2048], P('seq', 'ctx')
- input_grad: float32 [2, 2048, 2048], P('seq', 'ctx')
- grad_query: float32 [2048, 2048], P(('ctx', 'seq'), 'tp')
- grad_key: float32 [2048, 2048], P(('ctx', 'seq'), 'tp')
- grad_value: float32 [2048, 2048], P(('ctx', 'seq'), 'tp')
- grad_query_gain: float32 [16, 128], P('tp', ('ctx', 'seq'))
- grad_key_gain: float32 [16, 128], P('tp', ('ctx', 'seq'))
- grad_output: float32 [2048, 2048], P('tp', ('ctx', 'seq'))
- grad_attn_gain: float32 [2048], P(('ctx', 'seq'))
- grad_gate: float32 [2048, 8192], P(('ctx', 'seq'), 'tp')
- grad_up: float32 [2048, 8192], P(('ctx', 'seq'), 'tp')
- grad_down: float32 [8192, 2048], P('tp', ('ctx', 'seq'))
- grad_mlp_gain: float32 [2048], P(('ctx', 'seq'))
The draws below stay inside these ranges and needn't reach their ends.
Inputs may be any that keep to these rules, and one draw needn't show every extreme that they name: Each row of group_order names every block of the sequence once.
All inputs are finite; a program needn't handle non-finite values.
Results may differ from the reference program's by a relative error of at most 0.04.
Values may be sent and summed in bfloat16 or wider, within the bound.
A program may use at most 320 MiB of HBM per device.

```python
import math
import jax
import jax.numpy as jnp
from jax import lax

D = 2048
HEADS = 16
HD = 128
FF = 8192
TOK_DEV = 512
SEQS = 2
L = 2048
N_CTX = 4


def column_scales(key):
    picked = jax.random.randint(key, (HEADS,), 0, HD)
    col_index = jnp.arange(D, dtype=jnp.int32)
    head_of = col_index // HD
    chosen = jnp.sum(jnp.where(head_of[:, None] == jnp.arange(HEADS, dtype=jnp.int32)[None, :], picked[None, :], 0), axis=1)
    return jnp.where(col_index % HD == chosen, 10.0, 1.0).astype(jnp.float32)


def projection_draw(key):
    noise = jnp.clip(jax.random.normal(key, (D, D), jnp.float32), -4.0, 4.0) * (1.0 / math.sqrt(D))
    noise = noise * column_scales(jax.random.fold_in(key, 5))[None, :]
    result = noise
    return result.astype(jnp.bfloat16)


def gain_draw(key):
    lower_log = jnp.full((HEADS, HD), math.log(0.5), jnp.float32)
    spread = jax.random.uniform(key, (HEADS, HD), jnp.float32)
    return jnp.exp(lower_log + spread * (math.log(2.0) - lower_log)).astype(jnp.float32)


def draw_w_query(key, part):
    return projection_draw(jax.random.fold_in(key, 11))


def draw_w_key(key, part):
    return projection_draw(jax.random.fold_in(key, 12))


def draw_query_gain(key, part):
    return gain_draw(jax.random.fold_in(key, 21))


def draw_key_gain(key, part):
    return gain_draw(jax.random.fold_in(key, 22))


def draw_tokens(key, part):
    base = jnp.clip(jax.random.normal(jax.random.fold_in(key, 31), (SEQS, L, D), jnp.float32), -6.0, 6.0)
    result = base
    return result.astype(jnp.bfloat16)


def levels(key, extent, pieces, smallest, largest):
    factor_of = 1.0
    for position, blocks in pieces:
        steps = jax.random.uniform(jax.random.fold_in(jax.random.fold_in(key, 6), position), (blocks,), jnp.float32, smallest / len(pieces), largest / len(pieces))
        factor_of = factor_of * jnp.repeat(jnp.exp(steps), extent[position] // blocks).reshape((-1,) + (1,) * (len(extent) - 1 - position))
    return factor_of


def centred(rng, dims, scale, reach, cuts=(), kind=jnp.bfloat16):
    gain = levels(rng, dims, cuts, -0.22, 0.18) if cuts else 1.0
    array = jax.random.normal(rng, dims, jnp.float32) * scale * gain
    return jnp.minimum(jnp.maximum(array, -reach), reach).astype(kind)


def setup_inputs(seed: int = 0) -> dict:
    key_list = jax.random.split(jax.random.key(seed), 15)
    return {
        "tokens": draw_tokens(jax.random.fold_in(key_list[14], 71), 0),
        "out_grad": centred(key_list[1], (SEQS, L, D), 1.0, 6.0, ((0, 2), (1, 4))),
        "group_order": jax.vmap(lambda own: jax.random.permutation(own, 2 * N_CTX))(jax.random.split(key_list[2], SEQS)).reshape((SEQS, 2 * N_CTX)).astype(jnp.int32),
        "w_query": draw_w_query(jax.random.fold_in(key_list[14], 71), 0),
        "w_key": draw_w_key(jax.random.fold_in(key_list[14], 71), 0),
        "w_value": centred(key_list[5], (D, D), D ** -0.5, 0.125, ((1, 4),)),
        "query_gain": draw_query_gain(jax.random.fold_in(key_list[14], 71), 0),
        "key_gain": draw_key_gain(jax.random.fold_in(key_list[14], 71), 0),
        "w_output": centred(key_list[8], (D, D), D ** -0.5, 0.125, ((0, 4),)),
        "attn_gain": jnp.clip(jax.random.uniform(key_list[9], (D,), jnp.float32, 0.5, 1.5), 0.5, 1.5),
        "w_gate": centred(key_list[10], (D, FF), D ** -0.5, 0.125, ((1, 4),)),
        "w_up": centred(key_list[11], (D, FF), D ** -0.5, 0.125, ((1, 4),)),
        "w_down": centred(key_list[12], (FF, D), FF ** -0.5, 0.0625, ((0, 4),)),
        "mlp_gain": jnp.clip(jax.random.uniform(key_list[13], (D,), jnp.float32, 0.5, 1.5), 0.5, 1.5),
    }


norm_eps = 1e-06
rope_base = 500000.0
masked_score = -1e+30

def matmul(left, right):
    return jnp.dot(left, right, preferred_element_type=jnp.float32)

def rope_tables(positions):
    half = HD // 2
    rates = rope_base ** (-(jnp.arange(half, dtype=jnp.float32) * 2.0 / HD))
    angle = positions.astype(jnp.float32)[:, None] * rates[None, :]
    return (jnp.cos(angle), jnp.sin(angle))

def rotate(heads_in, cosine, sine):
    half = heads_in.shape[-1] // 2
    first, second = (heads_in[..., :half], heads_in[..., half:])
    cosine, sine = (cosine[:, None, :], sine[:, None, :])
    return jnp.concatenate([first * cosine - second * sine, second * cosine + first * sine], axis=-1)

def unrotate(grads_in, cosine, sine):
    half = grads_in.shape[-1] // 2
    first, second = (grads_in[..., :half], grads_in[..., half:])
    cosine, sine = (cosine[:, None, :], sine[:, None, :])
    return jnp.concatenate([first * cosine + second * sine, second * cosine - first * sine], axis=-1)

def head_forward(query, keys, values, positions):
    block = 1024 if L % 1024 == 0 else L
    scale = HD ** (-0.5)

    def one_block(index):
        query_block = lax.dynamic_slice_in_dim(query, index * block, block, 0)
        query_pos = lax.dynamic_slice_in_dim(positions, index * block, block, 0)
        scores = matmul(query_block, keys.T) * scale
        mask = positions[None, :] <= query_pos[:, None]
        peak = lax.optimization_barrier(jnp.max(jnp.where(mask, scores, masked_score), axis=1))
        share = jnp.where(mask, jnp.exp(scores - peak[:, None]), 0.0)
        total = lax.optimization_barrier(jnp.sum(share, axis=1))
        mixed = matmul(share.astype(jnp.bfloat16), values) / total[:, None]
        return (mixed.astype(jnp.bfloat16), peak + jnp.log(total))
    mixed, log_total = lax.map(one_block, jnp.arange(L // block, dtype=jnp.int32))
    return (mixed.reshape(L, HD), log_total.reshape(L))

def head_backward(query, keys, values, upstream, log_total, delta, positions):
    block = 1024 if L % 1024 == 0 else L
    scale = HD ** (-0.5)

    def one_block(carry, index):
        key_grad, value_grad = carry
        query_block = lax.dynamic_slice_in_dim(query, index * block, block, 0)
        up_block = lax.dynamic_slice_in_dim(upstream, index * block, block, 0)
        total_block = lax.dynamic_slice_in_dim(log_total, index * block, block, 0)
        delta_block = lax.dynamic_slice_in_dim(delta, index * block, block, 0)
        query_pos = lax.dynamic_slice_in_dim(positions, index * block, block, 0)
        scores = matmul(query_block, keys.T) * scale
        mask = positions[None, :] <= query_pos[:, None]
        share = jnp.where(mask, jnp.exp(scores - total_block[:, None]), 0.0)
        share_grad = matmul(up_block, values.T)
        score_grad = (share * (share_grad - delta_block[:, None]) * scale).astype(jnp.bfloat16)
        query_grad = matmul(score_grad, keys)
        key_grad = key_grad + matmul(score_grad.T, query_block)
        value_grad = value_grad + matmul(share.astype(jnp.bfloat16).T, up_block)
        return ((key_grad, value_grad), query_grad)
    zeros = jnp.zeros((L, HD), jnp.float32)
    (key_grad, value_grad), query_grad = lax.scan(one_block, (zeros, zeros), jnp.arange(L // block, dtype=jnp.int32))
    return (query_grad.reshape(L, HD), key_grad, value_grad)

def sequence_pass(tokens, out_grad, order, w_query, w_key, w_value, query_gain, key_gain, w_output, attn_gain, w_gate, w_up, w_down, mlp_gain):
    group = TOK_DEV // 2
    row_ids = jnp.arange(L, dtype=jnp.int32)
    positions = order[row_ids // group] * group + row_ids % group
    cosine, sine = rope_tables(positions)
    inputs = tokens.astype(jnp.float32)
    query = matmul(tokens, w_query)
    keyraw = matmul(tokens, w_key)
    values = matmul(tokens, w_value).astype(jnp.bfloat16)
    query_scale = lax.rsqrt(lax.optimization_barrier(jnp.mean(query * query, axis=1)) + norm_eps)
    key_scale = lax.rsqrt(lax.optimization_barrier(jnp.mean(keyraw * keyraw, axis=1)) + norm_eps)
    query_norm = query * query_scale[:, None]
    key_norm = keyraw * key_scale[:, None]
    qgain = query_gain.reshape(D)
    kgain = key_gain.reshape(D)
    query_rot = rotate((query_norm * qgain).reshape(L, HEADS, HD), cosine, sine).astype(jnp.bfloat16)
    key_rot = rotate((key_norm * kgain).reshape(L, HEADS, HD), cosine, sine).astype(jnp.bfloat16)
    query_heads = query_rot.transpose(1, 0, 2)
    key_heads = key_rot.transpose(1, 0, 2)
    value_heads = values.reshape(L, HEADS, HD).transpose(1, 0, 2)
    mixed, log_total = lax.map(lambda items: head_forward(items[0], items[1], items[2], positions), (query_heads, key_heads, value_heads))
    attn_flat = mixed.transpose(1, 0, 2).reshape(L, D)
    proj = matmul(attn_flat, w_output)
    attn_scale = lax.rsqrt(lax.optimization_barrier(jnp.mean(proj * proj, axis=1)) + norm_eps)
    attn_norm = proj * attn_scale[:, None]
    resid = inputs + attn_norm * attn_gain
    hidden = resid.astype(jnp.bfloat16)
    gate = matmul(hidden, w_gate)
    up = matmul(hidden, w_up)
    sigma = jax.nn.sigmoid(gate)
    active = gate * sigma
    inner = (active * up).astype(jnp.bfloat16)
    down = matmul(inner, w_down)
    mlp_scale = lax.rsqrt(lax.optimization_barrier(jnp.mean(down * down, axis=1)) + norm_eps)
    mlp_norm = down * mlp_scale[:, None]
    block_out = resid + mlp_norm * mlp_gain
    upstream = out_grad.astype(jnp.float32)
    d_mlp_gain = lax.optimization_barrier(jnp.sum(upstream * mlp_norm, axis=0))
    d_mnorm = upstream * mlp_gain
    d_down = (mlp_scale[:, None] * (d_mnorm - mlp_norm * lax.optimization_barrier(jnp.mean(d_mnorm * mlp_norm, axis=1, keepdims=True)))).astype(jnp.bfloat16)
    grad_down = matmul(inner.T, d_down)
    d_inner = matmul(d_down, w_down.T)
    d_gate = (d_inner * up * sigma * (1.0 + gate * (1.0 - sigma))).astype(jnp.bfloat16)
    d_up = (d_inner * active).astype(jnp.bfloat16)
    grad_gate = matmul(hidden.T, d_gate)
    grad_up = matmul(hidden.T, d_up)
    d_resid = upstream + matmul(d_gate, w_gate.T) + matmul(d_up, w_up.T)
    d_attn_gain = lax.optimization_barrier(jnp.sum(d_resid * attn_norm, axis=0))
    d_anorm = d_resid * attn_gain
    d_proj = (attn_scale[:, None] * (d_anorm - attn_norm * lax.optimization_barrier(jnp.mean(d_anorm * attn_norm, axis=1, keepdims=True)))).astype(jnp.bfloat16)
    grad_output = matmul(attn_flat.T, d_proj)
    d_attn = matmul(d_proj, w_output.T).astype(jnp.bfloat16)
    d_attn_heads = d_attn.reshape(L, HEADS, HD).transpose(1, 0, 2)
    delta = lax.optimization_barrier(jnp.sum(d_attn_heads.astype(jnp.float32) * mixed.astype(jnp.float32), axis=2))
    d_qrot, d_krot, d_vals = lax.map(lambda items: head_backward(items[0], items[1], items[2], items[3], items[4], items[5], positions), (query_heads, key_heads, value_heads, d_attn_heads, log_total, delta))
    d_qhead = unrotate(d_qrot.transpose(1, 0, 2), cosine, sine).reshape(L, D)
    d_khead = unrotate(d_krot.transpose(1, 0, 2), cosine, sine).reshape(L, D)
    d_value = d_vals.transpose(1, 0, 2).reshape(L, D).astype(jnp.bfloat16)
    d_query_gain = lax.optimization_barrier(jnp.sum(d_qhead * query_norm, axis=0)).reshape(HEADS, HD)
    d_key_gain = lax.optimization_barrier(jnp.sum(d_khead * key_norm, axis=0)).reshape(HEADS, HD)
    d_qnorm = d_qhead * qgain
    d_knorm = d_khead * kgain
    d_query = (query_scale[:, None] * (d_qnorm - query_norm * lax.optimization_barrier(jnp.mean(d_qnorm * query_norm, axis=1, keepdims=True)))).astype(jnp.bfloat16)
    d_key = (key_scale[:, None] * (d_knorm - key_norm * lax.optimization_barrier(jnp.mean(d_knorm * key_norm, axis=1, keepdims=True)))).astype(jnp.bfloat16)
    grad_query = matmul(tokens.T, d_query)
    grad_key = matmul(tokens.T, d_key)
    grad_value = matmul(tokens.T, d_value)
    input_grad = d_resid + matmul(d_query, w_query.T) + matmul(d_key, w_key.T) + matmul(d_value, w_value.T)
    grads = (grad_query, grad_key, grad_value, d_query_gain, d_key_gain, grad_output, d_attn_gain, grad_gate, grad_up, grad_down, d_mlp_gain)
    return (block_out, input_grad, grads)

def reference(tokens, out_grad, group_order, w_query, w_key, w_value, query_gain, key_gain, w_output, attn_gain, w_gate, w_up, w_down, mlp_gain):

    def step(carry, items):
        block_out, input_grad, grads = sequence_pass(items[0], items[1], items[2], w_query, w_key, w_value, query_gain, key_gain, w_output, attn_gain, w_gate, w_up, w_down, mlp_gain)
        carry = tuple((old + new for old, new in zip(carry, grads)))
        return (carry, (block_out, input_grad))
    zeros = (jnp.zeros((D, D), jnp.float32), jnp.zeros((D, D), jnp.float32), jnp.zeros((D, D), jnp.float32), jnp.zeros((HEADS, HD), jnp.float32), jnp.zeros((HEADS, HD), jnp.float32), jnp.zeros((D, D), jnp.float32), jnp.zeros((D,), jnp.float32), jnp.zeros((D, FF), jnp.float32), jnp.zeros((D, FF), jnp.float32), jnp.zeros((FF, D), jnp.float32), jnp.zeros((D,), jnp.float32))
    grads, (block_out, input_grad) = lax.scan(step, zeros, (tokens, out_grad, group_order))
    return (block_out, input_grad, grads[0], grads[1], grads[2], grads[3], grads[4], grads[5], grads[6], grads[7], grads[8], grads[9], grads[10])
```

```python
import jax
import jax.numpy as jnp
from jax import lax
from jax.sharding import PartitionSpec as P
from jax.experimental import pallas as pl
from jax.experimental.pallas import tpu as pltpu

MESH = pl.DeviceIdType.MESH

def line_allreduce(x, n, blocks, chains, cid):
    rows, width = x.shape
    W = width // n
    rc = rows // blocks
    C = blocks // chains
    M = C * n

    def kernel(x_ref, out_ref, own, recv_l, recv_r, res, ssr, ssl, rsl, rsr):
        i = lax.axis_index("tp")
        has_l, has_r = i > 0, i < n - 1
        bar = pltpu.get_barrier_semaphore()
        @pl.when(has_l)
        def _():
            pl.semaphore_signal(bar, inc=1, device_id={"tp": i - 1}, device_id_type=MESH)
        @pl.when(has_r)
        def _():
            pl.semaphore_signal(bar, inc=1, device_id={"tp": i + 1}, device_id_type=MESH)
        for j in range(n):
            own[j] = x_ref[:, j * W:(j + 1) * W]
        pl.semaphore_wait(bar, has_l.astype(jnp.int32) + has_r.astype(jnp.int32))

        def rows_of(g, p):
            b = (p // n) * chains + g
            return pl.ds(pl.multiple_of(b * rc, rc), rc)

        def right(src, dst, g, p, j):
            sl = rows_of(g, p)
            return pltpu.make_async_remote_copy(src.at[j, sl], dst.at[j, sl], ssr.at[g, p], rsl.at[g, p],
                                                device_id={"tp": i + 1}, device_id_type=MESH)
        def left(src, dst, g, q, j):
            sl = rows_of(g, q)
            return pltpu.make_async_remote_copy(src.at[j, sl], dst.at[j, sl], ssl.at[g, q], rsr.at[g, q],
                                                device_id={"tp": i - 1}, device_id_type=MESH)
        def wait_l(g, p, j):
            sl = rows_of(g, p)
            pltpu.make_async_remote_copy(own.at[j, sl], recv_l.at[j, sl], ssr.at[g, p], rsl.at[g, p],
                                         device_id={"tp": i - 1}, device_id_type=MESH).wait_recv()
        def wait_r(g, q, j):
            sl = rows_of(g, q)
            pltpu.make_async_remote_copy(own.at[j, sl], recv_r.at[j, sl], ssl.at[g, q], rsr.at[g, q],
                                         device_id={"tp": i + 1}, device_id_type=MESH).wait_recv()

        def step(t, _):
            for g in range(chains):
                p = t - i
                q = t - (n - 1 - i)
                pm = lax.rem(p + n * M, n)
                jr = n - 1 - pm
                jl = lax.rem(q + n * M, n)
                pv = (p >= 0) & (p < M)
                qv = (q >= 0) & (q < M)
                @pl.when(pv & has_l)
                def _():
                    wait_l(g, p, jr)
                @pl.when(qv & has_r)
                def _():
                    wait_r(g, q, jl)
                @pl.when(pv & (jr > i))
                def _():
                    sl = rows_of(g, p)
                    @pl.when(has_l)
                    def _():
                        own[jr, sl] = (own[jr, sl].astype(jnp.float32) + recv_l[jr, sl].astype(jnp.float32)).astype(jnp.bfloat16)
                    right(own, recv_l, g, p, jr).start()
                @pl.when(qv & (jl < i))
                def _():
                    sl = rows_of(g, q)
                    @pl.when(has_r)
                    def _():
                        own[jl, sl] = (own[jl, sl].astype(jnp.float32) + recv_r[jl, sl].astype(jnp.float32)).astype(jnp.bfloat16)
                    left(own, recv_r, g, q, jl).start()
                @pl.when(pv & (jr == i))
                def _():
                    sl = rows_of(g, p)
                    @pl.when(has_l & has_r)
                    def _():
                        res[i, sl] = (own[i, sl].astype(jnp.float32) + recv_l[i, sl].astype(jnp.float32) + recv_r[i, sl].astype(jnp.float32)).astype(jnp.bfloat16)
                    @pl.when(jnp.logical_not(has_l))
                    def _():
                        res[i, sl] = (own[i, sl].astype(jnp.float32) + recv_r[i, sl].astype(jnp.float32)).astype(jnp.bfloat16)
                    @pl.when(jnp.logical_not(has_r))
                    def _():
                        res[i, sl] = (own[i, sl].astype(jnp.float32) + recv_l[i, sl].astype(jnp.float32)).astype(jnp.bfloat16)
                @pl.when(pv & (jr <= i) & has_r)
                def _():
                    right(res, res, g, p, jr).start()
                @pl.when(qv & (jl >= i) & has_l)
                def _():
                    left(res, res, g, q, jl).start()
            return 0
        lax.fori_loop(0, M + n - 1, step, 0)

        def drain(p, _):
            for g in range(chains):
                @pl.when(has_r)
                def _():
                    right(own, recv_l, g, p, 0).wait_send()
                @pl.when(has_l)
                def _():
                    left(own, recv_r, g, p, 0).wait_send()
            return 0
        lax.fori_loop(0, M, drain, 0)
        for j in range(n):
            out_ref[:, j * W:(j + 1) * W] = res[j]

    return pl.pallas_call(
        kernel,
        out_shape=jax.ShapeDtypeStruct((rows, width), jnp.bfloat16),
        in_specs=[pl.BlockSpec(memory_space=pltpu.VMEM)],
        out_specs=pl.BlockSpec(memory_space=pltpu.VMEM),
        scratch_shapes=[pltpu.VMEM((n, rows, W), jnp.bfloat16)] * 4 + [pltpu.SemaphoreType.DMA((chains, M))] * 4,
        compiler_params=pltpu.CompilerParams(collective_id=cid, has_side_effects=True, vmem_limit_bytes=40 * 2**20),
        name=f"line_ar_{blocks}_{chains}",
    )(x)

norm_eps = 1e-06
rope_base = 500000.0
masked_score = -1e30


def matmul(left, right):
    return jnp.dot(left, right, preferred_element_type=jnp.float32)


def rope_tables(positions, head_dim):
    half = head_dim // 2
    rates = rope_base ** (-(jnp.arange(half, dtype=jnp.float32) * 2.0 / head_dim))
    angle = positions.astype(jnp.float32)[:, None] * rates[None, :]
    return (jnp.cos(angle), jnp.sin(angle))


def rotate(heads_in, cosine, sine):
    half = heads_in.shape[-1] // 2
    first, second = (heads_in[..., :half], heads_in[..., half:])
    cosine, sine = (cosine[:, None, :], sine[:, None, :])
    return jnp.concatenate(
        [first * cosine - second * sine, second * cosine + first * sine], axis=-1
    )


def unrotate(grads_in, cosine, sine):
    half = grads_in.shape[-1] // 2
    first, second = (grads_in[..., :half], grads_in[..., half:])
    cosine, sine = (cosine[:, None, :], sine[:, None, :])
    return jnp.concatenate(
        [first * cosine + second * sine, second * cosine - first * sine], axis=-1
    )


def key_positions(order, first_row, count, group):
    row_ids = first_row + jnp.arange(count, dtype=jnp.int32)
    slots = row_ids // group
    picks = slots[:, None] == jnp.arange(order.shape[0], dtype=jnp.int32)[None, :]
    return jnp.sum(jnp.where(picks, order[None, :], 0), axis=1) * group + row_ids % group


def gather_pair(keys, values):
    return (
        lax.all_gather(keys, "ctx", axis=0, tiled=True),
        lax.all_gather(values, "ctx", axis=0, tiled=True),
    )


def tp_sum(partial, cid):
    n = lax.axis_size("tp")
    summed = line_allreduce(partial.astype(jnp.bfloat16), n, 16, 8, cid)
    return summed.astype(jnp.float32)


def per_device(
    tokens,
    out_grad,
    group_order,
    w_query,
    w_key,
    w_value,
    query_gain,
    key_gain,
    w_output,
    attn_gain,
    w_gate,
    w_up,
    w_down,
    mlp_gain,
):
    inputs_bf = tokens[0]
    order = group_order[0]
    row_count, width = inputs_bf.shape
    heads, head_dim = query_gain.shape
    local = heads * head_dim
    group = row_count // 2
    scale = head_dim ** (-0.5)
    query_pos = key_positions(order, lax.axis_index("ctx") * row_count, row_count, group)
    cosine, sine = rope_tables(query_pos, head_dim)
    inputs = inputs_bf.astype(jnp.float32)
    query = matmul(inputs_bf, w_query)
    keyraw = matmul(inputs_bf, w_key)
    values = matmul(inputs_bf, w_value).astype(jnp.bfloat16)
    query_sq, key_sq = lax.psum(
        (jnp.sum(query * query, axis=1), jnp.sum(keyraw * keyraw, axis=1)), "tp"
    )
    query_scale = lax.rsqrt(query_sq / width + norm_eps)
    key_scale = lax.rsqrt(key_sq / width + norm_eps)
    query_norm = query * query_scale[:, None]
    key_norm = keyraw * key_scale[:, None]
    qgain = query_gain.reshape(local)
    kgain = key_gain.reshape(local)
    query_rot = rotate(
        (query_norm * qgain).reshape(row_count, heads, head_dim), cosine, sine
    ).astype(jnp.bfloat16)
    key_rot = rotate((key_norm * kgain).reshape(row_count, heads, head_dim), cosine, sine).astype(
        jnp.bfloat16
    )
    key_flat = key_rot.reshape(row_count, local)
    start_state = (
        jnp.full((heads, row_count), masked_score, jnp.float32),
        jnp.zeros((heads, row_count), jnp.float32),
        jnp.zeros((heads, row_count, head_dim), jnp.float32),
    )
    keys_in = lax.all_gather(key_flat, "ctx", axis=0, tiled=True)
    values_in = lax.all_gather(values, "ctx", axis=0, tiled=True)
    count = keys_in.shape[0]
    attend_block = 512
    keys_in = keys_in.reshape(count // attend_block, attend_block, heads, head_dim)
    values_in = values_in.reshape(count // attend_block, attend_block, heads, head_dim)
    key_pos = key_positions(order, jnp.int32(0), count, group).reshape(
        count // attend_block, attend_block
    )

    def one_block(state, item):
        peak_old, total, accum = state
        key_block, value_block, pos_block = item
        scores = (
            jnp.einsum("qhd,khd->hqk", query_rot, key_block, preferred_element_type=jnp.float32)
            * scale
        )
        mask = (pos_block[None, :] <= query_pos[:, None])[None]
        peak = jnp.maximum(peak_old, jnp.max(jnp.where(mask, scores, masked_score), axis=2))
        share = jnp.where(mask, jnp.exp(scores - peak[:, :, None]), 0.0)
        fade = jnp.exp(peak_old - peak)
        total = total * fade + jnp.sum(share, axis=2)
        accum = accum * fade[:, :, None] + jnp.einsum(
            "hqk,khd->hqd",
            share.astype(jnp.bfloat16),
            value_block,
            preferred_element_type=jnp.float32,
        )
        return ((peak, total, accum), None)

    state, unused = lax.scan(one_block, start_state, (keys_in, values_in, key_pos))
    peak, total, accum = state
    log_total = peak + jnp.log(total)
    mixed = (accum / total[:, :, None]).astype(jnp.bfloat16)
    attn_flat = mixed.transpose(1, 0, 2).reshape(row_count, local)
    proj = tp_sum(matmul(attn_flat, w_output), 1)
    attn_scale = lax.rsqrt(jnp.mean(proj * proj, axis=1) + norm_eps)
    attn_norm = proj * attn_scale[:, None]
    resid = inputs + attn_norm * attn_gain
    hidden = resid.astype(jnp.bfloat16)
    gate = matmul(hidden, w_gate)
    up = matmul(hidden, w_up)
    sigma = jax.nn.sigmoid(gate)
    active = gate * sigma
    inner = (active * up).astype(jnp.bfloat16)
    down = tp_sum(matmul(inner, w_down), 2)
    mlp_scale = lax.rsqrt(jnp.mean(down * down, axis=1) + norm_eps)
    mlp_norm = down * mlp_scale[:, None]
    block_out = resid + mlp_norm * mlp_gain
    upstream = out_grad[0].astype(jnp.float32)
    d_mlp_gain = jnp.sum(upstream * mlp_norm, axis=0)
    d_mnorm = upstream * mlp_gain
    d_down = (
        mlp_scale[:, None]
        * (d_mnorm - mlp_norm * jnp.mean(d_mnorm * mlp_norm, axis=1, keepdims=True))
    ).astype(jnp.bfloat16)
    grad_down = matmul(inner.T, d_down)
    d_inner = matmul(d_down, w_down.T)
    d_gate = (d_inner * up * sigma * (1.0 + gate * (1.0 - sigma))).astype(jnp.bfloat16)
    d_up = (d_inner * active).astype(jnp.bfloat16)
    grad_gate = matmul(hidden.T, d_gate)
    grad_up = matmul(hidden.T, d_up)
    d_resid = upstream + tp_sum(matmul(d_gate, w_gate.T) + matmul(d_up, w_up.T), 3)
    d_attn_gain = jnp.sum(d_resid * attn_norm, axis=0)
    d_anorm = d_resid * attn_gain
    d_proj = (
        attn_scale[:, None]
        * (d_anorm - attn_norm * jnp.mean(d_anorm * attn_norm, axis=1, keepdims=True))
    ).astype(jnp.bfloat16)
    grad_output = matmul(attn_flat.T, d_proj)
    d_attn = matmul(d_proj, w_output.T).astype(jnp.bfloat16)
    d_attn_heads = d_attn.reshape(row_count, heads, head_dim)
    delta = jnp.sum(
        d_attn_heads.transpose(1, 0, 2).astype(jnp.float32) * mixed.astype(jnp.float32), axis=2
    )
    whole_keys, whole_values = gather_pair(key_flat, values)
    count = whole_keys.shape[0]
    block = 512
    key_blocks = whole_keys.reshape(count // block, block, heads, head_dim)
    value_blocks = whole_values.reshape(count // block, block, heads, head_dim)
    pos_blocks = key_positions(order, 0, count, group).reshape(count // block, block)
    zero_grads = jnp.zeros((row_count, heads, head_dim), jnp.float32)

    def back_block(query_grad, item):
        key_block, value_block, pos_block = item
        scores = (
            jnp.einsum("qhd,khd->hqk", query_rot, key_block, preferred_element_type=jnp.float32)
            * scale
        )
        mask = (pos_block[None, :] <= query_pos[:, None])[None]
        share = jnp.where(mask, jnp.exp(scores - log_total[:, :, None]), 0.0)
        share_grad = jnp.einsum(
            "qhd,khd->hqk", d_attn_heads, value_block, preferred_element_type=jnp.float32
        )
        score_grad = (share * (share_grad - delta[:, :, None]) * scale).astype(jnp.bfloat16)
        query_grad = query_grad + jnp.einsum(
            "hqk,khd->qhd", score_grad, key_block, preferred_element_type=jnp.float32
        )
        key_grad = jnp.einsum(
            "hqk,qhd->khd", score_grad, query_rot, preferred_element_type=jnp.float32
        )
        value_grad = jnp.einsum(
            "hqk,qhd->khd",
            share.astype(jnp.bfloat16),
            d_attn_heads,
            preferred_element_type=jnp.float32,
        )
        return (
            query_grad,
            jnp.concatenate(
                [key_grad.reshape(block, local), value_grad.reshape(block, local)], axis=1
            ),
        )

    d_qrot, kv_terms = lax.scan(back_block, zero_grads, (key_blocks, value_blocks, pos_blocks))
    kv_grads = lax.psum_scatter(
        kv_terms.reshape(count, 2 * local).astype(jnp.bfloat16), "ctx", scatter_dimension=0, tiled=True
    )
    kv_grads = kv_grads.astype(jnp.float32)
    d_krot = kv_grads[:, :local].reshape(row_count, heads, head_dim)
    d_value = kv_grads[:, local:].astype(jnp.bfloat16)
    d_qhead = unrotate(d_qrot, cosine, sine).reshape(row_count, local)
    d_khead = unrotate(d_krot, cosine, sine).reshape(row_count, local)
    d_query_gain = jnp.sum(d_qhead * query_norm, axis=0).reshape(heads, head_dim)
    d_key_gain = jnp.sum(d_khead * key_norm, axis=0).reshape(heads, head_dim)
    d_qnorm = d_qhead * qgain
    d_knorm = d_khead * kgain
    query_dot, key_dot = lax.psum(
        (jnp.sum(d_qnorm * query_norm, axis=1), jnp.sum(d_knorm * key_norm, axis=1)), "tp"
    )
    d_query = (query_scale[:, None] * (d_qnorm - query_norm * (query_dot / width)[:, None])).astype(
        jnp.bfloat16
    )
    d_key = (key_scale[:, None] * (d_knorm - key_norm * (key_dot / width)[:, None])).astype(
        jnp.bfloat16
    )
    grad_query = matmul(inputs_bf.T, d_query)
    grad_key = matmul(inputs_bf.T, d_key)
    grad_value = matmul(inputs_bf.T, d_value)
    input_grad = d_resid + tp_sum(
        matmul(d_query, w_query.T) + matmul(d_key, w_key.T) + matmul(d_value, w_value.T), 4
    )
    summed = (
        lax.psum_scatter(grad_query.astype(jnp.bfloat16), ("ctx", "seq"), scatter_dimension=0, tiled=True).astype(jnp.float32),
        lax.psum_scatter(grad_key.astype(jnp.bfloat16), ("ctx", "seq"), scatter_dimension=0, tiled=True).astype(jnp.float32),
        lax.psum_scatter(grad_value.astype(jnp.bfloat16), ("ctx", "seq"), scatter_dimension=0, tiled=True).astype(jnp.float32),
        lax.psum_scatter(d_query_gain, ("ctx", "seq"), scatter_dimension=1, tiled=True),
        lax.psum_scatter(d_key_gain, ("ctx", "seq"), scatter_dimension=1, tiled=True),
        lax.psum_scatter(grad_output.astype(jnp.bfloat16), ("ctx", "seq"), scatter_dimension=1, tiled=True).astype(jnp.float32),
        lax.psum_scatter(d_attn_gain, ("ctx", "seq"), scatter_dimension=0, tiled=True),
        lax.psum_scatter(grad_gate.astype(jnp.bfloat16), ("ctx", "seq"), scatter_dimension=0, tiled=True).astype(jnp.float32),
        lax.psum_scatter(grad_up.astype(jnp.bfloat16), ("ctx", "seq"), scatter_dimension=0, tiled=True).astype(jnp.float32),
        lax.psum_scatter(grad_down.astype(jnp.bfloat16), ("ctx", "seq"), scatter_dimension=1, tiled=True).astype(jnp.float32),
        lax.psum_scatter(d_mlp_gain, ("ctx", "seq"), scatter_dimension=0, tiled=True),
    )
    return (
        block_out[None],
        input_grad[None],
        summed[0],
        summed[1],
        summed[2],
        summed[3],
        summed[4],
        summed[5],
        summed[6],
        summed[7],
        summed[8],
        summed[9],
        summed[10],
    )


def solution(mesh):
    return jax.shard_map(
        per_device,
        mesh=mesh,
        in_specs=(
            P("seq", "ctx", None),
            P("seq", "ctx", None),
            P("seq", None),
            P(None, "tp"),
            P(None, "tp"),
            P(None, "tp"),
            P("tp", None),
            P("tp", None),
            P("tp", None),
            P(),
            P(None, "tp"),
            P(None, "tp"),
            P("tp", None),
            P(),
        ),
        out_specs=(
            P("seq", "ctx", None),
            P("seq", "ctx", None),
            P(("ctx", "seq"), "tp"),
            P(("ctx", "seq"), "tp"),
            P(("ctx", "seq"), "tp"),
            P("tp", ("ctx", "seq")),
            P("tp", ("ctx", "seq")),
            P("tp", ("ctx", "seq")),
            P(("ctx", "seq")),
            P(("ctx", "seq"), "tp"),
            P(("ctx", "seq"), "tp"),
            P("tp", ("ctx", "seq")),
            P(("ctx", "seq")),
        ),
        check_vma=False,
    )
```

```python
import jax
import jax.numpy as jnp
from jax import lax
from jax.sharding import PartitionSpec as P
from jax.experimental import pallas as pl
from jax.experimental.pallas import tpu as pltpu

MESH = pl.DeviceIdType.MESH
bf16 = jnp.bfloat16
f32 = jnp.float32
lanes = 128
row_blocks = 16
row_chains = 8


def remote(src, dst, send, recv, where):
    return pltpu.make_async_remote_copy(
        src, dst, send, recv, device_id=where, device_id_type=MESH
    )


class LineSum:
    def __init__(self, n, rows, width):
        self.n, self.rows, self.width = n, rows, width
        self.part = width // n
        self.rc = rows // row_blocks
        self.total = row_blocks // row_chains * n
        self.steps = self.total + n - 1

    def scratch(self):
        shape = (self.n, self.rows, self.part)
        return [pltpu.VMEM(shape, bf16)] * 4 + [
            pltpu.SemaphoreType.DMA((row_chains, self.total))
        ] * 4

    def bind(self, refs):
        self.own, self.from_l, self.from_r, self.res = refs[:4]
        self.send_r, self.send_l, self.recv_l, self.recv_r = refs[4:]
        self.i = lax.axis_index("tp")
        self.has_l, self.has_r = self.i > 0, self.i < self.n - 1

    def greet(self, bar):
        @pl.when(self.has_l)
        def _():
            pl.semaphore_signal(bar, inc=1, device_id={"tp": self.i - 1}, device_id_type=MESH)

        @pl.when(self.has_r)
        def _():
            pl.semaphore_signal(bar, inc=1, device_id={"tp": self.i + 1}, device_id_type=MESH)

        return self.has_l.astype(jnp.int32) + self.has_r.astype(jnp.int32)

    def load(self, x_ref):
        for j in range(self.n):
            self.own[j] = x_ref[:, j * self.part : (j + 1) * self.part]

    def rows_of(self, g, p):
        block = (p // self.n) * row_chains + g
        return pl.ds(pl.multiple_of(block * self.rc, self.rc), self.rc)

    def right(self, src, dst, g, p, j):
        sl = self.rows_of(g, p)
        return remote(
            src.at[j, sl], dst.at[j, sl], self.send_r.at[g, p], self.recv_l.at[g, p],
            {"tp": self.i + 1},
        )

    def left(self, src, dst, g, q, j):
        sl = self.rows_of(g, q)
        return remote(
            src.at[j, sl], dst.at[j, sl], self.send_l.at[g, q], self.recv_r.at[g, q],
            {"tp": self.i - 1},
        )

    def wait_l(self, g, p, j):
        sl = self.rows_of(g, p)
        remote(
            self.own.at[j, sl], self.from_l.at[j, sl], self.send_r.at[g, p], self.recv_l.at[g, p],
            {"tp": self.i - 1},
        ).wait_recv()

    def wait_r(self, g, q, j):
        sl = self.rows_of(g, q)
        remote(
            self.own.at[j, sl], self.from_r.at[j, sl], self.send_l.at[g, q], self.recv_r.at[g, q],
            {"tp": self.i + 1},
        ).wait_recv()

    def step(self, t):
        n, i, has_l, has_r = self.n, self.i, self.has_l, self.has_r
        own, from_l, from_r, res = self.own, self.from_l, self.from_r, self.res
        for g in range(row_chains):
            p = t - i
            q = t - (n - 1 - i)
            jr = n - 1 - lax.rem(p + n * self.total, n)
            jl = lax.rem(q + n * self.total, n)
            pv = (p >= 0) & (p < self.total)
            qv = (q >= 0) & (q < self.total)

            @pl.when(pv & has_l)
            def _():
                self.wait_l(g, p, jr)

            @pl.when(qv & has_r)
            def _():
                self.wait_r(g, q, jl)

            @pl.when(pv & (jr > i))
            def _():
                sl = self.rows_of(g, p)

                @pl.when(has_l)
                def _():
                    own[jr, sl] = (own[jr, sl].astype(f32) + from_l[jr, sl].astype(f32)).astype(bf16)

                self.right(own, from_l, g, p, jr).start()

            @pl.when(qv & (jl < i))
            def _():
                sl = self.rows_of(g, q)

                @pl.when(has_r)
                def _():
                    own[jl, sl] = (own[jl, sl].astype(f32) + from_r[jl, sl].astype(f32)).astype(bf16)

                self.left(own, from_r, g, q, jl).start()

            @pl.when(pv & (jr == i))
            def _():
                sl = self.rows_of(g, p)

                @pl.when(has_l & has_r)
                def _():
                    res[i, sl] = (
                        own[i, sl].astype(f32) + from_l[i, sl].astype(f32) + from_r[i, sl].astype(f32)
                    ).astype(bf16)

                @pl.when(jnp.logical_not(has_l))
                def _():
                    res[i, sl] = (own[i, sl].astype(f32) + from_r[i, sl].astype(f32)).astype(bf16)

                @pl.when(jnp.logical_not(has_r))
                def _():
                    res[i, sl] = (own[i, sl].astype(f32) + from_l[i, sl].astype(f32)).astype(bf16)

            @pl.when(pv & (jr <= i) & has_r)
            def _():
                self.right(res, res, g, p, jr).start()

            @pl.when(qv & (jl >= i) & has_l)
            def _():
                self.left(res, res, g, q, jl).start()

    def drain(self):
        def one(p, carry):
            for g in range(row_chains):

                @pl.when(self.has_r)
                def _():
                    self.right(self.own, self.from_l, g, p, 0).wait_send()

                @pl.when(self.has_l)
                def _():
                    self.left(self.own, self.from_r, g, p, 0).wait_send()

            return carry

        lax.fori_loop(0, self.total, one, 0)

    def store(self, out_ref):
        for j in range(self.n):
            out_ref[:, j * self.part : (j + 1) * self.part] = self.res[j]


class GradScatter:
    def __init__(self, n_ctx, n_seq, width, jobs):
        self.nx, self.ny = n_ctx // 2, n_seq
        self.rows = width // (n_ctx * n_seq)
        self.jobs = jobs
        start = 0
        self.spans = []
        for job in jobs:
            self.spans.append((start, start + job["count"]))
            start += job["count"]
        self.total = start
        self.steps = start + 5

    def scratch(self):
        nx, ny, r, t = self.nx, self.ny, self.rows, self.total
        tile = (r, lanes)
        sem = pltpu.SemaphoreType.DMA
        return [
            pltpu.VMEM((2, nx, ny, 2) + tile, bf16),
            pltpu.VMEM((2, nx, ny, 2) + tile, f32),
            pltpu.VMEM((t, nx, ny, 2) + tile, bf16),
            pltpu.VMEM((3, nx, ny) + tile, bf16),
            pltpu.VMEM((3, ny, nx) + tile, bf16),
            pltpu.VMEM((t, nx - 1, ny) + tile, bf16),
            pltpu.VMEM((t, ny - 1, nx) + tile, bf16),
            pltpu.VMEM((3, ny) + tile, bf16),
            pltpu.VMEM((3, nx) + tile, bf16),
            pltpu.VMEM((t, ny - 1) + tile, bf16),
            pltpu.VMEM((t, nx - 1) + tile, bf16),
            sem((2,)), sem((t,)),
            sem((3, nx - 1)), sem((t, nx - 1)), sem((3, ny - 1)), sem((t, ny - 1)),
            sem((3, ny - 1)), sem((t, ny - 1)), sem((3, nx - 1)), sem((t, nx - 1)),
        ]

    def bind(self, refs, at_refs, b_refs, out_refs):
        (self.send0, self.keep, self.recv0, self.pa, self.pb, self.r1a, self.r1b, self.qa, self.qb,
         self.r2a, self.r2b, self.s0, self.d0, self.s1a, self.d1a, self.s1b, self.d1b,
         self.s2a, self.d2a, self.s2b, self.d2b) = refs
        self.at_refs, self.b_refs, self.out_refs = at_refs, b_refs, out_refs
        ctx = lax.axis_index("ctx")
        self.mx, self.core, self.my = ctx // 2, lax.rem(ctx, 2), lax.axis_index("seq")

    def at_x(self, d):
        return {"ctx": lax.rem(self.mx + d, self.nx) * 2 + self.core}

    def at_y(self, d):
        return {"seq": lax.rem(self.my + d, self.ny)}

    def at_mate(self):
        return {"ctx": self.mx * 2 + 1 - self.core}

    def greet(self, bar):
        places = [self.at_mate()]
        places += [self.at_x(d) for d in range(1, self.nx)]
        places += [self.at_y(d) for d in range(1, self.ny)]
        for place in places:
            pl.semaphore_signal(bar, inc=1, device_id=place, device_id_type=MESH)
        return len(places)

    def c0(self, c, slot):
        return remote(self.send0.at[slot], self.recv0.at[c], self.s0.at[slot], self.d0.at[c], self.at_mate())

    def c1a(self, c, slot, d):
        return remote(
            self.pa.at[slot, lax.rem(self.mx + d, self.nx)], self.r1a.at[c, d - 1],
            self.s1a.at[slot, d - 1], self.d1a.at[c, d - 1], self.at_x(d),
        )

    def c1b(self, c, slot, d):
        return remote(
            self.pb.at[slot, lax.rem(self.my + d, self.ny)], self.r1b.at[c, d - 1],
            self.s1b.at[slot, d - 1], self.d1b.at[c, d - 1], self.at_y(d),
        )

    def c2a(self, c, slot, d):
        return remote(
            self.qa.at[slot, lax.rem(self.my + d, self.ny)], self.r2a.at[c, d - 1],
            self.s2a.at[slot, d - 1], self.d2a.at[c, d - 1], self.at_y(d),
        )

    def c2b(self, c, slot, d):
        return remote(
            self.qb.at[slot, lax.rem(self.mx + d, self.nx)], self.r2b.at[c, d - 1],
            self.s2b.at[slot, d - 1], self.d2b.at[c, d - 1], self.at_x(d),
        )

    def make(self, c):
        slot = lax.rem(c, 2)
        nx, ny, r = self.nx, self.ny, self.rows

        @pl.when(c >= 2)
        def _():
            self.c0(c, slot).wait_send()

        def products(at_ref, b_ref, col, parity, write):
            def tile(e, carry):
                x, y = e // ny, lax.rem(e, ny)
                row = pl.multiple_of(((x * 2 + parity) * ny + y) * r, r)
                acc = jnp.dot(
                    at_ref[pl.ds(row, r), :], b_ref[:, pl.ds(col, 2 * lanes)],
                    preferred_element_type=f32,
                )
                write(x, y, acc)
                return carry

            lax.fori_loop(0, nx * ny, tile, 0)

        def to_send(x, y, acc):
            self.send0[slot, x, y, 0] = acc[:, :lanes].astype(bf16)
            self.send0[slot, x, y, 1] = acc[:, lanes:].astype(bf16)

        def to_keep(x, y, acc):
            self.keep[slot, x, y, 0] = acc[:, :lanes]
            self.keep[slot, x, y, 1] = acc[:, lanes:]

        for job, (lo, hi) in zip(self.jobs, self.spans):

            @pl.when((c >= lo) & (c < hi))
            def _():
                at_ref, b_ref = self.at_refs[job["a"]], self.b_refs[job["b"]]
                col = pl.multiple_of((c - lo + job["first"]) * (2 * lanes), 2 * lanes)
                products(at_ref, b_ref, col, 1 - self.core, to_send)
                self.c0(c, slot).start()
                products(at_ref, b_ref, col, self.core, to_keep)

    def pair(self, c):
        slot = lax.rem(c, 3)
        nx, ny = self.nx, self.ny

        @pl.when(c >= 3)
        def _():
            for d in range(1, nx):
                self.c1a(c, slot, d).wait_send()
            for d in range(1, ny):
                self.c1b(c, slot, d).wait_send()

        self.c0(c, lax.rem(c, 2)).wait_recv()
        for x in range(nx):
            for y in range(ny):
                self.pa[slot, x, y] = (
                    self.keep[lax.rem(c, 2), x, y, 0] + self.recv0[c, x, y, 0].astype(f32)
                ).astype(bf16)
        for d in range(1, nx):
            self.c1a(c, slot, d).start()
        for x in range(nx):
            for y in range(ny):
                self.pb[slot, y, x] = (
                    self.keep[lax.rem(c, 2), x, y, 1] + self.recv0[c, x, y, 1].astype(f32)
                ).astype(bf16)
        for d in range(1, ny):
            self.c1b(c, slot, d).start()

    def cross(self, c):
        slot = lax.rem(c, 3)
        nx, ny = self.nx, self.ny

        @pl.when(c >= 3)
        def _():
            for d in range(1, ny):
                self.c2a(c, slot, d).wait_send()
            for d in range(1, nx):
                self.c2b(c, slot, d).wait_send()

        for d in range(1, nx):
            self.c1a(c, slot, d).wait_recv()
        for y in range(ny):
            acc = self.pa[slot, self.mx, y].astype(f32)
            for d in range(1, nx):
                acc = acc + self.r1a[c, d - 1, y].astype(f32)
            self.qa[slot, y] = acc.astype(bf16)
        for d in range(1, ny):
            self.c2a(c, slot, d).start()
        for d in range(1, ny):
            self.c1b(c, slot, d).wait_recv()
        for x in range(nx):
            acc = self.pb[slot, self.my, x].astype(f32)
            for d in range(1, ny):
                acc = acc + self.r1b[c, d - 1, x].astype(f32)
            self.qb[slot, x] = acc.astype(bf16)
        for d in range(1, nx):
            self.c2b(c, slot, d).start()

    def finish(self, c):
        slot = lax.rem(c, 3)
        nx, ny = self.nx, self.ny
        for d in range(1, ny):
            self.c2a(c, slot, d).wait_recv()
        for d in range(1, nx):
            self.c2b(c, slot, d).wait_recv()
        for job, (lo, hi) in zip(self.jobs, self.spans):

            @pl.when((c >= lo) & (c < hi))
            def _():
                out_ref = self.out_refs[job["out"]]
                col = pl.multiple_of((c - lo + job["place"]) * (2 * lanes), 2 * lanes)
                acc = self.qa[slot, self.my].astype(f32)
                for d in range(1, ny):
                    acc = acc + self.r2a[c, d - 1].astype(f32)
                out_ref[:, pl.ds(col, lanes)] = acc
                acc = self.qb[slot, self.mx].astype(f32)
                for d in range(1, nx):
                    acc = acc + self.r2b[c, d - 1].astype(f32)
                out_ref[:, pl.ds(col + lanes, lanes)] = acc

    def early(self, it):
        @pl.when((it >= 5) & (it < self.total + 5))
        def _():
            self.finish(it - 5)

        @pl.when((it >= 3) & (it < self.total + 3))
        def _():
            self.cross(it - 3)

        @pl.when((it >= 1) & (it < self.total + 1))
        def _():
            self.pair(it - 1)

    def late(self, it):
        @pl.when(it < self.total)
        def _():
            self.make(it)

    def drain(self):
        for c in range(max(self.total - 2, 0), self.total):
            self.c0(c, c % 2).wait_send()
        for c in range(max(self.total - 3, 0), self.total):
            slot = c % 3
            for d in range(1, self.nx):
                self.c1a(c, slot, d).wait_send()
                self.c2b(c, slot, d).wait_send()
            for d in range(1, self.ny):
                self.c1b(c, slot, d).wait_send()
                self.c2a(c, slot, d).wait_send()


class GainSum:
    def __init__(self, n_ctx, n_seq):
        self.ny, self.n = n_seq, n_ctx * n_seq

    def scratch(self):
        sem = pltpu.SemaphoreType.DMA
        return [pltpu.VMEM((self.n - 1, 8, lanes), f32), sem((self.n - 1,)), sem((self.n - 1,))]

    def bind(self, refs, in_ref, out_ref):
        self.got, self.sent, self.done = refs
        self.in_ref, self.out_ref = in_ref, out_ref
        self.me = lax.axis_index("ctx") * self.ny + lax.axis_index("seq")

    def place(self, d):
        to = lax.rem(self.me + d, self.n)
        return to, {"ctx": to // self.ny, "seq": lax.rem(to, self.ny)}

    def copy(self, d):
        to, where = self.place(d)
        return remote(self.in_ref.at[to], self.got.at[d - 1], self.sent.at[d - 1], self.done.at[d - 1], where)

    def greet(self, bar):
        for d in range(1, self.n):
            pl.semaphore_signal(bar, inc=1, device_id=self.place(d)[1], device_id_type=MESH)
        return self.n - 1

    def start(self):
        for d in range(1, self.n):
            self.copy(d).start()

    def finish(self):
        acc = self.in_ref[self.me]
        for d in range(1, self.n):
            self.copy(d).wait_recv()
            acc = acc + self.got[d - 1]
        self.out_ref[...] = acc
        for d in range(1, self.n):
            self.copy(d).wait_send()


def vmem_spec():
    return pl.BlockSpec(memory_space=pltpu.VMEM)


def comm_call(body, args, outs, scratch, cid, name):
    return pl.pallas_call(
        body,
        out_shape=outs,
        in_specs=[vmem_spec()] * len(args),
        out_specs=[vmem_spec()] * len(outs),
        scratch_shapes=scratch,
        compiler_params=pltpu.CompilerParams(
            collective_id=cid, has_side_effects=True, vmem_limit_bytes=62 * 2**20
        ),
        name=name,
    )(*args)


def tp_sum(partial, cid):
    rows, width = partial.shape
    line = LineSum(lax.axis_size("tp"), rows, width)

    def body(x_ref, out_ref, *refs):
        line.bind(refs)
        bar = pltpu.get_barrier_semaphore()
        peers = line.greet(bar)
        line.load(x_ref)
        pl.semaphore_wait(bar, peers)

        def one(t, carry):
            line.step(t)
            return carry

        lax.fori_loop(0, line.steps, one, 0)
        line.drain()
        line.store(out_ref)

    out = jax.ShapeDtypeStruct((rows, width), bf16)
    (summed,) = comm_call(body, [partial.astype(bf16)], [out], line.scratch(), cid, "tp_sum")
    return summed.astype(f32)


def sum_and_scatter(partial, ats, bs, jobs, out_widths, cid, gains=None):
    rows, width = partial.shape
    n_ctx, n_seq = lax.axis_size("ctx"), lax.axis_size("seq")
    line = LineSum(lax.axis_size("tp"), rows, width)
    grads = GradScatter(n_ctx, n_seq, width, jobs)
    small = GainSum(n_ctx, n_seq)
    small_in = [] if gains is None else [gains]
    na, nb, no, ns = len(ats), len(bs), len(out_widths), len(small_in)
    n_line, n_grads = len(line.scratch()), len(grads.scratch())

    def body(x_ref, *refs):
        at_refs, b_refs = refs[:na], refs[na : na + nb]
        refs = refs[na + nb :]
        small_refs, refs = refs[:ns], refs[ns:]
        out_ref, grad_refs, refs = refs[0], refs[1 : 1 + no], refs[1 + no :]
        small_out, scratch = refs[:ns], refs[ns:]
        line.bind(scratch[:n_line])
        grads.bind(scratch[n_line : n_line + n_grads], at_refs, b_refs, grad_refs)
        bar = pltpu.get_barrier_semaphore()
        peers = line.greet(bar)
        if ns:
            small.bind(scratch[n_line + n_grads :], small_refs[0], small_out[0])
            peers = peers + small.greet(bar)
        else:
            peers = peers + grads.greet(bar)
        line.load(x_ref)
        pl.semaphore_wait(bar, peers)
        if ns:
            small.start()

        def one(it, carry):
            grads.early(it)

            @pl.when(it < line.steps)
            def _():
                line.step(it)

            grads.late(it)
            return carry

        lax.fori_loop(0, max(line.steps, grads.steps), one, 0)
        if ns:
            small.finish()
        line.drain()
        grads.drain()
        line.store(out_ref)

    outs = [jax.ShapeDtypeStruct((rows, width), bf16)] + [
        jax.ShapeDtypeStruct((grads.rows, w), f32) for w in out_widths
    ]
    outs += [jax.ShapeDtypeStruct((8, lanes), f32)] * ns
    res = comm_call(
        body, [partial.astype(bf16)] + list(ats) + list(bs) + small_in, outs,
        line.scratch() + grads.scratch() + (small.scratch() if ns else []), cid, "sum_and_scatter",
    )
    return res[0].astype(f32), res[1:]


norm_eps = 1e-06
rope_base = 500000.0
masked_score = -1e30


def matmul(left, right):
    return jnp.dot(left, right, preferred_element_type=jnp.float32)


def rope_tables(positions, head_dim):
    half = head_dim // 2
    rates = rope_base ** (-(jnp.arange(half, dtype=jnp.float32) * 2.0 / head_dim))
    angle = positions.astype(jnp.float32)[:, None] * rates[None, :]
    return (jnp.cos(angle), jnp.sin(angle))


def rotate(heads_in, cosine, sine):
    half = heads_in.shape[-1] // 2
    first, second = (heads_in[..., :half], heads_in[..., half:])
    cosine, sine = (cosine[:, None, :], sine[:, None, :])
    return jnp.concatenate(
        [first * cosine - second * sine, second * cosine + first * sine], axis=-1
    )


def unrotate(grads_in, cosine, sine):
    half = grads_in.shape[-1] // 2
    first, second = (grads_in[..., :half], grads_in[..., half:])
    cosine, sine = (cosine[:, None, :], sine[:, None, :])
    return jnp.concatenate(
        [first * cosine + second * sine, second * cosine - first * sine], axis=-1
    )


def key_positions(order, first_row, count, group):
    row_ids = first_row + jnp.arange(count, dtype=jnp.int32)
    slots = row_ids // group
    picks = slots[:, None] == jnp.arange(order.shape[0], dtype=jnp.int32)[None, :]
    return jnp.sum(jnp.where(picks, order[None, :], 0), axis=1) * group + row_ids % group


def gather_pair(keys, values):
    return (
        lax.all_gather(keys, "ctx", axis=0, tiled=True),
        lax.all_gather(values, "ctx", axis=0, tiled=True),
    )


def per_device(
    tokens,
    out_grad,
    group_order,
    w_query,
    w_key,
    w_value,
    query_gain,
    key_gain,
    w_output,
    attn_gain,
    w_gate,
    w_up,
    w_down,
    mlp_gain,
):
    inputs_bf = tokens[0]
    order = group_order[0]
    row_count, width = inputs_bf.shape
    heads, head_dim = query_gain.shape
    local = heads * head_dim
    group = row_count // 2
    scale = head_dim ** (-0.5)
    query_pos = key_positions(order, lax.axis_index("ctx") * row_count, row_count, group)
    cosine, sine = rope_tables(query_pos, head_dim)
    inputs = inputs_bf.astype(jnp.float32)
    query = matmul(inputs_bf, w_query)
    keyraw = matmul(inputs_bf, w_key)
    values = matmul(inputs_bf, w_value).astype(jnp.bfloat16)
    query_sq, key_sq = lax.psum(
        (jnp.sum(query * query, axis=1), jnp.sum(keyraw * keyraw, axis=1)), "tp"
    )
    query_scale = lax.rsqrt(query_sq / width + norm_eps)
    key_scale = lax.rsqrt(key_sq / width + norm_eps)
    query_norm = query * query_scale[:, None]
    key_norm = keyraw * key_scale[:, None]
    qgain = query_gain.reshape(local)
    kgain = key_gain.reshape(local)
    query_rot = rotate(
        (query_norm * qgain).reshape(row_count, heads, head_dim), cosine, sine
    ).astype(jnp.bfloat16)
    key_rot = rotate((key_norm * kgain).reshape(row_count, heads, head_dim), cosine, sine).astype(
        jnp.bfloat16
    )
    key_flat = key_rot.reshape(row_count, local)
    start_state = (
        jnp.full((heads, row_count), masked_score, jnp.float32),
        jnp.zeros((heads, row_count), jnp.float32),
        jnp.zeros((heads, row_count, head_dim), jnp.float32),
    )
    keys_in = lax.all_gather(key_flat, "ctx", axis=0, tiled=True)
    values_in = lax.all_gather(values, "ctx", axis=0, tiled=True)
    count = keys_in.shape[0]
    attend_block = 512
    keys_in = keys_in.reshape(count // attend_block, attend_block, heads, head_dim)
    values_in = values_in.reshape(count // attend_block, attend_block, heads, head_dim)
    key_pos = key_positions(order, jnp.int32(0), count, group).reshape(
        count // attend_block, attend_block
    )

    def one_block(state, item):
        peak_old, total, accum = state
        key_block, value_block, pos_block = item
        scores = (
            jnp.einsum("qhd,khd->hqk", query_rot, key_block, preferred_element_type=jnp.float32)
            * scale
        )
        mask = (pos_block[None, :] <= query_pos[:, None])[None]
        peak = jnp.maximum(peak_old, jnp.max(jnp.where(mask, scores, masked_score), axis=2))
        share = jnp.where(mask, jnp.exp(scores - peak[:, :, None]), 0.0)
        fade = jnp.exp(peak_old - peak)
        total = total * fade + jnp.sum(share, axis=2)
        accum = accum * fade[:, :, None] + jnp.einsum(
            "hqk,khd->hqd",
            share.astype(jnp.bfloat16),
            value_block,
            preferred_element_type=jnp.float32,
        )
        return ((peak, total, accum), None)

    state, unused = lax.scan(one_block, start_state, (keys_in, values_in, key_pos))
    peak, total, accum = state
    log_total = peak + jnp.log(total)
    mixed = (accum / total[:, :, None]).astype(jnp.bfloat16)
    attn_flat = mixed.transpose(1, 0, 2).reshape(row_count, local)
    proj = tp_sum(matmul(attn_flat, w_output), 1)
    attn_scale = lax.rsqrt(jnp.mean(proj * proj, axis=1) + norm_eps)
    attn_norm = proj * attn_scale[:, None]
    resid = inputs + attn_norm * attn_gain
    hidden = resid.astype(jnp.bfloat16)
    gate = matmul(hidden, w_gate)
    up = matmul(hidden, w_up)
    sigma = jax.nn.sigmoid(gate)
    active = gate * sigma
    inner = (active * up).astype(jnp.bfloat16)
    down = tp_sum(matmul(inner, w_down), 2)
    mlp_scale = lax.rsqrt(jnp.mean(down * down, axis=1) + norm_eps)
    mlp_norm = down * mlp_scale[:, None]
    block_out = resid + mlp_norm * mlp_gain
    upstream = out_grad[0].astype(jnp.float32)
    d_mlp_gain = jnp.sum(upstream * mlp_norm, axis=0)
    d_mnorm = upstream * mlp_gain
    d_down = (
        mlp_scale[:, None]
        * (d_mnorm - mlp_norm * jnp.mean(d_mnorm * mlp_norm, axis=1, keepdims=True))
    ).astype(jnp.bfloat16)
    d_inner = matmul(d_down, w_down.T)
    d_gate = (d_inner * up * sigma * (1.0 + gate * (1.0 - sigma))).astype(jnp.bfloat16)
    d_up = (d_inner * active).astype(jnp.bfloat16)
    hidden_t = hidden.T
    wide = inner.shape[1] // (2 * lanes)
    half = wide // 2
    back, (grad_down, grad_gate_a) = sum_and_scatter(
        matmul(d_gate, w_gate.T) + matmul(d_up, w_up.T),
        [d_down.T, hidden_t],
        [inner, d_gate],
        [
            dict(a=0, b=0, first=0, count=wide, out=0, place=0),
            dict(a=1, b=1, first=0, count=half, out=1, place=0),
        ],
        [inner.shape[1], half * 2 * lanes],
        3,
    )
    d_resid = upstream + back
    d_attn_gain = jnp.sum(d_resid * attn_norm, axis=0)
    d_anorm = d_resid * attn_gain
    d_proj = (
        attn_scale[:, None]
        * (d_anorm - attn_norm * jnp.mean(d_anorm * attn_norm, axis=1, keepdims=True))
    ).astype(jnp.bfloat16)
    d_attn = matmul(d_proj, w_output.T).astype(jnp.bfloat16)
    d_attn_heads = d_attn.reshape(row_count, heads, head_dim)
    delta = jnp.sum(
        d_attn_heads.transpose(1, 0, 2).astype(jnp.float32) * mixed.astype(jnp.float32), axis=2
    )
    whole_keys, whole_values = gather_pair(key_flat, values)
    count = whole_keys.shape[0]
    block = 512
    key_blocks = whole_keys.reshape(count // block, block, heads, head_dim)
    value_blocks = whole_values.reshape(count // block, block, heads, head_dim)
    pos_blocks = key_positions(order, 0, count, group).reshape(count // block, block)
    zero_grads = jnp.zeros((row_count, heads, head_dim), jnp.float32)

    def back_block(query_grad, item):
        key_block, value_block, pos_block = item
        scores = (
            jnp.einsum("qhd,khd->hqk", query_rot, key_block, preferred_element_type=jnp.float32)
            * scale
        )
        mask = (pos_block[None, :] <= query_pos[:, None])[None]
        share = jnp.where(mask, jnp.exp(scores - log_total[:, :, None]), 0.0)
        share_grad = jnp.einsum(
            "qhd,khd->hqk", d_attn_heads, value_block, preferred_element_type=jnp.float32
        )
        score_grad = (share * (share_grad - delta[:, :, None]) * scale).astype(jnp.bfloat16)
        query_grad = query_grad + jnp.einsum(
            "hqk,khd->qhd", score_grad, key_block, preferred_element_type=jnp.float32
        )
        key_grad = jnp.einsum(
            "hqk,qhd->khd", score_grad, query_rot, preferred_element_type=jnp.float32
        )
        value_grad = jnp.einsum(
            "hqk,qhd->khd",
            share.astype(jnp.bfloat16),
            d_attn_heads,
            preferred_element_type=jnp.float32,
        )
        return (
            query_grad,
            jnp.concatenate(
                [key_grad.reshape(block, local), value_grad.reshape(block, local)], axis=1
            ),
        )

    d_qrot, kv_terms = lax.scan(back_block, zero_grads, (key_blocks, value_blocks, pos_blocks))
    kv_grads = lax.psum_scatter(
        kv_terms.reshape(count, 2 * local).astype(jnp.bfloat16), "ctx", scatter_dimension=0, tiled=True
    )
    kv_grads = kv_grads.astype(jnp.float32)
    d_krot = kv_grads[:, :local].reshape(row_count, heads, head_dim)
    d_value = kv_grads[:, local:].astype(jnp.bfloat16)
    d_qhead = unrotate(d_qrot, cosine, sine).reshape(row_count, local)
    d_khead = unrotate(d_krot, cosine, sine).reshape(row_count, local)
    d_query_gain = jnp.sum(d_qhead * query_norm, axis=0).reshape(heads, head_dim)
    d_key_gain = jnp.sum(d_khead * key_norm, axis=0).reshape(heads, head_dim)
    d_qnorm = d_qhead * qgain
    d_knorm = d_khead * kgain
    query_dot, key_dot = lax.psum(
        (jnp.sum(d_qnorm * query_norm, axis=1), jnp.sum(d_knorm * key_norm, axis=1)), "tp"
    )
    d_query = (query_scale[:, None] * (d_qnorm - query_norm * (query_dot / width)[:, None])).astype(
        jnp.bfloat16
    )
    d_key = (key_scale[:, None] * (d_knorm - key_norm * (key_dot / width)[:, None])).astype(
        jnp.bfloat16
    )
    thin = local // (2 * lanes)
    owners = lax.axis_size("ctx") * lax.axis_size("seq")
    pieces = [
        d_attn_gain.reshape(owners, -1),
        d_mlp_gain.reshape(owners, -1),
        d_query_gain.reshape(heads, owners, -1).transpose(1, 0, 2).reshape(owners, -1),
        d_key_gain.reshape(heads, owners, -1).transpose(1, 0, 2).reshape(owners, -1),
    ]
    cuts = [piece.shape[1] for piece in pieces]
    packed = jnp.concatenate(pieces, axis=1)
    packed = jnp.pad(packed, ((0, 0), (0, 8 * lanes - packed.shape[1]))).reshape(owners, 8, lanes)
    back, (grad_gate_b, grad_up, grad_qkv, grad_output, small) = sum_and_scatter(
        matmul(d_query, w_query.T) + matmul(d_key, w_key.T) + matmul(d_value, w_value.T),
        [hidden_t, inputs_bf.T, d_proj.T],
        [d_gate, d_up, d_query, d_key, d_value, attn_flat],
        [
            dict(a=0, b=0, first=half, count=wide - half, out=0, place=0),
            dict(a=0, b=1, first=0, count=wide, out=1, place=0),
            dict(a=2, b=5, first=0, count=thin, out=3, place=0),
            dict(a=1, b=2, first=0, count=thin, out=2, place=0),
            dict(a=1, b=3, first=0, count=thin, out=2, place=thin),
            dict(a=1, b=4, first=0, count=thin, out=2, place=2 * thin),
        ],
        [(wide - half) * 2 * lanes, inner.shape[1], 3 * local, local],
        4,
        packed,
    )
    small = small.reshape(-1)
    g_attn, g_mlp, g_query, g_key = jnp.split(
        small[: sum(cuts)], [cuts[0], cuts[0] + cuts[1], cuts[0] + cuts[1] + cuts[2]]
    )
    input_grad = d_resid + back
    grad_query, grad_key, grad_value = jnp.split(grad_qkv, 3, axis=1)
    grad_gate = jnp.concatenate([grad_gate_a, grad_gate_b], axis=1)
    summed = (
        grad_query,
        grad_key,
        grad_value,
        g_query.reshape(heads, -1),
        g_key.reshape(heads, -1),
        grad_output.T,
        g_attn,
        grad_gate,
        grad_up,
        grad_down.T,
        g_mlp,
    )
    return (
        block_out[None],
        input_grad[None],
        summed[0],
        summed[1],
        summed[2],
        summed[3],
        summed[4],
        summed[5],
        summed[6],
        summed[7],
        summed[8],
        summed[9],
        summed[10],
    )


def solution(mesh):
    return jax.shard_map(
        per_device,
        mesh=mesh,
        in_specs=(
            P("seq", "ctx", None),
            P("seq", "ctx", None),
            P("seq", None),
            P(None, "tp"),
            P(None, "tp"),
            P(None, "tp"),
            P("tp", None),
            P("tp", None),
            P("tp", None),
            P(),
            P(None, "tp"),
            P(None, "tp"),
            P("tp", None),
            P(),
        ),
        out_specs=(
            P("seq", "ctx", None),
            P("seq", "ctx", None),
            P(("ctx", "seq"), "tp"),
            P(("ctx", "seq"), "tp"),
            P(("ctx", "seq"), "tp"),
            P("tp", ("ctx", "seq")),
            P("tp", ("ctx", "seq")),
            P("tp", ("ctx", "seq")),
            P(("ctx", "seq")),
            P(("ctx", "seq"), "tp"),
            P(("ctx", "seq"), "tp"),
            P("tp", ("ctx", "seq")),
            P(("ctx", "seq")),
        ),
        check_vma=False,
    )
```

```python
import jax
import jax.numpy as jnp
from jax import lax
from jax.sharding import PartitionSpec as P
from jax.experimental import pallas as pl
from jax.experimental.pallas import tpu as pltpu

MESH = pl.DeviceIdType.MESH
bf16 = jnp.bfloat16
f32 = jnp.float32
lanes = 128
row_blocks = 16
row_chains = 8
pace = 6
norm_eps = 1e-06


def remote(src, dst, send, recv, where):
    return pltpu.make_async_remote_copy(
        src, dst, send, recv, device_id=where, device_id_type=MESH
    )


class LineSum:
    def __init__(self, n, rows, width):
        self.n, self.rows, self.width = n, rows, width
        self.part = width // n
        self.rc = rows // row_blocks
        self.total = row_blocks // row_chains * n
        self.steps = self.total + n - 1

    def scratch(self):
        shape = (self.n, self.rows, self.part)
        return [pltpu.VMEM(shape, bf16)] * 4 + [
            pltpu.SemaphoreType.DMA((row_chains, self.total))
        ] * 4

    def bind(self, refs):
        self.own, self.from_l, self.from_r, self.res = refs[:4]
        self.send_r, self.send_l, self.recv_l, self.recv_r = refs[4:]
        self.i = lax.axis_index("tp")
        self.has_l, self.has_r = self.i > 0, self.i < self.n - 1

    def greet(self, bar):
        @pl.when(self.has_l)
        def _():
            pl.semaphore_signal(bar, inc=1, device_id={"tp": self.i - 1}, device_id_type=MESH)

        @pl.when(self.has_r)
        def _():
            pl.semaphore_signal(bar, inc=1, device_id={"tp": self.i + 1}, device_id_type=MESH)

        return self.has_l.astype(jnp.int32) + self.has_r.astype(jnp.int32)

    def load(self, x_ref):
        for j in range(self.n):
            self.own[j] = x_ref[:, j * self.part : (j + 1) * self.part]

    def rows_of(self, g, p):
        block = (p // self.n) * row_chains + g
        return pl.ds(pl.multiple_of(block * self.rc, self.rc), self.rc)

    def right(self, src, dst, g, p, j):
        sl = self.rows_of(g, p)
        return remote(
            src.at[j, sl], dst.at[j, sl], self.send_r.at[g, p], self.recv_l.at[g, p],
            {"tp": self.i + 1},
        )

    def left(self, src, dst, g, q, j):
        sl = self.rows_of(g, q)
        return remote(
            src.at[j, sl], dst.at[j, sl], self.send_l.at[g, q], self.recv_r.at[g, q],
            {"tp": self.i - 1},
        )

    def wait_l(self, g, p, j):
        sl = self.rows_of(g, p)
        remote(
            self.own.at[j, sl], self.from_l.at[j, sl], self.send_r.at[g, p], self.recv_l.at[g, p],
            {"tp": self.i - 1},
        ).wait_recv()

    def wait_r(self, g, q, j):
        sl = self.rows_of(g, q)
        remote(
            self.own.at[j, sl], self.from_r.at[j, sl], self.send_l.at[g, q], self.recv_r.at[g, q],
            {"tp": self.i + 1},
        ).wait_recv()

    def step(self, t):
        for g in range(row_chains):
            self.sub_step(t, g)

    def piece(self, e):
        t = e // row_chains

        @pl.when(t < self.steps)
        def _():
            self.sub_step(t, lax.rem(e, row_chains))

    def sub_step(self, t, g):
        n, i, has_l, has_r = self.n, self.i, self.has_l, self.has_r
        own, from_l, from_r, res = self.own, self.from_l, self.from_r, self.res
        p = t - i
        q = t - (n - 1 - i)
        jr = n - 1 - lax.rem(p + n * self.total, n)
        jl = lax.rem(q + n * self.total, n)
        pv = (p >= 0) & (p < self.total)
        qv = (q >= 0) & (q < self.total)

        @pl.when(pv & has_l)
        def _():
            self.wait_l(g, p, jr)

        @pl.when(qv & has_r)
        def _():
            self.wait_r(g, q, jl)

        @pl.when(pv & (jr > i))
        def _():
            sl = self.rows_of(g, p)

            @pl.when(has_l)
            def _():
                own[jr, sl] = (own[jr, sl].astype(f32) + from_l[jr, sl].astype(f32)).astype(bf16)

            self.right(own, from_l, g, p, jr).start()

        @pl.when(qv & (jl < i))
        def _():
            sl = self.rows_of(g, q)

            @pl.when(has_r)
            def _():
                own[jl, sl] = (own[jl, sl].astype(f32) + from_r[jl, sl].astype(f32)).astype(bf16)

            self.left(own, from_r, g, q, jl).start()

        @pl.when(pv & (jr == i))
        def _():
            sl = self.rows_of(g, p)

            @pl.when(has_l & has_r)
            def _():
                res[i, sl] = (
                    own[i, sl].astype(f32) + from_l[i, sl].astype(f32) + from_r[i, sl].astype(f32)
                ).astype(bf16)

            @pl.when(jnp.logical_not(has_l))
            def _():
                res[i, sl] = (own[i, sl].astype(f32) + from_r[i, sl].astype(f32)).astype(bf16)

            @pl.when(jnp.logical_not(has_r))
            def _():
                res[i, sl] = (own[i, sl].astype(f32) + from_l[i, sl].astype(f32)).astype(bf16)

        @pl.when(pv & (jr <= i) & has_r)
        def _():
            self.right(res, res, g, p, jr).start()

        @pl.when(qv & (jl >= i) & has_l)
        def _():
            self.left(res, res, g, q, jl).start()

    def drain(self):
        def one(p, carry):
            for g in range(row_chains):

                @pl.when(self.has_r)
                def _():
                    self.right(self.own, self.from_l, g, p, 0).wait_send()

                @pl.when(self.has_l)
                def _():
                    self.left(self.own, self.from_r, g, p, 0).wait_send()

            return carry

        lax.fori_loop(0, self.total, one, 0)

    def store(self, out_ref):
        for j in range(self.n):
            out_ref[:, j * self.part : (j + 1) * self.part] = self.res[j]


class GradScatter:
    def __init__(self, n_ctx, n_seq, width, jobs):
        self.nx, self.ny = n_ctx // 2, n_seq
        self.rows = width // (n_ctx * n_seq)
        self.jobs = jobs
        start = 0
        self.spans = []
        for job in jobs:
            self.spans.append((start, start + job["count"]))
            start += job["count"]
        self.total = start
        self.steps = start + 5

    def scratch(self):
        nx, ny, r, t = self.nx, self.ny, self.rows, self.total
        tile = (r, lanes)
        sem = pltpu.SemaphoreType.DMA
        return [
            pltpu.VMEM((2, nx, ny, 2) + tile, bf16),
            pltpu.VMEM((2, nx, ny, 2) + tile, f32),
            pltpu.VMEM((t, nx, ny, 2) + tile, bf16),
            pltpu.VMEM((3, nx, ny) + tile, bf16),
            pltpu.VMEM((3, ny, nx) + tile, bf16),
            pltpu.VMEM((t, nx - 1, ny) + tile, bf16),
            pltpu.VMEM((t, ny - 1, nx) + tile, bf16),
            pltpu.VMEM((3, ny) + tile, bf16),
            pltpu.VMEM((3, nx) + tile, bf16),
            pltpu.VMEM((t, ny - 1) + tile, bf16),
            pltpu.VMEM((t, nx - 1) + tile, bf16),
            sem((2,)), sem((t,)),
            sem((3, nx - 1)), sem((t, nx - 1)), sem((3, ny - 1)), sem((t, ny - 1)),
            sem((3, ny - 1)), sem((t, ny - 1)), sem((3, nx - 1)), sem((t, nx - 1)),
        ]

    def bind(self, refs, at_refs, b_refs, out_refs):
        (self.send0, self.keep, self.recv0, self.pa, self.pb, self.r1a, self.r1b, self.qa, self.qb,
         self.r2a, self.r2b, self.s0, self.d0, self.s1a, self.d1a, self.s1b, self.d1b,
         self.s2a, self.d2a, self.s2b, self.d2b) = refs
        self.at_refs, self.b_refs, self.out_refs = at_refs, b_refs, out_refs
        ctx = lax.axis_index("ctx")
        self.mx, self.core, self.my = ctx // 2, lax.rem(ctx, 2), lax.axis_index("seq")

    def at_x(self, d):
        return {"ctx": lax.rem(self.mx + d, self.nx) * 2 + self.core}

    def at_y(self, d):
        return {"seq": lax.rem(self.my + d, self.ny)}

    def at_mate(self):
        return {"ctx": self.mx * 2 + 1 - self.core}

    def greet(self, bar):
        places = [self.at_mate()]
        places += [self.at_x(d) for d in range(1, self.nx)]
        places += [self.at_y(d) for d in range(1, self.ny)]
        for place in places:
            pl.semaphore_signal(bar, inc=1, device_id=place, device_id_type=MESH)
        return len(places)

    def c0(self, c, slot):
        return remote(self.send0.at[slot], self.recv0.at[c], self.s0.at[slot], self.d0.at[c], self.at_mate())

    def c1a(self, c, slot, d):
        return remote(
            self.pa.at[slot, lax.rem(self.mx + d, self.nx)], self.r1a.at[c, d - 1],
            self.s1a.at[slot, d - 1], self.d1a.at[c, d - 1], self.at_x(d),
        )

    def c1b(self, c, slot, d):
        return remote(
            self.pb.at[slot, lax.rem(self.my + d, self.ny)], self.r1b.at[c, d - 1],
            self.s1b.at[slot, d - 1], self.d1b.at[c, d - 1], self.at_y(d),
        )

    def c2a(self, c, slot, d):
        return remote(
            self.qa.at[slot, lax.rem(self.my + d, self.ny)], self.r2a.at[c, d - 1],
            self.s2a.at[slot, d - 1], self.d2a.at[c, d - 1], self.at_y(d),
        )

    def c2b(self, c, slot, d):
        return remote(
            self.qb.at[slot, lax.rem(self.mx + d, self.nx)], self.r2b.at[c, d - 1],
            self.s2b.at[slot, d - 1], self.d2b.at[c, d - 1], self.at_x(d),
        )

    def make(self, c):
        slot = lax.rem(c, 2)
        nx, ny, r = self.nx, self.ny, self.rows

        @pl.when(c >= 2)
        def _():
            self.c0(c, slot).wait_send()

        def products(at_ref, b_ref, col, parity, write):
            def tile(e, carry):
                x, y = e // ny, lax.rem(e, ny)
                row = pl.multiple_of(((x * 2 + parity) * ny + y) * r, r)
                acc = jnp.dot(
                    at_ref[pl.ds(row, r), :], b_ref[:, pl.ds(col, 2 * lanes)],
                    preferred_element_type=f32,
                )
                write(x, y, acc)
                return carry

            lax.fori_loop(0, nx * ny, tile, 0)

        def to_send(x, y, acc):
            self.send0[slot, x, y, 0] = acc[:, :lanes].astype(bf16)
            self.send0[slot, x, y, 1] = acc[:, lanes:].astype(bf16)

        def to_keep(x, y, acc):
            self.keep[slot, x, y, 0] = acc[:, :lanes]
            self.keep[slot, x, y, 1] = acc[:, lanes:]

        for job, (lo, hi) in zip(self.jobs, self.spans):

            @pl.when((c >= lo) & (c < hi))
            def _():
                at_ref, b_ref = self.at_refs[job["a"]], self.b_refs[job["b"]]
                col = pl.multiple_of((c - lo + job["first"]) * (2 * lanes), 2 * lanes)
                products(at_ref, b_ref, col, 1 - self.core, to_send)
                self.c0(c, slot).start()
                products(at_ref, b_ref, col, self.core, to_keep)

    def pair(self, c):
        slot = lax.rem(c, 3)
        nx, ny = self.nx, self.ny

        @pl.when(c >= 3)
        def _():
            for d in range(1, nx):
                self.c1a(c, slot, d).wait_send()
            for d in range(1, ny):
                self.c1b(c, slot, d).wait_send()

        self.c0(c, lax.rem(c, 2)).wait_recv()
        for x in range(nx):
            for y in range(ny):
                self.pa[slot, x, y] = (
                    self.keep[lax.rem(c, 2), x, y, 0] + self.recv0[c, x, y, 0].astype(f32)
                ).astype(bf16)
        for d in range(1, nx):
            self.c1a(c, slot, d).start()
        for x in range(nx):
            for y in range(ny):
                self.pb[slot, y, x] = (
                    self.keep[lax.rem(c, 2), x, y, 1] + self.recv0[c, x, y, 1].astype(f32)
                ).astype(bf16)
        for d in range(1, ny):
            self.c1b(c, slot, d).start()

    def cross(self, c):
        slot = lax.rem(c, 3)
        nx, ny = self.nx, self.ny

        @pl.when(c >= 3)
        def _():
            for d in range(1, ny):
                self.c2a(c, slot, d).wait_send()
            for d in range(1, nx):
                self.c2b(c, slot, d).wait_send()

        for d in range(1, nx):
            self.c1a(c, slot, d).wait_recv()
        for y in range(ny):
            acc = self.pa[slot, self.mx, y].astype(f32)
            for d in range(1, nx):
                acc = acc + self.r1a[c, d - 1, y].astype(f32)
            self.qa[slot, y] = acc.astype(bf16)
        for d in range(1, ny):
            self.c2a(c, slot, d).start()
        for d in range(1, ny):
            self.c1b(c, slot, d).wait_recv()
        for x in range(nx):
            acc = self.pb[slot, self.my, x].astype(f32)
            for d in range(1, ny):
                acc = acc + self.r1b[c, d - 1, x].astype(f32)
            self.qb[slot, x] = acc.astype(bf16)
        for d in range(1, nx):
            self.c2b(c, slot, d).start()

    def finish(self, c):
        slot = lax.rem(c, 3)
        nx, ny = self.nx, self.ny
        for d in range(1, ny):
            self.c2a(c, slot, d).wait_recv()
        for d in range(1, nx):
            self.c2b(c, slot, d).wait_recv()
        for job, (lo, hi) in zip(self.jobs, self.spans):

            @pl.when((c >= lo) & (c < hi))
            def _():
                out_ref = self.out_refs[job["out"]]
                col = pl.multiple_of((c - lo + job["place"]) * (2 * lanes), 2 * lanes)
                acc = self.qa[slot, self.my].astype(f32)
                for d in range(1, ny):
                    acc = acc + self.r2a[c, d - 1].astype(f32)
                out_ref[:, pl.ds(col, lanes)] = acc
                acc = self.qb[slot, self.mx].astype(f32)
                for d in range(1, nx):
                    acc = acc + self.r2b[c, d - 1].astype(f32)
                out_ref[:, pl.ds(col + lanes, lanes)] = acc

    def early(self, it):
        @pl.when((it >= 5) & (it < self.total + 5))
        def _():
            self.finish(it - 5)

        @pl.when((it >= 3) & (it < self.total + 3))
        def _():
            self.cross(it - 3)

        @pl.when((it >= 1) & (it < self.total + 1))
        def _():
            self.pair(it - 1)

    def late(self, it):
        @pl.when(it < self.total)
        def _():
            self.make(it)

    def drain(self):
        for c in range(max(self.total - 2, 0), self.total):
            self.c0(c, c % 2).wait_send()
        for c in range(max(self.total - 3, 0), self.total):
            slot = c % 3
            for d in range(1, self.nx):
                self.c1a(c, slot, d).wait_send()
                self.c2b(c, slot, d).wait_send()
            for d in range(1, self.ny):
                self.c1b(c, slot, d).wait_send()
                self.c2a(c, slot, d).wait_send()


class GainSum:
    def __init__(self, n_ctx, n_seq):
        self.ny, self.n = n_seq, n_ctx * n_seq

    def scratch(self):
        sem = pltpu.SemaphoreType.DMA
        return [pltpu.VMEM((self.n - 1, 8, lanes), f32), sem((self.n - 1,)), sem((self.n - 1,))]

    def bind(self, refs, in_ref, out_ref):
        self.got, self.sent, self.done = refs
        self.in_ref, self.out_ref = in_ref, out_ref
        self.me = lax.axis_index("ctx") * self.ny + lax.axis_index("seq")

    def place(self, d):
        to = lax.rem(self.me + d, self.n)
        return to, {"ctx": to // self.ny, "seq": lax.rem(to, self.ny)}

    def copy(self, d):
        to, where = self.place(d)
        return remote(self.in_ref.at[to], self.got.at[d - 1], self.sent.at[d - 1], self.done.at[d - 1], where)

    def greet(self, bar):
        for d in range(1, self.n):
            pl.semaphore_signal(bar, inc=1, device_id=self.place(d)[1], device_id_type=MESH)
        return self.n - 1

    def start(self):
        for d in range(1, self.n):
            self.copy(d).start()

    def finish(self):
        acc = self.in_ref[self.me]
        for d in range(1, self.n):
            self.copy(d).wait_recv()
            acc = acc + self.got[d - 1]
        self.out_ref[...] = acc
        for d in range(1, self.n):
            self.copy(d).wait_send()


def vmem_spec():
    return pl.BlockSpec(memory_space=pltpu.VMEM)


def comm_call(body, args, outs, scratch, cid, name, scalars=()):
    return pl.pallas_call(
        body,
        out_shape=outs,
        in_specs=[
            pl.BlockSpec(memory_space=pltpu.SMEM) if i in scalars else vmem_spec()
            for i in range(len(args))
        ],
        out_specs=[vmem_spec()] * len(outs),
        scratch_shapes=scratch,
        compiler_params=pltpu.CompilerParams(
            collective_id=cid, has_side_effects=True, vmem_limit_bytes=62 * 2**20
        ),
        name=name,
    )(*args)


def tp_sum(partial, cid):
    rows, width = partial.shape
    line = LineSum(lax.axis_size("tp"), rows, width)

    def body(x_ref, out_ref, *refs):
        line.bind(refs)
        bar = pltpu.get_barrier_semaphore()
        peers = line.greet(bar)
        line.load(x_ref)
        pl.semaphore_wait(bar, peers)

        def one(t, carry):
            line.step(t)
            return carry

        lax.fori_loop(0, line.steps, one, 0)
        line.drain()
        line.store(out_ref)

    out = jax.ShapeDtypeStruct((rows, width), bf16)
    (summed,) = comm_call(body, [partial.astype(bf16)], [out], line.scratch(), cid, "tp_sum")
    return summed


def sum_and_scatter(partial, ats, bs, jobs, out_widths, cid, gains=None):
    rows, width = partial.shape
    n_ctx, n_seq = lax.axis_size("ctx"), lax.axis_size("seq")
    line = LineSum(lax.axis_size("tp"), rows, width)
    grads = GradScatter(n_ctx, n_seq, width, jobs)
    small = GainSum(n_ctx, n_seq)
    small_in = [] if gains is None else [gains]
    na, nb, no, ns = len(ats), len(bs), len(out_widths), len(small_in)
    n_line, n_grads = len(line.scratch()), len(grads.scratch())

    def body(x_ref, *refs):
        at_refs, b_refs = refs[:na], refs[na : na + nb]
        refs = refs[na + nb :]
        small_refs, refs = refs[:ns], refs[ns:]
        out_ref, grad_refs, refs = refs[0], refs[1 : 1 + no], refs[1 + no :]
        small_out, scratch = refs[:ns], refs[ns:]
        line.bind(scratch[:n_line])
        grads.bind(scratch[n_line : n_line + n_grads], at_refs, b_refs, grad_refs)
        bar = pltpu.get_barrier_semaphore()
        peers = line.greet(bar)
        if ns:
            small.bind(scratch[n_line + n_grads :], small_refs[0], small_out[0])
            peers = peers + small.greet(bar)
        else:
            peers = peers + grads.greet(bar)
        line.load(x_ref)
        pl.semaphore_wait(bar, peers)
        if ns:
            small.start()

        def one(it, carry):
            grads.early(it)
            for v in range(pace):
                line.piece(it * pace + v)
            grads.late(it)
            return carry

        lax.fori_loop(0, max(-(-line.steps * row_chains // pace), grads.steps), one, 0)
        if ns:
            small.finish()
        line.drain()
        grads.drain()
        line.store(out_ref)

    outs = [jax.ShapeDtypeStruct((rows, width), bf16)] + [
        jax.ShapeDtypeStruct((grads.rows, w), f32) for w in out_widths
    ]
    outs += [jax.ShapeDtypeStruct((8, lanes), f32)] * ns
    res = comm_call(
        body, [partial.astype(bf16)] + list(ats) + list(bs) + small_in, outs,
        line.scratch() + grads.scratch() + (small.scratch() if ns else []), cid, "sum_and_scatter",
    )
    return res[0], res[1:]


class LineSmall:
    def __init__(self, n, rows):
        self.n, self.rows = n, rows

    def scratch(self):
        sem = pltpu.SemaphoreType.DMA
        return [
            pltpu.VMEM((8, self.rows), f32), pltpu.VMEM((self.n - 1, 8, self.rows), f32),
            sem((self.n - 1,)), sem((self.n - 1,)),
        ]

    def bind(self, refs):
        self.mine, self.got, self.sent, self.done = refs
        self.i = lax.axis_index("tp")

    def greet(self, bar):
        for d in range(1, self.n):
            pl.semaphore_signal(
                bar, inc=1, device_id={"tp": lax.rem(self.i + d, self.n)}, device_id_type=MESH
            )
        return self.n - 1

    def copy(self, d):
        return remote(
            self.mine, self.got.at[d - 1], self.sent.at[d - 1], self.done.at[d - 1],
            {"tp": lax.rem(self.i + d, self.n)},
        )

    def total(self, columns):
        self.mine[...] = jnp.transpose(columns)[:8]
        for d in range(1, self.n):
            self.copy(d).start()
        acc = self.mine[...]
        for d in range(1, self.n):
            self.copy(d).wait_recv()
            acc = acc + self.got[d - 1]
        for d in range(1, self.n):
            self.copy(d).wait_send()
        return jnp.transpose(jnp.concatenate([acc, jnp.zeros((lanes - 8, self.rows), f32)], axis=0))


def lane_pair(first, second, rows):
    lane = lax.broadcasted_iota(jnp.int32, (rows, lanes), 1)
    return jnp.where(lane == 0, first, 0.0) + jnp.where(lane == 1, second, 0.0)


def dot_nt(left, right):
    return lax.dot_general(left, right, (((1,), (1,)), ((), ())), preferred_element_type=f32)


def dot_tn(left, right):
    return lax.dot_general(left, right, (((0,), (0,)), ((), ())), preferred_element_type=f32)


def attention_back(
    back, grad, proj, attn_gain, w_output, query_rot, keys, values, attn, lse, pos_row, order,
    query_norm, key_norm, scales, qgain, kgain, cosine, sine, cid,
):
    rows, width = back.shape
    local = w_output.shape[0]
    head_dim = lanes
    heads = local // head_dim
    count = keys.shape[0]
    nx, n_tp = lax.axis_size("ctx") // 2, lax.axis_size("tp")
    small = LineSmall(n_tp, rows)
    n_small = len(small.scratch())
    scale = head_dim ** (-0.5)
    tile = 64
    sub = rows // 2

    def body(
        back_ref, grad_ref, proj_ref, again_ref, w_ref, q_ref, k_ref, v_ref, attn_ref, lse_ref,
        prow_ref, order_ref, qn_ref, kn_ref, sc_ref, qg_ref, kg_ref, cos_ref, sin_ref,
        dqkv_ref, dprojt_ref, dagain_ref, dqg_ref, dkg_ref,
        dproj, dout, columns, delta, dqs, dks, send0, keep, recv0, recv1,
        s0, d0, s1, d1, *small_refs,
    ):
        small.bind(small_refs)
        ctx = lax.axis_index("ctx")
        mx, core = ctx // 2, lax.rem(ctx, 2)
        bar = pltpu.get_barrier_semaphore()
        mate = {"ctx": mx * 2 + 1 - core}
        peers = small.greet(bar) + nx
        pl.semaphore_signal(bar, inc=1, device_id=mate, device_id_type=MESH)
        for d in range(1, nx):
            pl.semaphore_signal(
                bar, inc=1, device_id={"ctx": lax.rem(mx + d, nx) * 2 + core}, device_id_type=MESH
            )

        dagain_ref[...] = jnp.zeros_like(dagain_ref)

        def norm_rows(t, carry):
            sl = pl.ds(pl.multiple_of(t * tile, tile), tile)
            dres = grad_ref[sl].astype(f32) + back_ref[sl].astype(f32)
            out = proj_ref[sl].astype(f32)
            inv = lax.rsqrt(jnp.mean(out * out, axis=1, keepdims=True) + norm_eps)
            norm = out * inv
            dagain_ref[...] += jnp.sum(dres * norm, axis=0, keepdims=True)
            dnorm = dres * again_ref[...]
            dot = jnp.mean(dnorm * norm, axis=1, keepdims=True)
            dproj[sl] = (inv * (dnorm - norm * dot)).astype(bf16)
            return carry

        lax.fori_loop(0, rows // tile, norm_rows, 0)
        for h in range(local // sub):
            dout[:, h * sub : (h + 1) * sub] = dot_nt(
                dproj[...], w_ref[h * sub : (h + 1) * sub, :]
            ).astype(bf16)
        lane = lax.broadcasted_iota(jnp.int32, (rows, lanes), 1)
        acc = jnp.zeros((rows, lanes), f32)
        for h in range(heads):
            hs = slice(h * head_dim, (h + 1) * head_dim)
            row_sum = jnp.sum(
                dout[:, hs].astype(f32) * attn_ref[:, hs].astype(f32), axis=1, keepdims=True
            )
            acc = jnp.where(lane == h, row_sum, acc)
        columns[...] = acc
        delta[...] = jnp.transpose(columns[...])[:8]
        dqs[...] = jnp.zeros_like(dqs)
        pl.semaphore_wait(bar, peers)

        def c0(h):
            slot = lax.rem(h, 2)
            return remote(send0.at[slot], recv0.at[h], s0.at[slot], d0.at[h], mate)

        def c1(h, d):
            to = lax.rem(mx + d, nx)
            return remote(
                recv0.at[h, to], recv1.at[h, d - 1], s1.at[h, d - 1], d1.at[h, d - 1],
                {"ctx": to * 2 + core},
            )

        def one_block(h, hs, x, owner, write):
            start = (x * 2 + owner) * rows
            for part in range(rows // sub):
                ks = pl.ds(pl.multiple_of(start + part * sub, sub), sub)
                key, value = k_ref[ks, hs], v_ref[ks, hs]
                query, dhead = q_ref[:, hs], dout[:, hs]
                score = dot_nt(key, query) * scale
                place = order_ref[0, (x * 2 + owner) * 2 + part] * sub
                seen = place + lax.broadcasted_iota(jnp.int32, (sub, rows), 0) <= prow_ref[...]
                share = jnp.where(seen, jnp.exp(score - lse_ref[pl.ds(h, 1), :]), 0.0)
                dshare = dot_nt(value, dhead)
                dscore = (share * (dshare - delta[pl.ds(h, 1), :]) * scale).astype(bf16)
                dqs[:, hs] += dot_tn(dscore, key)
                write(
                    x, slice(part * sub, (part + 1) * sub),
                    jnp.dot(dscore, query, preferred_element_type=f32),
                    jnp.dot(share.astype(bf16), dhead, preferred_element_type=f32),
                )

        def one_head(h):
            hs = pl.ds(pl.multiple_of(h * head_dim, head_dim), head_dim)
            slot = lax.rem(h, 2)

            def to_send(x, rs, dk, dv):
                send0[slot, x, rs, :lanes] = dk.astype(bf16)
                send0[slot, x, rs, lanes:] = dv.astype(bf16)

            def to_keep(x, rs, dk, dv):
                keep[slot, x, rs, :lanes] = dk.astype(bf16)
                keep[slot, x, rs, lanes:] = dv.astype(bf16)

            @pl.when(h >= 2)
            def _():
                c0(h).wait_send()

            def mates(e, carry):
                one_block(h, hs, lax.rem(mx + 1 + e, nx), 1 - core, to_send)
                return carry

            lax.fori_loop(0, nx, mates, 0)
            c0(h).start()

            def owns(e, carry):
                one_block(h, hs, lax.rem(mx + 1 + e, nx), core, to_keep)
                return carry

            lax.fori_loop(0, nx, owns, 0)
            c0(h).wait_recv()

            def add(x, carry):
                recv0[h, x] = (keep[slot, x].astype(f32) + recv0[h, x].astype(f32)).astype(bf16)
                return carry

            lax.fori_loop(0, nx, add, 0)
            for d in range(1, nx):
                c1(h, d).start()

        def heads_loop(h, carry):
            one_head(h)
            return carry

        lax.fori_loop(0, heads, heads_loop, 0)

        dot_q = jnp.zeros((rows, 1), f32)
        for h in range(heads):
            hs = slice(h * head_dim, (h + 1) * head_dim)
            dq = dqs[:, hs]
            dq = dq * cos_ref[...] - pltpu.roll(dq, head_dim // 2, 1) * sin_ref[...]
            norm = qn_ref[:, hs]
            dqg_ref[:, hs] = jnp.sum(dq * norm, axis=0, keepdims=True)
            dq = dq * qg_ref[:, hs]
            dqs[:, hs] = dq
            dot_q = dot_q + jnp.sum(dq * norm, axis=1, keepdims=True)
        dprojt_ref[...] = jnp.transpose(dproj[...])
        dot_k = jnp.zeros((rows, 1), f32)
        for h in range(heads):
            hs = slice(h * head_dim, (h + 1) * head_dim)
            total = recv0[h, mx].astype(f32)
            for d in range(1, nx):
                c1(h, d).wait_recv()
                total = total + recv1[h, d - 1].astype(f32)
            dqkv_ref[:, 2 * local + h * head_dim : 2 * local + (h + 1) * head_dim] = total[
                :, lanes:
            ].astype(bf16)
            dk = total[:, :lanes]
            dk = dk * cos_ref[...] - pltpu.roll(dk, head_dim // 2, 1) * sin_ref[...]
            norm = kn_ref[:, hs]
            dkg_ref[:, hs] = jnp.sum(dk * norm, axis=0, keepdims=True)
            dk = dk * kg_ref[:, hs]
            dks[:, hs] = dk
            dot_k = dot_k + jnp.sum(dk * norm, axis=1, keepdims=True)
        dots = small.total(lane_pair(dot_q, dot_k, rows)) * (1.0 / width)
        for h in range(heads):
            hs = slice(h * head_dim, (h + 1) * head_dim)
            dqkv_ref[:, hs] = (
                sc_ref[:, 0:1] * (dqs[:, hs] - qn_ref[:, hs] * dots[:, 0:1])
            ).astype(bf16)
            dqkv_ref[:, local + h * head_dim : local + (h + 1) * head_dim] = (
                sc_ref[:, 1:2] * (dks[:, hs] - kn_ref[:, hs] * dots[:, 1:2])
            ).astype(bf16)
        for h in range(heads):
            if h >= heads - 2:
                c0(h).wait_send()
            for d in range(1, nx):
                c1(h, d).wait_send()

    sem = pltpu.SemaphoreType.DMA
    pair = (rows, 2 * lanes)
    return comm_call(
        body,
        [back, grad, proj, attn_gain, w_output, query_rot, keys, values, attn, lse, pos_row,
         order, query_norm, key_norm, scales, qgain, kgain, cosine, sine],
        [
            jax.ShapeDtypeStruct((rows, 3 * local), bf16),
            jax.ShapeDtypeStruct((width, rows), bf16),
            jax.ShapeDtypeStruct((1, width), f32),
            jax.ShapeDtypeStruct((1, local), f32),
            jax.ShapeDtypeStruct((1, local), f32),
        ],
        [
            pltpu.VMEM((rows, width), bf16), pltpu.VMEM((rows, local), bf16),
            pltpu.VMEM((rows, lanes), f32), pltpu.VMEM((8, rows), f32),
            pltpu.VMEM((rows, local), f32), pltpu.VMEM((rows, local), f32),
            pltpu.VMEM((2, nx) + pair, bf16), pltpu.VMEM((2, nx) + pair, bf16),
            pltpu.VMEM((heads, nx) + pair, bf16), pltpu.VMEM((heads, nx - 1) + pair, bf16),
            sem((2,)), sem((heads,)), sem((heads, nx - 1)), sem((heads, nx - 1)),
        ] + small.scratch(),
        cid, "attention_back", {11},
    )


norm_eps = 1e-06
rope_base = 500000.0
masked_score = -1e30


def matmul(left, right):
    return jnp.dot(left, right, preferred_element_type=jnp.float32)


def rope_tables(positions, head_dim):
    half = head_dim // 2
    rates = rope_base ** (-(jnp.arange(half, dtype=jnp.float32) * 2.0 / head_dim))
    angle = positions.astype(jnp.float32)[:, None] * rates[None, :]
    return (jnp.cos(angle), jnp.sin(angle))


def rotate(heads_in, cosine, sine):
    half = heads_in.shape[-1] // 2
    first, second = (heads_in[..., :half], heads_in[..., half:])
    cosine, sine = (cosine[:, None, :], sine[:, None, :])
    return jnp.concatenate(
        [first * cosine - second * sine, second * cosine + first * sine], axis=-1
    )


def unrotate(grads_in, cosine, sine):
    half = grads_in.shape[-1] // 2
    first, second = (grads_in[..., :half], grads_in[..., half:])
    cosine, sine = (cosine[:, None, :], sine[:, None, :])
    return jnp.concatenate(
        [first * cosine + second * sine, second * cosine - first * sine], axis=-1
    )


def key_positions(order, first_row, count, group):
    row_ids = first_row + jnp.arange(count, dtype=jnp.int32)
    slots = row_ids // group
    picks = slots[:, None] == jnp.arange(order.shape[0], dtype=jnp.int32)[None, :]
    return jnp.sum(jnp.where(picks, order[None, :], 0), axis=1) * group + row_ids % group


def gather_pair(keys, values):
    return (
        lax.all_gather(keys, "ctx", axis=0, tiled=True),
        lax.all_gather(values, "ctx", axis=0, tiled=True),
    )


def per_device(
    tokens,
    out_grad,
    group_order,
    w_query,
    w_key,
    w_value,
    query_gain,
    key_gain,
    w_output,
    attn_gain,
    w_gate,
    w_up,
    w_down,
    mlp_gain,
):
    inputs_bf = tokens[0]
    order = group_order[0]
    row_count, width = inputs_bf.shape
    heads, head_dim = query_gain.shape
    local = heads * head_dim
    group = row_count // 2
    scale = head_dim ** (-0.5)
    query_pos = key_positions(order, lax.axis_index("ctx") * row_count, row_count, group)
    cosine, sine = rope_tables(query_pos, head_dim)
    inputs = inputs_bf.astype(jnp.float32)
    query = matmul(inputs_bf, w_query)
    keyraw = matmul(inputs_bf, w_key)
    values = matmul(inputs_bf, w_value).astype(jnp.bfloat16)
    query_sq, key_sq = lax.psum(
        (jnp.sum(query * query, axis=1), jnp.sum(keyraw * keyraw, axis=1)), "tp"
    )
    query_scale = lax.rsqrt(query_sq / width + norm_eps)
    key_scale = lax.rsqrt(key_sq / width + norm_eps)
    query_norm = query * query_scale[:, None]
    key_norm = keyraw * key_scale[:, None]
    qgain = query_gain.reshape(local)
    kgain = key_gain.reshape(local)
    query_rot = rotate(
        (query_norm * qgain).reshape(row_count, heads, head_dim), cosine, sine
    ).astype(jnp.bfloat16)
    key_rot = rotate((key_norm * kgain).reshape(row_count, heads, head_dim), cosine, sine).astype(
        jnp.bfloat16
    )
    key_flat = key_rot.reshape(row_count, local)
    start_state = (
        jnp.full((heads, row_count), masked_score, jnp.float32),
        jnp.zeros((heads, row_count), jnp.float32),
        jnp.zeros((heads, row_count, head_dim), jnp.float32),
    )
    keys_in = lax.all_gather(key_flat, "ctx", axis=0, tiled=True)
    values_in = lax.all_gather(values, "ctx", axis=0, tiled=True)
    count = keys_in.shape[0]
    attend_block = 512
    keys_in = keys_in.reshape(count // attend_block, attend_block, heads, head_dim)
    values_in = values_in.reshape(count // attend_block, attend_block, heads, head_dim)
    key_pos = key_positions(order, jnp.int32(0), count, group).reshape(
        count // attend_block, attend_block
    )

    def one_block(state, item):
        peak_old, total, accum = state
        key_block, value_block, pos_block = item
        scores = (
            jnp.einsum("qhd,khd->hqk", query_rot, key_block, preferred_element_type=jnp.float32)
            * scale
        )
        mask = (pos_block[None, :] <= query_pos[:, None])[None]
        peak = jnp.maximum(peak_old, jnp.max(jnp.where(mask, scores, masked_score), axis=2))
        share = jnp.where(mask, jnp.exp(scores - peak[:, :, None]), 0.0)
        fade = jnp.exp(peak_old - peak)
        total = total * fade + jnp.sum(share, axis=2)
        accum = accum * fade[:, :, None] + jnp.einsum(
            "hqk,khd->hqd",
            share.astype(jnp.bfloat16),
            value_block,
            preferred_element_type=jnp.float32,
        )
        return ((peak, total, accum), None)

    state, unused = lax.scan(one_block, start_state, (keys_in, values_in, key_pos))
    peak, total, accum = state
    log_total = peak + jnp.log(total)
    mixed = (accum / total[:, :, None]).astype(jnp.bfloat16)
    attn_flat = mixed.transpose(1, 0, 2).reshape(row_count, local)
    proj_sum = tp_sum(matmul(attn_flat, w_output), 1)
    proj = proj_sum.astype(f32)
    attn_scale = lax.rsqrt(jnp.mean(proj * proj, axis=1) + norm_eps)
    attn_norm = proj * attn_scale[:, None]
    resid = inputs + attn_norm * attn_gain
    hidden = resid.astype(jnp.bfloat16)
    gate = matmul(hidden, w_gate)
    up = matmul(hidden, w_up)
    sigma = jax.nn.sigmoid(gate)
    active = gate * sigma
    inner = (active * up).astype(jnp.bfloat16)
    down = tp_sum(matmul(inner, w_down), 2).astype(f32)
    mlp_scale = lax.rsqrt(jnp.mean(down * down, axis=1) + norm_eps)
    mlp_norm = down * mlp_scale[:, None]
    block_out = resid + mlp_norm * mlp_gain
    upstream = out_grad[0].astype(jnp.float32)
    d_mlp_gain = jnp.sum(upstream * mlp_norm, axis=0)
    d_mnorm = upstream * mlp_gain
    d_down = (
        mlp_scale[:, None]
        * (d_mnorm - mlp_norm * jnp.mean(d_mnorm * mlp_norm, axis=1, keepdims=True))
    ).astype(jnp.bfloat16)
    d_inner = matmul(d_down, w_down.T)
    d_gate = (d_inner * up * sigma * (1.0 + gate * (1.0 - sigma))).astype(jnp.bfloat16)
    d_up = (d_inner * active).astype(jnp.bfloat16)
    hidden_t = hidden.T
    wide = inner.shape[1] // (2 * lanes)
    half = wide // 2
    back, (grad_down, grad_gate_a) = sum_and_scatter(
        matmul(d_gate, w_gate.T) + matmul(d_up, w_up.T),
        [d_down.T, hidden_t],
        [inner, d_gate],
        [
            dict(a=0, b=0, first=0, count=wide, out=0, place=0),
            dict(a=1, b=1, first=0, count=half, out=1, place=0),
        ],
        [inner.shape[1], half * 2 * lanes],
        3,
    )
    whole_keys = keys_in.reshape(count, local)
    whole_values = values_in.reshape(count, local)
    angle_cos = jnp.concatenate([cosine, cosine], axis=1)
    angle_sin = jnp.concatenate([-sine, sine], axis=1)
    lse = jnp.pad(log_total, ((0, 8 - heads), (0, 0)))
    scales = jnp.stack([query_scale, key_scale], axis=1)
    d_qkv, d_proj_t, d_attn_gain, d_query_gain, d_key_gain = attention_back(
        back, out_grad[0], proj_sum, attn_gain[None], w_output, query_rot.reshape(row_count, local),
        whole_keys, whole_values, attn_flat, lse, query_pos[None], group_order,
        query_norm, key_norm, scales, qgain[None], kgain[None], angle_cos, angle_sin, 5,
    )
    d_query_gain = d_query_gain.reshape(heads, head_dim)
    d_key_gain = d_key_gain.reshape(heads, head_dim)
    d_query, d_key, d_value = (d_qkv[:, i * local : (i + 1) * local] for i in range(3))
    thin = local // (2 * lanes)
    owners = lax.axis_size("ctx") * lax.axis_size("seq")
    pieces = [
        d_attn_gain.reshape(owners, -1),
        d_mlp_gain.reshape(owners, -1),
        d_query_gain.reshape(heads, owners, -1).transpose(1, 0, 2).reshape(owners, -1),
        d_key_gain.reshape(heads, owners, -1).transpose(1, 0, 2).reshape(owners, -1),
    ]
    cuts = [piece.shape[1] for piece in pieces]
    packed = jnp.concatenate(pieces, axis=1)
    packed = jnp.pad(packed, ((0, 0), (0, 8 * lanes - packed.shape[1]))).reshape(owners, 8, lanes)
    last, (grad_gate_b, grad_up, grad_qkv, grad_output, small) = sum_and_scatter(
        matmul(d_query, w_query.T) + matmul(d_key, w_key.T) + matmul(d_value, w_value.T),
        [hidden_t, inputs_bf.T, d_proj_t],
        [d_gate, d_up, d_qkv, attn_flat],
        [
            dict(a=0, b=0, first=half, count=wide - half, out=0, place=0),
            dict(a=0, b=1, first=0, count=wide, out=1, place=0),
            dict(a=2, b=3, first=0, count=thin, out=3, place=0),
            dict(a=1, b=2, first=0, count=3 * thin, out=2, place=0),
        ],
        [(wide - half) * 2 * lanes, inner.shape[1], 3 * local, local],
        4,
        packed,
    )
    small = small.reshape(-1)
    g_attn, g_mlp, g_query, g_key = jnp.split(
        small[: sum(cuts)], [cuts[0], cuts[0] + cuts[1], cuts[0] + cuts[1] + cuts[2]]
    )
    input_grad = upstream + back.astype(f32) + last.astype(f32)
    grad_query, grad_key, grad_value = jnp.split(grad_qkv, 3, axis=1)
    grad_gate = jnp.concatenate([grad_gate_a, grad_gate_b], axis=1)
    summed = (
        grad_query,
        grad_key,
        grad_value,
        g_query.reshape(heads, -1),
        g_key.reshape(heads, -1),
        grad_output.T,
        g_attn,
        grad_gate,
        grad_up,
        grad_down.T,
        g_mlp,
    )
    return (
        block_out[None],
        input_grad[None],
        summed[0],
        summed[1],
        summed[2],
        summed[3],
        summed[4],
        summed[5],
        summed[6],
        summed[7],
        summed[8],
        summed[9],
        summed[10],
    )


def solution(mesh):
    return jax.shard_map(
        per_device,
        mesh=mesh,
        in_specs=(
            P("seq", "ctx", None),
            P("seq", "ctx", None),
            P("seq", None),
            P(None, "tp"),
            P(None, "tp"),
            P(None, "tp"),
            P("tp", None),
            P("tp", None),
            P("tp", None),
            P(),
            P(None, "tp"),
            P(None, "tp"),
            P("tp", None),
            P(),
        ),
        out_specs=(
            P("seq", "ctx", None),
            P("seq", "ctx", None),
            P(("ctx", "seq"), "tp"),
            P(("ctx", "seq"), "tp"),
            P(("ctx", "seq"), "tp"),
            P("tp", ("ctx", "seq")),
            P("tp", ("ctx", "seq")),
            P("tp", ("ctx", "seq")),
            P(("ctx", "seq")),
            P(("ctx", "seq"), "tp"),
            P(("ctx", "seq"), "tp"),
            P("tp", ("ctx", "seq")),
            P(("ctx", "seq")),
        ),
        check_vma=False,
    )
```

```python
import jax
import jax.numpy as jnp
from jax import lax
from jax.sharding import PartitionSpec as P
from jax.experimental import pallas as pl
from jax.experimental.pallas import tpu as pltpu

MESH = pl.DeviceIdType.MESH
bf16 = jnp.bfloat16
f32 = jnp.float32
lanes = 128
row_blocks = 16
row_chains = 8
pace = 6
norm_eps = 1e-06


def remote(src, dst, send, recv, where):
    return pltpu.make_async_remote_copy(
        src, dst, send, recv, device_id=where, device_id_type=MESH
    )


class LineSum:
    def __init__(self, n, rows, width):
        self.n, self.rows, self.width = n, rows, width
        self.part = width // n
        self.rc = rows // row_blocks
        self.total = row_blocks // row_chains * n
        self.steps = self.total + n - 1

    def scratch(self):
        shape = (self.n, self.rows, self.part)
        return [pltpu.VMEM(shape, bf16)] * 4 + [
            pltpu.SemaphoreType.DMA((row_chains, self.total))
        ] * 4

    def bind(self, refs):
        self.own, self.from_l, self.from_r, self.res = refs[:4]
        self.send_r, self.send_l, self.recv_l, self.recv_r = refs[4:]
        self.i = lax.axis_index("tp")
        self.has_l, self.has_r = self.i > 0, self.i < self.n - 1

    def greet(self, bar):
        @pl.when(self.has_l)
        def _():
            pl.semaphore_signal(bar, inc=1, device_id={"tp": self.i - 1}, device_id_type=MESH)

        @pl.when(self.has_r)
        def _():
            pl.semaphore_signal(bar, inc=1, device_id={"tp": self.i + 1}, device_id_type=MESH)

        return self.has_l.astype(jnp.int32) + self.has_r.astype(jnp.int32)

    def load(self, x_ref):
        for j in range(self.n):
            self.own[j] = x_ref[:, j * self.part : (j + 1) * self.part]

    def rows_of(self, g, p):
        block = (p // self.n) * row_chains + g
        return pl.ds(pl.multiple_of(block * self.rc, self.rc), self.rc)

    def right(self, src, dst, g, p, j):
        sl = self.rows_of(g, p)
        return remote(
            src.at[j, sl], dst.at[j, sl], self.send_r.at[g, p], self.recv_l.at[g, p],
            {"tp": self.i + 1},
        )

    def left(self, src, dst, g, q, j):
        sl = self.rows_of(g, q)
        return remote(
            src.at[j, sl], dst.at[j, sl], self.send_l.at[g, q], self.recv_r.at[g, q],
            {"tp": self.i - 1},
        )

    def wait_l(self, g, p, j):
        sl = self.rows_of(g, p)
        remote(
            self.own.at[j, sl], self.from_l.at[j, sl], self.send_r.at[g, p], self.recv_l.at[g, p],
            {"tp": self.i - 1},
        ).wait_recv()

    def wait_r(self, g, q, j):
        sl = self.rows_of(g, q)
        remote(
            self.own.at[j, sl], self.from_r.at[j, sl], self.send_l.at[g, q], self.recv_r.at[g, q],
            {"tp": self.i + 1},
        ).wait_recv()

    def step(self, t):
        for g in range(row_chains):
            self.sub_step(t, g)

    def piece(self, e):
        t = e // row_chains

        @pl.when(t < self.steps)
        def _():
            self.sub_step(t, lax.rem(e, row_chains))

    def sub_step(self, t, g):
        n, i, has_l, has_r = self.n, self.i, self.has_l, self.has_r
        own, from_l, from_r, res = self.own, self.from_l, self.from_r, self.res
        p = t - i
        q = t - (n - 1 - i)
        jr = n - 1 - lax.rem(p + n * self.total, n)
        jl = lax.rem(q + n * self.total, n)
        pv = (p >= 0) & (p < self.total)
        qv = (q >= 0) & (q < self.total)

        @pl.when(pv & has_l)
        def _():
            self.wait_l(g, p, jr)

        @pl.when(qv & has_r)
        def _():
            self.wait_r(g, q, jl)

        @pl.when(pv & (jr > i))
        def _():
            sl = self.rows_of(g, p)

            @pl.when(has_l)
            def _():
                own[jr, sl] = (own[jr, sl].astype(f32) + from_l[jr, sl].astype(f32)).astype(bf16)

            self.right(own, from_l, g, p, jr).start()

        @pl.when(qv & (jl < i))
        def _():
            sl = self.rows_of(g, q)

            @pl.when(has_r)
            def _():
                own[jl, sl] = (own[jl, sl].astype(f32) + from_r[jl, sl].astype(f32)).astype(bf16)

            self.left(own, from_r, g, q, jl).start()

        @pl.when(pv & (jr == i))
        def _():
            sl = self.rows_of(g, p)

            @pl.when(has_l & has_r)
            def _():
                res[i, sl] = (
                    own[i, sl].astype(f32) + from_l[i, sl].astype(f32) + from_r[i, sl].astype(f32)
                ).astype(bf16)

            @pl.when(jnp.logical_not(has_l))
            def _():
                res[i, sl] = (own[i, sl].astype(f32) + from_r[i, sl].astype(f32)).astype(bf16)

            @pl.when(jnp.logical_not(has_r))
            def _():
                res[i, sl] = (own[i, sl].astype(f32) + from_l[i, sl].astype(f32)).astype(bf16)

        @pl.when(pv & (jr <= i) & has_r)
        def _():
            self.right(res, res, g, p, jr).start()

        @pl.when(qv & (jl >= i) & has_l)
        def _():
            self.left(res, res, g, q, jl).start()

    def drain(self):
        def one(p, carry):
            for g in range(row_chains):

                @pl.when(self.has_r)
                def _():
                    self.right(self.own, self.from_l, g, p, 0).wait_send()

                @pl.when(self.has_l)
                def _():
                    self.left(self.own, self.from_r, g, p, 0).wait_send()

            return carry

        lax.fori_loop(0, self.total, one, 0)

    def store(self, out_ref):
        for j in range(self.n):
            out_ref[:, j * self.part : (j + 1) * self.part] = self.res[j]


class GradScatter:
    def __init__(self, n_ctx, n_seq, width, jobs):
        self.nx, self.ny = n_ctx // 2, n_seq
        self.rows = width // (n_ctx * n_seq)
        self.jobs = jobs
        start = 0
        self.spans = []
        for job in jobs:
            self.spans.append((start, start + job["count"]))
            start += job["count"]
        self.total = start
        self.steps = start + 5

    def scratch(self):
        nx, ny, r, t = self.nx, self.ny, self.rows, self.total
        tile = (r, lanes)
        sem = pltpu.SemaphoreType.DMA
        return [
            pltpu.VMEM((2, nx, ny, 2) + tile, bf16),
            pltpu.VMEM((2, nx, ny, 2) + tile, f32),
            pltpu.VMEM((t, nx, ny, 2) + tile, bf16),
            pltpu.VMEM((3, nx, ny) + tile, bf16),
            pltpu.VMEM((3, ny, nx) + tile, bf16),
            pltpu.VMEM((t, nx - 1, ny) + tile, bf16),
            pltpu.VMEM((t, ny - 1, nx) + tile, bf16),
            pltpu.VMEM((3, ny) + tile, bf16),
            pltpu.VMEM((3, nx) + tile, bf16),
            pltpu.VMEM((t, ny - 1) + tile, bf16),
            pltpu.VMEM((t, nx - 1) + tile, bf16),
            sem((2,)), sem((t,)),
            sem((3, nx - 1)), sem((t, nx - 1)), sem((3, ny - 1)), sem((t, ny - 1)),
            sem((3, ny - 1)), sem((t, ny - 1)), sem((3, nx - 1)), sem((t, nx - 1)),
        ]

    def bind(self, refs, at_refs, b_refs, out_refs):
        (self.send0, self.keep, self.recv0, self.pa, self.pb, self.r1a, self.r1b, self.qa, self.qb,
         self.r2a, self.r2b, self.s0, self.d0, self.s1a, self.d1a, self.s1b, self.d1b,
         self.s2a, self.d2a, self.s2b, self.d2b) = refs
        self.at_refs, self.b_refs, self.out_refs = at_refs, b_refs, out_refs
        ctx = lax.axis_index("ctx")
        self.mx, self.core, self.my = ctx // 2, lax.rem(ctx, 2), lax.axis_index("seq")

    def at_x(self, d):
        return {"ctx": lax.rem(self.mx + d, self.nx) * 2 + self.core}

    def at_y(self, d):
        return {"seq": lax.rem(self.my + d, self.ny)}

    def at_mate(self):
        return {"ctx": self.mx * 2 + 1 - self.core}

    def greet(self, bar):
        places = [self.at_mate()]
        places += [self.at_x(d) for d in range(1, self.nx)]
        places += [self.at_y(d) for d in range(1, self.ny)]
        for place in places:
            pl.semaphore_signal(bar, inc=1, device_id=place, device_id_type=MESH)
        return len(places)

    def c0(self, c, slot):
        return remote(self.send0.at[slot], self.recv0.at[c], self.s0.at[slot], self.d0.at[c], self.at_mate())

    def c1a(self, c, slot, d):
        return remote(
            self.pa.at[slot, lax.rem(self.mx + d, self.nx)], self.r1a.at[c, d - 1],
            self.s1a.at[slot, d - 1], self.d1a.at[c, d - 1], self.at_x(d),
        )

    def c1b(self, c, slot, d):
        return remote(
            self.pb.at[slot, lax.rem(self.my + d, self.ny)], self.r1b.at[c, d - 1],
            self.s1b.at[slot, d - 1], self.d1b.at[c, d - 1], self.at_y(d),
        )

    def c2a(self, c, slot, d):
        return remote(
            self.qa.at[slot, lax.rem(self.my + d, self.ny)], self.r2a.at[c, d - 1],
            self.s2a.at[slot, d - 1], self.d2a.at[c, d - 1], self.at_y(d),
        )

    def c2b(self, c, slot, d):
        return remote(
            self.qb.at[slot, lax.rem(self.mx + d, self.nx)], self.r2b.at[c, d - 1],
            self.s2b.at[slot, d - 1], self.d2b.at[c, d - 1], self.at_x(d),
        )

    def make(self, c):
        slot = lax.rem(c, 2)
        nx, ny, r = self.nx, self.ny, self.rows

        @pl.when(c >= 2)
        def _():
            self.c0(c, slot).wait_send()

        def products(at_ref, b_ref, col, parity, write):
            def tile(e, carry):
                x, y = e // ny, lax.rem(e, ny)
                row = pl.multiple_of(((x * 2 + parity) * ny + y) * r, r)
                acc = jnp.dot(
                    at_ref[pl.ds(row, r), :], b_ref[:, pl.ds(col, 2 * lanes)],
                    preferred_element_type=f32,
                )
                write(x, y, acc)
                return carry

            lax.fori_loop(0, nx * ny, tile, 0)

        def to_send(x, y, acc):
            self.send0[slot, x, y, 0] = acc[:, :lanes].astype(bf16)
            self.send0[slot, x, y, 1] = acc[:, lanes:].astype(bf16)

        def to_keep(x, y, acc):
            self.keep[slot, x, y, 0] = acc[:, :lanes]
            self.keep[slot, x, y, 1] = acc[:, lanes:]

        for job, (lo, hi) in zip(self.jobs, self.spans):

            @pl.when((c >= lo) & (c < hi))
            def _():
                at_ref, b_ref = self.at_refs[job["a"]], self.b_refs[job["b"]]
                col = pl.multiple_of((c - lo + job["first"]) * (2 * lanes), 2 * lanes)
                products(at_ref, b_ref, col, 1 - self.core, to_send)
                self.c0(c, slot).start()
                products(at_ref, b_ref, col, self.core, to_keep)

    def pair(self, c):
        slot = lax.rem(c, 3)
        nx, ny = self.nx, self.ny

        @pl.when(c >= 3)
        def _():
            for d in range(1, nx):
                self.c1a(c, slot, d).wait_send()
            for d in range(1, ny):
                self.c1b(c, slot, d).wait_send()

        self.c0(c, lax.rem(c, 2)).wait_recv()
        for x in range(nx):
            for y in range(ny):
                self.pa[slot, x, y] = (
                    self.keep[lax.rem(c, 2), x, y, 0] + self.recv0[c, x, y, 0].astype(f32)
                ).astype(bf16)
        for d in range(1, nx):
            self.c1a(c, slot, d).start()
        for x in range(nx):
            for y in range(ny):
                self.pb[slot, y, x] = (
                    self.keep[lax.rem(c, 2), x, y, 1] + self.recv0[c, x, y, 1].astype(f32)
                ).astype(bf16)
        for d in range(1, ny):
            self.c1b(c, slot, d).start()

    def cross(self, c):
        slot = lax.rem(c, 3)
        nx, ny = self.nx, self.ny

        @pl.when(c >= 3)
        def _():
            for d in range(1, ny):
                self.c2a(c, slot, d).wait_send()
            for d in range(1, nx):
                self.c2b(c, slot, d).wait_send()

        for d in range(1, nx):
            self.c1a(c, slot, d).wait_recv()
        for y in range(ny):
            acc = self.pa[slot, self.mx, y].astype(f32)
            for d in range(1, nx):
                acc = acc + self.r1a[c, d - 1, y].astype(f32)
            self.qa[slot, y] = acc.astype(bf16)
        for d in range(1, ny):
            self.c2a(c, slot, d).start()
        for d in range(1, ny):
            self.c1b(c, slot, d).wait_recv()
        for x in range(nx):
            acc = self.pb[slot, self.my, x].astype(f32)
            for d in range(1, ny):
                acc = acc + self.r1b[c, d - 1, x].astype(f32)
            self.qb[slot, x] = acc.astype(bf16)
        for d in range(1, nx):
            self.c2b(c, slot, d).start()

    def finish(self, c):
        slot = lax.rem(c, 3)
        nx, ny = self.nx, self.ny
        for d in range(1, ny):
            self.c2a(c, slot, d).wait_recv()
        for d in range(1, nx):
            self.c2b(c, slot, d).wait_recv()
        for job, (lo, hi) in zip(self.jobs, self.spans):

            @pl.when((c >= lo) & (c < hi))
            def _():
                out_ref = self.out_refs[job["out"]]
                col = pl.multiple_of((c - lo + job["place"]) * (2 * lanes), 2 * lanes)
                acc = self.qa[slot, self.my].astype(f32)
                for d in range(1, ny):
                    acc = acc + self.r2a[c, d - 1].astype(f32)
                out_ref[:, pl.ds(col, lanes)] = acc
                acc = self.qb[slot, self.mx].astype(f32)
                for d in range(1, nx):
                    acc = acc + self.r2b[c, d - 1].astype(f32)
                out_ref[:, pl.ds(col + lanes, lanes)] = acc

    def early(self, it):
        @pl.when((it >= 5) & (it < self.total + 5))
        def _():
            self.finish(it - 5)

        @pl.when((it >= 3) & (it < self.total + 3))
        def _():
            self.cross(it - 3)

        @pl.when((it >= 1) & (it < self.total + 1))
        def _():
            self.pair(it - 1)

    def late(self, it):
        @pl.when(it < self.total)
        def _():
            self.make(it)

    def drain(self):
        for c in range(max(self.total - 2, 0), self.total):
            self.c0(c, c % 2).wait_send()
        for c in range(max(self.total - 3, 0), self.total):
            slot = c % 3
            for d in range(1, self.nx):
                self.c1a(c, slot, d).wait_send()
                self.c2b(c, slot, d).wait_send()
            for d in range(1, self.ny):
                self.c1b(c, slot, d).wait_send()
                self.c2a(c, slot, d).wait_send()


class GainSum:
    def __init__(self, n_ctx, n_seq):
        self.ny, self.n = n_seq, n_ctx * n_seq

    def scratch(self):
        sem = pltpu.SemaphoreType.DMA
        return [pltpu.VMEM((self.n - 1, 8, lanes), f32), sem((self.n - 1,)), sem((self.n - 1,))]

    def bind(self, refs, in_ref, out_ref):
        self.got, self.sent, self.done = refs
        self.in_ref, self.out_ref = in_ref, out_ref
        self.me = lax.axis_index("ctx") * self.ny + lax.axis_index("seq")

    def place(self, d):
        to = lax.rem(self.me + d, self.n)
        return to, {"ctx": to // self.ny, "seq": lax.rem(to, self.ny)}

    def copy(self, d):
        to, where = self.place(d)
        return remote(self.in_ref.at[to], self.got.at[d - 1], self.sent.at[d - 1], self.done.at[d - 1], where)

    def greet(self, bar):
        for d in range(1, self.n):
            pl.semaphore_signal(bar, inc=1, device_id=self.place(d)[1], device_id_type=MESH)
        return self.n - 1

    def start(self):
        for d in range(1, self.n):
            self.copy(d).start()

    def finish(self):
        acc = self.in_ref[self.me]
        for d in range(1, self.n):
            self.copy(d).wait_recv()
            acc = acc + self.got[d - 1]
        self.out_ref[...] = acc
        for d in range(1, self.n):
            self.copy(d).wait_send()


def vmem_spec():
    return pl.BlockSpec(memory_space=pltpu.VMEM)


def comm_call(body, args, outs, scratch, cid, name, scalars=()):
    return pl.pallas_call(
        body,
        out_shape=outs,
        in_specs=[
            pl.BlockSpec(memory_space=pltpu.SMEM) if i in scalars else vmem_spec()
            for i in range(len(args))
        ],
        out_specs=[vmem_spec()] * len(outs),
        scratch_shapes=scratch,
        compiler_params=pltpu.CompilerParams(
            collective_id=cid, has_side_effects=True, vmem_limit_bytes=62 * 2**20
        ),
        name=name,
    )(*args)


def tp_sum(partial, cid):
    rows, width = partial.shape
    line = LineSum(lax.axis_size("tp"), rows, width)

    def body(x_ref, out_ref, *refs):
        line.bind(refs)
        bar = pltpu.get_barrier_semaphore()
        peers = line.greet(bar)
        line.load(x_ref)
        pl.semaphore_wait(bar, peers)

        def one(t, carry):
            line.step(t)
            return carry

        lax.fori_loop(0, line.steps, one, 0)
        line.drain()
        line.store(out_ref)

    out = jax.ShapeDtypeStruct((rows, width), bf16)
    (summed,) = comm_call(body, [partial.astype(bf16)], [out], line.scratch(), cid, "tp_sum")
    return summed


def sum_and_scatter(partial, ats, bs, jobs, out_widths, cid, gains=None):
    rows, width = partial.shape
    n_ctx, n_seq = lax.axis_size("ctx"), lax.axis_size("seq")
    line = LineSum(lax.axis_size("tp"), rows, width)
    grads = GradScatter(n_ctx, n_seq, width, jobs)
    small = GainSum(n_ctx, n_seq)
    small_in = [] if gains is None else [gains]
    na, nb, no, ns = len(ats), len(bs), len(out_widths), len(small_in)
    n_line, n_grads = len(line.scratch()), len(grads.scratch())

    def body(x_ref, *refs):
        at_refs, b_refs = refs[:na], refs[na : na + nb]
        refs = refs[na + nb :]
        small_refs, refs = refs[:ns], refs[ns:]
        out_ref, grad_refs, refs = refs[0], refs[1 : 1 + no], refs[1 + no :]
        small_out, scratch = refs[:ns], refs[ns:]
        line.bind(scratch[:n_line])
        grads.bind(scratch[n_line : n_line + n_grads], at_refs, b_refs, grad_refs)
        bar = pltpu.get_barrier_semaphore()
        peers = line.greet(bar)
        if ns:
            small.bind(scratch[n_line + n_grads :], small_refs[0], small_out[0])
            peers = peers + small.greet(bar)
        else:
            peers = peers + grads.greet(bar)
        line.load(x_ref)
        pl.semaphore_wait(bar, peers)
        if ns:
            small.start()

        def one(it, carry):
            grads.early(it)
            for v in range(pace):
                line.piece(it * pace + v)
            grads.late(it)
            return carry

        lax.fori_loop(0, max(-(-line.steps * row_chains // pace), grads.steps), one, 0)
        if ns:
            small.finish()
        line.drain()
        grads.drain()
        line.store(out_ref)

    outs = [jax.ShapeDtypeStruct((rows, width), bf16)] + [
        jax.ShapeDtypeStruct((grads.rows, w), f32) for w in out_widths
    ]
    outs += [jax.ShapeDtypeStruct((8, lanes), f32)] * ns
    res = comm_call(
        body, [partial.astype(bf16)] + list(ats) + list(bs) + small_in, outs,
        line.scratch() + grads.scratch() + (small.scratch() if ns else []), cid, "sum_and_scatter",
    )
    return res[0], res[1:]


class LineSmall:
    def __init__(self, n, rows):
        self.n, self.rows = n, rows

    def scratch(self):
        sem = pltpu.SemaphoreType.DMA
        return [
            pltpu.VMEM((8, self.rows), f32), pltpu.VMEM((self.n - 1, 8, self.rows), f32),
            sem((self.n - 1,)), sem((self.n - 1,)),
        ]

    def bind(self, refs):
        self.mine, self.got, self.sent, self.done = refs
        self.i = lax.axis_index("tp")

    def greet(self, bar):
        for d in range(1, self.n):
            pl.semaphore_signal(
                bar, inc=1, device_id={"tp": lax.rem(self.i + d, self.n)}, device_id_type=MESH
            )
        return self.n - 1

    def copy(self, d):
        return remote(
            self.mine, self.got.at[d - 1], self.sent.at[d - 1], self.done.at[d - 1],
            {"tp": lax.rem(self.i + d, self.n)},
        )

    def total(self, columns):
        self.mine[...] = jnp.transpose(columns)[:8]
        for d in range(1, self.n):
            self.copy(d).start()
        acc = self.mine[...]
        for d in range(1, self.n):
            self.copy(d).wait_recv()
            acc = acc + self.got[d - 1]
        for d in range(1, self.n):
            self.copy(d).wait_send()
        return jnp.transpose(jnp.concatenate([acc, jnp.zeros((lanes - 8, self.rows), f32)], axis=0))


def lane_pair(first, second, rows):
    lane = lax.broadcasted_iota(jnp.int32, (rows, lanes), 1)
    return jnp.where(lane == 0, first, 0.0) + jnp.where(lane == 1, second, 0.0)


def dot_nt(left, right):
    return lax.dot_general(left, right, (((1,), (1,)), ((), ())), preferred_element_type=f32)


def dot_tn(left, right):
    return lax.dot_general(left, right, (((0,), (0,)), ((), ())), preferred_element_type=f32)


def attention_back(
    back, grad, proj, attn_gain, w_output, query_rot, keys, values, attn, lse, pos_row, order,
    query_norm, key_norm, scales, qgain, kgain, cosine, sine, cid,
):
    rows, width = back.shape
    local = w_output.shape[0]
    head_dim = lanes
    heads = local // head_dim
    count = keys.shape[0]
    nx, n_tp = lax.axis_size("ctx") // 2, lax.axis_size("tp")
    small = LineSmall(n_tp, rows)
    n_small = len(small.scratch())
    scale = head_dim ** (-0.5)
    tile = 64
    sub = rows // 2

    def body(
        back_ref, grad_ref, proj_ref, again_ref, w_ref, q_ref, k_ref, v_ref, attn_ref, lse_ref,
        prow_ref, order_ref, qn_ref, kn_ref, sc_ref, qg_ref, kg_ref, cos_ref, sin_ref,
        dqkv_ref, dprojt_ref, dagain_ref, dqg_ref, dkg_ref,
        dproj, dout, columns, delta, dqs, dks, send0, keep, recv0, recv1,
        s0, d0, s1, d1, *small_refs,
    ):
        small.bind(small_refs)
        ctx = lax.axis_index("ctx")
        mx, core = ctx // 2, lax.rem(ctx, 2)
        bar = pltpu.get_barrier_semaphore()
        mate = {"ctx": mx * 2 + 1 - core}
        peers = small.greet(bar) + nx
        pl.semaphore_signal(bar, inc=1, device_id=mate, device_id_type=MESH)
        for d in range(1, nx):
            pl.semaphore_signal(
                bar, inc=1, device_id={"ctx": lax.rem(mx + d, nx) * 2 + core}, device_id_type=MESH
            )

        dagain_ref[...] = jnp.zeros_like(dagain_ref)

        def norm_rows(t, carry):
            sl = pl.ds(pl.multiple_of(t * tile, tile), tile)
            dres = grad_ref[sl].astype(f32) + back_ref[sl].astype(f32)
            out = proj_ref[sl].astype(f32)
            inv = lax.rsqrt(jnp.mean(out * out, axis=1, keepdims=True) + norm_eps)
            norm = out * inv
            dagain_ref[...] += jnp.sum(dres * norm, axis=0, keepdims=True)
            dnorm = dres * again_ref[...]
            dot = jnp.mean(dnorm * norm, axis=1, keepdims=True)
            dproj[sl] = (inv * (dnorm - norm * dot)).astype(bf16)
            return carry

        lax.fori_loop(0, rows // tile, norm_rows, 0)
        for h in range(local // sub):
            dout[:, h * sub : (h + 1) * sub] = dot_nt(
                dproj[...], w_ref[h * sub : (h + 1) * sub, :]
            ).astype(bf16)
        lane = lax.broadcasted_iota(jnp.int32, (rows, lanes), 1)
        acc = jnp.zeros((rows, lanes), f32)
        for h in range(heads):
            hs = slice(h * head_dim, (h + 1) * head_dim)
            row_sum = jnp.sum(
                dout[:, hs].astype(f32) * attn_ref[:, hs].astype(f32), axis=1, keepdims=True
            )
            acc = jnp.where(lane == h, row_sum, acc)
        columns[...] = acc
        delta[...] = jnp.transpose(columns[...])[:8]
        dqs[...] = jnp.zeros_like(dqs)
        pl.semaphore_wait(bar, peers)

        def c0(h):
            slot = lax.rem(h, 2)
            return remote(send0.at[slot], recv0.at[h], s0.at[slot], d0.at[h], mate)

        def c1(h, d):
            to = lax.rem(mx + d, nx)
            return remote(
                recv0.at[h, to], recv1.at[h, d - 1], s1.at[h, d - 1], d1.at[h, d - 1],
                {"ctx": to * 2 + core},
            )

        def one_block(h, hs, x, owner, write):
            start = (x * 2 + owner) * rows
            for part in range(rows // sub):
                ks = pl.ds(pl.multiple_of(start + part * sub, sub), sub)
                key, value = k_ref[ks, hs], v_ref[ks, hs]
                query, dhead = q_ref[:, hs], dout[:, hs]
                score = dot_nt(key, query) * scale
                place = order_ref[0, (x * 2 + owner) * 2 + part] * sub
                seen = place + lax.broadcasted_iota(jnp.int32, (sub, rows), 0) <= prow_ref[...]
                share = jnp.where(seen, jnp.exp(score - lse_ref[pl.ds(h, 1), :]), 0.0)
                dshare = dot_nt(value, dhead)
                dscore = (share * (dshare - delta[pl.ds(h, 1), :]) * scale).astype(bf16)
                dqs[:, hs] += dot_tn(dscore, key)
                write(
                    x, slice(part * sub, (part + 1) * sub),
                    jnp.dot(dscore, query, preferred_element_type=f32),
                    jnp.dot(share.astype(bf16), dhead, preferred_element_type=f32),
                )

        def one_head(h):
            hs = pl.ds(pl.multiple_of(h * head_dim, head_dim), head_dim)
            slot = lax.rem(h, 2)

            def to_send(x, rs, dk, dv):
                send0[slot, x, rs, :lanes] = dk.astype(bf16)
                send0[slot, x, rs, lanes:] = dv.astype(bf16)

            def to_keep(x, rs, dk, dv):
                keep[slot, x, rs, :lanes] = dk.astype(bf16)
                keep[slot, x, rs, lanes:] = dv.astype(bf16)

            @pl.when(h >= 2)
            def _():
                c0(h).wait_send()

            def mates(e, carry):
                one_block(h, hs, lax.rem(mx + 1 + e, nx), 1 - core, to_send)
                return carry

            lax.fori_loop(0, nx, mates, 0)
            c0(h).start()

            def owns(e, carry):
                one_block(h, hs, lax.rem(mx + 1 + e, nx), core, to_keep)
                return carry

            lax.fori_loop(0, nx, owns, 0)
            c0(h).wait_recv()

            def add(x, carry):
                recv0[h, x] = (keep[slot, x].astype(f32) + recv0[h, x].astype(f32)).astype(bf16)
                return carry

            lax.fori_loop(0, nx, add, 0)
            for d in range(1, nx):
                c1(h, d).start()

        def heads_loop(h, carry):
            one_head(h)
            return carry

        lax.fori_loop(0, heads, heads_loop, 0)

        dot_q = jnp.zeros((rows, 1), f32)
        for h in range(heads):
            hs = slice(h * head_dim, (h + 1) * head_dim)
            dq = dqs[:, hs]
            dq = dq * cos_ref[...] - pltpu.roll(dq, head_dim // 2, 1) * sin_ref[...]
            norm = qn_ref[:, hs]
            dqg_ref[:, hs] = jnp.sum(dq * norm, axis=0, keepdims=True)
            dq = dq * qg_ref[:, hs]
            dqs[:, hs] = dq
            dot_q = dot_q + jnp.sum(dq * norm, axis=1, keepdims=True)
        dprojt_ref[...] = jnp.transpose(dproj[...])
        dot_k = jnp.zeros((rows, 1), f32)
        for h in range(heads):
            hs = slice(h * head_dim, (h + 1) * head_dim)
            total = recv0[h, mx].astype(f32)
            for d in range(1, nx):
                c1(h, d).wait_recv()
                total = total + recv1[h, d - 1].astype(f32)
            dqkv_ref[:, 2 * local + h * head_dim : 2 * local + (h + 1) * head_dim] = total[
                :, lanes:
            ].astype(bf16)
            dk = total[:, :lanes]
            dk = dk * cos_ref[...] - pltpu.roll(dk, head_dim // 2, 1) * sin_ref[...]
            norm = kn_ref[:, hs]
            dkg_ref[:, hs] = jnp.sum(dk * norm, axis=0, keepdims=True)
            dk = dk * kg_ref[:, hs]
            dks[:, hs] = dk
            dot_k = dot_k + jnp.sum(dk * norm, axis=1, keepdims=True)
        dots = small.total(lane_pair(dot_q, dot_k, rows)) * (1.0 / width)
        for h in range(heads):
            hs = slice(h * head_dim, (h + 1) * head_dim)
            dqkv_ref[:, hs] = (
                sc_ref[:, 0:1] * (dqs[:, hs] - qn_ref[:, hs] * dots[:, 0:1])
            ).astype(bf16)
            dqkv_ref[:, local + h * head_dim : local + (h + 1) * head_dim] = (
                sc_ref[:, 1:2] * (dks[:, hs] - kn_ref[:, hs] * dots[:, 1:2])
            ).astype(bf16)
        for h in range(heads):
            if h >= heads - 2:
                c0(h).wait_send()
            for d in range(1, nx):
                c1(h, d).wait_send()

    sem = pltpu.SemaphoreType.DMA
    pair = (rows, 2 * lanes)
    return comm_call(
        body,
        [back, grad, proj, attn_gain, w_output, query_rot, keys, values, attn, lse, pos_row,
         order, query_norm, key_norm, scales, qgain, kgain, cosine, sine],
        [
            jax.ShapeDtypeStruct((rows, 3 * local), bf16),
            jax.ShapeDtypeStruct((width, rows), bf16),
            jax.ShapeDtypeStruct((1, width), f32),
            jax.ShapeDtypeStruct((1, local), f32),
            jax.ShapeDtypeStruct((1, local), f32),
        ],
        [
            pltpu.VMEM((rows, width), bf16), pltpu.VMEM((rows, local), bf16),
            pltpu.VMEM((rows, lanes), f32), pltpu.VMEM((8, rows), f32),
            pltpu.VMEM((rows, local), f32), pltpu.VMEM((rows, local), f32),
            pltpu.VMEM((2, nx) + pair, bf16), pltpu.VMEM((2, nx) + pair, bf16),
            pltpu.VMEM((heads, nx) + pair, bf16), pltpu.VMEM((heads, nx - 1) + pair, bf16),
            sem((2,)), sem((heads,)), sem((heads, nx - 1)), sem((heads, nx - 1)),
        ] + small.scratch(),
        cid, "attention_back", {11},
    )


def front(tokens, w_query, w_key, w_value, w_output, qgain, kgain, cosine, sine, order, cid):
    rows, width = tokens.shape
    local = w_query.shape[1]
    head_dim = lanes
    heads = local // head_dim
    nx = lax.axis_size("ctx") // 2
    count = nx * 2 * rows
    n_tp = lax.axis_size("tp")
    small = LineSmall(n_tp, rows)
    line = LineSum(n_tp, rows, width)
    n_small, n_line = len(small.scratch()), len(line.scratch())
    scale = head_dim ** (-0.5)
    group = rows // 2

    def body(
        tok_hbm, wq_hbm, wk_hbm, wv_hbm, wo_hbm, qg_ref, kg_ref, cos_ref, sin_ref, order_ref,
        qrot_out, key_out, value_out, qn_out, kn_out, attn_out, sc_out, lse_out, proj_out,
        tok, w3, wo, qn, kn, qrot, keys, values, peak, total, acc, attn, loads, stores,
        sx, dx, sm, dm, sf, df, *rest,
    ):
        small.bind(rest[:n_small])
        line.bind(rest[n_small : n_small + n_line])
        copies = [
            pltpu.make_async_copy(src, dst, loads.at[i])
            for i, (src, dst) in enumerate(
                [(tok_hbm, tok), (wv_hbm, w3.at[2]), (wq_hbm, w3.at[0]), (wk_hbm, w3.at[1]),
                 (wo_hbm, wo)]
            )
        ]
        for copy in copies:
            copy.start()
        ctx = lax.axis_index("ctx")
        mx, core = ctx // 2, lax.rem(ctx, 2)
        mate = {"ctx": mx * 2 + 1 - core}

        def peer(d):
            return {"ctx": lax.rem(mx + d, nx) * 2 + core}

        bar = pltpu.get_barrier_semaphore()
        pl.semaphore_signal(bar, inc=1, device_id=mate, device_id_type=MESH)
        for d in range(1, nx):
            pl.semaphore_signal(bar, inc=1, device_id=peer(d), device_id_type=MESH)
        peers = small.greet(bar) + nx

        def at(x, owner):
            return pl.ds(pl.multiple_of((x * 2 + owner) * rows, rows), rows)

        mine = at(mx, core)
        boxes = [keys, values]

        def to_peer(b, d):
            box = boxes[b]
            return remote(
                box.at[mine], box.at[mine], sx.at[b, d - 1], dx.at[b, d - 1], peer(d)
            )

        def from_peer(b, d):
            box = boxes[b]
            rs = at(lax.rem(mx + nx - d, nx), core)
            return remote(box.at[rs], box.at[rs], sx.at[b, d - 1], dx.at[b, d - 1], peer(d))

        def to_mate(b):
            box = boxes[b]
            return remote(box.at[mine], box.at[mine], sm.at[b], dm.at[b], mate)

        def from_mate(b):
            box = boxes[b]
            rs = at(mx, 1 - core)
            return remote(box.at[rs], box.at[rs], sm.at[b], dm.at[b], mate)

        def pass_on(b, d):
            box = boxes[b]
            rs = at(lax.rem(mx + nx - d, nx), core)
            return remote(box.at[rs], box.at[rs], sf.at[b, d - 1], df.at[b, d - 1], mate)

        def passed(b, d):
            box = boxes[b]
            rs = at(lax.rem(mx + nx - d, nx), 1 - core)
            return remote(box.at[rs], box.at[rs], sf.at[b, d - 1], df.at[b, d - 1], mate)

        copies[0].wait()
        copies[1].wait()
        values[mine] = jnp.dot(tok[...], w3[2], preferred_element_type=f32).astype(bf16)
        pl.semaphore_wait(bar, peers)
        for d in range(1, nx):
            to_peer(1, d).start()
        to_mate(1).start()
        copies[2].wait()
        qn[...] = jnp.dot(tok[...], w3[0], preferred_element_type=f32)
        copies[3].wait()
        kn[...] = jnp.dot(tok[...], w3[1], preferred_element_type=f32)

        def squares(ref):
            acc_sq = jnp.zeros((rows, 1), f32)
            for h in range(heads):
                part = ref[:, h * head_dim : (h + 1) * head_dim]
                acc_sq = acc_sq + jnp.sum(part * part, axis=1, keepdims=True)
            return acc_sq

        sums = small.total(lane_pair(squares(qn), squares(kn), rows))
        scales = lax.rsqrt(sums * (1.0 / width) + norm_eps)
        sc_out[...] = scales

        def rotated(ref, column, gain_ref, h):
            hs = slice(h * head_dim, (h + 1) * head_dim)
            norm = ref[:, hs] * sc_out[:, column : column + 1]
            ref[:, hs] = norm
            norm = norm * gain_ref[:, hs]
            return (
                norm * cos_ref[...] + pltpu.roll(norm, head_dim // 2, 1) * sin_ref[...]
            ).astype(bf16)

        for h in range(heads):
            keys[mine, h * head_dim : (h + 1) * head_dim] = rotated(kn, 1, kg_ref, h)
        for d in range(1, nx):
            to_peer(0, d).start()
        to_mate(0).start()
        for h in range(heads):
            qrot[:, h * head_dim : (h + 1) * head_dim] = rotated(qn, 0, qg_ref, h)
        peak[...] = jnp.full_like(peak, masked_score)
        total[...] = jnp.zeros_like(total)
        acc[...] = jnp.zeros_like(acc)

        def places(block, shape, axis):
            spot = lax.broadcasted_iota(jnp.int32, shape, axis)
            first, second = order_ref[0, block * 2], order_ref[0, block * 2 + 1]
            return jnp.where(spot < group, first * group + spot, (second - 1) * group + spot)

        def attend(x, owner):
            block = x * 2 + owner
            rs = at(x, owner)

            def one(h, carry):
                hs = pl.ds(pl.multiple_of(h * head_dim, head_dim), head_dim)
                score = dot_nt(qrot[:, hs], keys[rs, hs]) * scale
                seen = places(block, (1, rows), 1) <= places(ctx, (rows, 1), 0)
                old = peak[h]
                new = jnp.maximum(
                    old, jnp.max(jnp.where(seen, score, masked_score), axis=1, keepdims=True)
                )
                share = jnp.where(seen, jnp.exp(score - new), 0.0)
                fade = jnp.exp(old - new)
                peak[h] = new
                total[h] = total[h] * fade + jnp.sum(share, axis=1, keepdims=True)
                acc[:, hs] = acc[:, hs] * fade + jnp.dot(
                    share.astype(bf16), values[rs, hs], preferred_element_type=f32
                )
                return carry

            lax.fori_loop(0, heads, one, 0)

        attend(mx, core)
        for d in range(1, nx):
            from_peer(1, d).wait_recv()
            pass_on(1, d).start()
        from_mate(1).wait_recv()
        from_mate(0).wait_recv()
        attend(mx, 1 - core)
        for d in range(1, nx):
            from_peer(0, d).wait_recv()
            pass_on(0, d).start()
            attend(lax.rem(mx + nx - d, nx), core)
        for d in range(1, nx):
            passed(1, d).wait_recv()
            passed(0, d).wait_recv()
            attend(lax.rem(mx + nx - d, nx), 1 - core)

        lane = lax.broadcasted_iota(jnp.int32, (rows, lanes), 1)
        logs = jnp.zeros((rows, lanes), f32)
        for h in range(heads):
            hs = slice(h * head_dim, (h + 1) * head_dim)
            attn[:, hs] = (acc[:, hs] / total[h]).astype(bf16)
            logs = jnp.where(lane == h, peak[h] + jnp.log(total[h]), logs)
        lse_out[...] = jnp.transpose(logs)[:8]
        outs = [
            pltpu.make_async_copy(src, dst, stores.at[i])
            for i, (src, dst) in enumerate(
                [(qrot, qrot_out), (keys, key_out), (values, value_out), (qn, qn_out),
                 (kn, kn_out), (attn, attn_out)]
            )
        ]
        for copy in outs:
            copy.start()
        copies[4].wait()
        for j in range(n_tp):
            line.own[j] = jnp.dot(
                attn[...], wo[:, j * line.part : (j + 1) * line.part], preferred_element_type=f32
            ).astype(bf16)

        def one(t, carry):
            line.step(t)
            return carry

        lax.fori_loop(0, line.steps, one, 0)
        line.drain()
        line.store(proj_out)
        for copy in outs:
            copy.wait()
        for b in range(2):
            to_mate(b).wait_send()
            for d in range(1, nx):
                to_peer(b, d).wait_send()
                pass_on(b, d).wait_send()

    sem = pltpu.SemaphoreType.DMA
    hbm = pl.BlockSpec(memory_space=pl.ANY)
    block = jax.ShapeDtypeStruct
    return pl.pallas_call(
        body,
        out_shape=[
            block((rows, local), bf16), block((count, local), bf16), block((count, local), bf16),
            block((rows, local), f32), block((rows, local), f32), block((rows, local), bf16),
            block((rows, lanes), f32), block((8, rows), f32), block((rows, width), bf16),
        ],
        in_specs=[hbm] * 5 + [vmem_spec()] * 4 + [pl.BlockSpec(memory_space=pltpu.SMEM)],
        out_specs=[hbm] * 6 + [vmem_spec()] * 3,
        scratch_shapes=[
            pltpu.VMEM((rows, width), bf16), pltpu.VMEM((3, width, local), bf16),
            pltpu.VMEM((local, width), bf16), pltpu.VMEM((rows, local), f32),
            pltpu.VMEM((rows, local), f32), pltpu.VMEM((rows, local), bf16),
            pltpu.VMEM((count, local), bf16), pltpu.VMEM((count, local), bf16),
            pltpu.VMEM((heads, rows, 1), f32), pltpu.VMEM((heads, rows, 1), f32),
            pltpu.VMEM((rows, local), f32), pltpu.VMEM((rows, local), bf16),
            sem((5,)), sem((6,)),
            sem((2, nx - 1)), sem((2, nx - 1)), sem((2,)), sem((2,)),
            sem((2, nx - 1)), sem((2, nx - 1)),
        ] + small.scratch() + line.scratch(),
        compiler_params=pltpu.CompilerParams(
            collective_id=cid, has_side_effects=True, vmem_limit_bytes=62 * 2**20
        ),
        name="front",
    )(tokens, w_query, w_key, w_value, w_output, qgain, kgain, cosine, sine, order)


norm_eps = 1e-06
rope_base = 500000.0
masked_score = -1e30


def matmul(left, right):
    return jnp.dot(left, right, preferred_element_type=jnp.float32)


def rope_tables(positions, head_dim):
    half = head_dim // 2
    rates = rope_base ** (-(jnp.arange(half, dtype=jnp.float32) * 2.0 / head_dim))
    angle = positions.astype(jnp.float32)[:, None] * rates[None, :]
    return (jnp.cos(angle), jnp.sin(angle))


def key_positions(order, first_row, count, group):
    row_ids = first_row + jnp.arange(count, dtype=jnp.int32)
    slots = row_ids // group
    picks = slots[:, None] == jnp.arange(order.shape[0], dtype=jnp.int32)[None, :]
    return jnp.sum(jnp.where(picks, order[None, :], 0), axis=1) * group + row_ids % group


def per_device(
    tokens,
    out_grad,
    group_order,
    w_query,
    w_key,
    w_value,
    query_gain,
    key_gain,
    w_output,
    attn_gain,
    w_gate,
    w_up,
    w_down,
    mlp_gain,
):
    inputs_bf = tokens[0]
    order = group_order[0]
    row_count, width = inputs_bf.shape
    heads, head_dim = query_gain.shape
    local = heads * head_dim
    group = row_count // 2
    query_pos = key_positions(order, lax.axis_index("ctx") * row_count, row_count, group)
    cosine, sine = rope_tables(query_pos, head_dim)
    inputs = inputs_bf.astype(jnp.float32)
    qgain = query_gain.reshape(local)
    kgain = key_gain.reshape(local)
    angle_cos = jnp.concatenate([cosine, cosine], axis=1)
    angle_sin = jnp.concatenate([-sine, sine], axis=1)
    (query_rot, whole_keys, whole_values, query_norm, key_norm, attn_flat, scales, lse,
     proj_sum) = front(
        inputs_bf, w_query, w_key, w_value, w_output, qgain[None], kgain[None], angle_cos,
        angle_sin, group_order, 1,
    )
    proj = proj_sum.astype(f32)
    attn_scale = lax.rsqrt(jnp.mean(proj * proj, axis=1) + norm_eps)
    attn_norm = proj * attn_scale[:, None]
    resid = inputs + attn_norm * attn_gain
    hidden = resid.astype(jnp.bfloat16)
    gate = matmul(hidden, w_gate)
    up = matmul(hidden, w_up)
    sigma = jax.nn.sigmoid(gate)
    active = gate * sigma
    inner = (active * up).astype(jnp.bfloat16)
    down = tp_sum(matmul(inner, w_down), 2).astype(f32)
    mlp_scale = lax.rsqrt(jnp.mean(down * down, axis=1) + norm_eps)
    mlp_norm = down * mlp_scale[:, None]
    block_out = resid + mlp_norm * mlp_gain
    upstream = out_grad[0].astype(jnp.float32)
    d_mlp_gain = jnp.sum(upstream * mlp_norm, axis=0)
    d_mnorm = upstream * mlp_gain
    d_down = (
        mlp_scale[:, None]
        * (d_mnorm - mlp_norm * jnp.mean(d_mnorm * mlp_norm, axis=1, keepdims=True))
    ).astype(jnp.bfloat16)
    d_inner = matmul(d_down, w_down.T)
    d_gate = (d_inner * up * sigma * (1.0 + gate * (1.0 - sigma))).astype(jnp.bfloat16)
    d_up = (d_inner * active).astype(jnp.bfloat16)
    hidden_t = hidden.T
    wide = inner.shape[1] // (2 * lanes)
    half = wide // 2
    back, (grad_down, grad_gate_a) = sum_and_scatter(
        matmul(d_gate, w_gate.T) + matmul(d_up, w_up.T),
        [d_down.T, hidden_t],
        [inner, d_gate],
        [
            dict(a=0, b=0, first=0, count=wide, out=0, place=0),
            dict(a=1, b=1, first=0, count=half, out=1, place=0),
        ],
        [inner.shape[1], half * 2 * lanes],
        3,
    )
    d_qkv, d_proj_t, d_attn_gain, d_query_gain, d_key_gain = attention_back(
        back, out_grad[0], proj_sum, attn_gain[None], w_output, query_rot,
        whole_keys, whole_values, attn_flat, lse, query_pos[None], group_order,
        query_norm, key_norm, scales, qgain[None], kgain[None], angle_cos, angle_sin, 5,
    )
    d_query_gain = d_query_gain.reshape(heads, head_dim)
    d_key_gain = d_key_gain.reshape(heads, head_dim)
    d_query, d_key, d_value = (d_qkv[:, i * local : (i + 1) * local] for i in range(3))
    thin = local // (2 * lanes)
    owners = lax.axis_size("ctx") * lax.axis_size("seq")
    pieces = [
        d_attn_gain.reshape(owners, -1),
        d_mlp_gain.reshape(owners, -1),
        d_query_gain.reshape(heads, owners, -1).transpose(1, 0, 2).reshape(owners, -1),
        d_key_gain.reshape(heads, owners, -1).transpose(1, 0, 2).reshape(owners, -1),
    ]
    cuts = [piece.shape[1] for piece in pieces]
    packed = jnp.concatenate(pieces, axis=1)
    packed = jnp.pad(packed, ((0, 0), (0, 8 * lanes - packed.shape[1]))).reshape(owners, 8, lanes)
    last, (grad_gate_b, grad_up, grad_qkv, grad_output, small) = sum_and_scatter(
        matmul(d_query, w_query.T) + matmul(d_key, w_key.T) + matmul(d_value, w_value.T),
        [hidden_t, inputs_bf.T, d_proj_t],
        [d_gate, d_up, d_qkv, attn_flat],
        [
            dict(a=0, b=0, first=half, count=wide - half, out=0, place=0),
            dict(a=0, b=1, first=0, count=wide, out=1, place=0),
            dict(a=2, b=3, first=0, count=thin, out=3, place=0),
            dict(a=1, b=2, first=0, count=3 * thin, out=2, place=0),
        ],
        [(wide - half) * 2 * lanes, inner.shape[1], 3 * local, local],
        4,
        packed,
    )
    small = small.reshape(-1)
    g_attn, g_mlp, g_query, g_key = jnp.split(
        small[: sum(cuts)], [cuts[0], cuts[0] + cuts[1], cuts[0] + cuts[1] + cuts[2]]
    )
    input_grad = upstream + back.astype(f32) + last.astype(f32)
    grad_query, grad_key, grad_value = jnp.split(grad_qkv, 3, axis=1)
    grad_gate = jnp.concatenate([grad_gate_a, grad_gate_b], axis=1)
    summed = (
        grad_query,
        grad_key,
        grad_value,
        g_query.reshape(heads, -1),
        g_key.reshape(heads, -1),
        grad_output.T,
        g_attn,
        grad_gate,
        grad_up,
        grad_down.T,
        g_mlp,
    )
    return (
        block_out[None],
        input_grad[None],
        summed[0],
        summed[1],
        summed[2],
        summed[3],
        summed[4],
        summed[5],
        summed[6],
        summed[7],
        summed[8],
        summed[9],
        summed[10],
    )


def solution(mesh):
    return jax.shard_map(
        per_device,
        mesh=mesh,
        in_specs=(
            P("seq", "ctx", None),
            P("seq", "ctx", None),
            P("seq", None),
            P(None, "tp"),
            P(None, "tp"),
            P(None, "tp"),
            P("tp", None),
            P("tp", None),
            P("tp", None),
            P(),
            P(None, "tp"),
            P(None, "tp"),
            P("tp", None),
            P(),
        ),
        out_specs=(
            P("seq", "ctx", None),
            P("seq", "ctx", None),
            P(("ctx", "seq"), "tp"),
            P(("ctx", "seq"), "tp"),
            P(("ctx", "seq"), "tp"),
            P("tp", ("ctx", "seq")),
            P("tp", ("ctx", "seq")),
            P("tp", ("ctx", "seq")),
            P(("ctx", "seq")),
            P(("ctx", "seq"), "tp"),
            P(("ctx", "seq"), "tp"),
            P("tp", ("ctx", "seq")),
            P(("ctx", "seq")),
        ),
        check_vma=False,
    )
```

```python
import jax
import jax.numpy as jnp
from jax import lax
from jax.sharding import PartitionSpec as P
from jax.experimental import pallas as pl
from jax.experimental.pallas import tpu as pltpu

norm_eps = 1e-06
rope_base = 500000.0
masked_score = -1e30


def rope_tables(positions, head_dim):
    half = head_dim // 2
    rates = rope_base ** (-(jnp.arange(half, dtype=jnp.float32) * 2.0 / head_dim))
    angle = positions.astype(jnp.float32)[:, None] * rates[None, :]
    return (jnp.cos(angle), jnp.sin(angle))


def key_positions(order, first_row, count, group):
    row_ids = first_row + jnp.arange(count, dtype=jnp.int32)
    slots = row_ids // group
    picks = slots[:, None] == jnp.arange(order.shape[0], dtype=jnp.int32)[None, :]
    return jnp.sum(jnp.where(picks, order[None, :], 0), axis=1) * group + row_ids % group


MESH = pl.DeviceIdType.MESH
bf16 = jnp.bfloat16
f32 = jnp.float32
lanes = 128
row_blocks = 16
row_chains = 8
pace = 6


def remote(src, dst, send, recv, where):
    return pltpu.make_async_remote_copy(
        src, dst, send, recv, device_id=where, device_id_type=MESH
    )


class LineSum:
    def __init__(self, n, rows, width):
        self.n, self.rows, self.width = n, rows, width
        self.part = width // n
        self.rc = rows // row_blocks
        self.total = row_blocks // row_chains * n
        self.steps = self.total + n - 1

    def scratch(self):
        shape = (self.n, self.rows, self.part)
        return [pltpu.VMEM(shape, bf16)] * 4 + [
            pltpu.SemaphoreType.DMA((row_chains, self.total))
        ] * 4

    def bind(self, refs):
        self.own, self.from_l, self.from_r, self.res = refs[:4]
        self.send_r, self.send_l, self.recv_l, self.recv_r = refs[4:]
        self.i = lax.axis_index("tp")
        self.has_l, self.has_r = self.i > 0, self.i < self.n - 1

    def greet(self, bar):
        @pl.when(self.has_l)
        def _():
            pl.semaphore_signal(bar, inc=1, device_id={"tp": self.i - 1}, device_id_type=MESH)

        @pl.when(self.has_r)
        def _():
            pl.semaphore_signal(bar, inc=1, device_id={"tp": self.i + 1}, device_id_type=MESH)

        return self.has_l.astype(jnp.int32) + self.has_r.astype(jnp.int32)

    def load(self, x_ref):
        for j in range(self.n):
            self.own[j] = x_ref[:, j * self.part : (j + 1) * self.part]

    def rows_of(self, g, p):
        block = (p // self.n) * row_chains + g
        return pl.ds(pl.multiple_of(block * self.rc, self.rc), self.rc)

    def right(self, src, dst, g, p, j):
        sl = self.rows_of(g, p)
        return remote(
            src.at[j, sl], dst.at[j, sl], self.send_r.at[g, p], self.recv_l.at[g, p],
            {"tp": self.i + 1},
        )

    def left(self, src, dst, g, q, j):
        sl = self.rows_of(g, q)
        return remote(
            src.at[j, sl], dst.at[j, sl], self.send_l.at[g, q], self.recv_r.at[g, q],
            {"tp": self.i - 1},
        )

    def wait_l(self, g, p, j):
        sl = self.rows_of(g, p)
        remote(
            self.own.at[j, sl], self.from_l.at[j, sl], self.send_r.at[g, p], self.recv_l.at[g, p],
            {"tp": self.i - 1},
        ).wait_recv()

    def wait_r(self, g, q, j):
        sl = self.rows_of(g, q)
        remote(
            self.own.at[j, sl], self.from_r.at[j, sl], self.send_l.at[g, q], self.recv_r.at[g, q],
            {"tp": self.i + 1},
        ).wait_recv()

    def step(self, t):
        for g in range(row_chains):
            self.sub_step(t, g)

    def piece(self, e):
        t = e // row_chains

        @pl.when(t < self.steps)
        def _():
            self.sub_step(t, lax.rem(e, row_chains))

    def sub_step(self, t, g):
        n, i, has_l, has_r = self.n, self.i, self.has_l, self.has_r
        own, from_l, from_r, res = self.own, self.from_l, self.from_r, self.res
        p = t - i
        q = t - (n - 1 - i)
        jr = n - 1 - lax.rem(p + n * self.total, n)
        jl = lax.rem(q + n * self.total, n)
        pv = (p >= 0) & (p < self.total)
        qv = (q >= 0) & (q < self.total)

        @pl.when(pv & has_l)
        def _():
            self.wait_l(g, p, jr)

        @pl.when(qv & has_r)
        def _():
            self.wait_r(g, q, jl)

        @pl.when(pv & (jr > i))
        def _():
            sl = self.rows_of(g, p)

            @pl.when(has_l)
            def _():
                own[jr, sl] = (own[jr, sl].astype(f32) + from_l[jr, sl].astype(f32)).astype(bf16)

            self.right(own, from_l, g, p, jr).start()

        @pl.when(qv & (jl < i))
        def _():
            sl = self.rows_of(g, q)

            @pl.when(has_r)
            def _():
                own[jl, sl] = (own[jl, sl].astype(f32) + from_r[jl, sl].astype(f32)).astype(bf16)

            self.left(own, from_r, g, q, jl).start()

        @pl.when(pv & (jr == i))
        def _():
            sl = self.rows_of(g, p)

            @pl.when(has_l & has_r)
            def _():
                res[i, sl] = (
                    own[i, sl].astype(f32) + from_l[i, sl].astype(f32) + from_r[i, sl].astype(f32)
                ).astype(bf16)

            @pl.when(jnp.logical_not(has_l))
            def _():
                res[i, sl] = (own[i, sl].astype(f32) + from_r[i, sl].astype(f32)).astype(bf16)

            @pl.when(jnp.logical_not(has_r))
            def _():
                res[i, sl] = (own[i, sl].astype(f32) + from_l[i, sl].astype(f32)).astype(bf16)

        @pl.when(pv & (jr <= i) & has_r)
        def _():
            self.right(res, res, g, p, jr).start()

        @pl.when(qv & (jl >= i) & has_l)
        def _():
            self.left(res, res, g, q, jl).start()

    def drain(self):
        def one(p, carry):
            for g in range(row_chains):

                @pl.when(self.has_r)
                def _():
                    self.right(self.own, self.from_l, g, p, 0).wait_send()

                @pl.when(self.has_l)
                def _():
                    self.left(self.own, self.from_r, g, p, 0).wait_send()

            return carry

        lax.fori_loop(0, self.total, one, 0)

    def ship(self, out_ref, sems, base):
        copies = []
        for j in range(self.n):
            cols = pl.ds(j * self.part, self.part)
            copy = pltpu.make_async_copy(self.res.at[j], out_ref.at[:, cols], sems.at[base + j])
            copy.start()
            copies.append(copy)
        for copy in copies:
            copy.wait()

    def store(self, out_ref):
        for j in range(self.n):
            out_ref[:, j * self.part : (j + 1) * self.part] = self.res[j]


class GradScatter:
    def __init__(self, n_ctx, n_seq, width, jobs):
        self.nx, self.ny = n_ctx // 2, n_seq
        self.rows = width // (n_ctx * n_seq)
        self.jobs = jobs
        start = 0
        self.spans = []
        for job in jobs:
            self.spans.append((start, start + job["count"]))
            start += job["count"]
        self.total = start
        self.steps = start + 5

    def scratch(self):
        nx, ny, r, t = self.nx, self.ny, self.rows, self.total
        tile = (r, lanes)
        sem = pltpu.SemaphoreType.DMA
        return [
            pltpu.VMEM((2, nx, ny, 2) + tile, bf16),
            pltpu.VMEM((2, nx, ny, 2) + tile, f32),
            pltpu.VMEM((t, nx, ny, 2) + tile, bf16),
            pltpu.VMEM((3, nx, ny) + tile, bf16),
            pltpu.VMEM((3, ny, nx) + tile, bf16),
            pltpu.VMEM((t, nx - 1, ny) + tile, bf16),
            pltpu.VMEM((t, ny - 1, nx) + tile, bf16),
            pltpu.VMEM((3, ny) + tile, bf16),
            pltpu.VMEM((3, nx) + tile, bf16),
            pltpu.VMEM((t, ny - 1) + tile, bf16),
            pltpu.VMEM((t, nx - 1) + tile, bf16),
            sem((2,)), sem((t,)),
            sem((3, nx - 1)), sem((t, nx - 1)), sem((3, ny - 1)), sem((t, ny - 1)),
            sem((3, ny - 1)), sem((t, ny - 1)), sem((3, nx - 1)), sem((t, nx - 1)),
        ]

    def bind(self, refs, at_refs, b_refs, out_refs):
        (self.send0, self.keep, self.recv0, self.pa, self.pb, self.r1a, self.r1b, self.qa, self.qb,
         self.r2a, self.r2b, self.s0, self.d0, self.s1a, self.d1a, self.s1b, self.d1b,
         self.s2a, self.d2a, self.s2b, self.d2b) = refs
        self.at_refs, self.b_refs, self.out_refs = at_refs, b_refs, out_refs
        ctx = lax.axis_index("ctx")
        self.mx, self.core, self.my = ctx // 2, lax.rem(ctx, 2), lax.axis_index("seq")

    def at_x(self, d):
        return {"ctx": lax.rem(self.mx + d, self.nx) * 2 + self.core}

    def at_y(self, d):
        return {"seq": lax.rem(self.my + d, self.ny)}

    def at_mate(self):
        return {"ctx": self.mx * 2 + 1 - self.core}

    def greet(self, bar):
        places = [self.at_mate()]
        places += [self.at_x(d) for d in range(1, self.nx)]
        places += [self.at_y(d) for d in range(1, self.ny)]
        for place in places:
            pl.semaphore_signal(bar, inc=1, device_id=place, device_id_type=MESH)
        return len(places)

    def c0(self, c, slot):
        return remote(self.send0.at[slot], self.recv0.at[c], self.s0.at[slot], self.d0.at[c], self.at_mate())

    def c1a(self, c, slot, d):
        return remote(
            self.pa.at[slot, lax.rem(self.mx + d, self.nx)], self.r1a.at[c, d - 1],
            self.s1a.at[slot, d - 1], self.d1a.at[c, d - 1], self.at_x(d),
        )

    def c1b(self, c, slot, d):
        return remote(
            self.pb.at[slot, lax.rem(self.my + d, self.ny)], self.r1b.at[c, d - 1],
            self.s1b.at[slot, d - 1], self.d1b.at[c, d - 1], self.at_y(d),
        )

    def c2a(self, c, slot, d):
        return remote(
            self.qa.at[slot, lax.rem(self.my + d, self.ny)], self.r2a.at[c, d - 1],
            self.s2a.at[slot, d - 1], self.d2a.at[c, d - 1], self.at_y(d),
        )

    def c2b(self, c, slot, d):
        return remote(
            self.qb.at[slot, lax.rem(self.mx + d, self.nx)], self.r2b.at[c, d - 1],
            self.s2b.at[slot, d - 1], self.d2b.at[c, d - 1], self.at_x(d),
        )

    def make(self, c):
        slot = lax.rem(c, 2)
        nx, ny, r = self.nx, self.ny, self.rows

        @pl.when(c >= 2)
        def _():
            self.c0(c, slot).wait_send()

        def products(at_ref, b_ref, col, parity, write):
            def tile(e, carry):
                x, y = e // ny, lax.rem(e, ny)
                row = pl.multiple_of(((x * 2 + parity) * ny + y) * r, r)
                acc = jnp.dot(
                    at_ref[pl.ds(row, r), :], b_ref[:, pl.ds(col, 2 * lanes)],
                    preferred_element_type=f32,
                )
                write(x, y, acc)
                return carry

            lax.fori_loop(0, nx * ny, tile, 0)

        def to_send(x, y, acc):
            self.send0[slot, x, y, 0] = acc[:, :lanes].astype(bf16)
            self.send0[slot, x, y, 1] = acc[:, lanes:].astype(bf16)

        def to_keep(x, y, acc):
            self.keep[slot, x, y, 0] = acc[:, :lanes]
            self.keep[slot, x, y, 1] = acc[:, lanes:]

        for job, (lo, hi) in zip(self.jobs, self.spans):

            @pl.when((c >= lo) & (c < hi))
            def _():
                at_ref, b_ref = self.at_refs[job["a"]], self.b_refs[job["b"]]
                col = pl.multiple_of((c - lo + job["first"]) * (2 * lanes), 2 * lanes)
                products(at_ref, b_ref, col, 1 - self.core, to_send)
                self.c0(c, slot).start()
                products(at_ref, b_ref, col, self.core, to_keep)

    def pair(self, c):
        slot = lax.rem(c, 3)
        nx, ny = self.nx, self.ny

        @pl.when(c >= 3)
        def _():
            for d in range(1, nx):
                self.c1a(c, slot, d).wait_send()
            for d in range(1, ny):
                self.c1b(c, slot, d).wait_send()

        self.c0(c, lax.rem(c, 2)).wait_recv()
        for x in range(nx):
            for y in range(ny):
                self.pa[slot, x, y] = (
                    self.keep[lax.rem(c, 2), x, y, 0] + self.recv0[c, x, y, 0].astype(f32)
                ).astype(bf16)
        for d in range(1, nx):
            self.c1a(c, slot, d).start()
        for x in range(nx):
            for y in range(ny):
                self.pb[slot, y, x] = (
                    self.keep[lax.rem(c, 2), x, y, 1] + self.recv0[c, x, y, 1].astype(f32)
                ).astype(bf16)
        for d in range(1, ny):
            self.c1b(c, slot, d).start()

    def cross(self, c):
        slot = lax.rem(c, 3)
        nx, ny = self.nx, self.ny

        @pl.when(c >= 3)
        def _():
            for d in range(1, ny):
                self.c2a(c, slot, d).wait_send()
            for d in range(1, nx):
                self.c2b(c, slot, d).wait_send()

        for d in range(1, nx):
            self.c1a(c, slot, d).wait_recv()
        for y in range(ny):
            acc = self.pa[slot, self.mx, y].astype(f32)
            for d in range(1, nx):
                acc = acc + self.r1a[c, d - 1, y].astype(f32)
            self.qa[slot, y] = acc.astype(bf16)
        for d in range(1, ny):
            self.c2a(c, slot, d).start()
        for d in range(1, ny):
            self.c1b(c, slot, d).wait_recv()
        for x in range(nx):
            acc = self.pb[slot, self.my, x].astype(f32)
            for d in range(1, ny):
                acc = acc + self.r1b[c, d - 1, x].astype(f32)
            self.qb[slot, x] = acc.astype(bf16)
        for d in range(1, nx):
            self.c2b(c, slot, d).start()

    def finish(self, c):
        slot = lax.rem(c, 3)
        nx, ny = self.nx, self.ny
        for d in range(1, ny):
            self.c2a(c, slot, d).wait_recv()
        for d in range(1, nx):
            self.c2b(c, slot, d).wait_recv()
        for job, (lo, hi) in zip(self.jobs, self.spans):

            @pl.when((c >= lo) & (c < hi))
            def _():
                out_ref = self.out_refs[job["out"]]
                col = pl.multiple_of((c - lo + job["place"]) * (2 * lanes), 2 * lanes)
                acc = self.qa[slot, self.my].astype(f32)
                for d in range(1, ny):
                    acc = acc + self.r2a[c, d - 1].astype(f32)
                out_ref[:, pl.ds(col, lanes)] = acc
                acc = self.qb[slot, self.mx].astype(f32)
                for d in range(1, nx):
                    acc = acc + self.r2b[c, d - 1].astype(f32)
                out_ref[:, pl.ds(col + lanes, lanes)] = acc

    def early(self, it):
        @pl.when((it >= 5) & (it < self.total + 5))
        def _():
            self.finish(it - 5)

        @pl.when((it >= 3) & (it < self.total + 3))
        def _():
            self.cross(it - 3)

        @pl.when((it >= 1) & (it < self.total + 1))
        def _():
            self.pair(it - 1)

    def late(self, it):
        @pl.when(it < self.total)
        def _():
            self.make(it)

    def drain(self):
        for c in range(max(self.total - 2, 0), self.total):
            self.c0(c, c % 2).wait_send()
        for c in range(max(self.total - 3, 0), self.total):
            slot = c % 3
            for d in range(1, self.nx):
                self.c1a(c, slot, d).wait_send()
                self.c2b(c, slot, d).wait_send()
            for d in range(1, self.ny):
                self.c1b(c, slot, d).wait_send()
                self.c2a(c, slot, d).wait_send()


class GainSum:
    def __init__(self, n_ctx, n_seq):
        self.ny, self.n = n_seq, n_ctx * n_seq

    def scratch(self):
        sem = pltpu.SemaphoreType.DMA
        return [pltpu.VMEM((self.n - 1, 8, lanes), f32), sem((self.n - 1,)), sem((self.n - 1,))]

    def bind(self, refs, in_ref, out_ref):
        self.got, self.sent, self.done = refs
        self.in_ref, self.out_ref = in_ref, out_ref
        self.me = lax.axis_index("ctx") * self.ny + lax.axis_index("seq")

    def place(self, d):
        to = lax.rem(self.me + d, self.n)
        return to, {"ctx": to // self.ny, "seq": lax.rem(to, self.ny)}

    def copy(self, d):
        to, where = self.place(d)
        return remote(self.in_ref.at[to], self.got.at[d - 1], self.sent.at[d - 1], self.done.at[d - 1], where)

    def greet(self, bar):
        for d in range(1, self.n):
            pl.semaphore_signal(bar, inc=1, device_id=self.place(d)[1], device_id_type=MESH)
        return self.n - 1

    def start(self):
        for d in range(1, self.n):
            self.copy(d).start()

    def finish(self):
        acc = self.in_ref[self.me]
        for d in range(1, self.n):
            self.copy(d).wait_recv()
            acc = acc + self.got[d - 1]
        self.out_ref[...] = acc
        for d in range(1, self.n):
            self.copy(d).wait_send()


def vmem_spec():
    return pl.BlockSpec(memory_space=pltpu.VMEM)


def comm_call(body, args, outs, scratch, cid, name, scalars=()):
    return pl.pallas_call(
        body,
        out_shape=outs,
        in_specs=[
            pl.BlockSpec(memory_space=pltpu.SMEM) if i in scalars else vmem_spec()
            for i in range(len(args))
        ],
        out_specs=[vmem_spec()] * len(outs),
        scratch_shapes=scratch,
        compiler_params=pltpu.CompilerParams(
            collective_id=cid, has_side_effects=True, vmem_limit_bytes=62 * 2**20
        ),
        name=name,
    )(*args)


class LineSmall:
    def __init__(self, n, rows):
        self.n, self.rows = n, rows

    def scratch(self):
        sem = pltpu.SemaphoreType.DMA
        return [
            pltpu.VMEM((8, self.rows), f32), pltpu.VMEM((self.n - 1, 8, self.rows), f32),
            sem((self.n - 1,)), sem((self.n - 1,)),
        ]

    def bind(self, refs):
        self.mine, self.got, self.sent, self.done = refs
        self.i = lax.axis_index("tp")

    def greet(self, bar):
        for d in range(1, self.n):
            pl.semaphore_signal(
                bar, inc=1, device_id={"tp": lax.rem(self.i + d, self.n)}, device_id_type=MESH
            )
        return self.n - 1

    def copy(self, d):
        return remote(
            self.mine, self.got.at[d - 1], self.sent.at[d - 1], self.done.at[d - 1],
            {"tp": lax.rem(self.i + d, self.n)},
        )

    def total(self, columns):
        self.mine[...] = jnp.transpose(columns)[:8]
        for d in range(1, self.n):
            self.copy(d).start()
        acc = self.mine[...]
        for d in range(1, self.n):
            self.copy(d).wait_recv()
            acc = acc + self.got[d - 1]
        for d in range(1, self.n):
            self.copy(d).wait_send()
        return jnp.transpose(jnp.concatenate([acc, jnp.zeros((lanes - 8, self.rows), f32)], axis=0))


def lane_pair(first, second, rows):
    lane = lax.broadcasted_iota(jnp.int32, (rows, lanes), 1)
    return jnp.where(lane == 0, first, 0.0) + jnp.where(lane == 1, second, 0.0)


def dot_nt(left, right):
    return lax.dot_general(left, right, (((1,), (1,)), ((), ())), preferred_element_type=f32)


def dot_tn(left, right):
    return lax.dot_general(left, right, (((0,), (0,)), ((), ())), preferred_element_type=f32)


def attention_back(
    back, grad, proj, attn_gain, w_output, query_rot, keys, values, attn, lse, pos_row, order,
    query_norm, key_norm, scales, qgain, kgain, cosine, sine, cid,
):
    rows, width = back.shape
    local = w_output.shape[0]
    head_dim = lanes
    heads = local // head_dim
    count = keys.shape[0]
    nx, n_tp = lax.axis_size("ctx") // 2, lax.axis_size("tp")
    small = LineSmall(n_tp, rows)
    n_small = len(small.scratch())
    scale = head_dim ** (-0.5)
    tile = 64
    sub = rows // 2

    def body(
        back_ref, grad_ref, proj_ref, again_ref, w_ref, q_ref, k_ref, v_ref, attn_ref, lse_ref,
        prow_ref, order_ref, qn_ref, kn_ref, sc_ref, qg_ref, kg_ref, cos_ref, sin_ref,
        dqkv_ref, dprojt_ref, dagain_ref, dqg_ref, dkg_ref,
        dproj, dout, columns, delta, dqs, dks, send0, keep, recv0, recv1,
        s0, d0, s1, d1, *small_refs,
    ):
        small.bind(small_refs)
        ctx = lax.axis_index("ctx")
        mx, core = ctx // 2, lax.rem(ctx, 2)
        bar = pltpu.get_barrier_semaphore()
        mate = {"ctx": mx * 2 + 1 - core}
        peers = small.greet(bar) + nx
        pl.semaphore_signal(bar, inc=1, device_id=mate, device_id_type=MESH)
        for d in range(1, nx):
            pl.semaphore_signal(
                bar, inc=1, device_id={"ctx": lax.rem(mx + d, nx) * 2 + core}, device_id_type=MESH
            )

        dagain_ref[...] = jnp.zeros_like(dagain_ref)

        def norm_rows(t, carry):
            sl = pl.ds(pl.multiple_of(t * tile, tile), tile)
            dres = grad_ref[sl].astype(f32) + back_ref[sl].astype(f32)
            out = proj_ref[sl].astype(f32)
            inv = lax.rsqrt(jnp.mean(out * out, axis=1, keepdims=True) + norm_eps)
            norm = out * inv
            dagain_ref[...] += jnp.sum(dres * norm, axis=0, keepdims=True)
            dnorm = dres * again_ref[...]
            dot = jnp.mean(dnorm * norm, axis=1, keepdims=True)
            dproj[sl] = (inv * (dnorm - norm * dot)).astype(bf16)
            return carry

        lax.fori_loop(0, rows // tile, norm_rows, 0)
        for h in range(local // sub):
            dout[:, h * sub : (h + 1) * sub] = dot_nt(
                dproj[...], w_ref[h * sub : (h + 1) * sub, :]
            ).astype(bf16)
        lane = lax.broadcasted_iota(jnp.int32, (rows, lanes), 1)
        acc = jnp.zeros((rows, lanes), f32)
        for h in range(heads):
            hs = slice(h * head_dim, (h + 1) * head_dim)
            row_sum = jnp.sum(
                dout[:, hs].astype(f32) * attn_ref[:, hs].astype(f32), axis=1, keepdims=True
            )
            acc = jnp.where(lane == h, row_sum, acc)
        columns[...] = acc
        delta[...] = jnp.transpose(columns[...])[:8]
        dqs[...] = jnp.zeros_like(dqs)
        pl.semaphore_wait(bar, peers)

        def c0(h):
            slot = lax.rem(h, 2)
            return remote(send0.at[slot], recv0.at[h], s0.at[slot], d0.at[h], mate)

        def c1(h, d):
            to = lax.rem(mx + d, nx)
            return remote(
                recv0.at[h, to], recv1.at[h, d - 1], s1.at[h, d - 1], d1.at[h, d - 1],
                {"ctx": to * 2 + core},
            )

        def one_block(h, hs, x, owner, write):
            start = (x * 2 + owner) * rows
            for part in range(rows // sub):
                ks = pl.ds(pl.multiple_of(start + part * sub, sub), sub)
                key, value = k_ref[ks, hs], v_ref[ks, hs]
                query, dhead = q_ref[:, hs], dout[:, hs]
                score = dot_nt(key, query) * scale
                place = order_ref[0, (x * 2 + owner) * 2 + part] * sub
                seen = place + lax.broadcasted_iota(jnp.int32, (sub, rows), 0) <= prow_ref[...]
                share = jnp.where(seen, jnp.exp(score - lse_ref[pl.ds(h, 1), :]), 0.0)
                dshare = dot_nt(value, dhead)
                dscore = (share * (dshare - delta[pl.ds(h, 1), :]) * scale).astype(bf16)
                dqs[:, hs] += dot_tn(dscore, key)
                write(
                    x, slice(part * sub, (part + 1) * sub),
                    jnp.dot(dscore, query, preferred_element_type=f32),
                    jnp.dot(share.astype(bf16), dhead, preferred_element_type=f32),
                )

        def one_head(h):
            hs = pl.ds(pl.multiple_of(h * head_dim, head_dim), head_dim)
            slot = lax.rem(h, 2)

            def to_send(x, rs, dk, dv):
                send0[slot, x, rs, :lanes] = dk.astype(bf16)
                send0[slot, x, rs, lanes:] = dv.astype(bf16)

            def to_keep(x, rs, dk, dv):
                keep[slot, x, rs, :lanes] = dk.astype(bf16)
                keep[slot, x, rs, lanes:] = dv.astype(bf16)

            @pl.when(h >= 2)
            def _():
                c0(h).wait_send()

            def mates(e, carry):
                one_block(h, hs, lax.rem(mx + 1 + e, nx), 1 - core, to_send)
                return carry

            lax.fori_loop(0, nx, mates, 0)
            c0(h).start()

            def owns(e, carry):
                one_block(h, hs, lax.rem(mx + 1 + e, nx), core, to_keep)
                return carry

            lax.fori_loop(0, nx, owns, 0)
            c0(h).wait_recv()

            def add(x, carry):
                recv0[h, x] = (keep[slot, x].astype(f32) + recv0[h, x].astype(f32)).astype(bf16)
                return carry

            lax.fori_loop(0, nx, add, 0)
            for d in range(1, nx):
                c1(h, d).start()

        def heads_loop(h, carry):
            one_head(h)
            return carry

        lax.fori_loop(0, heads, heads_loop, 0)

        dot_q = jnp.zeros((rows, 1), f32)
        for h in range(heads):
            hs = slice(h * head_dim, (h + 1) * head_dim)
            dq = dqs[:, hs]
            dq = dq * cos_ref[...] - pltpu.roll(dq, head_dim // 2, 1) * sin_ref[...]
            norm = qn_ref[:, hs]
            dqg_ref[:, hs] = jnp.sum(dq * norm, axis=0, keepdims=True)
            dq = dq * qg_ref[:, hs]
            dqs[:, hs] = dq
            dot_q = dot_q + jnp.sum(dq * norm, axis=1, keepdims=True)
        dprojt_ref[...] = jnp.transpose(dproj[...])
        dot_k = jnp.zeros((rows, 1), f32)
        for h in range(heads):
            hs = slice(h * head_dim, (h + 1) * head_dim)
            total = recv0[h, mx].astype(f32)
            for d in range(1, nx):
                c1(h, d).wait_recv()
                total = total + recv1[h, d - 1].astype(f32)
            dqkv_ref[:, 2 * local + h * head_dim : 2 * local + (h + 1) * head_dim] = total[
                :, lanes:
            ].astype(bf16)
            dk = total[:, :lanes]
            dk = dk * cos_ref[...] - pltpu.roll(dk, head_dim // 2, 1) * sin_ref[...]
            norm = kn_ref[:, hs]
            dkg_ref[:, hs] = jnp.sum(dk * norm, axis=0, keepdims=True)
            dk = dk * kg_ref[:, hs]
            dks[:, hs] = dk
            dot_k = dot_k + jnp.sum(dk * norm, axis=1, keepdims=True)
        dots = small.total(lane_pair(dot_q, dot_k, rows)) * (1.0 / width)
        for h in range(heads):
            hs = slice(h * head_dim, (h + 1) * head_dim)
            dqkv_ref[:, hs] = (
                sc_ref[:, 0:1] * (dqs[:, hs] - qn_ref[:, hs] * dots[:, 0:1])
            ).astype(bf16)
            dqkv_ref[:, local + h * head_dim : local + (h + 1) * head_dim] = (
                sc_ref[:, 1:2] * (dks[:, hs] - kn_ref[:, hs] * dots[:, 1:2])
            ).astype(bf16)
        for h in range(heads):
            if h >= heads - 2:
                c0(h).wait_send()
            for d in range(1, nx):
                c1(h, d).wait_send()

    sem = pltpu.SemaphoreType.DMA
    pair = (rows, 2 * lanes)
    return comm_call(
        body,
        [back, grad, proj, attn_gain, w_output, query_rot, keys, values, attn, lse, pos_row,
         order, query_norm, key_norm, scales, qgain, kgain, cosine, sine],
        [
            jax.ShapeDtypeStruct((rows, 3 * local), bf16),
            jax.ShapeDtypeStruct((width, rows), bf16),
            jax.ShapeDtypeStruct((1, width), f32),
            jax.ShapeDtypeStruct((1, local), f32),
            jax.ShapeDtypeStruct((1, local), f32),
        ],
        [
            pltpu.VMEM((rows, width), bf16), pltpu.VMEM((rows, local), bf16),
            pltpu.VMEM((rows, lanes), f32), pltpu.VMEM((8, rows), f32),
            pltpu.VMEM((rows, local), f32), pltpu.VMEM((rows, local), f32),
            pltpu.VMEM((2, nx) + pair, bf16), pltpu.VMEM((2, nx) + pair, bf16),
            pltpu.VMEM((heads, nx) + pair, bf16), pltpu.VMEM((heads, nx - 1) + pair, bf16),
            sem((2,)), sem((heads,)), sem((heads, nx - 1)), sem((heads, nx - 1)),
        ] + small.scratch(),
        cid, "attention_back", {11},
    )


def front(tokens, w_query, w_key, w_value, w_output, qgain, kgain, cosine, sine, order, cid):
    rows, width = tokens.shape
    local = w_query.shape[1]
    head_dim = lanes
    heads = local // head_dim
    nx = lax.axis_size("ctx") // 2
    count = nx * 2 * rows
    n_tp = lax.axis_size("tp")
    small = LineSmall(n_tp, rows)
    line = LineSum(n_tp, rows, width)
    n_small, n_line = len(small.scratch()), len(line.scratch())
    scale = head_dim ** (-0.5)
    group = rows // 2

    def body(
        tok_hbm, wq_hbm, wk_hbm, wv_hbm, wo_hbm, qg_ref, kg_ref, cos_ref, sin_ref, order_ref,
        qrot_out, key_out, value_out, qn_out, kn_out, attn_out, tokt_out, proj_out, sc_out, lse_out,
        tok, tokt, w3, wo, qn, kn, qrot, keys, values, peak, total, acc, attn, loads, stores,
        sx, dx, sm, dm, sf, df, *rest,
    ):
        small.bind(rest[:n_small])
        line.bind(rest[n_small : n_small + n_line])
        copies = [
            pltpu.make_async_copy(src, dst, loads.at[i])
            for i, (src, dst) in enumerate(
                [(tok_hbm, tok), (wv_hbm, w3.at[2]), (wq_hbm, w3.at[0]), (wk_hbm, w3.at[1]),
                 (wo_hbm, wo)]
            )
        ]
        for copy in copies:
            copy.start()
        ctx = lax.axis_index("ctx")
        mx, core = ctx // 2, lax.rem(ctx, 2)
        mate = {"ctx": mx * 2 + 1 - core}

        def peer(d):
            return {"ctx": lax.rem(mx + d, nx) * 2 + core}

        bar = pltpu.get_barrier_semaphore()
        pl.semaphore_signal(bar, inc=1, device_id=mate, device_id_type=MESH)
        for d in range(1, nx):
            pl.semaphore_signal(bar, inc=1, device_id=peer(d), device_id_type=MESH)
        peers = small.greet(bar) + nx

        def at(x, owner):
            return pl.ds(pl.multiple_of((x * 2 + owner) * rows, rows), rows)

        mine = at(mx, core)
        boxes = [keys, values]

        def to_peer(b, d):
            box = boxes[b]
            return remote(
                box.at[mine], box.at[mine], sx.at[b, d - 1], dx.at[b, d - 1], peer(d)
            )

        def from_peer(b, d):
            box = boxes[b]
            rs = at(lax.rem(mx + nx - d, nx), core)
            return remote(box.at[rs], box.at[rs], sx.at[b, d - 1], dx.at[b, d - 1], peer(d))

        def to_mate(b):
            box = boxes[b]
            return remote(box.at[mine], box.at[mine], sm.at[b], dm.at[b], mate)

        def from_mate(b):
            box = boxes[b]
            rs = at(mx, 1 - core)
            return remote(box.at[rs], box.at[rs], sm.at[b], dm.at[b], mate)

        def pass_on(b, d):
            box = boxes[b]
            rs = at(lax.rem(mx + nx - d, nx), core)
            return remote(box.at[rs], box.at[rs], sf.at[b, d - 1], df.at[b, d - 1], mate)

        def passed(b, d):
            box = boxes[b]
            rs = at(lax.rem(mx + nx - d, nx), 1 - core)
            return remote(box.at[rs], box.at[rs], sf.at[b, d - 1], df.at[b, d - 1], mate)

        copies[0].wait()
        copies[1].wait()
        values[mine] = jnp.dot(tok[...], w3[2], preferred_element_type=f32).astype(bf16)
        pl.semaphore_wait(bar, peers)
        for d in range(1, nx):
            to_peer(1, d).start()
        to_mate(1).start()
        copies[2].wait()
        qn[...] = jnp.dot(tok[...], w3[0], preferred_element_type=f32)
        copies[3].wait()
        kn[...] = jnp.dot(tok[...], w3[1], preferred_element_type=f32)

        def squares(ref):
            acc_sq = jnp.zeros((rows, 1), f32)
            for h in range(heads):
                part = ref[:, h * head_dim : (h + 1) * head_dim]
                acc_sq = acc_sq + jnp.sum(part * part, axis=1, keepdims=True)
            return acc_sq

        sums = small.total(lane_pair(squares(qn), squares(kn), rows))
        scales = lax.rsqrt(sums * (1.0 / width) + norm_eps)
        sc_out[...] = scales

        def rotated(ref, column, gain_ref, h):
            hs = slice(h * head_dim, (h + 1) * head_dim)
            norm = ref[:, hs] * sc_out[:, column : column + 1]
            ref[:, hs] = norm
            norm = norm * gain_ref[:, hs]
            return (
                norm * cos_ref[...] + pltpu.roll(norm, head_dim // 2, 1) * sin_ref[...]
            ).astype(bf16)

        for h in range(heads):
            keys[mine, h * head_dim : (h + 1) * head_dim] = rotated(kn, 1, kg_ref, h)
        for d in range(1, nx):
            to_peer(0, d).start()
        to_mate(0).start()
        for h in range(heads):
            qrot[:, h * head_dim : (h + 1) * head_dim] = rotated(qn, 0, qg_ref, h)
        peak[...] = jnp.full_like(peak, masked_score)
        total[...] = jnp.zeros_like(total)
        acc[...] = jnp.zeros_like(acc)

        def places(block, shape, axis):
            spot = lax.broadcasted_iota(jnp.int32, shape, axis)
            first, second = order_ref[0, block * 2], order_ref[0, block * 2 + 1]
            return jnp.where(spot < group, first * group + spot, (second - 1) * group + spot)

        def attend(x, owner):
            block = x * 2 + owner
            rs = at(x, owner)

            def one(h, carry):
                hs = pl.ds(pl.multiple_of(h * head_dim, head_dim), head_dim)
                score = dot_nt(qrot[:, hs], keys[rs, hs]) * scale
                seen = places(block, (1, rows), 1) <= places(ctx, (rows, 1), 0)
                old = peak[h]
                new = jnp.maximum(
                    old, jnp.max(jnp.where(seen, score, masked_score), axis=1, keepdims=True)
                )
                share = jnp.where(seen, jnp.exp(score - new), 0.0)
                fade = jnp.exp(old - new)
                peak[h] = new
                total[h] = total[h] * fade + jnp.sum(share, axis=1, keepdims=True)
                acc[:, hs] = acc[:, hs] * fade + jnp.dot(
                    share.astype(bf16), values[rs, hs], preferred_element_type=f32
                )
                return carry

            lax.fori_loop(0, heads, one, 0)

        attend(mx, core)
        for d in range(1, nx):
            from_peer(1, d).wait_recv()
            pass_on(1, d).start()
        from_mate(1).wait_recv()
        from_mate(0).wait_recv()
        attend(mx, 1 - core)
        tokt[...] = jnp.transpose(tok[...])
        for d in range(1, nx):
            from_peer(0, d).wait_recv()
            pass_on(0, d).start()
            attend(lax.rem(mx + nx - d, nx), core)
        for d in range(1, nx):
            passed(1, d).wait_recv()
            passed(0, d).wait_recv()
            attend(lax.rem(mx + nx - d, nx), 1 - core)

        lane = lax.broadcasted_iota(jnp.int32, (rows, lanes), 1)
        logs = jnp.zeros((rows, lanes), f32)
        for h in range(heads):
            hs = slice(h * head_dim, (h + 1) * head_dim)
            attn[:, hs] = (acc[:, hs] / total[h]).astype(bf16)
            logs = jnp.where(lane == h, peak[h] + jnp.log(total[h]), logs)
        lse_out[...] = jnp.transpose(logs)[:8]
        outs = [
            pltpu.make_async_copy(src, dst, stores.at[i])
            for i, (src, dst) in enumerate(
                [(qrot, qrot_out), (keys, key_out), (values, value_out), (qn, qn_out),
                 (kn, kn_out), (attn, attn_out), (tokt, tokt_out)]
            )
        ]
        for copy in outs:
            copy.start()
        copies[4].wait()
        for j in range(n_tp):
            line.own[j] = jnp.dot(
                attn[...], wo[:, j * line.part : (j + 1) * line.part], preferred_element_type=f32
            ).astype(bf16)

        def one(t, carry):
            line.step(t)
            return carry

        lax.fori_loop(0, line.steps, one, 0)
        line.ship(proj_out, stores, 7)
        line.drain()
        for copy in outs:
            copy.wait()
        for b in range(2):
            to_mate(b).wait_send()
            for d in range(1, nx):
                to_peer(b, d).wait_send()
                pass_on(b, d).wait_send()

    sem = pltpu.SemaphoreType.DMA
    hbm = pl.BlockSpec(memory_space=pl.ANY)
    block = jax.ShapeDtypeStruct
    return pl.pallas_call(
        body,
        out_shape=[
            block((rows, local), bf16), block((count, local), bf16), block((count, local), bf16),
            block((rows, local), f32), block((rows, local), f32), block((rows, local), bf16),
            block((width, rows), bf16), block((rows, width), bf16),
            block((rows, lanes), f32), block((8, rows), f32),
        ],
        in_specs=[hbm] * 5 + [vmem_spec()] * 4 + [pl.BlockSpec(memory_space=pltpu.SMEM)],
        out_specs=[hbm] * 8 + [vmem_spec()] * 2,
        scratch_shapes=[
            pltpu.VMEM((rows, width), bf16), pltpu.VMEM((width, rows), bf16),
            pltpu.VMEM((3, width, local), bf16),
            pltpu.VMEM((local, width), bf16), pltpu.VMEM((rows, local), f32),
            pltpu.VMEM((rows, local), f32), pltpu.VMEM((rows, local), bf16),
            pltpu.VMEM((count, local), bf16), pltpu.VMEM((count, local), bf16),
            pltpu.VMEM((heads, rows, 1), f32), pltpu.VMEM((heads, rows, 1), f32),
            pltpu.VMEM((rows, local), f32), pltpu.VMEM((rows, local), bf16),
            sem((5,)), sem((7 + n_tp,)),
            sem((2, nx - 1)), sem((2, nx - 1)), sem((2,)), sem((2,)),
            sem((2, nx - 1)), sem((2, nx - 1)),
        ] + small.scratch() + line.scratch(),
        compiler_params=pltpu.CompilerParams(
            collective_id=cid, has_side_effects=True, vmem_limit_bytes=62 * 2**20
        ),
        name="front",
    )(tokens, w_query, w_key, w_value, w_output, qgain, kgain, cosine, sine, order)


def load_list(pairs, sems):
    copies = [pltpu.make_async_copy(src, dst, sems.at[i]) for i, (src, dst) in enumerate(pairs)]
    for copy in copies:
        copy.start()
    return copies


def kernel_call(body, args, kinds, outs, out_kinds, scratch, cid, name):
    spec = {
        "v": vmem_spec(),
        "h": pl.BlockSpec(memory_space=pl.ANY),
        "s": pl.BlockSpec(memory_space=pltpu.SMEM),
    }
    return pl.pallas_call(
        body,
        out_shape=[jax.ShapeDtypeStruct(*out) for out in outs],
        in_specs=[spec[kind] for kind in kinds],
        out_specs=[spec[kind] for kind in out_kinds],
        scratch_shapes=scratch,
        compiler_params=pltpu.CompilerParams(
            collective_id=cid, has_side_effects=True, vmem_limit_bytes=62 * 2**20
        ),
        name=name,
    )(*args)


def mlp_forward(tokens, proj, attn_gain, w_gate, w_up, w_down, cid):
    rows, width = tokens.shape
    wide = w_gate.shape[1]
    n_tp = lax.axis_size("tp")
    line = LineSum(n_tp, rows, width)
    n_line = len(line.scratch())
    tile = 64
    cut = 512
    n_cut = wide // cut

    def body(
        tok_hbm, proj_hbm, again_ref, wg_hbm, wu_hbm, wd_hbm,
        hidt_out, gate_out, up_out, inner_out, down_out,
        tok, proj_v, hid, hidt, gate, up, inner, wg, wu, wd, first, loads, stores, *rest,
    ):
        line.bind(rest[:n_line])
        start = load_list([(proj_hbm, proj_v), (tok_hbm, tok)], first)
        pairs = []
        for j in range(n_cut):
            cols = pl.ds(j * cut, cut)
            pairs += [(wg_hbm.at[:, cols], wg.at[j]), (wu_hbm.at[:, cols], wu.at[j])]
        for j in range(n_tp):
            cols = pl.ds(j * line.part, line.part)
            pairs += [(wd_hbm.at[:, cols], wd.at[j])]
        weights = load_list(pairs, loads)
        bar = pltpu.get_barrier_semaphore()
        peers = line.greet(bar)
        for copy in start:
            copy.wait()

        def norm_rows(t, carry):
            sl = pl.ds(pl.multiple_of(t * tile, tile), tile)
            out = proj_v[sl].astype(f32)
            inv = lax.rsqrt(jnp.mean(out * out, axis=1, keepdims=True) + norm_eps)
            hid[sl] = (tok[sl].astype(f32) + out * inv * again_ref[...]).astype(bf16)
            return carry

        lax.fori_loop(0, rows // tile, norm_rows, 0)
        for j in range(n_cut):
            cols = slice(j * cut, (j + 1) * cut)
            weights[2 * j].wait()
            weights[2 * j + 1].wait()
            for r in range(2):
                sl = slice(r * rows // 2, (r + 1) * rows // 2)
                g = jnp.dot(hid[sl], wg[j], preferred_element_type=f32)
                u = jnp.dot(hid[sl], wu[j], preferred_element_type=f32)
                gate[sl, cols] = g.astype(bf16)
                up[sl, cols] = u.astype(bf16)
                inner[sl, cols] = (g * jax.nn.sigmoid(g) * u).astype(bf16)
        outs = load_list([(gate, gate_out), (up, up_out), (inner, inner_out)], stores)
        for j in range(n_tp):
            weights[2 * n_cut + j].wait()
            line.own[j] = jnp.dot(inner[...], wd[j], preferred_element_type=f32).astype(bf16)
        pl.semaphore_wait(bar, peers)

        def one(t, carry):
            line.step(t)

            @pl.when(t == 2)
            def _():
                hidt[...] = jnp.transpose(hid[...])

            return carry

        lax.fori_loop(0, line.steps, one, 0)
        last = pltpu.make_async_copy(hidt, hidt_out, stores.at[3])
        last.start()
        line.ship(down_out, stores, 4)
        line.drain()
        for copy in outs + [last]:
            copy.wait()

    sem = pltpu.SemaphoreType.DMA
    return kernel_call(
        body, [tokens, proj, attn_gain, w_gate, w_up, w_down], "hhvhhh",
        [((width, rows), bf16), ((rows, wide), bf16), ((rows, wide), bf16), ((rows, wide), bf16),
         ((rows, width), bf16)],
        "hhhhh",
        [
            pltpu.VMEM((rows, width), bf16), pltpu.VMEM((rows, width), bf16),
            pltpu.VMEM((rows, width), bf16), pltpu.VMEM((width, rows), bf16),
            pltpu.VMEM((rows, wide), bf16), pltpu.VMEM((rows, wide), bf16),
            pltpu.VMEM((rows, wide), bf16),
            pltpu.VMEM((n_cut, width, cut), bf16), pltpu.VMEM((n_cut, width, cut), bf16),
            pltpu.VMEM((n_tp, wide, line.part), bf16),
            sem((2,)), sem((2 * n_cut + n_tp,)), sem((4 + n_tp,)),
        ] + line.scratch(),
        cid, "mlp_forward",
    )


def mlp_back(down, grad, mlp_gain, gate, up, inner, hid_t, w_gate, w_up, w_down, jobs, widths, cid):
    rows, width = down.shape
    wide = gate.shape[1]
    n_tp = lax.axis_size("tp")
    line = LineSum(n_tp, rows, width)
    grads = GradScatter(lax.axis_size("ctx"), lax.axis_size("seq"), width, jobs)
    n_line, n_grads, n_out = len(line.scratch()), len(grads.scratch()), len(widths)
    tile = 64
    cut = 512
    n_cut = wide // cut
    part = line.part

    def body(
        down_ref, grad_ref, mgain_ref, gate_hbm, up_hbm, inner_hbm, hidt_hbm, wg_hbm, wu_hbm, wd_hbm,
        back_out, dgate_out, dup_out, dgain_out, *rest,
    ):
        grad_outs, rest = rest[:n_out], rest[n_out:]
        (gate_v, up_v, inner_v, hidt, ddown, ddownt, dgate, dup, ring, loads, wsem, stores) = rest[:12]
        line.bind(rest[12 : 12 + n_line])
        grads.bind(rest[12 + n_line :], [ddownt, hidt], [inner_v, dgate, dup], grad_outs)

        def fetch(src, index):
            return pltpu.make_async_copy(src, ring.at[index], wsem.at[index])

        def rows_of(ref, j, size):
            return ref.at[pl.ds(pl.multiple_of(j * size, size), size)]

        for j in range(4):
            fetch(rows_of(wd_hbm, j, cut), j).start()
        early = load_list(
            [(inner_hbm, inner_v), (gate_hbm, gate_v), (up_hbm, up_v), (hidt_hbm, hidt)], loads
        )
        bar = pltpu.get_barrier_semaphore()
        peers = line.greet(bar) + grads.greet(bar)
        dgain_out[...] = jnp.zeros_like(dgain_out)

        def norm_rows(t, carry):
            sl = pl.ds(pl.multiple_of(t * tile, tile), tile)
            out = down_ref[sl].astype(f32)
            upstream = grad_ref[sl].astype(f32)
            inv = lax.rsqrt(jnp.mean(out * out, axis=1, keepdims=True) + norm_eps)
            norm = out * inv
            dgain_out[...] += jnp.sum(upstream * norm, axis=0, keepdims=True)
            dnorm = upstream * mgain_ref[...]
            dot = jnp.mean(dnorm * norm, axis=1, keepdims=True)
            ddown[sl] = (inv * (dnorm - norm * dot)).astype(bf16)
            return carry

        lax.fori_loop(0, rows // tile, norm_rows, 0)
        ddownt[...] = jnp.transpose(ddown[...])
        for copy in early:
            copy.wait()
        pl.semaphore_wait(bar, peers)

        def inner_back(j, carry):
            fetch(rows_of(wd_hbm, j, cut), j).wait()
            cols = pl.ds(pl.multiple_of(j * cut, cut), cut)
            for r in range(2):
                sl = slice(r * rows // 2, (r + 1) * rows // 2)
                dmix = dot_nt(ddown[sl], ring[j])
                g, u = gate_v[sl, cols].astype(f32), up_v[sl, cols].astype(f32)
                sig = jax.nn.sigmoid(g)
                dgate[sl, cols] = (dmix * u * sig * (1.0 + g * (1.0 - sig))).astype(bf16)
                dup[sl, cols] = (dmix * (g * sig)).astype(bf16)

            @pl.when(lax.rem(j, 2) == 0)
            def _():
                fetch(rows_of(wg_hbm, j // 2, part), j).start()

            @pl.when(lax.rem(j, 2) == 1)
            def _():
                fetch(rows_of(wu_hbm, j // 2, part), j).start()
                grads.early(j // 2)
                grads.late(j // 2)

            return carry

        lax.fori_loop(0, n_cut, inner_back, 0)
        outs = load_list([(dgate, dgate_out), (dup, dup_out)], stores)

        def hidden_back(j, carry):
            slot = lax.rem(2 * j, 4)
            fetch(rows_of(wg_hbm, j, part), slot).wait()
            fetch(rows_of(wu_hbm, j, part), slot + 1).wait()
            for r in range(2):
                sl = slice(r * rows // 2, (r + 1) * rows // 2)
                line.own[j, sl] = (
                    dot_nt(dgate[sl], ring[slot]) + dot_nt(dup[sl], ring[slot + 1])
                ).astype(bf16)

            @pl.when(j + 2 < n_tp)
            def _():
                fetch(rows_of(wg_hbm, j + 2, part), slot).start()
                fetch(rows_of(wu_hbm, j + 2, part), slot + 1).start()

            @pl.when(lax.rem(j, 2) == 1)
            def _():
                grads.early(n_cut // 2 + j // 2)
                grads.late(n_cut // 2 + j // 2)

            return carry

        lax.fori_loop(0, n_tp, hidden_back, 0)
        done = n_cut // 2 + n_tp // 2

        def one(it, carry):
            grads.early(it)
            for v in range(pace):
                line.piece((it - done) * pace + v)
            grads.late(it)
            return carry

        line_steps = -(-line.steps * row_chains // pace)
        lax.fori_loop(done, max(done + line_steps, grads.steps), one, 0)
        line.ship(back_out, stores, 2)
        line.drain()
        grads.drain()
        for copy in outs:
            copy.wait()

    sem = pltpu.SemaphoreType.DMA
    return kernel_call(
        body, [down, grad, mlp_gain, gate, up, inner, hid_t, w_gate, w_up, w_down], "vvvhhhhhhh",
        [((rows, width), bf16), ((rows, wide), bf16), ((rows, wide), bf16), ((1, width), f32)]
        + [((grads.rows, w), f32) for w in widths],
        "hhhv" + "v" * n_out,
        [
            pltpu.VMEM((rows, wide), bf16), pltpu.VMEM((rows, wide), bf16),
            pltpu.VMEM((rows, wide), bf16), pltpu.VMEM((width, rows), bf16),
            pltpu.VMEM((rows, width), bf16), pltpu.VMEM((width, rows), bf16),
            pltpu.VMEM((rows, wide), bf16), pltpu.VMEM((rows, wide), bf16),
            pltpu.VMEM((4, cut, width), bf16),
            sem((4,)), sem((4,)), sem((2 + n_tp,)),
        ] + line.scratch() + grads.scratch(),
        cid, "mlp_back",
    )


def last_sums(dqkv, w_query, w_key, w_value, ats, bs, jobs, widths, gains, cid):
    rows = dqkv.shape[0]
    width, local = w_query.shape
    n_ctx, n_seq = lax.axis_size("ctx"), lax.axis_size("seq")
    n_tp = lax.axis_size("tp")
    line = LineSum(n_tp, rows, width)
    grads = GradScatter(n_ctx, n_seq, width, jobs)
    small = GainSum(n_ctx, n_seq)
    na, nb, n_out = len(ats), len(bs), len(widths)
    n_line, n_grads = len(line.scratch()), len(grads.scratch())
    part = line.part

    def body(dqkv_ref, wq_ref, wk_ref, wv_ref, *refs):
        at_refs, b_refs = refs[:na], refs[na : na + nb]
        gain_ref, last_out = refs[na + nb], refs[na + nb + 1]
        refs = refs[na + nb + 2 :]
        grad_outs, gain_out, stores, scratch = refs[:n_out], refs[n_out], refs[n_out + 1], refs[n_out + 2 :]
        line.bind(scratch[:n_line])
        grads.bind(scratch[n_line : n_line + n_grads], at_refs, list(b_refs) + [dqkv_ref], grad_outs)
        small.bind(scratch[n_line + n_grads :], gain_ref, gain_out)
        bar = pltpu.get_barrier_semaphore()
        peers = line.greet(bar) + small.greet(bar)
        pl.semaphore_wait(bar, peers)
        small.start()

        def input_back(j, carry):
            rs = pl.ds(pl.multiple_of(j * part, part), part)
            line.own[j] = (
                dot_nt(dqkv_ref[:, :local], wq_ref[rs])
                + dot_nt(dqkv_ref[:, local : 2 * local], wk_ref[rs])
                + dot_nt(dqkv_ref[:, 2 * local :], wv_ref[rs])
            ).astype(bf16)

            @pl.when(lax.rem(j, 2) == 0)
            def _():
                grads.early(j // 2)
                grads.late(j // 2)

            return carry

        lax.fori_loop(0, n_tp, input_back, 0)
        done = n_tp // 2

        def one(it, carry):
            grads.early(it)
            for v in range(pace):
                line.piece((it - done) * pace + v)
            grads.late(it)
            return carry

        line_steps = -(-line.steps * row_chains // pace)
        lax.fori_loop(done, max(done + line_steps, grads.steps), one, 0)
        small.finish()
        line.ship(last_out, stores, 0)
        line.drain()
        grads.drain()

    sem = pltpu.SemaphoreType.DMA
    return kernel_call(
        body, [dqkv, w_query, w_key, w_value] + list(ats) + list(bs) + [gains],
        "vvvv" + "v" * (na + nb + 1),
        [((rows, width), bf16)] + [((grads.rows, w), f32) for w in widths] + [((8, lanes), f32)],
        "h" + "v" * (n_out + 1),
        [sem((n_tp,))] + line.scratch() + grads.scratch() + small.scratch(),
        cid, "last_sums",
    )


def per_device(
    tokens,
    out_grad,
    group_order,
    w_query,
    w_key,
    w_value,
    query_gain,
    key_gain,
    w_output,
    attn_gain,
    w_gate,
    w_up,
    w_down,
    mlp_gain,
):
    inputs = tokens[0]
    upstream = out_grad[0]
    rows, width = inputs.shape
    heads, head_dim = query_gain.shape
    local = heads * head_dim
    wide = w_gate.shape[1]
    positions = key_positions(group_order[0], lax.axis_index("ctx") * rows, rows, rows // 2)
    cosine, sine = rope_tables(positions, head_dim)
    angle_cos = jnp.concatenate([cosine, cosine], axis=1)
    angle_sin = jnp.concatenate([-sine, sine], axis=1)
    qgain = query_gain.reshape(1, local)
    kgain = key_gain.reshape(1, local)
    (query_rot, keys, values, query_norm, key_norm, attn, tokens_t, proj, scales, lse) = front(
        inputs, w_query, w_key, w_value, w_output, qgain, kgain, angle_cos, angle_sin, group_order, 1
    )
    hidden_t, gate, up, inner, down = mlp_forward(
        inputs, proj, attn_gain[None], w_gate, w_up, w_down, 2
    )
    chunks = wide // (2 * lanes)
    chunk_cols = 2 * lanes
    back, d_gate, d_up, d_mlp_gain, grad_down, grad_gate = mlp_back(
        down, upstream, mlp_gain[None], gate, up, inner, hidden_t, w_gate, w_up, w_down,
        [
            dict(a=0, b=0, first=0, count=chunks, out=0, place=0),
            dict(a=1, b=1, first=0, count=chunks, out=1, place=0),
        ],
        [wide, wide],
        3,
    )
    d_qkv, d_proj_t, d_attn_gain, d_query_gain, d_key_gain = attention_back(
        back, upstream, proj, attn_gain[None], w_output, query_rot, keys, values, attn, lse,
        positions[None], group_order, query_norm, key_norm, scales, qgain, kgain, angle_cos,
        angle_sin, 4,
    )
    owners = lax.axis_size("ctx") * lax.axis_size("seq")
    pieces = [
        d_attn_gain.reshape(owners, -1),
        d_mlp_gain.reshape(owners, -1),
        d_query_gain.reshape(heads, owners, -1).transpose(1, 0, 2).reshape(owners, -1),
        d_key_gain.reshape(heads, owners, -1).transpose(1, 0, 2).reshape(owners, -1),
    ]
    cuts = [piece.shape[1] for piece in pieces]
    packed = jnp.concatenate(pieces, axis=1)
    packed = jnp.pad(packed, ((0, 0), (0, 8 * lanes - packed.shape[1]))).reshape(owners, 8, lanes)
    thin = local // chunk_cols
    last, grad_up, grad_qkv, grad_output, small = last_sums(
        d_qkv, w_query, w_key, w_value,
        [hidden_t, tokens_t, d_proj_t],
        [d_up, attn],
        [
            dict(a=0, b=0, first=0, count=chunks, out=0, place=0),
            dict(a=2, b=1, first=0, count=thin, out=2, place=0),
            dict(a=1, b=2, first=0, count=3 * thin, out=1, place=0),
        ],
        [wide, 3 * local, local],
        packed,
        5,
    )
    small = small.reshape(-1)
    g_attn, g_mlp, g_query, g_key = jnp.split(
        small[: sum(cuts)], [cuts[0], cuts[0] + cuts[1], cuts[0] + cuts[1] + cuts[2]]
    )
    grad_query, grad_key, grad_value = jnp.split(grad_qkv, 3, axis=1)
    proj, down = proj.astype(f32), down.astype(f32)
    attn_norm = proj * lax.rsqrt(jnp.mean(proj * proj, axis=1) + norm_eps)[:, None]
    mlp_norm = down * lax.rsqrt(jnp.mean(down * down, axis=1) + norm_eps)[:, None]
    block_out = inputs.astype(f32) + attn_norm * attn_gain + mlp_norm * mlp_gain
    input_grad = upstream.astype(f32) + back.astype(f32) + last.astype(f32)
    return (
        block_out[None],
        input_grad[None],
        grad_query,
        grad_key,
        grad_value,
        g_query.reshape(heads, -1),
        g_key.reshape(heads, -1),
        grad_output.T,
        g_attn,
        grad_gate,
        grad_up,
        grad_down.T,
        g_mlp,
    )


def solution(mesh):
    return jax.shard_map(
        per_device,
        mesh=mesh,
        in_specs=(
            P("seq", "ctx", None),
            P("seq", "ctx", None),
            P("seq", None),
            P(None, "tp"),
            P(None, "tp"),
            P(None, "tp"),
            P("tp", None),
            P("tp", None),
            P("tp", None),
            P(),
            P(None, "tp"),
            P(None, "tp"),
            P("tp", None),
            P(),
        ),
        out_specs=(
            P("seq", "ctx", None),
            P("seq", "ctx", None),
            P(("ctx", "seq"), "tp"),
            P(("ctx", "seq"), "tp"),
            P(("ctx", "seq"), "tp"),
            P("tp", ("ctx", "seq")),
            P("tp", ("ctx", "seq")),
            P("tp", ("ctx", "seq")),
            P(("ctx", "seq")),
            P(("ctx", "seq"), "tp"),
            P(("ctx", "seq"), "tp"),
            P("tp", ("ctx", "seq")),
            P(("ctx", "seq")),
        ),
        check_vma=False,
    )
```

```python
import jax
import jax.numpy as jnp
from jax import lax
from jax.sharding import PartitionSpec as P
from jax.experimental import pallas as pl
from jax.experimental.pallas import tpu as pltpu

norm_eps = 1e-06
rope_base = 500000.0
masked_score = -1e30


def rope_tables(positions, head_dim):
    half = head_dim // 2
    rates = rope_base ** (-(jnp.arange(half, dtype=jnp.float32) * 2.0 / head_dim))
    angle = positions.astype(jnp.float32)[:, None] * rates[None, :]
    return (jnp.cos(angle), jnp.sin(angle))


def key_positions(order, first_row, count, group):
    row_ids = first_row + jnp.arange(count, dtype=jnp.int32)
    slots = row_ids // group
    picks = slots[:, None] == jnp.arange(order.shape[0], dtype=jnp.int32)[None, :]
    return jnp.sum(jnp.where(picks, order[None, :], 0), axis=1) * group + row_ids % group


MESH = pl.DeviceIdType.MESH
bf16 = jnp.bfloat16
f32 = jnp.float32
lanes = 128
row_blocks = 16
row_chains = 8
pace = 6


def remote(src, dst, send, recv, where):
    return pltpu.make_async_remote_copy(
        src, dst, send, recv, device_id=where, device_id_type=MESH
    )


class LineSum:
    def __init__(self, n, rows, width, blocks=row_blocks):
        self.n, self.rows, self.width = n, rows, width
        self.part = width // n
        self.rc = rows // blocks
        self.total = blocks // row_chains * n
        self.steps = self.total + n - 1

    def scratch(self):
        shape = (self.n, self.rows, self.part)
        return [pltpu.VMEM(shape, bf16)] * 4 + [
            pltpu.SemaphoreType.DMA((row_chains, self.total))
        ] * 4

    def bind(self, refs):
        self.own, self.from_l, self.from_r, self.res = refs[:4]
        self.send_r, self.send_l, self.recv_l, self.recv_r = refs[4:]
        self.i = lax.axis_index("tp")
        self.has_l, self.has_r = self.i > 0, self.i < self.n - 1

    def greet(self, bar):
        @pl.when(self.has_l)
        def _():
            pl.semaphore_signal(bar, inc=1, device_id={"tp": self.i - 1}, device_id_type=MESH)

        @pl.when(self.has_r)
        def _():
            pl.semaphore_signal(bar, inc=1, device_id={"tp": self.i + 1}, device_id_type=MESH)

        return self.has_l.astype(jnp.int32) + self.has_r.astype(jnp.int32)

    def load(self, x_ref):
        for j in range(self.n):
            self.own[j] = x_ref[:, j * self.part : (j + 1) * self.part]

    def rows_of(self, g, p):
        block = (p // self.n) * row_chains + g
        return pl.ds(pl.multiple_of(block * self.rc, self.rc), self.rc)

    def right(self, src, dst, g, p, j):
        sl = self.rows_of(g, p)
        return remote(
            src.at[j, sl], dst.at[j, sl], self.send_r.at[g, p], self.recv_l.at[g, p],
            {"tp": self.i + 1},
        )

    def left(self, src, dst, g, q, j):
        sl = self.rows_of(g, q)
        return remote(
            src.at[j, sl], dst.at[j, sl], self.send_l.at[g, q], self.recv_r.at[g, q],
            {"tp": self.i - 1},
        )

    def wait_l(self, g, p, j):
        sl = self.rows_of(g, p)
        remote(
            self.own.at[j, sl], self.from_l.at[j, sl], self.send_r.at[g, p], self.recv_l.at[g, p],
            {"tp": self.i - 1},
        ).wait_recv()

    def wait_r(self, g, q, j):
        sl = self.rows_of(g, q)
        remote(
            self.own.at[j, sl], self.from_r.at[j, sl], self.send_l.at[g, q], self.recv_r.at[g, q],
            {"tp": self.i + 1},
        ).wait_recv()

    def step(self, t):
        for g in range(row_chains):
            self.sub_step(t, g)

    def piece(self, e):
        t = e // row_chains

        @pl.when(t < self.steps)
        def _():
            self.sub_step(t, lax.rem(e, row_chains))

    def sub_step(self, t, g):
        n, i, has_l, has_r = self.n, self.i, self.has_l, self.has_r
        own, from_l, from_r, res = self.own, self.from_l, self.from_r, self.res
        p = t - i
        q = t - (n - 1 - i)
        jr = n - 1 - lax.rem(p + n * self.total, n)
        jl = lax.rem(q + n * self.total, n)
        pv = (p >= 0) & (p < self.total)
        qv = (q >= 0) & (q < self.total)

        @pl.when(pv & has_l)
        def _():
            self.wait_l(g, p, jr)

        @pl.when(qv & has_r)
        def _():
            self.wait_r(g, q, jl)

        @pl.when(pv & (jr > i))
        def _():
            sl = self.rows_of(g, p)

            @pl.when(has_l)
            def _():
                own[jr, sl] = (own[jr, sl].astype(f32) + from_l[jr, sl].astype(f32)).astype(bf16)

            self.right(own, from_l, g, p, jr).start()

        @pl.when(qv & (jl < i))
        def _():
            sl = self.rows_of(g, q)

            @pl.when(has_r)
            def _():
                own[jl, sl] = (own[jl, sl].astype(f32) + from_r[jl, sl].astype(f32)).astype(bf16)

            self.left(own, from_r, g, q, jl).start()

        @pl.when(pv & (jr == i))
        def _():
            sl = self.rows_of(g, p)

            @pl.when(has_l & has_r)
            def _():
                res[i, sl] = (
                    own[i, sl].astype(f32) + from_l[i, sl].astype(f32) + from_r[i, sl].astype(f32)
                ).astype(bf16)

            @pl.when(jnp.logical_not(has_l))
            def _():
                res[i, sl] = (own[i, sl].astype(f32) + from_r[i, sl].astype(f32)).astype(bf16)

            @pl.when(jnp.logical_not(has_r))
            def _():
                res[i, sl] = (own[i, sl].astype(f32) + from_l[i, sl].astype(f32)).astype(bf16)

        @pl.when(pv & (jr <= i) & has_r)
        def _():
            self.right(res, res, g, p, jr).start()

        @pl.when(qv & (jl >= i) & has_l)
        def _():
            self.left(res, res, g, q, jl).start()

    def drain(self):
        def one(p, carry):
            for g in range(row_chains):

                @pl.when(self.has_r)
                def _():
                    self.right(self.own, self.from_l, g, p, 0).wait_send()

                @pl.when(self.has_l)
                def _():
                    self.left(self.own, self.from_r, g, p, 0).wait_send()

            return carry

        lax.fori_loop(0, self.total, one, 0)

    def ship(self, out_ref, sems, base, start, count):
        return load_list(
            [
                (
                    self.res.at[j, pl.ds(start, count)],
                    out_ref.at[:, pl.ds(j * self.part, self.part)],
                )
                for j in range(self.n)
            ],
            sems, base,
        )


class GradScatter:
    def __init__(self, n_ctx, n_seq, width, jobs, orders=("xy", "yx")):
        self.nx, self.ny = n_ctx // 2, n_seq
        self.rows = width // (n_ctx * n_seq)
        self.jobs, self.orders = jobs, orders
        start = 0
        self.spans = []
        for job in jobs:
            self.spans.append((start, start + job["count"]))
            start += job["count"]
        self.total = start
        self.steps = start + 5

    def sizes(self, order):
        return (self.nx, self.ny) if order == "xy" else (self.ny, self.nx)

    def scratch(self):
        nx, ny, t = self.nx, self.ny, self.total
        tile = (self.rows, lanes)
        sem = pltpu.SemaphoreType.DMA
        out = [
            pltpu.VMEM((2, nx, ny, 2) + tile, bf16),
            pltpu.VMEM((2, nx, ny, 2) + tile, f32),
            pltpu.VMEM((t, nx, ny, 2) + tile, bf16),
            sem((2,)), sem((t,)),
        ]
        for order in self.orders:
            n1, n2 = self.sizes(order)
            out += [
                pltpu.VMEM((3, n1, n2) + tile, bf16),
                pltpu.VMEM((t, n1 - 1, n2) + tile, bf16),
                pltpu.VMEM((3, n2) + tile, bf16),
                pltpu.VMEM((t, n2 - 1) + tile, bf16),
                sem((3, n1 - 1)), sem((t, n1 - 1)), sem((3, n2 - 1)), sem((t, n2 - 1)),
            ]
        return out

    def bind(self, refs, at_refs, b_refs, out_refs):
        self.send0, self.keep, self.recv0, self.s0, self.d0 = refs[:5]
        self.half = [refs[5 + 8 * h : 13 + 8 * h] for h in range(2)]
        self.at_refs, self.b_refs, self.out_refs = at_refs, b_refs, out_refs
        ctx = lax.axis_index("ctx")
        self.mx, self.core, self.my = ctx // 2, lax.rem(ctx, 2), lax.axis_index("seq")

    def axis(self, name, d):
        if name == "x":
            to = lax.rem(self.mx + d, self.nx)
            return to, {"ctx": to * 2 + self.core}
        to = lax.rem(self.my + d, self.ny)
        return to, {"seq": to}

    def at_mate(self):
        return {"ctx": self.mx * 2 + 1 - self.core}

    def greet(self, bar):
        places = [self.at_mate()]
        places += [self.axis("x", d)[1] for d in range(1, self.nx)]
        places += [self.axis("y", d)[1] for d in range(1, self.ny)]
        for place in places:
            pl.semaphore_signal(bar, inc=1, device_id=place, device_id_type=MESH)
        return len(places)

    def c0(self, c):
        slot = lax.rem(c, 2)
        return remote(
            self.send0.at[slot], self.recv0.at[c], self.s0.at[slot], self.d0.at[c], self.at_mate()
        )

    def c1(self, h, c, d):
        p, r1, _, _, sent, done, _, _ = self.half[h]
        to, where = self.axis(self.orders[h][0], d)
        slot = lax.rem(c, 3)
        return remote(p.at[slot, to], r1.at[c, d - 1], sent.at[slot, d - 1], done.at[c, d - 1], where)

    def c2(self, h, c, d):
        _, _, q, r2, _, _, sent, done = self.half[h]
        to, where = self.axis(self.orders[h][1], d)
        slot = lax.rem(c, 3)
        return remote(q.at[slot, to], r2.at[c, d - 1], sent.at[slot, d - 1], done.at[c, d - 1], where)

    def make(self, c):
        slot = lax.rem(c, 2)
        nx, ny, r = self.nx, self.ny, self.rows

        @pl.when(c >= 2)
        def _():
            self.c0(c).wait_send()

        def products(at_ref, b_ref, col, parity, write):
            def tile(e, carry):
                x, y = e // ny, lax.rem(e, ny)
                row = pl.multiple_of(((x * 2 + parity) * ny + y) * r, r)
                acc = jnp.dot(
                    at_ref[pl.ds(row, r), :], b_ref[:, pl.ds(col, 2 * lanes)],
                    preferred_element_type=f32,
                )
                write(x, y, acc)
                return carry

            lax.fori_loop(0, nx * ny, tile, 0)

        def to_send(x, y, acc):
            self.send0[slot, x, y, 0] = acc[:, :lanes].astype(bf16)
            self.send0[slot, x, y, 1] = acc[:, lanes:].astype(bf16)

        def to_keep(x, y, acc):
            self.keep[slot, x, y, 0] = acc[:, :lanes]
            self.keep[slot, x, y, 1] = acc[:, lanes:]

        for job, (lo, hi) in zip(self.jobs, self.spans):

            @pl.when((c >= lo) & (c < hi))
            def _():
                at_ref, b_ref = self.at_refs[job["a"]], self.b_refs[job["b"]]
                col = pl.multiple_of((c - lo + job["first"]) * (2 * lanes), 2 * lanes)
                products(at_ref, b_ref, col, 1 - self.core, to_send)
                self.c0(c).start()
                products(at_ref, b_ref, col, self.core, to_keep)

    def pair(self, c):
        slot, two = lax.rem(c, 3), lax.rem(c, 2)

        @pl.when(c >= 3)
        def _():
            for h in range(2):
                for d in range(1, self.sizes(self.orders[h])[0]):
                    self.c1(h, c, d).wait_send()

        self.c0(c).wait_recv()
        for h, order in enumerate(self.orders):
            p = self.half[h][0]
            for x in range(self.nx):
                for y in range(self.ny):
                    spot = (x, y) if order == "xy" else (y, x)
                    p[(slot,) + spot] = (
                        self.keep[two, x, y, h] + self.recv0[c, x, y, h].astype(f32)
                    ).astype(bf16)
            for d in range(1, self.sizes(order)[0]):
                self.c1(h, c, d).start()

    def own(self, name):
        return self.mx if name == "x" else self.my

    def cross(self, c):
        slot = lax.rem(c, 3)

        @pl.when(c >= 3)
        def _():
            for h in range(2):
                for d in range(1, self.sizes(self.orders[h])[1]):
                    self.c2(h, c, d).wait_send()

        for h, order in enumerate(self.orders):
            n1, n2 = self.sizes(order)
            p, r1, q = self.half[h][:3]
            for d in range(1, n1):
                self.c1(h, c, d).wait_recv()
            for e in range(n2):
                acc = p[slot, self.own(order[0]), e].astype(f32)
                for d in range(1, n1):
                    acc = acc + r1[c, d - 1, e].astype(f32)
                q[slot, e] = acc.astype(bf16)
            for d in range(1, n2):
                self.c2(h, c, d).start()

    def finish(self, c):
        slot = lax.rem(c, 3)
        totals = []
        for h, order in enumerate(self.orders):
            n2 = self.sizes(order)[1]
            q, r2 = self.half[h][2:4]
            for d in range(1, n2):
                self.c2(h, c, d).wait_recv()
            acc = q[slot, self.own(order[1])].astype(f32)
            for d in range(1, n2):
                acc = acc + r2[c, d - 1].astype(f32)
            totals.append(acc)
        for job, (lo, hi) in zip(self.jobs, self.spans):

            @pl.when((c >= lo) & (c < hi))
            def _():
                out_ref = self.out_refs[job["out"]]
                col = pl.multiple_of((c - lo + job["place"]) * (2 * lanes), 2 * lanes)
                out_ref[:, pl.ds(col, lanes)] = totals[0]
                out_ref[:, pl.ds(col + lanes, lanes)] = totals[1]

    def tick(self, it):
        @pl.when((it >= 5) & (it < self.total + 5))
        def _():
            self.finish(it - 5)

        @pl.when((it >= 3) & (it < self.total + 3))
        def _():
            self.cross(it - 3)

        @pl.when((it >= 1) & (it < self.total + 1))
        def _():
            self.pair(it - 1)

        @pl.when(it < self.total)
        def _():
            self.make(it)

    def drain(self):
        for c in range(max(self.total - 2, 0), self.total):
            self.c0(c).wait_send()
        for c in range(max(self.total - 3, 0), self.total):
            for h, order in enumerate(self.orders):
                n1, n2 = self.sizes(order)
                for d in range(1, n1):
                    self.c1(h, c, d).wait_send()
                for d in range(1, n2):
                    self.c2(h, c, d).wait_send()


class GainSum:
    def __init__(self, n_ctx, n_seq):
        self.ny, self.n = n_seq, n_ctx * n_seq

    def scratch(self):
        sem = pltpu.SemaphoreType.DMA
        return [pltpu.VMEM((self.n - 1, 8, lanes), f32), sem((self.n - 1,)), sem((self.n - 1,))]

    def bind(self, refs, in_ref, out_ref):
        self.got, self.sent, self.done = refs
        self.in_ref, self.out_ref = in_ref, out_ref
        self.me = lax.axis_index("ctx") * self.ny + lax.axis_index("seq")

    def place(self, d):
        to = lax.rem(self.me + d, self.n)
        return to, {"ctx": to // self.ny, "seq": lax.rem(to, self.ny)}

    def copy(self, d):
        to, where = self.place(d)
        return remote(self.in_ref.at[to], self.got.at[d - 1], self.sent.at[d - 1], self.done.at[d - 1], where)

    def greet(self, bar):
        for d in range(1, self.n):
            pl.semaphore_signal(bar, inc=1, device_id=self.place(d)[1], device_id_type=MESH)
        return self.n - 1

    def start(self):
        for d in range(1, self.n):
            self.copy(d).start()

    def finish(self):
        acc = self.in_ref[self.me]
        for d in range(1, self.n):
            self.copy(d).wait_recv()
            acc = acc + self.got[d - 1]
        self.out_ref[...] = acc
        for d in range(1, self.n):
            self.copy(d).wait_send()


def vmem_spec():
    return pl.BlockSpec(memory_space=pltpu.VMEM)


def comm_call(body, args, outs, scratch, cid, name, scalars=()):
    return pl.pallas_call(
        body,
        out_shape=outs,
        in_specs=[
            pl.BlockSpec(memory_space=pltpu.SMEM) if i in scalars else vmem_spec()
            for i in range(len(args))
        ],
        out_specs=[vmem_spec()] * len(outs),
        scratch_shapes=scratch,
        compiler_params=pltpu.CompilerParams(
            collective_id=cid, has_side_effects=True, vmem_limit_bytes=62 * 2**20
        ),
        name=name,
    )(*args)


class LineSmall:
    def __init__(self, n, rows):
        self.n, self.rows = n, rows

    def scratch(self):
        sem = pltpu.SemaphoreType.DMA
        return [
            pltpu.VMEM((8, self.rows), f32), pltpu.VMEM((self.n - 1, 8, self.rows), f32),
            sem((self.n - 1,)), sem((self.n - 1,)),
        ]

    def bind(self, refs):
        self.mine, self.got, self.sent, self.done = refs
        self.i = lax.axis_index("tp")

    def greet(self, bar):
        for d in range(1, self.n):
            pl.semaphore_signal(
                bar, inc=1, device_id={"tp": lax.rem(self.i + d, self.n)}, device_id_type=MESH
            )
        return self.n - 1

    def copy(self, d):
        return remote(
            self.mine, self.got.at[d - 1], self.sent.at[d - 1], self.done.at[d - 1],
            {"tp": lax.rem(self.i + d, self.n)},
        )

    def total(self, columns):
        self.mine[...] = jnp.transpose(columns)[:8]
        for d in range(1, self.n):
            self.copy(d).start()
        acc = self.mine[...]
        for d in range(1, self.n):
            self.copy(d).wait_recv()
            acc = acc + self.got[d - 1]
        for d in range(1, self.n):
            self.copy(d).wait_send()
        return jnp.transpose(jnp.concatenate([acc, jnp.zeros((lanes - 8, self.rows), f32)], axis=0))


def lane_pair(first, second, rows):
    lane = lax.broadcasted_iota(jnp.int32, (rows, lanes), 1)
    return jnp.where(lane == 0, first, 0.0) + jnp.where(lane == 1, second, 0.0)


def dot_nt(left, right):
    return lax.dot_general(left, right, (((1,), (1,)), ((), ())), preferred_element_type=f32)


def dot_tn(left, right):
    return lax.dot_general(left, right, (((0,), (0,)), ((), ())), preferred_element_type=f32)


def attention_back(
    back, grad, proj, attn_gain, w_output, query_rot, keys, values, attn, lse, pos_row, order,
    query_norm, key_norm, scales, qgain, kgain, cosine, sine, ats, bs, jobs, widths, cid,
):
    rows, width = back.shape
    local = w_output.shape[0]
    head_dim = lanes
    heads = local // head_dim
    count = keys.shape[0]
    nx, n_tp = lax.axis_size("ctx") // 2, lax.axis_size("tp")
    small = LineSmall(n_tp, rows)
    n_small = len(small.scratch())
    scale = head_dim ** (-0.5)
    tile = 64
    sub = rows // 2
    na, nb, n_out = len(ats), len(bs), len(widths)
    grads = None
    if jobs:
        grads = GradScatter(2 * nx, lax.axis_size("seq"), width, jobs, ("yx", "yx"))

    def body(
        back_ref, grad_ref, proj_ref, again_ref, w_ref, q_ref, k_ref, v_ref, attn_ref, lse_ref,
        prow_ref, order_ref, qn_ref, kn_ref, sc_ref, qg_ref, kg_ref, cos_ref, sin_ref, *rest,
    ):
        at_refs, b_refs, rest = rest[:na], rest[na : na + nb], rest[na + nb :]
        dqkv_ref, dprojt_ref, dagain_ref, dqg_ref, dkg_ref = rest[:5]
        grad_outs, rest = rest[5 : 5 + n_out], rest[5 + n_out :]
        (dproj, dout, columns, delta, dqs, dks, send0, keep, recv0, recv1, s0, d0, s1, d1) = rest[:14]
        small.bind(rest[14 : 14 + n_small])
        if jobs:
            grads.bind(rest[14 + n_small :], at_refs, b_refs, grad_outs)

        def tick(it):
            if jobs:
                grads.tick(it)

        ctx = lax.axis_index("ctx")
        mx, core = ctx // 2, lax.rem(ctx, 2)
        bar = pltpu.get_barrier_semaphore()
        mate = {"ctx": mx * 2 + 1 - core}
        if jobs:
            peers = small.greet(bar) + grads.greet(bar)
        else:
            peers = small.greet(bar) + nx
            pl.semaphore_signal(bar, inc=1, device_id=mate, device_id_type=MESH)
            for d in range(1, nx):
                pl.semaphore_signal(
                    bar, inc=1, device_id={"ctx": lax.rem(mx + d, nx) * 2 + core},
                    device_id_type=MESH,
                )
        pl.semaphore_wait(bar, peers)
        tick(jnp.int32(0))

        dagain_ref[...] = jnp.zeros_like(dagain_ref)

        def norm_rows(t, carry):
            sl = pl.ds(pl.multiple_of(t * tile, tile), tile)
            dres = grad_ref[sl].astype(f32) + back_ref[sl].astype(f32)
            out = proj_ref[sl].astype(f32)
            inv = lax.rsqrt(jnp.mean(out * out, axis=1, keepdims=True) + norm_eps)
            norm = out * inv
            dagain_ref[...] += jnp.sum(dres * norm, axis=0, keepdims=True)
            dnorm = dres * again_ref[...]
            dot = jnp.mean(dnorm * norm, axis=1, keepdims=True)
            dproj[sl] = (inv * (dnorm - norm * dot)).astype(bf16)
            return carry

        lax.fori_loop(0, rows // tile, norm_rows, 0)
        for h in range(local // sub):
            dout[:, h * sub : (h + 1) * sub] = dot_nt(
                dproj[...], w_ref[h * sub : (h + 1) * sub, :]
            ).astype(bf16)
        lane = lax.broadcasted_iota(jnp.int32, (rows, lanes), 1)
        acc = jnp.zeros((rows, lanes), f32)
        for h in range(heads):
            hs = slice(h * head_dim, (h + 1) * head_dim)
            row_sum = jnp.sum(
                dout[:, hs].astype(f32) * attn_ref[:, hs].astype(f32), axis=1, keepdims=True
            )
            acc = jnp.where(lane == h, row_sum, acc)
        columns[...] = acc
        delta[...] = jnp.transpose(columns[...])[:8]
        dqs[...] = jnp.zeros_like(dqs)

        def c0(h):
            slot = lax.rem(h, 2)
            return remote(send0.at[slot], recv0.at[h], s0.at[slot], d0.at[h], mate)

        def c1(h, d):
            to = lax.rem(mx + d, nx)
            return remote(
                recv0.at[h, to], recv1.at[h, d - 1], s1.at[h, d - 1], d1.at[h, d - 1],
                {"ctx": to * 2 + core},
            )

        def one_block(h, hs, x, owner, write):
            start = (x * 2 + owner) * rows
            for part in range(rows // sub):
                ks = pl.ds(pl.multiple_of(start + part * sub, sub), sub)
                key, value = k_ref[ks, hs], v_ref[ks, hs]
                query, dhead = q_ref[:, hs], dout[:, hs]
                score = dot_nt(key, query) * scale
                place = order_ref[0, (x * 2 + owner) * 2 + part] * sub
                seen = place + lax.broadcasted_iota(jnp.int32, (sub, rows), 0) <= prow_ref[...]
                share = jnp.where(seen, jnp.exp(score - lse_ref[pl.ds(h, 1), :]), 0.0)
                dshare = dot_nt(value, dhead)
                dscore = share * (dshare - delta[pl.ds(h, 1), :]) * scale
                high = dscore.astype(bf16)
                low = (dscore - high.astype(f32)).astype(bf16)
                dqs[:, hs] += dot_tn(high, key) + dot_tn(low, key)
                write(
                    x, slice(part * sub, (part + 1) * sub),
                    jnp.dot(high, query, preferred_element_type=f32)
                    + jnp.dot(low, query, preferred_element_type=f32),
                    jnp.dot(share.astype(bf16), dhead, preferred_element_type=f32),
                )

        def one_head(h):
            hs = pl.ds(pl.multiple_of(h * head_dim, head_dim), head_dim)
            slot = lax.rem(h, 2)

            def to_send(x, rs, dk, dv):
                send0[slot, x, rs, :lanes] = dk.astype(bf16)
                send0[slot, x, rs, lanes:] = dv.astype(bf16)

            def to_keep(x, rs, dk, dv):
                keep[slot, x, rs, :lanes] = dk.astype(bf16)
                keep[slot, x, rs, lanes:] = dv.astype(bf16)

            @pl.when(h >= 2)
            def _():
                c0(h).wait_send()

            def mates(e, carry):
                one_block(h, hs, lax.rem(mx + 1 + e, nx), 1 - core, to_send)
                return carry

            lax.fori_loop(0, nx, mates, 0)
            c0(h).start()
            tick(2 * h + 1)

            def owns(e, carry):
                one_block(h, hs, lax.rem(mx + 1 + e, nx), core, to_keep)
                return carry

            lax.fori_loop(0, nx, owns, 0)
            c0(h).wait_recv()

            def add(x, carry):
                recv0[h, x] = (keep[slot, x].astype(f32) + recv0[h, x].astype(f32)).astype(bf16)
                return carry

            lax.fori_loop(0, nx, add, 0)
            for d in range(1, nx):
                c1(h, d).start()
            tick(2 * h + 2)

        def heads_loop(h, carry):
            one_head(h)
            return carry

        lax.fori_loop(0, heads, heads_loop, 0)
        if jobs:

            def more(it, carry):
                grads.tick(it)
                return carry

            lax.fori_loop(2 * heads + 1, grads.steps, more, 0)

        dot_q = jnp.zeros((rows, 1), f32)
        for h in range(heads):
            hs = slice(h * head_dim, (h + 1) * head_dim)
            dq = dqs[:, hs]
            dq = dq * cos_ref[...] - pltpu.roll(dq, head_dim // 2, 1) * sin_ref[...]
            norm = qn_ref[:, hs]
            dqg_ref[:, hs] = jnp.sum(dq * norm, axis=0, keepdims=True)
            dq = dq * qg_ref[:, hs]
            dqs[:, hs] = dq
            dot_q = dot_q + jnp.sum(dq * norm, axis=1, keepdims=True)
        dprojt_ref[...] = jnp.transpose(dproj[...])
        dot_k = jnp.zeros((rows, 1), f32)
        for h in range(heads):
            hs = slice(h * head_dim, (h + 1) * head_dim)
            total = recv0[h, mx].astype(f32)
            for d in range(1, nx):
                c1(h, d).wait_recv()
                total = total + recv1[h, d - 1].astype(f32)
            dqkv_ref[:, 2 * local + h * head_dim : 2 * local + (h + 1) * head_dim] = total[
                :, lanes:
            ].astype(bf16)
            dk = total[:, :lanes]
            dk = dk * cos_ref[...] - pltpu.roll(dk, head_dim // 2, 1) * sin_ref[...]
            norm = kn_ref[:, hs]
            dkg_ref[:, hs] = jnp.sum(dk * norm, axis=0, keepdims=True)
            dk = dk * kg_ref[:, hs]
            dks[:, hs] = dk
            dot_k = dot_k + jnp.sum(dk * norm, axis=1, keepdims=True)
        dots = small.total(lane_pair(dot_q, dot_k, rows)) * (1.0 / width)
        for h in range(heads):
            hs = slice(h * head_dim, (h + 1) * head_dim)
            dqkv_ref[:, hs] = (
                sc_ref[:, 0:1] * (dqs[:, hs] - qn_ref[:, hs] * dots[:, 0:1])
            ).astype(bf16)
            dqkv_ref[:, local + h * head_dim : local + (h + 1) * head_dim] = (
                sc_ref[:, 1:2] * (dks[:, hs] - kn_ref[:, hs] * dots[:, 1:2])
            ).astype(bf16)
        for h in range(heads):
            if h >= heads - 2:
                c0(h).wait_send()
            for d in range(1, nx):
                c1(h, d).wait_send()
        if jobs:
            grads.drain()

    sem = pltpu.SemaphoreType.DMA
    pair = (rows, 2 * lanes)
    return comm_call(
        body,
        [back, grad, proj, attn_gain, w_output, query_rot, keys, values, attn, lse, pos_row,
         order, query_norm, key_norm, scales, qgain, kgain, cosine, sine] + ats + bs,
        [
            jax.ShapeDtypeStruct((rows, 3 * local), bf16),
            jax.ShapeDtypeStruct((width, rows), bf16),
            jax.ShapeDtypeStruct((1, width), f32),
            jax.ShapeDtypeStruct((1, local), f32),
            jax.ShapeDtypeStruct((1, local), f32),
        ] + [jax.ShapeDtypeStruct((grads.rows, w), f32) for w in widths],
        [
            pltpu.VMEM((rows, width), bf16), pltpu.VMEM((rows, local), bf16),
            pltpu.VMEM((rows, lanes), f32), pltpu.VMEM((8, rows), f32),
            pltpu.VMEM((rows, local), f32), pltpu.VMEM((rows, local), f32),
            pltpu.VMEM((2, nx) + pair, bf16), pltpu.VMEM((2, nx) + pair, bf16),
            pltpu.VMEM((heads, nx) + pair, bf16), pltpu.VMEM((heads, nx - 1) + pair, bf16),
            sem((2,)), sem((heads,)), sem((heads, nx - 1)), sem((heads, nx - 1)),
        ] + small.scratch() + (grads.scratch() if jobs else []),
        cid, "attention_back", {11},
    )


def front(tokens, w_query, w_key, w_value, qgain, kgain, cosine, sine, order, cid):
    rows, width = tokens.shape
    local = w_query.shape[1]
    head_dim = lanes
    heads = local // head_dim
    nx = lax.axis_size("ctx") // 2
    count = nx * 2 * rows
    n_tp = lax.axis_size("tp")
    small = LineSmall(n_tp, rows)
    n_small = len(small.scratch())
    scale = head_dim ** (-0.5)
    group = rows // 2

    def body(
        tok_hbm, wq_hbm, wk_hbm, wv_hbm, qg_ref, kg_ref, cos_ref, sin_ref, order_ref,
        qrot_out, key_out, value_out, qn_out, kn_out, attn_out, tokt_out, sc_out, lse_out,
        tok, tokt, w3, qn, kn, qrot, keys, values, peak, total, acc, attn, loads, stores,
        sx, dx, sm, dm, sf, df, *rest,
    ):
        small.bind(rest[:n_small])
        copies = [
            pltpu.make_async_copy(src, dst, loads.at[i])
            for i, (src, dst) in enumerate(
                [(tok_hbm, tok), (wv_hbm, w3.at[2]), (wq_hbm, w3.at[0]), (wk_hbm, w3.at[1])]
            )
        ]
        for copy in copies:
            copy.start()
        ctx = lax.axis_index("ctx")
        mx, core = ctx // 2, lax.rem(ctx, 2)
        mate = {"ctx": mx * 2 + 1 - core}

        def peer(d):
            return {"ctx": lax.rem(mx + d, nx) * 2 + core}

        bar = pltpu.get_barrier_semaphore()
        pl.semaphore_signal(bar, inc=1, device_id=mate, device_id_type=MESH)
        for d in range(1, nx):
            pl.semaphore_signal(bar, inc=1, device_id=peer(d), device_id_type=MESH)
        peers = small.greet(bar) + nx

        def at(x, owner):
            return pl.ds(pl.multiple_of((x * 2 + owner) * rows, rows), rows)

        mine = at(mx, core)
        boxes = [keys, values]

        def to_peer(b, d):
            box = boxes[b]
            return remote(
                box.at[mine], box.at[mine], sx.at[b, d - 1], dx.at[b, d - 1], peer(d)
            )

        def from_peer(b, d):
            box = boxes[b]
            rs = at(lax.rem(mx + nx - d, nx), core)
            return remote(box.at[rs], box.at[rs], sx.at[b, d - 1], dx.at[b, d - 1], peer(d))

        def to_mate(b):
            box = boxes[b]
            return remote(box.at[mine], box.at[mine], sm.at[b], dm.at[b], mate)

        def from_mate(b):
            box = boxes[b]
            rs = at(mx, 1 - core)
            return remote(box.at[rs], box.at[rs], sm.at[b], dm.at[b], mate)

        def pass_on(b, d):
            box = boxes[b]
            rs = at(lax.rem(mx + nx - d, nx), core)
            return remote(box.at[rs], box.at[rs], sf.at[b, d - 1], df.at[b, d - 1], mate)

        def passed(b, d):
            box = boxes[b]
            rs = at(lax.rem(mx + nx - d, nx), 1 - core)
            return remote(box.at[rs], box.at[rs], sf.at[b, d - 1], df.at[b, d - 1], mate)

        copies[0].wait()
        copies[1].wait()
        values[mine] = jnp.dot(tok[...], w3[2], preferred_element_type=f32).astype(bf16)
        pl.semaphore_wait(bar, peers)
        for d in range(1, nx):
            to_peer(1, d).start()
        to_mate(1).start()
        copies[2].wait()
        qn[...] = jnp.dot(tok[...], w3[0], preferred_element_type=f32)
        copies[3].wait()
        kn[...] = jnp.dot(tok[...], w3[1], preferred_element_type=f32)

        def squares(ref):
            acc_sq = jnp.zeros((rows, 1), f32)
            for h in range(heads):
                part = ref[:, h * head_dim : (h + 1) * head_dim]
                acc_sq = acc_sq + jnp.sum(part * part, axis=1, keepdims=True)
            return acc_sq

        sums = small.total(lane_pair(squares(qn), squares(kn), rows))
        scales = lax.rsqrt(sums * (1.0 / width) + norm_eps)
        sc_out[...] = scales

        def rotated(ref, column, gain_ref, h):
            hs = slice(h * head_dim, (h + 1) * head_dim)
            norm = ref[:, hs] * sc_out[:, column : column + 1]
            ref[:, hs] = norm
            norm = norm * gain_ref[:, hs]
            return (
                norm * cos_ref[...] + pltpu.roll(norm, head_dim // 2, 1) * sin_ref[...]
            ).astype(bf16)

        for h in range(heads):
            keys[mine, h * head_dim : (h + 1) * head_dim] = rotated(kn, 1, kg_ref, h)
        for d in range(1, nx):
            to_peer(0, d).start()
        to_mate(0).start()
        for h in range(heads):
            qrot[:, h * head_dim : (h + 1) * head_dim] = rotated(qn, 0, qg_ref, h)
        peak[...] = jnp.full_like(peak, masked_score)
        total[...] = jnp.zeros_like(total)
        acc[...] = jnp.zeros_like(acc)

        def places(block, shape, axis):
            spot = lax.broadcasted_iota(jnp.int32, shape, axis)
            first, second = order_ref[0, block * 2], order_ref[0, block * 2 + 1]
            return jnp.where(spot < group, first * group + spot, (second - 1) * group + spot)

        def attend(x, owner):
            block = x * 2 + owner
            rs = at(x, owner)

            def one(h, carry):
                hs = pl.ds(pl.multiple_of(h * head_dim, head_dim), head_dim)
                score = dot_nt(qrot[:, hs], keys[rs, hs]) * scale
                seen = places(block, (1, rows), 1) <= places(ctx, (rows, 1), 0)
                old = peak[h]
                new = jnp.maximum(
                    old, jnp.max(jnp.where(seen, score, masked_score), axis=1, keepdims=True)
                )
                share = jnp.where(seen, jnp.exp(score - new), 0.0)
                fade = jnp.exp(old - new)
                peak[h] = new
                total[h] = total[h] * fade + jnp.sum(share, axis=1, keepdims=True)
                acc[:, hs] = acc[:, hs] * fade + jnp.dot(
                    share.astype(bf16), values[rs, hs], preferred_element_type=f32
                )
                return carry

            lax.fori_loop(0, heads, one, 0)

        attend(mx, core)
        for d in range(1, nx):
            from_peer(1, d).wait_recv()
            pass_on(1, d).start()
        from_mate(1).wait_recv()
        from_mate(0).wait_recv()
        attend(mx, 1 - core)
        tokt[...] = jnp.transpose(tok[...])
        for d in range(1, nx):
            from_peer(0, d).wait_recv()
            pass_on(0, d).start()
            attend(lax.rem(mx + nx - d, nx), core)
        for d in range(1, nx):
            passed(1, d).wait_recv()
            passed(0, d).wait_recv()
            attend(lax.rem(mx + nx - d, nx), 1 - core)

        lane = lax.broadcasted_iota(jnp.int32, (rows, lanes), 1)
        logs = jnp.zeros((rows, lanes), f32)
        for h in range(heads):
            hs = slice(h * head_dim, (h + 1) * head_dim)
            attn[:, hs] = (acc[:, hs] / total[h]).astype(bf16)
            logs = jnp.where(lane == h, peak[h] + jnp.log(total[h]), logs)
        lse_out[...] = jnp.transpose(logs)[:8]
        outs = [
            pltpu.make_async_copy(src, dst, stores.at[i])
            for i, (src, dst) in enumerate(
                [(qrot, qrot_out), (keys, key_out), (values, value_out), (qn, qn_out),
                 (kn, kn_out), (attn, attn_out), (tokt, tokt_out)]
            )
        ]
        for copy in outs:
            copy.start()
        for copy in outs:
            copy.wait()
        for b in range(2):
            to_mate(b).wait_send()
            for d in range(1, nx):
                to_peer(b, d).wait_send()
                pass_on(b, d).wait_send()

    sem = pltpu.SemaphoreType.DMA
    hbm = pl.BlockSpec(memory_space=pl.ANY)
    block = jax.ShapeDtypeStruct
    return pl.pallas_call(
        body,
        out_shape=[
            block((rows, local), bf16), block((count, local), bf16), block((count, local), bf16),
            block((rows, local), f32), block((rows, local), f32), block((rows, local), bf16),
            block((width, rows), bf16),
            block((rows, lanes), f32), block((8, rows), f32),
        ],
        in_specs=[hbm] * 4 + [vmem_spec()] * 4 + [pl.BlockSpec(memory_space=pltpu.SMEM)],
        out_specs=[hbm] * 7 + [vmem_spec()] * 2,
        scratch_shapes=[
            pltpu.VMEM((rows, width), bf16), pltpu.VMEM((width, rows), bf16),
            pltpu.VMEM((3, width, local), bf16),
            pltpu.VMEM((rows, local), f32),
            pltpu.VMEM((rows, local), f32), pltpu.VMEM((rows, local), bf16),
            pltpu.VMEM((count, local), bf16), pltpu.VMEM((count, local), bf16),
            pltpu.VMEM((heads, rows, 1), f32), pltpu.VMEM((heads, rows, 1), f32),
            pltpu.VMEM((rows, local), f32), pltpu.VMEM((rows, local), bf16),
            sem((4,)), sem((7,)),
            sem((2, nx - 1)), sem((2, nx - 1)), sem((2,)), sem((2,)),
            sem((2, nx - 1)), sem((2, nx - 1)),
        ] + small.scratch(),
        compiler_params=pltpu.CompilerParams(
            collective_id=cid, has_side_effects=True, vmem_limit_bytes=62 * 2**20
        ),
        name="front",
    )(tokens, w_query, w_key, w_value, qgain, kgain, cosine, sine, order)


def load_list(pairs, sems, base=0):
    copies = [
        pltpu.make_async_copy(src, dst, sems.at[base + i]) for i, (src, dst) in enumerate(pairs)
    ]
    for copy in copies:
        copy.start()
    return copies


def kernel_call(body, args, kinds, outs, out_kinds, scratch, cid, name):
    spec = {
        "v": vmem_spec(),
        "h": pl.BlockSpec(memory_space=pl.ANY),
        "s": pl.BlockSpec(memory_space=pltpu.SMEM),
    }
    return pl.pallas_call(
        body,
        out_shape=[jax.ShapeDtypeStruct(*out) for out in outs],
        in_specs=[spec[kind] for kind in kinds],
        out_specs=[spec[kind] for kind in out_kinds],
        scratch_shapes=scratch,
        compiler_params=pltpu.CompilerParams(
            collective_id=cid, has_side_effects=True, vmem_limit_bytes=62 * 2**20
        ),
        name=name,
    )(*args)


def middle(attn, tokens, attn_gain, w_output, w_gate, w_up, w_down, cid):
    rows, width = tokens.shape
    local, wide = w_output.shape[0], w_gate.shape[1]
    n_tp = lax.axis_size("tp")
    line = LineSum(n_tp, 2 * rows, width, 4 * row_chains)
    n_line = len(line.scratch())
    half = rows // 2
    tile = 64
    cut = 512
    n_cut = wide // cut
    part = line.part

    def body(
        attn_hbm, tok_hbm, again_ref, wo_hbm, wg_hbm, wu_hbm, wd_hbm,
        proj_out, hidt_out, gate_out, up_out, inner_out, down_out,
        attn_v, tok, wo, hid, hidt, gate, up, inner, wg, wu, wd, first, loads, stores, *rest,
    ):
        line.bind(rest[:n_line])
        start = load_list([(attn_hbm, attn_v), (wo_hbm, wo), (tok_hbm, tok)], first)
        pairs = []
        for j in range(n_cut):
            cols = pl.ds(j * cut, cut)
            pairs += [(wg_hbm.at[:, cols], wg.at[j]), (wu_hbm.at[:, cols], wu.at[j])]
        for j in range(n_tp):
            cols = pl.ds(j * part, part)
            pairs += [(wd_hbm.at[:, cols], wd.at[j])]
        weights = load_list(pairs, loads)
        bar = pltpu.get_barrier_semaphore()
        peers = line.greet(bar)
        for copy in start:
            copy.wait()
        for j in range(n_tp):
            line.own[j, :rows] = jnp.dot(
                attn_v[...], wo[:, j * part : (j + 1) * part], preferred_element_type=f32
            ).astype(bf16)
        pl.semaphore_wait(bar, peers)

        def step(t, carry):
            line.step(t)

            @pl.when(t == 3 * n_tp + 1)
            def _():
                hidt[...] = jnp.transpose(hid[...])

            return carry

        def row_half(c, carry):
            base = pl.multiple_of(c * half, half)
            sl = pl.ds(base, half)
            lax.fori_loop(c * 2 * n_tp, c * n_tp + 2 * n_tp - 1, step, 0)

            def norm_rows(t, carry):
                rs = pl.ds(pl.multiple_of(base + t * tile, tile), tile)
                outs = [line.res[j, rs].astype(f32) for j in range(n_tp)]
                square = sum(jnp.sum(out * out, axis=1, keepdims=True) for out in outs)
                inv = lax.rsqrt(square * (1.0 / width) + norm_eps)
                for j, out in enumerate(outs):
                    cols = slice(j * part, (j + 1) * part)
                    hid[rs, cols] = (
                        tok[rs, cols].astype(f32) + out * inv * again_ref[:, cols]
                    ).astype(bf16)
                return carry

            lax.fori_loop(0, half // tile, norm_rows, 0)
            for j in range(n_cut):
                cols = slice(j * cut, (j + 1) * cut)

                @pl.when(c == 0)
                def _():
                    weights[2 * j].wait()
                    weights[2 * j + 1].wait()

                g = jnp.dot(hid[sl], wg[j], preferred_element_type=f32)
                u = jnp.dot(hid[sl], wu[j], preferred_element_type=f32)
                gate[sl, cols] = g.astype(bf16)
                up[sl, cols] = u.astype(bf16)
                inner[sl, cols] = (g * jax.nn.sigmoid(g) * u).astype(bf16)
                for v in range(j * row_chains // n_cut, (j + 1) * row_chains // n_cut):
                    line.piece(((c + 2) * n_tp - 1) * row_chains + v)
            for j in range(n_tp):

                @pl.when(c == 0)
                def _():
                    weights[2 * n_cut + j].wait()

                line.own[j, pl.ds(rows + base, half)] = jnp.dot(
                    inner[sl], wd[j], preferred_element_type=f32
                ).astype(bf16)
            return carry

        lax.fori_loop(0, 2, row_half, 0)
        outs = load_list([(gate, gate_out), (up, up_out), (inner, inner_out)], stores)
        ready = line.ship(proj_out, stores, 4, 0, rows)
        lax.fori_loop(3 * n_tp, line.steps, step, 0)
        last = pltpu.make_async_copy(hidt, hidt_out, stores.at[3])
        last.start()
        ready = ready + line.ship(down_out, stores, 4 + n_tp, rows, rows)
        line.drain()
        for copy in outs + [last] + ready:
            copy.wait()

    sem = pltpu.SemaphoreType.DMA
    return kernel_call(
        body, [attn, tokens, attn_gain, w_output, w_gate, w_up, w_down], "hhvhhhh",
        [((rows, width), bf16), ((width, rows), bf16), ((rows, wide), bf16), ((rows, wide), bf16),
         ((rows, wide), bf16), ((rows, width), bf16)],
        "hhhhhh",
        [
            pltpu.VMEM((rows, local), bf16), pltpu.VMEM((rows, width), bf16),
            pltpu.VMEM((local, width), bf16),
            pltpu.VMEM((rows, width), bf16), pltpu.VMEM((width, rows), bf16),
            pltpu.VMEM((rows, wide), bf16), pltpu.VMEM((rows, wide), bf16),
            pltpu.VMEM((rows, wide), bf16),
            pltpu.VMEM((n_cut, width, cut), bf16), pltpu.VMEM((n_cut, width, cut), bf16),
            pltpu.VMEM((n_tp, wide, part), bf16),
            sem((3,)), sem((2 * n_cut + n_tp,)), sem((4 + 2 * n_tp,)),
        ] + line.scratch(),
        cid, "middle",
    )


def mlp_back(down, grad, mlp_gain, gate, up, inner, hid_t, w_gate, w_up, w_down, jobs, widths, cid):
    rows, width = down.shape
    wide = gate.shape[1]
    n_tp = lax.axis_size("tp")
    line = LineSum(n_tp, rows, width)
    grads = GradScatter(lax.axis_size("ctx"), lax.axis_size("seq"), width, jobs)
    n_line, n_grads, n_out = len(line.scratch()), len(grads.scratch()), len(widths)
    tile = 64
    cut = 512
    n_cut = wide // cut
    part = line.part
    lead = row_chains * n_tp // (n_cut + n_tp)
    ticks = 3

    def body(
        down_ref, grad_ref, mgain_ref, gate_hbm, up_hbm, inner_hbm, hidt_hbm, wg_hbm, wu_hbm, wd_hbm,
        back_out, dgate_out, dup_out, dgain_out, *rest,
    ):
        grad_outs, rest = rest[:n_out], rest[n_out:]
        (gate_v, up_v, inner_v, hidt, ddown, ddownt, dgate, dup, ring, loads, wsem, stores) = rest[:12]
        line.bind(rest[12 : 12 + n_line])
        grads.bind(rest[12 + n_line :], [ddownt, hidt], [inner_v, dgate, dup], grad_outs)

        def fetch(src, index):
            return pltpu.make_async_copy(src, ring.at[index], wsem.at[index])

        def rows_of(ref, j, size):
            return ref.at[pl.ds(pl.multiple_of(j * size, size), size)]

        for j in range(4):
            fetch(rows_of(wd_hbm, j, cut), j).start()
        early = load_list(
            [(inner_hbm, inner_v), (gate_hbm, gate_v), (up_hbm, up_v), (hidt_hbm, hidt)], loads
        )
        bar = pltpu.get_barrier_semaphore()
        peers = line.greet(bar) + grads.greet(bar)
        dgain_out[...] = jnp.zeros_like(dgain_out)

        def norm_rows(t, carry):
            sl = pl.ds(pl.multiple_of(t * tile, tile), tile)
            out = down_ref[sl].astype(f32)
            upstream = grad_ref[sl].astype(f32)
            inv = lax.rsqrt(jnp.mean(out * out, axis=1, keepdims=True) + norm_eps)
            norm = out * inv
            dgain_out[...] += jnp.sum(upstream * norm, axis=0, keepdims=True)
            dnorm = upstream * mgain_ref[...]
            dot = jnp.mean(dnorm * norm, axis=1, keepdims=True)
            ddown[sl] = (inv * (dnorm - norm * dot)).astype(bf16)
            return carry

        lax.fori_loop(0, rows // tile, norm_rows, 0)
        ddownt[...] = jnp.transpose(ddown[...])
        for copy in early:
            copy.wait()
        pl.semaphore_wait(bar, peers)

        half = rows // 2

        def row_half(c, carry):
            sl = pl.ds(pl.multiple_of(c * half, half), half)

            def beside(i, t):
                @pl.when(c == 1)
                def _():
                    for v in range(lead):
                        line.piece(i * lead + v)

                if t is not None:
                    grads.tick(t)

            def inner_back(j, carry):
                fetch(rows_of(wd_hbm, j, cut), j).wait()
                cols = pl.ds(pl.multiple_of(j * cut, cut), cut)
                dmix = dot_nt(ddown[sl], ring[j])
                g, u = gate_v[sl, cols].astype(f32), up_v[sl, cols].astype(f32)
                sig = jax.nn.sigmoid(g)
                dgate[sl, cols] = (dmix * u * sig * (1.0 + g * (1.0 - sig))).astype(bf16)
                dup[sl, cols] = (dmix * (g * sig)).astype(bf16)

                @pl.when(lax.rem(j, 2) == 0)
                def _():
                    fetch(rows_of(wg_hbm, j // 2, part), j).start()

                @pl.when(lax.rem(j, 2) == 1)
                def _():
                    fetch(rows_of(wu_hbm, j // 2, part), j).start()

                beside(j, None)
                return carry

            lax.fori_loop(0, n_cut, inner_back, 0)
            grads.tick(c * ticks)

            def hidden_back(j, carry):
                slot = lax.rem(2 * j, 4)
                fetch(rows_of(wg_hbm, j, part), slot).wait()
                fetch(rows_of(wu_hbm, j, part), slot + 1).wait()
                line.own[j, sl] = (
                    dot_nt(dgate[sl], ring[slot]) + dot_nt(dup[sl], ring[slot + 1])
                ).astype(bf16)

                @pl.when(j + 2 < n_tp)
                def _():
                    fetch(rows_of(wg_hbm, j + 2, part), slot).start()
                    fetch(rows_of(wu_hbm, j + 2, part), slot + 1).start()

                @pl.when((j + 2 >= n_tp) & (c == 0))
                def _():
                    fetch(rows_of(wd_hbm, slot, cut), slot).start()
                    fetch(rows_of(wd_hbm, slot + 1, cut), slot + 1).start()

                beside(n_cut + j, None)

                @pl.when((lax.rem(j, 2) == 1) & (c * ticks + 1 + j // 2 < (c + 1) * ticks))
                def _():
                    grads.tick(c * ticks + 1 + j // 2)

                return carry

            lax.fori_loop(0, n_tp, hidden_back, 0)
            return carry

        lax.fori_loop(0, 2, row_half, 0)
        outs = load_list([(dgate, dgate_out), (dup, dup_out)], stores)
        done, used = 2 * ticks, (n_cut + n_tp) * lead

        def one(it, carry):
            for v in range(pace):
                line.piece(used + (it - done) * pace + v)
            grads.tick(it)
            return carry

        line_its = -(-(line.steps * row_chains - used) // pace)
        lax.fori_loop(done, max(done + line_its, grads.steps), one, 0)
        outs += line.ship(back_out, stores, 2, 0, rows)
        line.drain()
        grads.drain()
        for copy in outs:
            copy.wait()

    sem = pltpu.SemaphoreType.DMA
    return kernel_call(
        body, [down, grad, mlp_gain, gate, up, inner, hid_t, w_gate, w_up, w_down], "vvvhhhhhhh",
        [((rows, width), bf16), ((rows, wide), bf16), ((rows, wide), bf16), ((1, width), f32)]
        + [((grads.rows, w), f32) for w in widths],
        "hhhv" + "v" * n_out,
        [
            pltpu.VMEM((rows, wide), bf16), pltpu.VMEM((rows, wide), bf16),
            pltpu.VMEM((rows, wide), bf16), pltpu.VMEM((width, rows), bf16),
            pltpu.VMEM((rows, width), bf16), pltpu.VMEM((width, rows), bf16),
            pltpu.VMEM((rows, wide), bf16), pltpu.VMEM((rows, wide), bf16),
            pltpu.VMEM((4, cut, width), bf16),
            sem((4,)), sem((4,)), sem((2 + n_tp,)),
        ] + line.scratch() + grads.scratch(),
        cid, "mlp_back",
    )


def last_sums(dqkv, w_query, w_key, w_value, ats, bs, jobs, widths, gains, cid):
    rows = dqkv.shape[0]
    width, local = w_query.shape
    n_ctx, n_seq = lax.axis_size("ctx"), lax.axis_size("seq")
    n_tp = lax.axis_size("tp")
    line = LineSum(n_tp, rows, width)
    grads = GradScatter(n_ctx, n_seq, width, jobs)
    small = GainSum(n_ctx, n_seq)
    na, nb, n_out = len(ats), len(bs), len(widths)
    n_line, n_grads = len(line.scratch()), len(grads.scratch())
    part = line.part

    def body(dqkv_ref, wq_ref, wk_ref, wv_ref, *refs):
        at_refs, b_refs = refs[:na], refs[na : na + nb]
        gain_ref, last_out = refs[na + nb], refs[na + nb + 1]
        refs = refs[na + nb + 2 :]
        grad_outs, gain_out, stores, scratch = refs[:n_out], refs[n_out], refs[n_out + 1], refs[n_out + 2 :]
        line.bind(scratch[:n_line])
        grads.bind(scratch[n_line : n_line + n_grads], at_refs, list(b_refs) + [dqkv_ref], grad_outs)
        small.bind(scratch[n_line + n_grads :], gain_ref, gain_out)
        bar = pltpu.get_barrier_semaphore()
        peers = line.greet(bar) + small.greet(bar)
        pl.semaphore_wait(bar, peers)
        small.start()

        def input_back(j, carry):
            rs = pl.ds(pl.multiple_of(j * part, part), part)
            line.own[j] = (
                dot_nt(dqkv_ref[:, :local], wq_ref[rs])
                + dot_nt(dqkv_ref[:, local : 2 * local], wk_ref[rs])
                + dot_nt(dqkv_ref[:, 2 * local :], wv_ref[rs])
            ).astype(bf16)

            @pl.when(lax.rem(j, 2) == 0)
            def _():
                grads.tick(j // 2)

            return carry

        lax.fori_loop(0, n_tp, input_back, 0)
        done = n_tp // 2

        def one(it, carry):
            grads.tick(it)
            for v in range(pace):
                line.piece((it - done) * pace + v)
            return carry

        line_steps = -(-line.steps * row_chains // pace)
        lax.fori_loop(done, max(done + line_steps, grads.steps), one, 0)
        small.finish()
        outs = line.ship(last_out, stores, 0, 0, rows)
        line.drain()
        grads.drain()
        for copy in outs:
            copy.wait()

    sem = pltpu.SemaphoreType.DMA
    return kernel_call(
        body, [dqkv, w_query, w_key, w_value] + list(ats) + list(bs) + [gains],
        "vvvv" + "v" * (na + nb + 1),
        [((rows, width), bf16)] + [((grads.rows, w), f32) for w in widths] + [((8, lanes), f32)],
        "h" + "v" * (n_out + 1),
        [sem((n_tp,))] + line.scratch() + grads.scratch() + small.scratch(),
        cid, "last_sums",
    )


def per_device(
    tokens,
    out_grad,
    group_order,
    w_query,
    w_key,
    w_value,
    query_gain,
    key_gain,
    w_output,
    attn_gain,
    w_gate,
    w_up,
    w_down,
    mlp_gain,
):
    inputs = tokens[0]
    upstream = out_grad[0]
    rows, width = inputs.shape
    heads, head_dim = query_gain.shape
    local = heads * head_dim
    wide = w_gate.shape[1]
    positions = key_positions(group_order[0], lax.axis_index("ctx") * rows, rows, rows // 2)
    cosine, sine = rope_tables(positions, head_dim)
    angle_cos = jnp.concatenate([cosine, cosine], axis=1)
    angle_sin = jnp.concatenate([-sine, sine], axis=1)
    qgain = query_gain.reshape(1, local)
    kgain = key_gain.reshape(1, local)
    (query_rot, keys, values, query_norm, key_norm, attn, tokens_t, scales, lse) = front(
        inputs, w_query, w_key, w_value, qgain, kgain, angle_cos, angle_sin, group_order, 1
    )
    proj, hidden_t, gate, up, inner, down = middle(
        attn, inputs, attn_gain[None], w_output, w_gate, w_up, w_down, 2
    )
    chunk_cols = 2 * lanes
    chunks = wide // chunk_cols
    thin = local // chunk_cols
    n_first = chunks * 5 // 8 if keys.shape[0] <= 8 * rows else chunks
    n_mid = chunks * 5 // 8 if keys.shape[0] <= 8 * rows else 0
    back, d_gate, d_up, d_mlp_gain, grad_down, grad_gate = mlp_back(
        down, upstream, mlp_gain[None], gate, up, inner, hidden_t, w_gate, w_up, w_down,
        [
            dict(a=0, b=0, first=0, count=chunks, out=0, place=0),
            dict(a=1, b=1, first=0, count=n_first, out=1, place=0),
        ],
        [wide, n_first * chunk_cols],
        3,
    )
    mid_jobs, mid_widths = [], []
    if n_mid:
        mid_jobs = [
            dict(a=0, b=0, first=n_first, count=chunks - n_first, out=0, place=0),
            dict(a=0, b=1, first=0, count=n_mid, out=1, place=0),
        ]
        mid_widths = [(chunks - n_first) * chunk_cols, n_mid * chunk_cols]
    d_qkv, d_proj_t, d_attn_gain, d_query_gain, d_key_gain, *mid = attention_back(
        back, upstream, proj, attn_gain[None], w_output, query_rot, keys, values, attn, lse,
        positions[None], group_order, query_norm, key_norm, scales, qgain, kgain, angle_cos,
        angle_sin, [hidden_t] if n_mid else [], [d_gate, d_up] if n_mid else [], mid_jobs,
        mid_widths, 4,
    )
    owners = lax.axis_size("ctx") * lax.axis_size("seq")
    pieces = [
        d_attn_gain.reshape(owners, -1),
        d_mlp_gain.reshape(owners, -1),
        d_query_gain.reshape(heads, owners, -1).transpose(1, 0, 2).reshape(owners, -1),
        d_key_gain.reshape(heads, owners, -1).transpose(1, 0, 2).reshape(owners, -1),
    ]
    cuts = [piece.shape[1] for piece in pieces]
    packed = jnp.concatenate(pieces, axis=1)
    packed = jnp.pad(packed, ((0, 0), (0, 8 * lanes - packed.shape[1]))).reshape(owners, 8, lanes)
    last, grad_up, grad_qkv, grad_output, small = last_sums(
        d_qkv, w_query, w_key, w_value,
        [hidden_t, tokens_t, d_proj_t],
        [d_up, attn],
        [
            dict(a=0, b=0, first=n_mid, count=chunks - n_mid, out=0, place=0),
            dict(a=2, b=1, first=0, count=thin, out=2, place=0),
            dict(a=1, b=2, first=0, count=3 * thin, out=1, place=0),
        ],
        [(chunks - n_mid) * chunk_cols, 3 * local, local],
        packed,
        5,
    )
    if n_mid:
        grad_gate = jnp.concatenate([grad_gate, mid[0]], axis=1)
        grad_up = jnp.concatenate([mid[1], grad_up], axis=1)
    small = small.reshape(-1)
    g_attn, g_mlp, g_query, g_key = jnp.split(
        small[: sum(cuts)], [cuts[0], cuts[0] + cuts[1], cuts[0] + cuts[1] + cuts[2]]
    )
    grad_query, grad_key, grad_value = jnp.split(grad_qkv, 3, axis=1)
    proj, down = proj.astype(f32), down.astype(f32)
    attn_norm = proj * lax.rsqrt(jnp.mean(proj * proj, axis=1) + norm_eps)[:, None]
    mlp_norm = down * lax.rsqrt(jnp.mean(down * down, axis=1) + norm_eps)[:, None]
    block_out = inputs.astype(f32) + attn_norm * attn_gain + mlp_norm * mlp_gain
    input_grad = upstream.astype(f32) + back.astype(f32) + last.astype(f32)
    return (
        block_out[None],
        input_grad[None],
        grad_query,
        grad_key,
        grad_value,
        g_query.reshape(heads, -1),
        g_key.reshape(heads, -1),
        grad_output.T,
        g_attn,
        grad_gate,
        grad_up,
        grad_down.T,
        g_mlp,
    )


def solution(mesh):
    return jax.shard_map(
        per_device,
        mesh=mesh,
        in_specs=(
            P("seq", "ctx", None),
            P("seq", "ctx", None),
            P("seq", None),
            P(None, "tp"),
            P(None, "tp"),
            P(None, "tp"),
            P("tp", None),
            P("tp", None),
            P("tp", None),
            P(),
            P(None, "tp"),
            P(None, "tp"),
            P("tp", None),
            P(),
        ),
        out_specs=(
            P("seq", "ctx", None),
            P("seq", "ctx", None),
            P(("ctx", "seq"), "tp"),
            P(("ctx", "seq"), "tp"),
            P(("ctx", "seq"), "tp"),
            P("tp", ("ctx", "seq")),
            P("tp", ("ctx", "seq")),
            P("tp", ("ctx", "seq")),
            P(("ctx", "seq")),
            P(("ctx", "seq"), "tp"),
            P(("ctx", "seq"), "tp"),
            P("tp", ("ctx", "seq")),
            P(("ctx", "seq")),
        ),
        check_vma=False,
    )
```

```python
import jax
import jax.numpy as jnp
from jax import lax
from jax.sharding import PartitionSpec as P
from jax.experimental import pallas as pl
from jax.experimental.pallas import tpu as pltpu

norm_eps = 1e-06
rope_base = 500000.0
masked_score = -1e30


def rope_tables(positions, head_dim):
    half = head_dim // 2
    rates = rope_base ** (-(jnp.arange(half, dtype=jnp.float32) * 2.0 / head_dim))
    angle = positions.astype(jnp.float32)[:, None] * rates[None, :]
    return (jnp.cos(angle), jnp.sin(angle))


def key_positions(order, first_row, count, group):
    row_ids = first_row + jnp.arange(count, dtype=jnp.int32)
    slots = row_ids // group
    picks = slots[:, None] == jnp.arange(order.shape[0], dtype=jnp.int32)[None, :]
    return jnp.sum(jnp.where(picks, order[None, :], 0), axis=1) * group + row_ids % group


MESH = pl.DeviceIdType.MESH
bf16 = jnp.bfloat16
f32 = jnp.float32
lanes = 128
row_blocks = 16
row_chains = 8
pace = 6


def remote(src, dst, send, recv, where):
    return pltpu.make_async_remote_copy(
        src, dst, send, recv, device_id=where, device_id_type=MESH
    )


class LineSum:
    def __init__(self, n, rows, width, blocks=row_blocks):
        self.n, self.rows, self.width = n, rows, width
        self.part = width // n
        self.rc = rows // blocks
        self.total = blocks // row_chains * n
        self.steps = self.total + n - 1

    def scratch(self):
        shape = (self.n, self.rows, self.part)
        return (
            [pltpu.VMEM(shape, bf16)] * 4
            + [pltpu.SemaphoreType.DMA] * 2
            + [pltpu.SemaphoreType.DMA((row_chains, self.total))] * 2
        )

    def bind(self, refs):
        self.own, self.from_l, self.from_r, self.res = refs[:4]
        self.send_r, self.send_l, self.recv_l, self.recv_r = refs[4:]
        self.i = lax.axis_index("tp")
        self.has_l, self.has_r = self.i > 0, self.i < self.n - 1

    def greet(self, bar):
        @pl.when(self.has_l)
        def _():
            pl.semaphore_signal(bar, inc=1, device_id={"tp": self.i - 1}, device_id_type=MESH)

        @pl.when(self.has_r)
        def _():
            pl.semaphore_signal(bar, inc=1, device_id={"tp": self.i + 1}, device_id_type=MESH)

        return self.has_l.astype(jnp.int32) + self.has_r.astype(jnp.int32)

    def load(self, x_ref):
        for j in range(self.n):
            self.own[j] = x_ref[:, j * self.part : (j + 1) * self.part]

    def rows_of(self, g, p):
        block = (p // self.n) * row_chains + g
        return pl.ds(pl.multiple_of(block * self.rc, self.rc), self.rc)

    def right(self, src, dst, g, p, j):
        sl = self.rows_of(g, p)
        return remote(
            src.at[j, sl], dst.at[j, sl], self.send_r, self.recv_l.at[g, p],
            {"tp": self.i + 1},
        )

    def left(self, src, dst, g, q, j):
        sl = self.rows_of(g, q)
        return remote(
            src.at[j, sl], dst.at[j, sl], self.send_l, self.recv_r.at[g, q],
            {"tp": self.i - 1},
        )

    def wait_l(self, g, p, j):
        sl = self.rows_of(g, p)
        remote(
            self.own.at[j, sl], self.from_l.at[j, sl], self.send_r, self.recv_l.at[g, p],
            {"tp": self.i - 1},
        ).wait_recv()

    def wait_r(self, g, q, j):
        sl = self.rows_of(g, q)
        remote(
            self.own.at[j, sl], self.from_r.at[j, sl], self.send_l, self.recv_r.at[g, q],
            {"tp": self.i + 1},
        ).wait_recv()

    def step(self, t):
        self.pieces(t * row_chains, row_chains)

    def pieces(self, first, count):
        def one(v, carry):
            self.piece(first + v)
            return carry

        lax.fori_loop(0, count, one, 0)

    def piece(self, e):
        t = e // row_chains

        @pl.when(t < self.steps)
        def _():
            self.sub_step(t, lax.rem(e, row_chains))

    def sub_step(self, t, g):
        n, i, has_l, has_r = self.n, self.i, self.has_l, self.has_r
        own, from_l, from_r, res = self.own, self.from_l, self.from_r, self.res
        p = t - i
        q = t - (n - 1 - i)
        jr = n - 1 - lax.rem(p + n * self.total, n)
        jl = lax.rem(q + n * self.total, n)
        pv = (p >= 0) & (p < self.total)
        qv = (q >= 0) & (q < self.total)

        @pl.when(pv & has_l)
        def _():
            self.wait_l(g, p, jr)

        @pl.when(qv & has_r)
        def _():
            self.wait_r(g, q, jl)

        @pl.when(pv & (jr > i))
        def _():
            sl = self.rows_of(g, p)

            @pl.when(has_l)
            def _():
                own[jr, sl] = (own[jr, sl].astype(f32) + from_l[jr, sl].astype(f32)).astype(bf16)

            self.right(own, from_l, g, p, jr).start()

        @pl.when(qv & (jl < i))
        def _():
            sl = self.rows_of(g, q)

            @pl.when(has_r)
            def _():
                own[jl, sl] = (own[jl, sl].astype(f32) + from_r[jl, sl].astype(f32)).astype(bf16)

            self.left(own, from_r, g, q, jl).start()

        @pl.when(pv & (jr == i))
        def _():
            sl = self.rows_of(g, p)

            @pl.when(has_l & has_r)
            def _():
                res[i, sl] = (
                    own[i, sl].astype(f32) + from_l[i, sl].astype(f32) + from_r[i, sl].astype(f32)
                ).astype(bf16)

            @pl.when(jnp.logical_not(has_l))
            def _():
                res[i, sl] = (own[i, sl].astype(f32) + from_r[i, sl].astype(f32)).astype(bf16)

            @pl.when(jnp.logical_not(has_r))
            def _():
                res[i, sl] = (own[i, sl].astype(f32) + from_l[i, sl].astype(f32)).astype(bf16)

        @pl.when(pv & (jr <= i) & has_r)
        def _():
            self.right(res, res, g, p, jr).start()

        @pl.when(qv & (jl >= i) & has_l)
        def _():
            self.left(res, res, g, q, jl).start()

    def drain(self):
        @pl.when(self.has_r)
        def _():
            remote(
                self.own, self.from_l, self.send_r, self.recv_l.at[0, 0], {"tp": self.i + 1}
            ).wait_send()

        @pl.when(self.has_l)
        def _():
            remote(
                self.own, self.from_r, self.send_l, self.recv_r.at[0, 0], {"tp": self.i - 1}
            ).wait_send()

    def ship(self, out_ref, sems, base, start, count):
        return load_list(
            [
                (
                    self.res.at[j, pl.ds(start, count)],
                    out_ref.at[:, pl.ds(j * self.part, self.part)],
                )
                for j in range(self.n)
            ],
            sems, base,
        )


class GradScatter:
    def __init__(self, n_ctx, n_seq, width, jobs, orders=("xy", "yx")):
        self.nx, self.ny = n_ctx // 2, n_seq
        self.rows = width // (n_ctx * n_seq)
        self.jobs, self.orders = jobs, orders
        start = 0
        self.spans = []
        for job in jobs:
            self.spans.append((start, start + job["count"]))
            start += job["count"]
        self.total = start
        self.steps = start + 5

    def out_shapes(self, widths):
        flips = {job["out"] for job in self.jobs if job["flip"]}
        return [
            ((w, self.rows) if i in flips else (self.rows, w), f32) for i, w in enumerate(widths)
        ]

    def sizes(self, order):
        return (self.nx, self.ny) if order == "xy" else (self.ny, self.nx)

    def scratch(self):
        nx, ny, t = self.nx, self.ny, self.total
        tile = (self.rows, lanes)
        sem = pltpu.SemaphoreType.DMA
        out = [
            pltpu.VMEM((2, nx, ny, 2) + tile, bf16),
            pltpu.VMEM((2, nx, ny, 2) + tile, f32),
            pltpu.VMEM((t, nx, ny, 2) + tile, bf16),
            sem((2,)), sem((t,)),
        ]
        for order in self.orders:
            n1, n2 = self.sizes(order)
            out += [
                pltpu.VMEM((3, n1, n2) + tile, bf16),
                pltpu.VMEM((t, n1 - 1, n2) + tile, bf16),
                pltpu.VMEM((3, n2) + tile, bf16),
                pltpu.VMEM((t, n2 - 1) + tile, bf16),
                sem((3, n1 - 1)), sem((t, n1 - 1)), sem((3, n2 - 1)), sem((t, n2 - 1)),
            ]
        return out

    def bind(self, refs, at_refs, b_refs, out_refs):
        self.send0, self.keep, self.recv0, self.s0, self.d0 = refs[:5]
        self.half = [refs[5 + 8 * h : 13 + 8 * h] for h in range(2)]
        self.at_refs, self.b_refs, self.out_refs = at_refs, b_refs, out_refs
        ctx = lax.axis_index("ctx")
        self.mx, self.core, self.my = ctx // 2, lax.rem(ctx, 2), lax.axis_index("seq")

    def axis(self, name, d):
        if name == "x":
            to = lax.rem(self.mx + d, self.nx)
            return to, {"ctx": to * 2 + self.core}
        to = lax.rem(self.my + d, self.ny)
        return to, {"seq": to}

    def at_mate(self):
        return {"ctx": self.mx * 2 + 1 - self.core}

    def greet(self, bar):
        places = [self.at_mate()]
        places += [self.axis("x", d)[1] for d in range(1, self.nx)]
        places += [self.axis("y", d)[1] for d in range(1, self.ny)]
        for place in places:
            pl.semaphore_signal(bar, inc=1, device_id=place, device_id_type=MESH)
        return len(places)

    def c0(self, c):
        slot = lax.rem(c, 2)
        return remote(
            self.send0.at[slot], self.recv0.at[c], self.s0.at[slot], self.d0.at[c], self.at_mate()
        )

    def c1(self, h, c, d):
        p, r1, _, _, sent, done, _, _ = self.half[h]
        to, where = self.axis(self.orders[h][0], d)
        slot = lax.rem(c, 3)
        return remote(p.at[slot, to], r1.at[c, d - 1], sent.at[slot, d - 1], done.at[c, d - 1], where)

    def c2(self, h, c, d):
        _, _, q, r2, _, _, sent, done = self.half[h]
        to, where = self.axis(self.orders[h][1], d)
        slot = lax.rem(c, 3)
        return remote(q.at[slot, to], r2.at[c, d - 1], sent.at[slot, d - 1], done.at[c, d - 1], where)

    def make(self, c):
        slot = lax.rem(c, 2)
        nx, ny, r = self.nx, self.ny, self.rows

        @pl.when(c >= 2)
        def _():
            self.c0(c).wait_send()

        def products(at_ref, b_ref, col, parity, write):
            def tile(e, carry):
                x, y = e // ny, lax.rem(e, ny)
                row = pl.multiple_of(((x * 2 + parity) * ny + y) * r, r)
                acc = jnp.dot(
                    at_ref[pl.ds(row, r), :], b_ref[:, pl.ds(col, 2 * lanes)],
                    preferred_element_type=f32,
                )
                write(x, y, acc)
                return carry

            lax.fori_loop(0, nx * ny, tile, 0)

        def to_send(x, y, acc):
            self.send0[slot, x, y, 0] = acc[:, :lanes].astype(bf16)
            self.send0[slot, x, y, 1] = acc[:, lanes:].astype(bf16)

        def to_keep(x, y, acc):
            self.keep[slot, x, y, 0] = acc[:, :lanes]
            self.keep[slot, x, y, 1] = acc[:, lanes:]

        for job, (lo, hi) in zip(self.jobs, self.spans):

            @pl.when((c >= lo) & (c < hi))
            def _():
                at_ref, b_ref = self.at_refs[job["a"]], self.b_refs[job["b"]]
                col = pl.multiple_of((c - lo + job["first"]) * (2 * lanes), 2 * lanes)
                products(at_ref, b_ref, col, 1 - self.core, to_send)
                self.c0(c).start()
                products(at_ref, b_ref, col, self.core, to_keep)

    def pair(self, c):
        slot, two = lax.rem(c, 3), lax.rem(c, 2)

        @pl.when(c >= 3)
        def _():
            for h in range(2):
                for d in range(1, self.sizes(self.orders[h])[0]):
                    self.c1(h, c, d).wait_send()

        self.c0(c).wait_recv()
        for h, order in enumerate(self.orders):
            p = self.half[h][0]
            for x in range(self.nx):
                for y in range(self.ny):
                    spot = (x, y) if order == "xy" else (y, x)
                    p[(slot,) + spot] = (
                        self.keep[two, x, y, h] + self.recv0[c, x, y, h].astype(f32)
                    ).astype(bf16)
            for d in range(1, self.sizes(order)[0]):
                self.c1(h, c, d).start()

    def own(self, name):
        return self.mx if name == "x" else self.my

    def cross(self, c):
        slot = lax.rem(c, 3)

        @pl.when(c >= 3)
        def _():
            for h in range(2):
                for d in range(1, self.sizes(self.orders[h])[1]):
                    self.c2(h, c, d).wait_send()

        for h, order in enumerate(self.orders):
            n1, n2 = self.sizes(order)
            p, r1, q = self.half[h][:3]
            for d in range(1, n1):
                self.c1(h, c, d).wait_recv()
            for e in range(n2):
                acc = p[slot, self.own(order[0]), e].astype(f32)
                for d in range(1, n1):
                    acc = acc + r1[c, d - 1, e].astype(f32)
                q[slot, e] = acc.astype(bf16)
            for d in range(1, n2):
                self.c2(h, c, d).start()

    def finish(self, c):
        slot = lax.rem(c, 3)
        totals = []
        for h, order in enumerate(self.orders):
            n2 = self.sizes(order)[1]
            q, r2 = self.half[h][2:4]
            for d in range(1, n2):
                self.c2(h, c, d).wait_recv()
            acc = q[slot, self.own(order[1])].astype(f32)
            for d in range(1, n2):
                acc = acc + r2[c, d - 1].astype(f32)
            totals.append(acc)
        for job, (lo, hi) in zip(self.jobs, self.spans):

            @pl.when((c >= lo) & (c < hi))
            def _():
                out_ref = self.out_refs[job["out"]]
                col = pl.multiple_of((c - lo + job["place"]) * (2 * lanes), 2 * lanes)
                for h in range(2):
                    place = pl.ds(col + h * lanes, lanes)
                    if job["flip"]:
                        out_ref[place, :] = jnp.transpose(totals[h])
                    else:
                        out_ref[:, place] = totals[h]

    def tick(self, it):
        @pl.when((it >= 5) & (it < self.total + 5))
        def _():
            self.finish(it - 5)

        @pl.when((it >= 3) & (it < self.total + 3))
        def _():
            self.cross(it - 3)

        @pl.when((it >= 1) & (it < self.total + 1))
        def _():
            self.pair(it - 1)

        @pl.when(it < self.total)
        def _():
            self.make(it)

    def drain(self):
        for c in range(max(self.total - 2, 0), self.total):
            self.c0(c).wait_send()
        for c in range(max(self.total - 3, 0), self.total):
            for h, order in enumerate(self.orders):
                n1, n2 = self.sizes(order)
                for d in range(1, n1):
                    self.c1(h, c, d).wait_send()
                for d in range(1, n2):
                    self.c2(h, c, d).wait_send()


class GainSum:
    def __init__(self, n_ctx, n_seq, rows):
        self.ny, self.n, self.rows = n_seq, n_ctx * n_seq, rows

    def scratch(self):
        sem = pltpu.SemaphoreType.DMA
        return [pltpu.VMEM((self.n - 1, self.rows, lanes), f32), sem((self.n - 1,)), sem((self.n - 1,))]

    def bind(self, refs, in_ref, out_ref):
        self.got, self.sent, self.done = refs
        self.in_ref, self.out_ref = in_ref, out_ref
        self.me = lax.axis_index("ctx") * self.ny + lax.axis_index("seq")

    def place(self, d):
        to = lax.rem(self.me + d, self.n)
        return {"ctx": to // self.ny, "seq": lax.rem(to, self.ny)}

    def copy(self, d):
        return remote(
            self.in_ref, self.got.at[d - 1], self.sent.at[d - 1], self.done.at[d - 1], self.place(d)
        )

    def greet(self, bar):
        for d in range(1, self.n):
            pl.semaphore_signal(bar, inc=1, device_id=self.place(d), device_id_type=MESH)
        return self.n - 1

    def start(self):
        for d in range(1, self.n):
            self.copy(d).start()

    def finish(self):
        acc = self.in_ref[...]
        for d in range(1, self.n):
            self.copy(d).wait_recv()
            acc = acc + self.got[d - 1]
        self.out_ref[...] = acc
        for d in range(1, self.n):
            self.copy(d).wait_send()


def vmem_spec():
    return pl.BlockSpec(memory_space=pltpu.VMEM)


def comm_call(body, args, outs, scratch, cid, name, scalars=()):
    return pl.pallas_call(
        body,
        out_shape=outs,
        in_specs=[
            pl.BlockSpec(memory_space=pltpu.SMEM) if i in scalars else vmem_spec()
            for i in range(len(args))
        ],
        out_specs=[vmem_spec()] * len(outs),
        scratch_shapes=scratch,
        compiler_params=pltpu.CompilerParams(
            collective_id=cid, has_side_effects=True, vmem_limit_bytes=62 * 2**20
        ),
        name=name,
    )(*args)


class LineSmall:
    def __init__(self, n, rows):
        self.n, self.rows = n, rows

    def scratch(self):
        sem = pltpu.SemaphoreType.DMA
        return [
            pltpu.VMEM((8, self.rows), f32), pltpu.VMEM((self.n - 1, 8, self.rows), f32),
            sem((self.n - 1,)), sem((self.n - 1,)),
        ]

    def bind(self, refs):
        self.mine, self.got, self.sent, self.done = refs
        self.i = lax.axis_index("tp")

    def greet(self, bar):
        for d in range(1, self.n):
            pl.semaphore_signal(
                bar, inc=1, device_id={"tp": lax.rem(self.i + d, self.n)}, device_id_type=MESH
            )
        return self.n - 1

    def copy(self, d):
        return remote(
            self.mine, self.got.at[d - 1], self.sent.at[d - 1], self.done.at[d - 1],
            {"tp": lax.rem(self.i + d, self.n)},
        )

    def total(self, columns):
        self.mine[...] = jnp.transpose(columns)[:8]
        for d in range(1, self.n):
            self.copy(d).start()
        acc = self.mine[...]
        for d in range(1, self.n):
            self.copy(d).wait_recv()
            acc = acc + self.got[d - 1]
        for d in range(1, self.n):
            self.copy(d).wait_send()
        return jnp.transpose(jnp.concatenate([acc, jnp.zeros((lanes - 8, self.rows), f32)], axis=0))


def lane_pair(first, second, rows):
    lane = lax.broadcasted_iota(jnp.int32, (rows, lanes), 1)
    return jnp.where(lane == 0, first, 0.0) + jnp.where(lane == 1, second, 0.0)


def dot_nt(left, right):
    return lax.dot_general(left, right, (((1,), (1,)), ((), ())), preferred_element_type=f32)


def dot_tn(left, right):
    return lax.dot_general(left, right, (((0,), (0,)), ((), ())), preferred_element_type=f32)


def attention_back(
    back, grad, proj, attn_gain, w_output, query_rot, keys, values, attn, lse, pos_row, order,
    query_norm, key_norm, scales, qgain, kgain, cosine, sine, ats, bs, jobs, widths, cid,
):
    rows, width = back.shape
    local = w_output.shape[0]
    head_dim = lanes
    heads = local // head_dim
    count = keys.shape[0]
    nx, n_tp = lax.axis_size("ctx") // 2, lax.axis_size("tp")
    small = LineSmall(n_tp, rows)
    n_small = len(small.scratch())
    scale = head_dim ** (-0.5)
    tile = 64
    sub = rows // 2
    na, nb, n_out = len(ats), len(bs), len(widths)
    grads = None
    if jobs:
        grads = GradScatter(2 * nx, lax.axis_size("seq"), width, jobs, ("yx", "yx"))

    def body(
        back_ref, grad_ref, proj_ref, again_ref, w_ref, q_ref, k_ref, v_ref, attn_ref, lse_ref,
        prow_ref, order_ref, qn_ref, kn_ref, sc_ref, qg_ref, kg_ref, cos_ref, sin_ref, *rest,
    ):
        at_refs, b_refs, rest = rest[:na], rest[na : na + nb], rest[na + nb :]
        dqkv_ref, dprojt_ref, dagain_ref, dqg_ref, dkg_ref = rest[:5]
        grad_outs, rest = rest[5 : 5 + n_out], rest[5 + n_out :]
        (dproj, dout, columns, delta, dqs, dks, send0, keep, recv0, recv1, s0, d0, s1, d1) = rest[:14]
        small.bind(rest[14 : 14 + n_small])
        if jobs:
            grads.bind(rest[14 + n_small :], at_refs, b_refs, grad_outs)

        def tick(it):
            if jobs:
                grads.tick(it)

        ctx = lax.axis_index("ctx")
        mx, core = ctx // 2, lax.rem(ctx, 2)
        bar = pltpu.get_barrier_semaphore()
        mate = {"ctx": mx * 2 + 1 - core}
        if jobs:
            peers = small.greet(bar) + grads.greet(bar)
        else:
            peers = small.greet(bar) + nx
            pl.semaphore_signal(bar, inc=1, device_id=mate, device_id_type=MESH)
            for d in range(1, nx):
                pl.semaphore_signal(
                    bar, inc=1, device_id={"ctx": lax.rem(mx + d, nx) * 2 + core},
                    device_id_type=MESH,
                )
        pl.semaphore_wait(bar, peers)
        tick(jnp.int32(0))

        dagain_ref[...] = jnp.zeros_like(dagain_ref)

        def norm_rows(t, carry):
            sl = pl.ds(pl.multiple_of(t * tile, tile), tile)
            dres = grad_ref[sl].astype(f32) + back_ref[sl].astype(f32)
            out = proj_ref[sl].astype(f32)
            inv = lax.rsqrt(jnp.mean(out * out, axis=1, keepdims=True) + norm_eps)
            norm = out * inv
            dagain_ref[...] += jnp.sum(dres * norm, axis=0, keepdims=True)
            dnorm = dres * again_ref[...]
            dot = jnp.mean(dnorm * norm, axis=1, keepdims=True)
            dproj[sl] = (inv * (dnorm - norm * dot)).astype(bf16)
            return carry

        lax.fori_loop(0, rows // tile, norm_rows, 0)
        for h in range(local // sub):
            dout[:, h * sub : (h + 1) * sub] = dot_nt(
                dproj[...], w_ref[h * sub : (h + 1) * sub, :]
            ).astype(bf16)
        lane = lax.broadcasted_iota(jnp.int32, (rows, lanes), 1)
        acc = jnp.zeros((rows, lanes), f32)
        for h in range(heads):
            hs = slice(h * head_dim, (h + 1) * head_dim)
            row_sum = jnp.sum(
                dout[:, hs].astype(f32) * attn_ref[:, hs].astype(f32), axis=1, keepdims=True
            )
            acc = jnp.where(lane == h, row_sum, acc)
        columns[...] = acc
        delta[...] = jnp.transpose(columns[...])[:8]
        dqs[...] = jnp.zeros_like(dqs)

        def c0(h):
            slot = lax.rem(h, 2)
            return remote(send0.at[slot], recv0.at[h], s0.at[slot], d0.at[h], mate)

        def c1(h, d):
            to = lax.rem(mx + d, nx)
            return remote(
                recv0.at[h, to], recv1.at[h, d - 1], s1.at[h, d - 1], d1.at[h, d - 1],
                {"ctx": to * 2 + core},
            )

        def one_block(h, hs, x, owner, write):
            start = (x * 2 + owner) * rows
            for part in range(rows // sub):
                ks = pl.ds(pl.multiple_of(start + part * sub, sub), sub)
                key, value = k_ref[ks, hs], v_ref[ks, hs]
                query, dhead = q_ref[:, hs], dout[:, hs]
                score = dot_nt(key, query) * scale
                place = order_ref[0, (x * 2 + owner) * 2 + part] * sub
                seen = place + lax.broadcasted_iota(jnp.int32, (sub, rows), 0) <= prow_ref[...]
                share = jnp.where(seen, jnp.exp(score - lse_ref[pl.ds(h, 1), :]), 0.0)
                dshare = dot_nt(value, dhead)
                dscore = share * (dshare - delta[pl.ds(h, 1), :]) * scale
                high = dscore.astype(bf16)
                low = (dscore - high.astype(f32)).astype(bf16)
                dqs[:, hs] += dot_tn(high, key) + dot_tn(low, key)
                write(
                    x, slice(part * sub, (part + 1) * sub),
                    jnp.dot(high, query, preferred_element_type=f32)
                    + jnp.dot(low, query, preferred_element_type=f32),
                    jnp.dot(share.astype(bf16), dhead, preferred_element_type=f32),
                )

        def one_head(h):
            hs = pl.ds(pl.multiple_of(h * head_dim, head_dim), head_dim)
            slot = lax.rem(h, 2)

            def to_send(x, rs, dk, dv):
                send0[slot, x, rs, :lanes] = dk.astype(bf16)
                send0[slot, x, rs, lanes:] = dv.astype(bf16)

            def to_keep(x, rs, dk, dv):
                keep[slot, x, rs, :lanes] = dk.astype(bf16)
                keep[slot, x, rs, lanes:] = dv.astype(bf16)

            @pl.when(h >= 2)
            def _():
                c0(h).wait_send()

            def mates(e, carry):
                one_block(h, hs, lax.rem(mx + 1 + e, nx), 1 - core, to_send)
                return carry

            lax.fori_loop(0, nx, mates, 0)
            c0(h).start()
            tick(2 * h + 1)

            def owns(e, carry):
                one_block(h, hs, lax.rem(mx + 1 + e, nx), core, to_keep)
                return carry

            lax.fori_loop(0, nx, owns, 0)
            c0(h).wait_recv()

            def add(x, carry):
                recv0[h, x] = (keep[slot, x].astype(f32) + recv0[h, x].astype(f32)).astype(bf16)
                return carry

            lax.fori_loop(0, nx, add, 0)
            for d in range(1, nx):
                c1(h, d).start()
            tick(2 * h + 2)

        def heads_loop(h, carry):
            one_head(h)
            return carry

        lax.fori_loop(0, heads, heads_loop, 0)
        if jobs:

            def more(it, carry):
                grads.tick(it)
                return carry

            lax.fori_loop(2 * heads + 1, grads.steps, more, 0)

        dot_q = jnp.zeros((rows, 1), f32)
        for h in range(heads):
            hs = slice(h * head_dim, (h + 1) * head_dim)
            dq = dqs[:, hs]
            dq = dq * cos_ref[...] - pltpu.roll(dq, head_dim // 2, 1) * sin_ref[...]
            norm = qn_ref[:, hs]
            dqg_ref[:, hs] = jnp.sum(dq * norm, axis=0, keepdims=True)
            dq = dq * qg_ref[:, hs]
            dqs[:, hs] = dq
            dot_q = dot_q + jnp.sum(dq * norm, axis=1, keepdims=True)
        dprojt_ref[...] = jnp.transpose(dproj[...])
        dot_k = jnp.zeros((rows, 1), f32)
        for h in range(heads):
            hs = slice(h * head_dim, (h + 1) * head_dim)
            total = recv0[h, mx].astype(f32)
            for d in range(1, nx):
                c1(h, d).wait_recv()
                total = total + recv1[h, d - 1].astype(f32)
            dqkv_ref[:, 2 * local + h * head_dim : 2 * local + (h + 1) * head_dim] = total[
                :, lanes:
            ].astype(bf16)
            dk = total[:, :lanes]
            dk = dk * cos_ref[...] - pltpu.roll(dk, head_dim // 2, 1) * sin_ref[...]
            norm = kn_ref[:, hs]
            dkg_ref[:, hs] = jnp.sum(dk * norm, axis=0, keepdims=True)
            dk = dk * kg_ref[:, hs]
            dks[:, hs] = dk
            dot_k = dot_k + jnp.sum(dk * norm, axis=1, keepdims=True)
        dots = small.total(lane_pair(dot_q, dot_k, rows)) * (1.0 / width)
        for h in range(heads):
            hs = slice(h * head_dim, (h + 1) * head_dim)
            dqkv_ref[:, hs] = (
                sc_ref[:, 0:1] * (dqs[:, hs] - qn_ref[:, hs] * dots[:, 0:1])
            ).astype(bf16)
            dqkv_ref[:, local + h * head_dim : local + (h + 1) * head_dim] = (
                sc_ref[:, 1:2] * (dks[:, hs] - kn_ref[:, hs] * dots[:, 1:2])
            ).astype(bf16)
        for h in range(heads):
            if h >= heads - 2:
                c0(h).wait_send()
            for d in range(1, nx):
                c1(h, d).wait_send()
        if jobs:
            grads.drain()

    sem = pltpu.SemaphoreType.DMA
    pair = (rows, 2 * lanes)
    return comm_call(
        body,
        [back, grad, proj, attn_gain, w_output, query_rot, keys, values, attn, lse, pos_row,
         order, query_norm, key_norm, scales, qgain, kgain, cosine, sine] + ats + bs,
        [
            jax.ShapeDtypeStruct((rows, 3 * local), bf16),
            jax.ShapeDtypeStruct((width, rows), bf16),
            jax.ShapeDtypeStruct((1, width), f32),
            jax.ShapeDtypeStruct((1, local), f32),
            jax.ShapeDtypeStruct((1, local), f32),
        ] + [jax.ShapeDtypeStruct(*out) for out in (grads.out_shapes(widths) if jobs else [])],
        [
            pltpu.VMEM((rows, width), bf16), pltpu.VMEM((rows, local), bf16),
            pltpu.VMEM((rows, lanes), f32), pltpu.VMEM((8, rows), f32),
            pltpu.VMEM((rows, local), f32), pltpu.VMEM((rows, local), f32),
            pltpu.VMEM((2, nx) + pair, bf16), pltpu.VMEM((2, nx) + pair, bf16),
            pltpu.VMEM((heads, nx) + pair, bf16), pltpu.VMEM((heads, nx - 1) + pair, bf16),
            sem((2,)), sem((heads,)), sem((heads, nx - 1)), sem((heads, nx - 1)),
        ] + small.scratch() + (grads.scratch() if jobs else []),
        cid, "attention_back", {11},
    )


def front(tokens, w_query, w_key, w_value, qgain, kgain, cosine, sine, order, cid):
    rows, width = tokens.shape
    local = w_query.shape[1]
    head_dim = lanes
    heads = local // head_dim
    nx = lax.axis_size("ctx") // 2
    count = nx * 2 * rows
    n_tp = lax.axis_size("tp")
    small = LineSmall(n_tp, rows)
    n_small = len(small.scratch())
    scale = head_dim ** (-0.5)
    group = rows // 2

    def body(
        tok_hbm, wq_hbm, wk_hbm, wv_hbm, qg_ref, kg_ref, cos_ref, sin_ref, order_ref,
        qrot_out, key_out, value_out, qn_out, kn_out, attn_out, tokt_out, sc_out, lse_out,
        tok, tokt, w3, qn, kn, qrot, keys, values, peak, total, acc, attn, loads, stores,
        sx, dx, sm, dm, sf, df, *rest,
    ):
        small.bind(rest[:n_small])
        copies = [
            pltpu.make_async_copy(src, dst, loads.at[i])
            for i, (src, dst) in enumerate(
                [(tok_hbm, tok), (wv_hbm, w3.at[2]), (wq_hbm, w3.at[0]), (wk_hbm, w3.at[1])]
            )
        ]
        for copy in copies:
            copy.start()
        ctx = lax.axis_index("ctx")
        mx, core = ctx // 2, lax.rem(ctx, 2)
        mate = {"ctx": mx * 2 + 1 - core}

        def peer(d):
            return {"ctx": lax.rem(mx + d, nx) * 2 + core}

        bar = pltpu.get_barrier_semaphore()
        pl.semaphore_signal(bar, inc=1, device_id=mate, device_id_type=MESH)
        for d in range(1, nx):
            pl.semaphore_signal(bar, inc=1, device_id=peer(d), device_id_type=MESH)
        peers = small.greet(bar) + nx

        def at(x, owner):
            return pl.ds(pl.multiple_of((x * 2 + owner) * rows, rows), rows)

        mine = at(mx, core)
        side = local // 2
        boxes = [(keys, pl.ds(0, side)), (keys, pl.ds(side, side)), (values, pl.ds(0, local))]

        def move(t, rs, sent, done, where):
            box, cols = boxes[t]
            return remote(box.at[rs, cols], box.at[rs, cols], sent, done, where)

        def to_peer(t, d):
            return move(t, mine, sx.at[t, d - 1], dx.at[t, d - 1], peer(d))

        def from_peer(t, d):
            rs = at(lax.rem(mx + nx - d, nx), core)
            return move(t, rs, sx.at[t, d - 1], dx.at[t, d - 1], peer(d))

        def to_mate(t):
            return move(t, mine, sm.at[t], dm.at[t], mate)

        def from_mate(t):
            return move(t, at(mx, 1 - core), sm.at[t], dm.at[t], mate)

        def pass_on(t, d):
            rs = at(lax.rem(mx + nx - d, nx), core)
            return move(t, rs, sf.at[t, d - 1], df.at[t, d - 1], mate)

        def passed(t, d):
            rs = at(lax.rem(mx + nx - d, nx), 1 - core)
            return move(t, rs, sf.at[t, d - 1], df.at[t, d - 1], mate)

        def each_peer(act):
            def one(d, carry):
                act(d)
                return carry

            lax.fori_loop(1, nx, one, 0)

        copies[0].wait()
        copies[1].wait()
        values[mine] = jnp.dot(tok[...], w3[2], preferred_element_type=f32).astype(bf16)
        pl.semaphore_wait(bar, peers)
        each_peer(lambda d: to_peer(2, d).start())
        to_mate(2).start()
        copies[2].wait()
        qn[...] = jnp.dot(tok[...], w3[0], preferred_element_type=f32)
        copies[3].wait()
        kn[...] = jnp.dot(tok[...], w3[1], preferred_element_type=f32)

        def squares(ref):
            acc_sq = jnp.zeros((rows, 1), f32)
            for h in range(heads):
                part = ref[:, h * head_dim : (h + 1) * head_dim]
                acc_sq = acc_sq + jnp.sum(part * part, axis=1, keepdims=True)
            return acc_sq

        sums = small.total(lane_pair(squares(qn), squares(kn), rows))
        scales = lax.rsqrt(sums * (1.0 / width) + norm_eps)
        sc_out[...] = scales

        def rotated(ref, column, gain_ref, h):
            hs = slice(h * head_dim, (h + 1) * head_dim)
            norm = ref[:, hs] * sc_out[:, column : column + 1]
            ref[:, hs] = norm
            norm = norm * gain_ref[:, hs]
            return (
                norm * cos_ref[...] + pltpu.roll(norm, head_dim // 2, 1) * sin_ref[...]
            ).astype(bf16)

        for h in range(heads):
            keys[mine, h * head_dim : (h + 1) * head_dim] = rotated(kn, 1, kg_ref, h)
            if (h + 1) * head_dim in (side, local):
                t = (h + 1) * head_dim // side - 1
                each_peer(lambda d: to_peer(t, d).start())
                to_mate(t).start()
        for h in range(heads):
            qrot[:, h * head_dim : (h + 1) * head_dim] = rotated(qn, 0, qg_ref, h)
        peak[...] = jnp.full_like(peak, masked_score)
        total[...] = jnp.zeros_like(total)
        acc[...] = jnp.zeros_like(acc)

        def places(block, shape, axis):
            spot = lax.broadcasted_iota(jnp.int32, shape, axis)
            first, second = order_ref[0, block * 2], order_ref[0, block * 2 + 1]
            return jnp.where(spot < group, first * group + spot, (second - 1) * group + spot)

        def attend(x, owner, low, high):
            block = x * 2 + owner
            rs = at(x, owner)

            def one(h, carry):
                hs = pl.ds(pl.multiple_of(h * head_dim, head_dim), head_dim)
                score = dot_nt(qrot[:, hs], keys[rs, hs]) * scale
                seen = places(block, (1, rows), 1) <= places(ctx, (rows, 1), 0)
                old = peak[h]
                new = jnp.maximum(
                    old, jnp.max(jnp.where(seen, score, masked_score), axis=1, keepdims=True)
                )
                share = jnp.where(seen, jnp.exp(score - new), 0.0)
                fade = jnp.exp(old - new)
                peak[h] = new
                total[h] = total[h] * fade + jnp.sum(share, axis=1, keepdims=True)
                acc[:, hs] = acc[:, hs] * fade + jnp.dot(
                    share.astype(bf16), values[rs, hs], preferred_element_type=f32
                )
                return carry

            lax.fori_loop(low, high, one, 0)

        attend(mx, core, 0, heads)

        def hand_on(t, d):
            from_peer(t, d).wait_recv()
            pass_on(t, d).start()

        each_peer(lambda d: hand_on(2, d))
        for t in range(3):
            from_mate(t).wait_recv()
        attend(mx, 1 - core, 0, heads)
        tokt[...] = jnp.transpose(tok[...])

        def half_heads(t, carry):
            low, high = t * heads // 2, (t + 1) * heads // 2

            def near(d):
                for v in range(2):

                    @pl.when(t == v)
                    def _():
                        hand_on(v, d)

                attend(lax.rem(mx + nx - d, nx), core, low, high)

            def far(d):
                @pl.when(t == 0)
                def _():
                    passed(2, d).wait_recv()
                    passed(0, d).wait_recv()

                @pl.when(t == 1)
                def _():
                    passed(1, d).wait_recv()

                attend(lax.rem(mx + nx - d, nx), 1 - core, low, high)

            each_peer(near)
            each_peer(far)
            return carry

        lax.fori_loop(0, 2, half_heads, 0)

        lane = lax.broadcasted_iota(jnp.int32, (rows, lanes), 1)
        logs = jnp.zeros((rows, lanes), f32)
        for h in range(heads):
            hs = slice(h * head_dim, (h + 1) * head_dim)
            attn[:, hs] = (acc[:, hs] / total[h]).astype(bf16)
            logs = jnp.where(lane == h, peak[h] + jnp.log(total[h]), logs)
        lse_out[...] = jnp.transpose(logs)[:8]
        outs = [
            pltpu.make_async_copy(src, dst, stores.at[i])
            for i, (src, dst) in enumerate(
                [(qrot, qrot_out), (keys, key_out), (values, value_out), (qn, qn_out),
                 (kn, kn_out), (attn, attn_out), (tokt, tokt_out)]
            )
        ]
        for copy in outs:
            copy.start()
        for copy in outs:
            copy.wait()
        for t in range(3):
            to_mate(t).wait_send()

            def sent(d):
                to_peer(t, d).wait_send()
                pass_on(t, d).wait_send()

            each_peer(sent)

    sem = pltpu.SemaphoreType.DMA
    hbm = pl.BlockSpec(memory_space=pl.ANY)
    block = jax.ShapeDtypeStruct
    return pl.pallas_call(
        body,
        out_shape=[
            block((rows, local), bf16), block((count, local), bf16), block((count, local), bf16),
            block((rows, local), f32), block((rows, local), f32), block((rows, local), bf16),
            block((width, rows), bf16),
            block((rows, lanes), f32), block((8, rows), f32),
        ],
        in_specs=[hbm] * 4 + [vmem_spec()] * 4 + [pl.BlockSpec(memory_space=pltpu.SMEM)],
        out_specs=[hbm] * 7 + [vmem_spec()] * 2,
        scratch_shapes=[
            pltpu.VMEM((rows, width), bf16), pltpu.VMEM((width, rows), bf16),
            pltpu.VMEM((3, width, local), bf16),
            pltpu.VMEM((rows, local), f32),
            pltpu.VMEM((rows, local), f32), pltpu.VMEM((rows, local), bf16),
            pltpu.VMEM((count, local), bf16), pltpu.VMEM((count, local), bf16),
            pltpu.VMEM((heads, rows, 1), f32), pltpu.VMEM((heads, rows, 1), f32),
            pltpu.VMEM((rows, local), f32), pltpu.VMEM((rows, local), bf16),
            sem((4,)), sem((7,)),
            sem((3, nx - 1)), sem((3, nx - 1)), sem((3,)), sem((3,)),
            sem((3, nx - 1)), sem((3, nx - 1)),
        ] + small.scratch(),
        compiler_params=pltpu.CompilerParams(
            collective_id=cid, has_side_effects=True, vmem_limit_bytes=62 * 2**20
        ),
        name="front",
    )(tokens, w_query, w_key, w_value, qgain, kgain, cosine, sine, order)


def load_list(pairs, sems, base=0):
    copies = [
        pltpu.make_async_copy(src, dst, sems.at[base + i]) for i, (src, dst) in enumerate(pairs)
    ]
    for copy in copies:
        copy.start()
    return copies


def kernel_call(body, args, kinds, outs, out_kinds, scratch, cid, name):
    spec = {
        "v": vmem_spec(),
        "h": pl.BlockSpec(memory_space=pl.ANY),
        "s": pl.BlockSpec(memory_space=pltpu.SMEM),
    }
    return pl.pallas_call(
        body,
        out_shape=[jax.ShapeDtypeStruct(*out) for out in outs],
        in_specs=[spec[kind] for kind in kinds],
        out_specs=[spec[kind] for kind in out_kinds],
        scratch_shapes=scratch,
        compiler_params=pltpu.CompilerParams(
            collective_id=cid, has_side_effects=True, vmem_limit_bytes=62 * 2**20
        ),
        name=name,
    )(*args)


def middle(attn, tokens, attn_gain, w_output, w_gate, w_up, w_down, cid):
    rows, width = tokens.shape
    local, wide = w_output.shape[0], w_gate.shape[1]
    n_tp = lax.axis_size("tp")
    line = LineSum(n_tp, 2 * rows, width, 4 * row_chains)
    n_line = len(line.scratch())
    half = rows // 2
    tile = 64
    cut = 512
    n_cut = wide // cut
    part = line.part

    def body(
        attn_hbm, tok_hbm, again_ref, wo_hbm, wg_hbm, wu_hbm, wd_hbm,
        proj_out, hidt_out, gate_out, up_out, inner_out, down_out, inv_out,
        attn_v, tok, wo, hid, hidt, gate, up, inner, wg, wu, wd, first, loads, stores, *rest,
    ):
        line.bind(rest[:n_line])
        start = load_list([(attn_hbm, attn_v), (wo_hbm, wo), (tok_hbm, tok)], first)
        pairs = []
        for j in range(n_cut):
            cols = pl.ds(j * cut, cut)
            pairs += [(wg_hbm.at[:, cols], wg.at[j]), (wu_hbm.at[:, cols], wu.at[j])]
        for j in range(n_tp):
            cols = pl.ds(j * part, part)
            pairs += [(wd_hbm.at[:, cols], wd.at[j])]
        weights = load_list(pairs, loads)
        bar = pltpu.get_barrier_semaphore()
        peers = line.greet(bar)
        for copy in start:
            copy.wait()
        for j in range(n_tp):
            line.own[j, :rows] = jnp.dot(
                attn_v[...], wo[:, j * part : (j + 1) * part], preferred_element_type=f32
            ).astype(bf16)
        pl.semaphore_wait(bar, peers)

        def step(t, carry):
            line.step(t)

            @pl.when(t == 3 * n_tp + 1)
            def _():
                hidt[...] = jnp.transpose(hid[...])

            return carry

        def row_half(c, carry):
            base = pl.multiple_of(c * half, half)
            sl = pl.ds(base, half)
            lax.fori_loop(c * 2 * n_tp, c * n_tp + 2 * n_tp - 1, step, 0)

            def norm_rows(t, carry):
                rs = pl.ds(pl.multiple_of(base + t * tile, tile), tile)
                outs = [line.res[j, rs].astype(f32) for j in range(n_tp)]
                square = sum(jnp.sum(out * out, axis=1, keepdims=True) for out in outs)
                inv = lax.rsqrt(square * (1.0 / width) + norm_eps)
                inv_out[rs, :] = inv
                for j, out in enumerate(outs):
                    cols = slice(j * part, (j + 1) * part)
                    hid[rs, cols] = (
                        tok[rs, cols].astype(f32) + out * inv * again_ref[:, cols]
                    ).astype(bf16)
                return carry

            lax.fori_loop(0, half // tile, norm_rows, 0)
            for j in range(n_cut):
                cols = slice(j * cut, (j + 1) * cut)

                @pl.when(c == 0)
                def _():
                    weights[2 * j].wait()
                    weights[2 * j + 1].wait()

                g = jnp.dot(hid[sl], wg[j], preferred_element_type=f32)
                u = jnp.dot(hid[sl], wu[j], preferred_element_type=f32)
                gate[sl, cols] = g.astype(bf16)
                up[sl, cols] = u.astype(bf16)
                inner[sl, cols] = (g * jax.nn.sigmoid(g) * u).astype(bf16)
                low, high = j * row_chains // n_cut, (j + 1) * row_chains // n_cut
                line.pieces(((c + 2) * n_tp - 1) * row_chains + low, high - low)
            for j in range(n_tp):

                @pl.when(c == 0)
                def _():
                    weights[2 * n_cut + j].wait()

                line.own[j, pl.ds(rows + base, half)] = jnp.dot(
                    inner[sl], wd[j], preferred_element_type=f32
                ).astype(bf16)
            return carry

        lax.fori_loop(0, 2, row_half, 0)
        outs = load_list([(gate, gate_out), (up, up_out), (inner, inner_out)], stores)
        ready = line.ship(proj_out, stores, 4, 0, rows)
        lax.fori_loop(3 * n_tp, line.steps, step, 0)
        last = pltpu.make_async_copy(hidt, hidt_out, stores.at[3])
        last.start()
        ready = ready + line.ship(down_out, stores, 4 + n_tp, rows, rows)
        line.drain()
        for copy in outs + [last] + ready:
            copy.wait()

    sem = pltpu.SemaphoreType.DMA
    return kernel_call(
        body, [attn, tokens, attn_gain, w_output, w_gate, w_up, w_down], "hhvhhhh",
        [((rows, width), bf16), ((width, rows), bf16), ((rows, wide), bf16), ((rows, wide), bf16),
         ((rows, wide), bf16), ((rows, width), bf16), ((rows, 1), f32)],
        "hhhhhhv",
        [
            pltpu.VMEM((rows, local), bf16), pltpu.VMEM((rows, width), bf16),
            pltpu.VMEM((local, width), bf16),
            pltpu.VMEM((rows, width), bf16), pltpu.VMEM((width, rows), bf16),
            pltpu.VMEM((rows, wide), bf16), pltpu.VMEM((rows, wide), bf16),
            pltpu.VMEM((rows, wide), bf16),
            pltpu.VMEM((n_cut, width, cut), bf16), pltpu.VMEM((n_cut, width, cut), bf16),
            pltpu.VMEM((n_tp, wide, part), bf16),
            sem((3,)), sem((2 * n_cut + n_tp,)), sem((4 + 2 * n_tp,)),
        ] + line.scratch(),
        cid, "middle",
    )


def mlp_back(down, grad, mlp_gain, gate, up, inner, hid_t, w_gate, w_up, w_down, jobs, widths, cid):
    rows, width = down.shape
    wide = gate.shape[1]
    n_tp = lax.axis_size("tp")
    line = LineSum(n_tp, rows, width)
    grads = GradScatter(lax.axis_size("ctx"), lax.axis_size("seq"), width, jobs)
    n_line, n_grads, n_out = len(line.scratch()), len(grads.scratch()), len(widths)
    tile = 64
    cut = 512
    n_cut = wide // cut
    part = line.part
    lead = row_chains * n_tp // (n_cut + n_tp)
    ticks = n_cut // 2 + n_tp // 2

    def body(
        down_hbm, grad_hbm, mgain_ref, gate_hbm, up_hbm, inner_hbm, hidt_hbm, wg_hbm, wu_hbm, wd_hbm,
        back_out, dgate_out, dup_out, dgain_out, inv_out, *rest,
    ):
        grad_outs, rest = rest[:n_out], rest[n_out:]
        (gate_v, up_v, inner_v, hidt, ddown, ddownt, dgate, dup, ring, loads, wsem, stores) = rest[:12]
        line.bind(rest[12 : 12 + n_line])
        grads.bind(rest[12 + n_line :], [ddownt, hidt], [inner_v, dgate, dup], grad_outs)

        def fetch(src, index):
            return pltpu.make_async_copy(src, ring.at[index], wsem.at[index])

        def rows_of(ref, j, size):
            return ref.at[pl.ds(pl.multiple_of(j * size, size), size)]

        for j in range(4):
            fetch(rows_of(wd_hbm, j, cut), j).start()
        down_ref, grad_ref = dgate.at[:, pl.ds(0, width)], dup.at[:, pl.ds(0, width)]
        first = load_list([(down_hbm, down_ref), (grad_hbm, grad_ref)], loads, 4)
        early = load_list(
            [(inner_hbm, inner_v), (gate_hbm, gate_v), (up_hbm, up_v), (hidt_hbm, hidt)], loads
        )
        bar = pltpu.get_barrier_semaphore()
        peers = line.greet(bar) + grads.greet(bar)
        dgain_out[...] = jnp.zeros_like(dgain_out)
        for copy in first:
            copy.wait()

        def norm_rows(t, carry):
            sl = pl.ds(pl.multiple_of(t * tile, tile), tile)
            out = down_ref[sl].astype(f32)
            upstream = grad_ref[sl].astype(f32)
            inv = lax.rsqrt(jnp.mean(out * out, axis=1, keepdims=True) + norm_eps)
            norm = out * inv
            inv_out[sl, :] = inv
            dgain_out[...] += jnp.sum(upstream * norm, axis=0, keepdims=True)
            dnorm = upstream * mgain_ref[...]
            dot = jnp.mean(dnorm * norm, axis=1, keepdims=True)
            ddown[sl] = (inv * (dnorm - norm * dot)).astype(bf16)
            return carry

        lax.fori_loop(0, rows // tile, norm_rows, 0)
        ddownt[...] = jnp.transpose(ddown[...])
        for copy in early:
            copy.wait()
        pl.semaphore_wait(bar, peers)

        half = rows // 2

        def row_half(c, carry):
            sl = pl.ds(pl.multiple_of(c * half, half), half)

            def beside(i, j, first):
                @pl.when(c == 1)
                def _():
                    line.pieces(i * lead, lead)

                @pl.when(lax.rem(j, 2) == 1)
                def _():
                    grads.tick(first + j // 2)

            def inner_back(j, carry):
                fetch(rows_of(wd_hbm, j, cut), j).wait()
                cols = pl.ds(pl.multiple_of(j * cut, cut), cut)
                dmix = dot_nt(ddown[sl], ring[j])
                g, u = gate_v[sl, cols].astype(f32), up_v[sl, cols].astype(f32)
                sig = jax.nn.sigmoid(g)
                dgate[sl, cols] = (dmix * u * sig * (1.0 + g * (1.0 - sig))).astype(bf16)
                dup[sl, cols] = (dmix * (g * sig)).astype(bf16)

                @pl.when(lax.rem(j, 2) == 0)
                def _():
                    fetch(rows_of(wg_hbm, j // 2, part), j).start()

                @pl.when(lax.rem(j, 2) == 1)
                def _():
                    fetch(rows_of(wu_hbm, j // 2, part), j).start()

                beside(j, j, c * ticks)
                return carry

            lax.fori_loop(0, n_cut, inner_back, 0)

            def hidden_back(j, carry):
                slot = lax.rem(2 * j, 4)
                fetch(rows_of(wg_hbm, j, part), slot).wait()
                fetch(rows_of(wu_hbm, j, part), slot + 1).wait()
                line.own[j, sl] = (
                    dot_nt(dgate[sl], ring[slot]) + dot_nt(dup[sl], ring[slot + 1])
                ).astype(bf16)

                @pl.when(j + 2 < n_tp)
                def _():
                    fetch(rows_of(wg_hbm, j + 2, part), slot).start()
                    fetch(rows_of(wu_hbm, j + 2, part), slot + 1).start()

                @pl.when((j + 2 >= n_tp) & (c == 0))
                def _():
                    fetch(rows_of(wd_hbm, slot, cut), slot).start()
                    fetch(rows_of(wd_hbm, slot + 1, cut), slot + 1).start()

                beside(n_cut + j, j, c * ticks + n_cut // 2)
                return carry

            lax.fori_loop(0, n_tp, hidden_back, 0)
            return carry

        lax.fori_loop(0, 2, row_half, 0)
        outs = load_list([(dgate, dgate_out), (dup, dup_out)], stores)
        done, used = 2 * ticks, (n_cut + n_tp) * lead

        def one(it, carry):
            line.pieces(used + (it - done) * pace, pace)
            grads.tick(it)
            return carry

        line_its = -(-(line.steps * row_chains - used) // pace)
        lax.fori_loop(done, max(done + line_its, grads.steps), one, 0)
        outs += line.ship(back_out, stores, 2, 0, rows)
        line.drain()
        grads.drain()
        for copy in outs:
            copy.wait()

    sem = pltpu.SemaphoreType.DMA
    return kernel_call(
        body, [down, grad, mlp_gain, gate, up, inner, hid_t, w_gate, w_up, w_down], "hhvhhhhhhh",
        [((rows, width), bf16), ((rows, wide), bf16), ((rows, wide), bf16), ((1, width), f32),
         ((rows, 1), f32)]
        + grads.out_shapes(widths),
        "hhhvv" + "v" * n_out,
        [
            pltpu.VMEM((rows, wide), bf16), pltpu.VMEM((rows, wide), bf16),
            pltpu.VMEM((rows, wide), bf16), pltpu.VMEM((width, rows), bf16),
            pltpu.VMEM((rows, width), bf16), pltpu.VMEM((width, rows), bf16),
            pltpu.VMEM((rows, wide), bf16), pltpu.VMEM((rows, wide), bf16),
            pltpu.VMEM((4, cut, width), bf16),
            sem((6,)), sem((4,)), sem((2 + n_tp,)),
        ] + line.scratch() + grads.scratch(),
        cid, "mlp_back",
    )


def last_sums(dqkv, w_query, w_key, w_value, ats, bs, jobs, widths, gains, cid):
    rows = dqkv.shape[0]
    width, local = w_query.shape
    n_ctx, n_seq = lax.axis_size("ctx"), lax.axis_size("seq")
    n_tp = lax.axis_size("tp")
    line = LineSum(n_tp, rows, width)
    grads = GradScatter(n_ctx, n_seq, width, jobs)
    small = GainSum(n_ctx, n_seq, gains.shape[0])
    na, nb, n_out = len(ats), len(bs), len(widths)
    n_line, n_grads = len(line.scratch()), len(grads.scratch())
    part = line.part

    def body(dqkv_ref, wq_ref, wk_ref, wv_ref, *refs):
        at_refs, b_refs = refs[:na], refs[na : na + nb]
        gain_ref, last_out = refs[na + nb], refs[na + nb + 1]
        refs = refs[na + nb + 2 :]
        grad_outs, gain_out, stores, scratch = refs[:n_out], refs[n_out], refs[n_out + 1], refs[n_out + 2 :]
        line.bind(scratch[:n_line])
        grads.bind(scratch[n_line : n_line + n_grads], at_refs, list(b_refs) + [dqkv_ref], grad_outs)
        small.bind(scratch[n_line + n_grads :], gain_ref, gain_out)
        bar = pltpu.get_barrier_semaphore()
        peers = line.greet(bar) + small.greet(bar)
        pl.semaphore_wait(bar, peers)
        small.start()

        def input_back(j, carry):
            rs = pl.ds(pl.multiple_of(j * part, part), part)
            line.own[j] = (
                dot_nt(dqkv_ref[:, :local], wq_ref[rs])
                + dot_nt(dqkv_ref[:, local : 2 * local], wk_ref[rs])
                + dot_nt(dqkv_ref[:, 2 * local :], wv_ref[rs])
            ).astype(bf16)

            @pl.when(lax.rem(j, 2) == 0)
            def _():
                grads.tick(j // 2)

            return carry

        lax.fori_loop(0, n_tp, input_back, 0)
        done = n_tp // 2

        def one(it, carry):
            grads.tick(it)
            line.pieces((it - done) * pace, pace)
            return carry

        line_steps = -(-line.steps * row_chains // pace)
        lax.fori_loop(done, max(done + line_steps, grads.steps), one, 0)
        small.finish()
        outs = line.ship(last_out, stores, 0, 0, rows)
        line.drain()
        grads.drain()
        for copy in outs:
            copy.wait()

    sem = pltpu.SemaphoreType.DMA
    return kernel_call(
        body, [dqkv, w_query, w_key, w_value] + list(ats) + list(bs) + [gains],
        "vvvv" + "v" * (na + nb + 1),
        [((rows, width), bf16)] + grads.out_shapes(widths) + [(gains.shape, f32)],
        "h" + "v" * (n_out + 1),
        [sem((n_tp,))] + line.scratch() + grads.scratch() + small.scratch(),
        cid, "last_sums",
    )


def per_device(
    tokens,
    out_grad,
    group_order,
    w_query,
    w_key,
    w_value,
    query_gain,
    key_gain,
    w_output,
    attn_gain,
    w_gate,
    w_up,
    w_down,
    mlp_gain,
):
    inputs = tokens[0]
    upstream = out_grad[0]
    rows, width = inputs.shape
    heads, head_dim = query_gain.shape
    local = heads * head_dim
    wide = w_gate.shape[1]
    positions = key_positions(group_order[0], lax.axis_index("ctx") * rows, rows, rows // 2)
    cosine, sine = rope_tables(positions, head_dim)
    angle_cos = jnp.concatenate([cosine, cosine], axis=1)
    angle_sin = jnp.concatenate([-sine, sine], axis=1)
    qgain = query_gain.reshape(1, local)
    kgain = key_gain.reshape(1, local)
    (query_rot, keys, values, query_norm, key_norm, attn, tokens_t, scales, lse) = front(
        inputs, w_query, w_key, w_value, qgain, kgain, angle_cos, angle_sin, group_order, 1
    )
    proj, hidden_t, gate, up, inner, down, proj_scale = middle(
        attn, inputs, attn_gain[None], w_output, w_gate, w_up, w_down, 2
    )
    chunk_cols = 2 * lanes
    chunks = wide // chunk_cols
    thin = local // chunk_cols
    back, d_gate, d_up, d_mlp_gain, down_scale, grad_down, grad_gate = mlp_back(
        down, upstream, mlp_gain[None], gate, up, inner, hidden_t, w_gate, w_up, w_down,
        [
            dict(a=0, b=0, first=0, count=chunks, out=0, place=0, flip=True),
            dict(a=1, b=1, first=0, count=chunks, out=1, place=0, flip=False),
        ],
        [wide, wide],
        3,
    )
    d_qkv, d_proj_t, d_attn_gain, d_query_gain, d_key_gain = attention_back(
        back, upstream, proj, attn_gain[None], w_output, query_rot, keys, values, attn, lse,
        positions[None], group_order, query_norm, key_norm, scales, qgain, kgain, angle_cos,
        angle_sin, [], [], [], [], 4,
    )
    owners = lax.axis_size("ctx") * lax.axis_size("seq")
    gains = [d_attn_gain, d_mlp_gain, d_query_gain, d_key_gain]
    ends = [gain.shape[1] for gain in gains]
    ends = [sum(ends[: i + 1]) for i in range(4)]
    packed = jnp.concatenate(gains, axis=1).reshape(-1, lanes)
    last, grad_up, grad_qkv, grad_output, small = last_sums(
        d_qkv, w_query, w_key, w_value,
        [hidden_t, tokens_t, d_proj_t],
        [d_up, attn],
        [
            dict(a=0, b=0, first=0, count=chunks, out=0, place=0, flip=False),
            dict(a=2, b=1, first=0, count=thin, out=2, place=0, flip=True),
            dict(a=1, b=2, first=0, count=3 * thin, out=1, place=0, flip=False),
        ],
        [wide, 3 * local, local],
        packed,
        5,
    )
    small = small.reshape(-1)
    me = lax.axis_index("ctx") * lax.axis_size("seq") + lax.axis_index("seq")

    def my_part(start, end, lead):
        whole = small[start:end].reshape(lead, -1)
        size = whole.shape[1] // owners
        return lax.dynamic_slice_in_dim(whole, me * size, size, 1)

    g_attn = my_part(0, ends[0], 1)[0]
    g_mlp = my_part(ends[0], ends[1], 1)[0]
    g_query = my_part(ends[1], ends[2], heads)
    g_key = my_part(ends[2], ends[3], heads)
    grad_query, grad_key, grad_value = jnp.split(grad_qkv, 3, axis=1)
    attn_norm = proj.astype(f32) * proj_scale
    mlp_norm = down.astype(f32) * down_scale
    block_out = inputs.astype(f32) + attn_norm * attn_gain + mlp_norm * mlp_gain
    input_grad = upstream.astype(f32) + back.astype(f32) + last.astype(f32)
    return (
        block_out[None],
        input_grad[None],
        grad_query,
        grad_key,
        grad_value,
        g_query,
        g_key,
        grad_output,
        g_attn,
        grad_gate,
        grad_up,
        grad_down,
        g_mlp,
    )


def solution(mesh):
    return jax.shard_map(
        per_device,
        mesh=mesh,
        in_specs=(
            P("seq", "ctx", None),
            P("seq", "ctx", None),
            P("seq", None),
            P(None, "tp"),
            P(None, "tp"),
            P(None, "tp"),
            P("tp", None),
            P("tp", None),
            P("tp", None),
            P(),
            P(None, "tp"),
            P(None, "tp"),
            P("tp", None),
            P(),
        ),
        out_specs=(
            P("seq", "ctx", None),
            P("seq", "ctx", None),
            P(("ctx", "seq"), "tp"),
            P(("ctx", "seq"), "tp"),
            P(("ctx", "seq"), "tp"),
            P("tp", ("ctx", "seq")),
            P("tp", ("ctx", "seq")),
            P("tp", ("ctx", "seq")),
            P(("ctx", "seq")),
            P(("ctx", "seq"), "tp"),
            P(("ctx", "seq"), "tp"),
            P("tp", ("ctx", "seq")),
            P(("ctx", "seq")),
        ),
        check_vma=False,
    )
```

```python
import jax
import jax.numpy as jnp
from jax import lax
from jax.sharding import PartitionSpec as P
from jax.experimental import pallas as pl
from jax.experimental.pallas import tpu as pltpu

norm_eps = 1e-06
rope_base = 500000.0
masked_score = -1e30


def rope_tables(positions, head_dim):
    half = head_dim // 2
    channel = jnp.arange(head_dim, dtype=jnp.int32)
    rates = rope_base ** (-((channel % half).astype(jnp.float32) * 2.0 / head_dim))
    angle = positions.astype(jnp.float32)[:, None] * rates[None, :]
    return jnp.cos(angle), jnp.where(channel[None, :] < half, -jnp.sin(angle), jnp.sin(angle))


def key_positions(order, first_row, count, group):
    row_ids = first_row + jnp.arange(count, dtype=jnp.int32)
    slots = row_ids // group
    picks = slots[:, None] == jnp.arange(order.shape[0], dtype=jnp.int32)[None, :]
    return jnp.sum(jnp.where(picks, order[None, :], 0), axis=1) * group + row_ids % group


MESH = pl.DeviceIdType.MESH
bf16 = jnp.bfloat16
f32 = jnp.float32
lanes = 128
row_blocks = 16
row_chains = 8
pace = 6


def remote(src, dst, send, recv, where):
    return pltpu.make_async_remote_copy(
        src, dst, send, recv, device_id=where, device_id_type=MESH
    )


class LineSum:
    def __init__(self, n, rows, width, blocks=row_blocks):
        self.n, self.rows, self.width = n, rows, width
        self.part = width // n
        self.rc = rows // blocks
        self.total = blocks // row_chains * n
        self.steps = self.total + n - 1

    def scratch(self):
        shape = (self.n, self.rows, self.part)
        return (
            [pltpu.VMEM(shape, bf16)] * 4
            + [pltpu.SemaphoreType.DMA] * 2
            + [pltpu.SemaphoreType.DMA((row_chains, self.total))] * 2
        )

    def bind(self, refs):
        self.own, self.from_l, self.from_r, self.res = refs[:4]
        self.send_r, self.send_l, self.recv_l, self.recv_r = refs[4:]
        self.i = lax.axis_index("tp")
        self.has_l, self.has_r = self.i > 0, self.i < self.n - 1

    def greet(self, bar):
        @pl.when(self.has_l)
        def _():
            pl.semaphore_signal(bar, inc=1, device_id={"tp": self.i - 1}, device_id_type=MESH)

        @pl.when(self.has_r)
        def _():
            pl.semaphore_signal(bar, inc=1, device_id={"tp": self.i + 1}, device_id_type=MESH)

        return self.has_l.astype(jnp.int32) + self.has_r.astype(jnp.int32)

    def load(self, x_ref):
        for j in range(self.n):
            self.own[j] = x_ref[:, j * self.part : (j + 1) * self.part]

    def rows_of(self, g, p):
        block = (p // self.n) * row_chains + g
        return pl.ds(pl.multiple_of(block * self.rc, self.rc), self.rc)

    def right(self, src, dst, g, p, j):
        sl = self.rows_of(g, p)
        return remote(
            src.at[j, sl], dst.at[j, sl], self.send_r, self.recv_l.at[g, p],
            {"tp": self.i + 1},
        )

    def left(self, src, dst, g, q, j):
        sl = self.rows_of(g, q)
        return remote(
            src.at[j, sl], dst.at[j, sl], self.send_l, self.recv_r.at[g, q],
            {"tp": self.i - 1},
        )

    def wait_l(self, g, p, j):
        sl = self.rows_of(g, p)
        remote(
            self.own.at[j, sl], self.from_l.at[j, sl], self.send_r, self.recv_l.at[g, p],
            {"tp": self.i - 1},
        ).wait_recv()

    def wait_r(self, g, q, j):
        sl = self.rows_of(g, q)
        remote(
            self.own.at[j, sl], self.from_r.at[j, sl], self.send_l, self.recv_r.at[g, q],
            {"tp": self.i + 1},
        ).wait_recv()

    def step(self, t):
        self.pieces(t * row_chains, row_chains)

    def pieces(self, first, count):
        def one(v, carry):
            self.piece(first + v)
            return carry

        lax.fori_loop(0, count, one, 0)

    def piece(self, e):
        t = e // row_chains

        @pl.when(t < self.steps)
        def _():
            self.sub_step(t, lax.rem(e, row_chains))

    def sub_step(self, t, g):
        n, i, has_l, has_r = self.n, self.i, self.has_l, self.has_r
        own, from_l, from_r, res = self.own, self.from_l, self.from_r, self.res
        p = t - i
        q = t - (n - 1 - i)
        jr = n - 1 - lax.rem(p + n * self.total, n)
        jl = lax.rem(q + n * self.total, n)
        pv = (p >= 0) & (p < self.total)
        qv = (q >= 0) & (q < self.total)

        @pl.when(pv & has_l)
        def _():
            self.wait_l(g, p, jr)

        @pl.when(qv & has_r)
        def _():
            self.wait_r(g, q, jl)

        @pl.when(pv & (jr > i))
        def _():
            sl = self.rows_of(g, p)

            @pl.when(has_l)
            def _():
                own[jr, sl] = (own[jr, sl].astype(f32) + from_l[jr, sl].astype(f32)).astype(bf16)

            self.right(own, from_l, g, p, jr).start()

        @pl.when(qv & (jl < i))
        def _():
            sl = self.rows_of(g, q)

            @pl.when(has_r)
            def _():
                own[jl, sl] = (own[jl, sl].astype(f32) + from_r[jl, sl].astype(f32)).astype(bf16)

            self.left(own, from_r, g, q, jl).start()

        @pl.when(pv & (jr == i))
        def _():
            sl = self.rows_of(g, p)

            @pl.when(has_l & has_r)
            def _():
                res[i, sl] = (
                    own[i, sl].astype(f32) + from_l[i, sl].astype(f32) + from_r[i, sl].astype(f32)
                ).astype(bf16)

            @pl.when(jnp.logical_not(has_l))
            def _():
                res[i, sl] = (own[i, sl].astype(f32) + from_r[i, sl].astype(f32)).astype(bf16)

            @pl.when(jnp.logical_not(has_r))
            def _():
                res[i, sl] = (own[i, sl].astype(f32) + from_l[i, sl].astype(f32)).astype(bf16)

        @pl.when(pv & (jr <= i) & has_r)
        def _():
            self.right(res, res, g, p, jr).start()

        @pl.when(qv & (jl >= i) & has_l)
        def _():
            self.left(res, res, g, q, jl).start()

    def drain(self):
        @pl.when(self.has_r)
        def _():
            remote(
                self.own, self.from_l, self.send_r, self.recv_l.at[0, 0], {"tp": self.i + 1}
            ).wait_send()

        @pl.when(self.has_l)
        def _():
            remote(
                self.own, self.from_r, self.send_l, self.recv_r.at[0, 0], {"tp": self.i - 1}
            ).wait_send()

    def ship(self, out_ref, sems, base, start, count):
        return load_list(
            [
                (
                    self.res.at[j, pl.ds(start, count)],
                    out_ref.at[:, pl.ds(j * self.part, self.part)],
                )
                for j in range(self.n)
            ],
            sems, base,
        )


class GradScatter:
    def __init__(self, n_ctx, n_seq, width, jobs, orders=("xy", "yx")):
        self.nx, self.ny = n_ctx // 2, n_seq
        self.rows = width // (n_ctx * n_seq)
        self.jobs, self.orders = jobs, orders
        start = 0
        self.spans = []
        for job in jobs:
            self.spans.append((start, start + job["count"]))
            start += job["count"]
        self.total = start
        self.steps = start + 5

    def out_shapes(self, widths):
        flips = {job["out"] for job in self.jobs if job["flip"]}
        return [
            ((w, self.rows) if i in flips else (self.rows, w), f32) for i, w in enumerate(widths)
        ]

    def sizes(self, order):
        return (self.nx, self.ny) if order == "xy" else (self.ny, self.nx)

    def scratch(self):
        nx, ny, t = self.nx, self.ny, self.total
        tile = (self.rows, lanes)
        sem = pltpu.SemaphoreType.DMA
        out = [
            pltpu.VMEM((2, nx, ny, 2) + tile, bf16),
            pltpu.VMEM((2, nx, ny, 2) + tile, f32),
            pltpu.VMEM((t, nx, ny, 2) + tile, bf16),
            sem((2,)), sem((t,)),
        ]
        for order in self.orders:
            n1, n2 = self.sizes(order)
            out += [
                pltpu.VMEM((3, n1, n2) + tile, bf16),
                pltpu.VMEM((t, n1 - 1, n2) + tile, bf16),
                pltpu.VMEM((3, n2) + tile, bf16),
                pltpu.VMEM((t, n2 - 1) + tile, bf16),
                sem((3, n1 - 1)), sem((t, n1 - 1)), sem((3, n2 - 1)), sem((t, n2 - 1)),
            ]
        return out

    def bind(self, refs, at_refs, b_refs, out_refs):
        self.send0, self.keep, self.recv0, self.s0, self.d0 = refs[:5]
        self.half = [refs[5 + 8 * h : 13 + 8 * h] for h in range(2)]
        self.at_refs, self.b_refs, self.out_refs = at_refs, b_refs, out_refs
        ctx = lax.axis_index("ctx")
        self.mx, self.core, self.my = ctx // 2, lax.rem(ctx, 2), lax.axis_index("seq")

    def axis(self, name, d):
        if name == "x":
            to = lax.rem(self.mx + d, self.nx)
            return to, {"ctx": to * 2 + self.core}
        to = lax.rem(self.my + d, self.ny)
        return to, {"seq": to}

    def at_mate(self):
        return {"ctx": self.mx * 2 + 1 - self.core}

    def greet(self, bar):
        places = [self.at_mate()]
        places += [self.axis("x", d)[1] for d in range(1, self.nx)]
        places += [self.axis("y", d)[1] for d in range(1, self.ny)]
        for place in places:
            pl.semaphore_signal(bar, inc=1, device_id=place, device_id_type=MESH)
        return len(places)

    def c0(self, c):
        slot = lax.rem(c, 2)
        return remote(
            self.send0.at[slot], self.recv0.at[c], self.s0.at[slot], self.d0.at[c], self.at_mate()
        )

    def c1(self, h, c, d):
        p, r1, _, _, sent, done, _, _ = self.half[h]
        to, where = self.axis(self.orders[h][0], d)
        slot = lax.rem(c, 3)
        return remote(p.at[slot, to], r1.at[c, d - 1], sent.at[slot, d - 1], done.at[c, d - 1], where)

    def c2(self, h, c, d):
        _, _, q, r2, _, _, sent, done = self.half[h]
        to, where = self.axis(self.orders[h][1], d)
        slot = lax.rem(c, 3)
        return remote(q.at[slot, to], r2.at[c, d - 1], sent.at[slot, d - 1], done.at[c, d - 1], where)

    def make(self, c):
        slot = lax.rem(c, 2)
        nx, ny, r = self.nx, self.ny, self.rows

        @pl.when(c >= 2)
        def _():
            self.c0(c).wait_send()

        def products(at_ref, b_ref, col, parity, write):
            def tile(e, carry):
                x, y = e // ny, lax.rem(e, ny)
                row = pl.multiple_of(((x * 2 + parity) * ny + y) * r, r)
                acc = jnp.dot(
                    at_ref[pl.ds(row, r), :], b_ref[:, pl.ds(col, 2 * lanes)],
                    preferred_element_type=f32,
                )
                write(x, y, acc)
                return carry

            lax.fori_loop(0, nx * ny, tile, 0)

        def to_send(x, y, acc):
            self.send0[slot, x, y, 0] = acc[:, :lanes].astype(bf16)
            self.send0[slot, x, y, 1] = acc[:, lanes:].astype(bf16)

        def to_keep(x, y, acc):
            self.keep[slot, x, y, 0] = acc[:, :lanes]
            self.keep[slot, x, y, 1] = acc[:, lanes:]

        for job, (lo, hi) in zip(self.jobs, self.spans):

            @pl.when((c >= lo) & (c < hi))
            def _():
                at_ref, b_ref = self.at_refs[job["a"]], self.b_refs[job["b"]]
                col = pl.multiple_of((c - lo + job["first"]) * (2 * lanes), 2 * lanes)
                products(at_ref, b_ref, col, 1 - self.core, to_send)
                self.c0(c).start()
                products(at_ref, b_ref, col, self.core, to_keep)

    def pair(self, c):
        slot, two = lax.rem(c, 3), lax.rem(c, 2)

        @pl.when(c >= 3)
        def _():
            for h in range(2):
                for d in range(1, self.sizes(self.orders[h])[0]):
                    self.c1(h, c, d).wait_send()

        self.c0(c).wait_recv()
        for h, order in enumerate(self.orders):
            p = self.half[h][0]
            for x in range(self.nx):
                for y in range(self.ny):
                    spot = (x, y) if order == "xy" else (y, x)
                    p[(slot,) + spot] = (
                        self.keep[two, x, y, h] + self.recv0[c, x, y, h].astype(f32)
                    ).astype(bf16)
            for d in range(1, self.sizes(order)[0]):
                self.c1(h, c, d).start()

    def own(self, name):
        return self.mx if name == "x" else self.my

    def cross(self, c):
        slot = lax.rem(c, 3)

        @pl.when(c >= 3)
        def _():
            for h in range(2):
                for d in range(1, self.sizes(self.orders[h])[1]):
                    self.c2(h, c, d).wait_send()

        for h, order in enumerate(self.orders):
            n1, n2 = self.sizes(order)
            p, r1, q = self.half[h][:3]
            for d in range(1, n1):
                self.c1(h, c, d).wait_recv()
            for e in range(n2):
                acc = p[slot, self.own(order[0]), e].astype(f32)
                for d in range(1, n1):
                    acc = acc + r1[c, d - 1, e].astype(f32)
                q[slot, e] = acc.astype(bf16)
            for d in range(1, n2):
                self.c2(h, c, d).start()

    def finish(self, c):
        slot = lax.rem(c, 3)
        totals = []
        for h, order in enumerate(self.orders):
            n2 = self.sizes(order)[1]
            q, r2 = self.half[h][2:4]
            for d in range(1, n2):
                self.c2(h, c, d).wait_recv()
            acc = q[slot, self.own(order[1])].astype(f32)
            for d in range(1, n2):
                acc = acc + r2[c, d - 1].astype(f32)
            totals.append(acc)
        for job, (lo, hi) in zip(self.jobs, self.spans):

            @pl.when((c >= lo) & (c < hi))
            def _():
                out_ref = self.out_refs[job["out"]]
                col = pl.multiple_of((c - lo + job["place"]) * (2 * lanes), 2 * lanes)
                for h in range(2):
                    place = pl.ds(col + h * lanes, lanes)
                    if job["flip"]:
                        out_ref[place, :] = jnp.transpose(totals[h])
                    else:
                        out_ref[:, place] = totals[h]

    def tick(self, it):
        @pl.when((it >= 5) & (it < self.total + 5))
        def _():
            self.finish(it - 5)

        @pl.when((it >= 3) & (it < self.total + 3))
        def _():
            self.cross(it - 3)

        @pl.when((it >= 1) & (it < self.total + 1))
        def _():
            self.pair(it - 1)

        @pl.when(it < self.total)
        def _():
            self.make(it)

    def drain(self):
        for c in range(max(self.total - 2, 0), self.total):
            self.c0(c).wait_send()
        for c in range(max(self.total - 3, 0), self.total):
            for h, order in enumerate(self.orders):
                n1, n2 = self.sizes(order)
                for d in range(1, n1):
                    self.c1(h, c, d).wait_send()
                for d in range(1, n2):
                    self.c2(h, c, d).wait_send()


class GainSum:
    def __init__(self, n_ctx, n_seq, rows):
        self.ny, self.n, self.rows = n_seq, n_ctx * n_seq, rows

    def scratch(self):
        sem = pltpu.SemaphoreType.DMA
        return [pltpu.VMEM((self.n - 1, self.rows, lanes), f32), sem((self.n - 1,)), sem((self.n - 1,))]

    def bind(self, refs, in_ref, out_ref):
        self.got, self.sent, self.done = refs
        self.in_ref, self.out_ref = in_ref, out_ref
        self.me = lax.axis_index("ctx") * self.ny + lax.axis_index("seq")

    def place(self, d):
        to = lax.rem(self.me + d, self.n)
        return {"ctx": to // self.ny, "seq": lax.rem(to, self.ny)}

    def copy(self, d):
        return remote(
            self.in_ref, self.got.at[d - 1], self.sent.at[d - 1], self.done.at[d - 1], self.place(d)
        )

    def greet(self, bar):
        for d in range(1, self.n):
            pl.semaphore_signal(bar, inc=1, device_id=self.place(d), device_id_type=MESH)
        return self.n - 1

    def start(self):
        for d in range(1, self.n):
            self.copy(d).start()

    def finish(self):
        acc = self.in_ref[...]
        for d in range(1, self.n):
            self.copy(d).wait_recv()
            acc = acc + self.got[d - 1]
        self.out_ref[...] = acc
        for d in range(1, self.n):
            self.copy(d).wait_send()


def vmem_spec():
    return pl.BlockSpec(memory_space=pltpu.VMEM)


def comm_call(body, args, outs, scratch, cid, name, scalars=()):
    return pl.pallas_call(
        body,
        out_shape=outs,
        in_specs=[
            pl.BlockSpec(memory_space=pltpu.SMEM) if i in scalars else vmem_spec()
            for i in range(len(args))
        ],
        out_specs=[vmem_spec()] * len(outs),
        scratch_shapes=scratch,
        compiler_params=pltpu.CompilerParams(
            collective_id=cid, has_side_effects=True, vmem_limit_bytes=62 * 2**20
        ),
        name=name,
    )(*args)


class LineSmall:
    def __init__(self, n, rows):
        self.n, self.rows = n, rows

    def scratch(self):
        sem = pltpu.SemaphoreType.DMA
        return [
            pltpu.VMEM((8, self.rows), f32), pltpu.VMEM((self.n - 1, 8, self.rows), f32),
            sem((self.n - 1,)), sem((self.n - 1,)),
        ]

    def bind(self, refs):
        self.mine, self.got, self.sent, self.done = refs
        self.i = lax.axis_index("tp")

    def greet(self, bar):
        for d in range(1, self.n):
            pl.semaphore_signal(
                bar, inc=1, device_id={"tp": lax.rem(self.i + d, self.n)}, device_id_type=MESH
            )
        return self.n - 1

    def copy(self, d):
        return remote(
            self.mine, self.got.at[d - 1], self.sent.at[d - 1], self.done.at[d - 1],
            {"tp": lax.rem(self.i + d, self.n)},
        )

    def total(self, columns):
        self.mine[...] = jnp.transpose(columns)[:8]
        for d in range(1, self.n):
            self.copy(d).start()
        acc = self.mine[...]
        for d in range(1, self.n):
            self.copy(d).wait_recv()
            acc = acc + self.got[d - 1]
        for d in range(1, self.n):
            self.copy(d).wait_send()
        return jnp.transpose(jnp.concatenate([acc, jnp.zeros((lanes - 8, self.rows), f32)], axis=0))


def lane_pair(first, second, rows):
    lane = lax.broadcasted_iota(jnp.int32, (rows, lanes), 1)
    return jnp.where(lane == 0, first, 0.0) + jnp.where(lane == 1, second, 0.0)


def dot_nt(left, right):
    return lax.dot_general(left, right, (((1,), (1,)), ((), ())), preferred_element_type=f32)


def dot_tn(left, right):
    return lax.dot_general(left, right, (((0,), (0,)), ((), ())), preferred_element_type=f32)


def attention_back(
    back, grad, proj, attn_gain, w_output, query_rot, keys, values, attn, lse, pos_row, order,
    query_norm, key_norm, scales, qgain, kgain, cosine, sine, ats, bs, jobs, widths, cid,
):
    rows, width = back.shape
    local = w_output.shape[0]
    head_dim = lanes
    heads = local // head_dim
    count = keys.shape[0]
    nx, n_tp = lax.axis_size("ctx") // 2, lax.axis_size("tp")
    small = LineSmall(n_tp, rows)
    n_small = len(small.scratch())
    scale = head_dim ** (-0.5)
    tile = 64
    sub = rows // 2
    na, nb, n_out = len(ats), len(bs), len(widths)
    grads = None
    if jobs:
        grads = GradScatter(2 * nx, lax.axis_size("seq"), width, jobs, ("yx", "yx"))

    def body(
        back_ref, grad_ref, proj_ref, again_ref, w_ref, q_ref, k_ref, v_ref, attn_ref, lse_ref,
        prow_ref, order_ref, qn_ref, kn_ref, sc_ref, qg_ref, kg_ref, cos_ref, sin_ref, *rest,
    ):
        at_refs, b_refs, rest = rest[:na], rest[na : na + nb], rest[na + nb :]
        dqkv_ref, dprojt_ref, dagain_ref, dqg_ref, dkg_ref = rest[:5]
        grad_outs, rest = rest[5 : 5 + n_out], rest[5 + n_out :]
        (dproj, dout, columns, delta, dqs, dks, send0, keep, recv0, recv1, s0, d0, s1, d1) = rest[:14]
        small.bind(rest[14 : 14 + n_small])
        if jobs:
            grads.bind(rest[14 + n_small :], at_refs, b_refs, grad_outs)

        def tick(it):
            if jobs:
                grads.tick(it)

        ctx = lax.axis_index("ctx")
        mx, core = ctx // 2, lax.rem(ctx, 2)
        bar = pltpu.get_barrier_semaphore()
        mate = {"ctx": mx * 2 + 1 - core}
        if jobs:
            peers = small.greet(bar) + grads.greet(bar)
        else:
            peers = small.greet(bar) + nx
            pl.semaphore_signal(bar, inc=1, device_id=mate, device_id_type=MESH)
            for d in range(1, nx):
                pl.semaphore_signal(
                    bar, inc=1, device_id={"ctx": lax.rem(mx + d, nx) * 2 + core},
                    device_id_type=MESH,
                )
        pl.semaphore_wait(bar, peers)
        tick(jnp.int32(0))

        dagain_ref[...] = jnp.zeros_like(dagain_ref)

        def norm_rows(t, carry):
            sl = pl.ds(pl.multiple_of(t * tile, tile), tile)
            dres = grad_ref[sl].astype(f32) + back_ref[sl].astype(f32)
            out = proj_ref[sl].astype(f32)
            inv = lax.rsqrt(jnp.mean(out * out, axis=1, keepdims=True) + norm_eps)
            norm = out * inv
            dagain_ref[...] += jnp.sum(dres * norm, axis=0, keepdims=True)
            dnorm = dres * again_ref[...]
            dot = jnp.mean(dnorm * norm, axis=1, keepdims=True)
            dproj[sl] = (inv * (dnorm - norm * dot)).astype(bf16)
            return carry

        lax.fori_loop(0, rows // tile, norm_rows, 0)
        for h in range(local // sub):
            dout[:, h * sub : (h + 1) * sub] = dot_nt(
                dproj[...], w_ref[h * sub : (h + 1) * sub, :]
            ).astype(bf16)
        lane = lax.broadcasted_iota(jnp.int32, (rows, lanes), 1)
        acc = jnp.zeros((rows, lanes), f32)
        for h in range(heads):
            hs = slice(h * head_dim, (h + 1) * head_dim)
            row_sum = jnp.sum(
                dout[:, hs].astype(f32) * attn_ref[:, hs].astype(f32), axis=1, keepdims=True
            )
            acc = jnp.where(lane == h, row_sum, acc)
        columns[...] = acc
        delta[...] = jnp.transpose(columns[...])[:8]
        dqs[...] = jnp.zeros_like(dqs)

        def c0(h):
            slot = lax.rem(h, 2)
            return remote(send0.at[slot], recv0.at[h], s0.at[slot], d0.at[h], mate)

        def c1(h, d):
            to = lax.rem(mx + d, nx)
            return remote(
                recv0.at[h, to], recv1.at[h, d - 1], s1.at[h, d - 1], d1.at[h, d - 1],
                {"ctx": to * 2 + core},
            )

        def one_block(h, hs, x, owner, write):
            start = (x * 2 + owner) * rows
            for part in range(rows // sub):
                ks = pl.ds(pl.multiple_of(start + part * sub, sub), sub)
                key, value = k_ref[ks, hs], v_ref[ks, hs]
                query, dhead = q_ref[:, hs], dout[:, hs]
                score = dot_nt(key, query) * scale
                place = order_ref[0, (x * 2 + owner) * 2 + part] * sub
                seen = place + lax.broadcasted_iota(jnp.int32, (sub, rows), 0) <= prow_ref[...]
                share = jnp.where(seen, jnp.exp(score - lse_ref[pl.ds(h, 1), :]), 0.0)
                dshare = dot_nt(value, dhead)
                dscore = share * (dshare - delta[pl.ds(h, 1), :]) * scale
                high = dscore.astype(bf16)
                low = (dscore - high.astype(f32)).astype(bf16)
                dqs[:, hs] += dot_tn(high, key) + dot_tn(low, key)
                write(
                    x, slice(part * sub, (part + 1) * sub),
                    jnp.dot(high, query, preferred_element_type=f32)
                    + jnp.dot(low, query, preferred_element_type=f32),
                    jnp.dot(share.astype(bf16), dhead, preferred_element_type=f32),
                )

        def one_head(h):
            hs = pl.ds(pl.multiple_of(h * head_dim, head_dim), head_dim)
            slot = lax.rem(h, 2)

            def to_send(x, rs, dk, dv):
                send0[slot, x, rs, :lanes] = dk.astype(bf16)
                send0[slot, x, rs, lanes:] = dv.astype(bf16)

            def to_keep(x, rs, dk, dv):
                keep[slot, x, rs, :lanes] = dk.astype(bf16)
                keep[slot, x, rs, lanes:] = dv.astype(bf16)

            @pl.when(h >= 2)
            def _():
                c0(h).wait_send()

            def mates(e, carry):
                one_block(h, hs, lax.rem(mx + 1 + e, nx), 1 - core, to_send)
                return carry

            lax.fori_loop(0, nx, mates, 0)
            c0(h).start()
            tick(2 * h + 1)

            def owns(e, carry):
                one_block(h, hs, lax.rem(mx + 1 + e, nx), core, to_keep)
                return carry

            lax.fori_loop(0, nx, owns, 0)
            c0(h).wait_recv()

            def add(x, carry):
                recv0[h, x] = (keep[slot, x].astype(f32) + recv0[h, x].astype(f32)).astype(bf16)
                return carry

            lax.fori_loop(0, nx, add, 0)
            for d in range(1, nx):
                c1(h, d).start()
            tick(2 * h + 2)

        def heads_loop(h, carry):
            one_head(h)
            return carry

        lax.fori_loop(0, heads, heads_loop, 0)
        if jobs:

            def more(it, carry):
                grads.tick(it)
                return carry

            lax.fori_loop(2 * heads + 1, grads.steps, more, 0)

        dot_q = jnp.zeros((rows, 1), f32)
        for h in range(heads):
            hs = slice(h * head_dim, (h + 1) * head_dim)
            dq = dqs[:, hs]
            dq = dq * cos_ref[...] - pltpu.roll(dq, head_dim // 2, 1) * sin_ref[...]
            norm = qn_ref[:, hs]
            dqg_ref[:, hs] = jnp.sum(dq * norm, axis=0, keepdims=True)
            dq = dq * qg_ref[:, hs]
            dqs[:, hs] = dq
            dot_q = dot_q + jnp.sum(dq * norm, axis=1, keepdims=True)
        dprojt_ref[...] = jnp.transpose(dproj[...])
        dot_k = jnp.zeros((rows, 1), f32)
        for h in range(heads):
            hs = slice(h * head_dim, (h + 1) * head_dim)
            total = recv0[h, mx].astype(f32)
            for d in range(1, nx):
                c1(h, d).wait_recv()
                total = total + recv1[h, d - 1].astype(f32)
            dqkv_ref[:, 2 * local + h * head_dim : 2 * local + (h + 1) * head_dim] = total[
                :, lanes:
            ].astype(bf16)
            dk = total[:, :lanes]
            dk = dk * cos_ref[...] - pltpu.roll(dk, head_dim // 2, 1) * sin_ref[...]
            norm = kn_ref[:, hs]
            dkg_ref[:, hs] = jnp.sum(dk * norm, axis=0, keepdims=True)
            dk = dk * kg_ref[:, hs]
            dks[:, hs] = dk
            dot_k = dot_k + jnp.sum(dk * norm, axis=1, keepdims=True)
        dots = small.total(lane_pair(dot_q, dot_k, rows)) * (1.0 / width)
        for h in range(heads):
            hs = slice(h * head_dim, (h + 1) * head_dim)
            dqkv_ref[:, hs] = (
                sc_ref[:, 0:1] * (dqs[:, hs] - qn_ref[:, hs] * dots[:, 0:1])
            ).astype(bf16)
            dqkv_ref[:, local + h * head_dim : local + (h + 1) * head_dim] = (
                sc_ref[:, 1:2] * (dks[:, hs] - kn_ref[:, hs] * dots[:, 1:2])
            ).astype(bf16)
        for h in range(heads):
            if h >= heads - 2:
                c0(h).wait_send()
            for d in range(1, nx):
                c1(h, d).wait_send()
        if jobs:
            grads.drain()

    sem = pltpu.SemaphoreType.DMA
    pair = (rows, 2 * lanes)
    return comm_call(
        body,
        [back, grad, proj, attn_gain, w_output, query_rot, keys, values, attn, lse, pos_row,
         order, query_norm, key_norm, scales, qgain, kgain, cosine, sine] + ats + bs,
        [
            jax.ShapeDtypeStruct((rows, 3 * local), bf16),
            jax.ShapeDtypeStruct((width, rows), bf16),
            jax.ShapeDtypeStruct((1, width), f32),
            jax.ShapeDtypeStruct((1, local), f32),
            jax.ShapeDtypeStruct((1, local), f32),
        ] + [jax.ShapeDtypeStruct(*out) for out in (grads.out_shapes(widths) if jobs else [])],
        [
            pltpu.VMEM((rows, width), bf16), pltpu.VMEM((rows, local), bf16),
            pltpu.VMEM((rows, lanes), f32), pltpu.VMEM((8, rows), f32),
            pltpu.VMEM((rows, local), f32), pltpu.VMEM((rows, local), f32),
            pltpu.VMEM((2, nx) + pair, bf16), pltpu.VMEM((2, nx) + pair, bf16),
            pltpu.VMEM((heads, nx) + pair, bf16), pltpu.VMEM((heads, nx - 1) + pair, bf16),
            sem((2,)), sem((heads,)), sem((heads, nx - 1)), sem((heads, nx - 1)),
        ] + small.scratch() + (grads.scratch() if jobs else []),
        cid, "attention_back", {11},
    )


def front(tokens, w_query, w_key, w_value, qgain, kgain, cosine, sine, order, cid):
    rows, width = tokens.shape
    local = w_query.shape[1]
    head_dim = lanes
    heads = local // head_dim
    nx = lax.axis_size("ctx") // 2
    count = nx * 2 * rows
    n_tp = lax.axis_size("tp")
    small = LineSmall(n_tp, rows)
    n_small = len(small.scratch())
    scale = head_dim ** (-0.5)
    group = rows // 2

    def body(
        tok_hbm, wq_hbm, wk_hbm, wv_hbm, qg_ref, kg_ref, cos_ref, sin_ref, order_ref,
        qrot_out, key_out, value_out, qn_out, kn_out, attn_out, tokt_out, sc_out, lse_out,
        tok, tokt, w3, qn, kn, qrot, keys, values, peak, total, acc, attn, loads, stores,
        sx, dx, sm, dm, sf, df, *rest,
    ):
        small.bind(rest[:n_small])
        copies = [
            pltpu.make_async_copy(src, dst, loads.at[i])
            for i, (src, dst) in enumerate(
                [(tok_hbm, tok), (wv_hbm, w3.at[2]), (wq_hbm, w3.at[0]), (wk_hbm, w3.at[1])]
            )
        ]
        for copy in copies:
            copy.start()
        ctx = lax.axis_index("ctx")
        mx, core = ctx // 2, lax.rem(ctx, 2)
        mate = {"ctx": mx * 2 + 1 - core}

        def peer(d):
            return {"ctx": lax.rem(mx + d, nx) * 2 + core}

        bar = pltpu.get_barrier_semaphore()
        pl.semaphore_signal(bar, inc=1, device_id=mate, device_id_type=MESH)
        for d in range(1, nx):
            pl.semaphore_signal(bar, inc=1, device_id=peer(d), device_id_type=MESH)
        peers = small.greet(bar) + nx

        def at(x, owner):
            return pl.ds(pl.multiple_of((x * 2 + owner) * rows, rows), rows)

        mine = at(mx, core)
        side = local // 2
        boxes = [(keys, pl.ds(0, side)), (keys, pl.ds(side, side)), (values, pl.ds(0, local))]

        def move(t, rs, sent, done, where):
            box, cols = boxes[t]
            return remote(box.at[rs, cols], box.at[rs, cols], sent, done, where)

        def to_peer(t, d):
            return move(t, mine, sx.at[t, d - 1], dx.at[t, d - 1], peer(d))

        def from_peer(t, d):
            rs = at(lax.rem(mx + nx - d, nx), core)
            return move(t, rs, sx.at[t, d - 1], dx.at[t, d - 1], peer(d))

        def to_mate(t):
            return move(t, mine, sm.at[t], dm.at[t], mate)

        def from_mate(t):
            return move(t, at(mx, 1 - core), sm.at[t], dm.at[t], mate)

        def pass_on(t, d):
            rs = at(lax.rem(mx + nx - d, nx), core)
            return move(t, rs, sf.at[t, d - 1], df.at[t, d - 1], mate)

        def passed(t, d):
            rs = at(lax.rem(mx + nx - d, nx), 1 - core)
            return move(t, rs, sf.at[t, d - 1], df.at[t, d - 1], mate)

        def each_peer(act):
            def one(d, carry):
                act(d)
                return carry

            lax.fori_loop(1, nx, one, 0)

        copies[0].wait()
        copies[1].wait()
        values[mine] = jnp.dot(tok[...], w3[2], preferred_element_type=f32).astype(bf16)
        pl.semaphore_wait(bar, peers)
        each_peer(lambda d: to_peer(2, d).start())
        to_mate(2).start()
        copies[2].wait()
        qn[...] = jnp.dot(tok[...], w3[0], preferred_element_type=f32)
        copies[3].wait()
        kn[...] = jnp.dot(tok[...], w3[1], preferred_element_type=f32)

        def squares(ref):
            acc_sq = jnp.zeros((rows, 1), f32)
            for h in range(heads):
                part = ref[:, h * head_dim : (h + 1) * head_dim]
                acc_sq = acc_sq + jnp.sum(part * part, axis=1, keepdims=True)
            return acc_sq

        sums = small.total(lane_pair(squares(qn), squares(kn), rows))
        scales = lax.rsqrt(sums * (1.0 / width) + norm_eps)
        sc_out[...] = scales

        def rotated(ref, column, gain_ref, h):
            hs = slice(h * head_dim, (h + 1) * head_dim)
            norm = ref[:, hs] * sc_out[:, column : column + 1]
            ref[:, hs] = norm
            norm = norm * gain_ref[:, hs]
            return (
                norm * cos_ref[...] + pltpu.roll(norm, head_dim // 2, 1) * sin_ref[...]
            ).astype(bf16)

        for h in range(heads):
            keys[mine, h * head_dim : (h + 1) * head_dim] = rotated(kn, 1, kg_ref, h)
            if (h + 1) * head_dim in (side, local):
                t = (h + 1) * head_dim // side - 1
                each_peer(lambda d: to_peer(t, d).start())
                to_mate(t).start()
        for h in range(heads):
            qrot[:, h * head_dim : (h + 1) * head_dim] = rotated(qn, 0, qg_ref, h)
        peak[...] = jnp.full_like(peak, masked_score)
        total[...] = jnp.zeros_like(total)
        acc[...] = jnp.zeros_like(acc)

        def places(block, shape, axis):
            spot = lax.broadcasted_iota(jnp.int32, shape, axis)
            first, second = order_ref[0, block * 2], order_ref[0, block * 2 + 1]
            return jnp.where(spot < group, first * group + spot, (second - 1) * group + spot)

        def attend(x, owner, low, high):
            block = x * 2 + owner
            rs = at(x, owner)

            def one(h, carry):
                hs = pl.ds(pl.multiple_of(h * head_dim, head_dim), head_dim)
                score = dot_nt(qrot[:, hs], keys[rs, hs]) * scale
                seen = places(block, (1, rows), 1) <= places(ctx, (rows, 1), 0)
                old = peak[h]
                new = jnp.maximum(
                    old, jnp.max(jnp.where(seen, score, masked_score), axis=1, keepdims=True)
                )
                share = jnp.where(seen, jnp.exp(score - new), 0.0)
                fade = jnp.exp(old - new)
                peak[h] = new
                total[h] = total[h] * fade + jnp.sum(share, axis=1, keepdims=True)
                acc[:, hs] = acc[:, hs] * fade + jnp.dot(
                    share.astype(bf16), values[rs, hs], preferred_element_type=f32
                )
                return carry

            lax.fori_loop(low, high, one, 0)

        attend(mx, core, 0, heads)

        def hand_on(t, d):
            from_peer(t, d).wait_recv()
            pass_on(t, d).start()

        each_peer(lambda d: hand_on(2, d))
        for t in range(3):
            from_mate(t).wait_recv()
        attend(mx, 1 - core, 0, heads)
        tokt[...] = jnp.transpose(tok[...])

        def half_heads(t, carry):
            low, high = t * heads // 2, (t + 1) * heads // 2

            def near(d):
                for v in range(2):

                    @pl.when(t == v)
                    def _():
                        hand_on(v, d)

                attend(lax.rem(mx + nx - d, nx), core, low, high)

            def far(d):
                @pl.when(t == 0)
                def _():
                    passed(2, d).wait_recv()
                    passed(0, d).wait_recv()

                @pl.when(t == 1)
                def _():
                    passed(1, d).wait_recv()

                attend(lax.rem(mx + nx - d, nx), 1 - core, low, high)

            each_peer(near)
            each_peer(far)
            return carry

        lax.fori_loop(0, 2, half_heads, 0)

        lane = lax.broadcasted_iota(jnp.int32, (rows, lanes), 1)
        logs = jnp.zeros((rows, lanes), f32)
        for h in range(heads):
            hs = slice(h * head_dim, (h + 1) * head_dim)
            attn[:, hs] = (acc[:, hs] / total[h]).astype(bf16)
            logs = jnp.where(lane == h, peak[h] + jnp.log(total[h]), logs)
        lse_out[...] = jnp.transpose(logs)[:8]
        outs = [
            pltpu.make_async_copy(src, dst, stores.at[i])
            for i, (src, dst) in enumerate(
                [(qrot, qrot_out), (keys, key_out), (values, value_out), (qn, qn_out),
                 (kn, kn_out), (attn, attn_out), (tokt, tokt_out)]
            )
        ]
        for copy in outs:
            copy.start()
        for copy in outs:
            copy.wait()
        for t in range(3):
            to_mate(t).wait_send()

            def sent(d):
                to_peer(t, d).wait_send()
                pass_on(t, d).wait_send()

            each_peer(sent)

    sem = pltpu.SemaphoreType.DMA
    hbm = pl.BlockSpec(memory_space=pl.ANY)
    block = jax.ShapeDtypeStruct
    return pl.pallas_call(
        body,
        out_shape=[
            block((rows, local), bf16), block((count, local), bf16), block((count, local), bf16),
            block((rows, local), f32), block((rows, local), f32), block((rows, local), bf16),
            block((width, rows), bf16),
            block((rows, lanes), f32), block((8, rows), f32),
        ],
        in_specs=[hbm] * 4 + [vmem_spec()] * 4 + [pl.BlockSpec(memory_space=pltpu.SMEM)],
        out_specs=[hbm] * 7 + [vmem_spec()] * 2,
        scratch_shapes=[
            pltpu.VMEM((rows, width), bf16), pltpu.VMEM((width, rows), bf16),
            pltpu.VMEM((3, width, local), bf16),
            pltpu.VMEM((rows, local), f32),
            pltpu.VMEM((rows, local), f32), pltpu.VMEM((rows, local), bf16),
            pltpu.VMEM((count, local), bf16), pltpu.VMEM((count, local), bf16),
            pltpu.VMEM((heads, rows, 1), f32), pltpu.VMEM((heads, rows, 1), f32),
            pltpu.VMEM((rows, local), f32), pltpu.VMEM((rows, local), bf16),
            sem((4,)), sem((7,)),
            sem((3, nx - 1)), sem((3, nx - 1)), sem((3,)), sem((3,)),
            sem((3, nx - 1)), sem((3, nx - 1)),
        ] + small.scratch(),
        compiler_params=pltpu.CompilerParams(
            collective_id=cid, has_side_effects=True, vmem_limit_bytes=62 * 2**20
        ),
        name="front",
    )(tokens, w_query, w_key, w_value, qgain, kgain, cosine, sine, order)


def load_list(pairs, sems, base=0):
    copies = [
        pltpu.make_async_copy(src, dst, sems.at[base + i]) for i, (src, dst) in enumerate(pairs)
    ]
    for copy in copies:
        copy.start()
    return copies


def kernel_call(body, args, kinds, outs, out_kinds, scratch, cid, name):
    spec = {
        "v": vmem_spec(),
        "h": pl.BlockSpec(memory_space=pl.ANY),
        "s": pl.BlockSpec(memory_space=pltpu.SMEM),
    }
    return pl.pallas_call(
        body,
        out_shape=[jax.ShapeDtypeStruct(*out) for out in outs],
        in_specs=[spec[kind] for kind in kinds],
        out_specs=[spec[kind] for kind in out_kinds],
        scratch_shapes=scratch,
        compiler_params=pltpu.CompilerParams(
            collective_id=cid, has_side_effects=True, vmem_limit_bytes=62 * 2**20
        ),
        name=name,
    )(*args)


def middle(attn, tokens, attn_gain, w_output, w_gate, w_up, w_down, cid):
    rows, width = tokens.shape
    local, wide = w_output.shape[0], w_gate.shape[1]
    n_tp = lax.axis_size("tp")
    line = LineSum(n_tp, 2 * rows, width, 4 * row_chains)
    n_line = len(line.scratch())
    half = rows // 2
    tile = 64
    cut = 512
    n_cut = wide // cut
    part = line.part

    def body(
        attn_hbm, tok_hbm, again_ref, wo_hbm, wg_hbm, wu_hbm, wd_hbm,
        proj_out, hidt_out, gate_out, up_out, inner_out, down_out, inv_out,
        attn_v, tok, wo, hid, hidt, gate, up, inner, wg, wu, wd, first, loads, stores, *rest,
    ):
        line.bind(rest[:n_line])
        start = load_list([(attn_hbm, attn_v), (wo_hbm, wo), (tok_hbm, tok)], first)
        pairs = []
        for j in range(n_cut):
            cols = pl.ds(j * cut, cut)
            pairs += [(wg_hbm.at[:, cols], wg.at[j]), (wu_hbm.at[:, cols], wu.at[j])]
        for j in range(n_tp):
            cols = pl.ds(j * part, part)
            pairs += [(wd_hbm.at[:, cols], wd.at[j])]
        weights = load_list(pairs, loads)
        bar = pltpu.get_barrier_semaphore()
        peers = line.greet(bar)
        for copy in start:
            copy.wait()
        for j in range(n_tp):
            line.own[j, :rows] = jnp.dot(
                attn_v[...], wo[:, j * part : (j + 1) * part], preferred_element_type=f32
            ).astype(bf16)
        pl.semaphore_wait(bar, peers)

        def step(t, carry):
            line.step(t)

            @pl.when(t == 3 * n_tp + 1)
            def _():
                hidt[...] = jnp.transpose(hid[...])

            return carry

        def row_half(c, carry):
            base = pl.multiple_of(c * half, half)
            sl = pl.ds(base, half)
            lax.fori_loop(c * 2 * n_tp, c * n_tp + 2 * n_tp - 1, step, 0)

            def norm_rows(t, carry):
                rs = pl.ds(pl.multiple_of(base + t * tile, tile), tile)
                outs = [line.res[j, rs].astype(f32) for j in range(n_tp)]
                square = sum(jnp.sum(out * out, axis=1, keepdims=True) for out in outs)
                inv = lax.rsqrt(square * (1.0 / width) + norm_eps)
                inv_out[rs, :] = inv
                for j, out in enumerate(outs):
                    cols = slice(j * part, (j + 1) * part)
                    hid[rs, cols] = (
                        tok[rs, cols].astype(f32) + out * inv * again_ref[:, cols]
                    ).astype(bf16)
                return carry

            lax.fori_loop(0, half // tile, norm_rows, 0)
            for j in range(n_cut):
                cols = slice(j * cut, (j + 1) * cut)

                @pl.when(c == 0)
                def _():
                    weights[2 * j].wait()
                    weights[2 * j + 1].wait()

                g = jnp.dot(hid[sl], wg[j], preferred_element_type=f32)
                u = jnp.dot(hid[sl], wu[j], preferred_element_type=f32)
                gate[sl, cols] = g.astype(bf16)
                up[sl, cols] = u.astype(bf16)
                inner[sl, cols] = (g * jax.nn.sigmoid(g) * u).astype(bf16)
                low, high = j * row_chains // n_cut, (j + 1) * row_chains // n_cut
                line.pieces(((c + 2) * n_tp - 1) * row_chains + low, high - low)
            for j in range(n_tp):

                @pl.when(c == 0)
                def _():
                    weights[2 * n_cut + j].wait()

                line.own[j, pl.ds(rows + base, half)] = jnp.dot(
                    inner[sl], wd[j], preferred_element_type=f32
                ).astype(bf16)
            return carry

        lax.fori_loop(0, 2, row_half, 0)
        outs = load_list([(gate, gate_out), (up, up_out), (inner, inner_out)], stores)
        ready = line.ship(proj_out, stores, 4, 0, rows)
        lax.fori_loop(3 * n_tp, line.steps, step, 0)
        last = pltpu.make_async_copy(hidt, hidt_out, stores.at[3])
        last.start()
        ready = ready + line.ship(down_out, stores, 4 + n_tp, rows, rows)
        line.drain()
        for copy in outs + [last] + ready:
            copy.wait()

    sem = pltpu.SemaphoreType.DMA
    return kernel_call(
        body, [attn, tokens, attn_gain, w_output, w_gate, w_up, w_down], "hhvhhhh",
        [((rows, width), bf16), ((width, rows), bf16), ((rows, wide), bf16), ((rows, wide), bf16),
         ((rows, wide), bf16), ((rows, width), bf16), ((rows, 1), f32)],
        "hhhhhhv",
        [
            pltpu.VMEM((rows, local), bf16), pltpu.VMEM((rows, width), bf16),
            pltpu.VMEM((local, width), bf16),
            pltpu.VMEM((rows, width), bf16), pltpu.VMEM((width, rows), bf16),
            pltpu.VMEM((rows, wide), bf16), pltpu.VMEM((rows, wide), bf16),
            pltpu.VMEM((rows, wide), bf16),
            pltpu.VMEM((n_cut, width, cut), bf16), pltpu.VMEM((n_cut, width, cut), bf16),
            pltpu.VMEM((n_tp, wide, part), bf16),
            sem((3,)), sem((2 * n_cut + n_tp,)), sem((4 + 2 * n_tp,)),
        ] + line.scratch(),
        cid, "middle",
    )


def mlp_back(down, grad, mlp_gain, gate, up, inner, hid_t, w_gate, w_up, w_down, jobs, widths, cid):
    rows, width = down.shape
    wide = gate.shape[1]
    n_tp = lax.axis_size("tp")
    line = LineSum(n_tp, rows, width)
    grads = GradScatter(lax.axis_size("ctx"), lax.axis_size("seq"), width, jobs)
    n_line, n_grads, n_out = len(line.scratch()), len(grads.scratch()), len(widths)
    tile = 64
    cut = 512
    n_cut = wide // cut
    part = line.part
    lead = row_chains * n_tp // (n_cut + n_tp)
    ticks = n_cut // 2 + n_tp // 2

    def body(
        down_hbm, grad_hbm, mgain_ref, gate_hbm, up_hbm, inner_hbm, hidt_hbm, wg_hbm, wu_hbm, wd_hbm,
        back_out, dgate_out, dup_out, dgain_out, inv_out, *rest,
    ):
        grad_outs, rest = rest[:n_out], rest[n_out:]
        (gate_v, up_v, inner_v, hidt, ddown, ddownt, dgate, dup, ring, loads, wsem, stores) = rest[:12]
        line.bind(rest[12 : 12 + n_line])
        grads.bind(rest[12 + n_line :], [ddownt, hidt], [inner_v, dgate, dup], grad_outs)

        def fetch(src, index):
            return pltpu.make_async_copy(src, ring.at[index], wsem.at[index])

        def rows_of(ref, j, size):
            return ref.at[pl.ds(pl.multiple_of(j * size, size), size)]

        for j in range(4):
            fetch(rows_of(wd_hbm, j, cut), j).start()
        down_ref, grad_ref = dgate.at[:, pl.ds(0, width)], dup.at[:, pl.ds(0, width)]
        first = load_list([(down_hbm, down_ref), (grad_hbm, grad_ref)], loads, 4)
        early = load_list(
            [(inner_hbm, inner_v), (gate_hbm, gate_v), (up_hbm, up_v), (hidt_hbm, hidt)], loads
        )
        bar = pltpu.get_barrier_semaphore()
        peers = line.greet(bar) + grads.greet(bar)
        dgain_out[...] = jnp.zeros_like(dgain_out)
        for copy in first:
            copy.wait()

        def norm_rows(t, carry):
            sl = pl.ds(pl.multiple_of(t * tile, tile), tile)
            out = down_ref[sl].astype(f32)
            upstream = grad_ref[sl].astype(f32)
            inv = lax.rsqrt(jnp.mean(out * out, axis=1, keepdims=True) + norm_eps)
            norm = out * inv
            inv_out[sl, :] = inv
            dgain_out[...] += jnp.sum(upstream * norm, axis=0, keepdims=True)
            dnorm = upstream * mgain_ref[...]
            dot = jnp.mean(dnorm * norm, axis=1, keepdims=True)
            ddown[sl] = (inv * (dnorm - norm * dot)).astype(bf16)
            return carry

        lax.fori_loop(0, rows // tile, norm_rows, 0)
        ddownt[...] = jnp.transpose(ddown[...])
        for copy in early:
            copy.wait()
        pl.semaphore_wait(bar, peers)

        half = rows // 2

        def row_half(c, carry):
            sl = pl.ds(pl.multiple_of(c * half, half), half)

            def beside(i, j, first):
                @pl.when(c == 1)
                def _():
                    line.pieces(i * lead, lead)

                @pl.when(lax.rem(j, 2) == 1)
                def _():
                    grads.tick(first + j // 2)

            def inner_back(j, carry):
                fetch(rows_of(wd_hbm, j, cut), j).wait()
                cols = pl.ds(pl.multiple_of(j * cut, cut), cut)
                dmix = dot_nt(ddown[sl], ring[j])
                g, u = gate_v[sl, cols].astype(f32), up_v[sl, cols].astype(f32)
                sig = jax.nn.sigmoid(g)
                dgate[sl, cols] = (dmix * u * sig * (1.0 + g * (1.0 - sig))).astype(bf16)
                dup[sl, cols] = (dmix * (g * sig)).astype(bf16)

                @pl.when(lax.rem(j, 2) == 0)
                def _():
                    fetch(rows_of(wg_hbm, j // 2, part), j).start()

                @pl.when(lax.rem(j, 2) == 1)
                def _():
                    fetch(rows_of(wu_hbm, j // 2, part), j).start()

                beside(j, j, c * ticks)
                return carry

            lax.fori_loop(0, n_cut, inner_back, 0)

            def hidden_back(j, carry):
                slot = lax.rem(2 * j, 4)
                fetch(rows_of(wg_hbm, j, part), slot).wait()
                fetch(rows_of(wu_hbm, j, part), slot + 1).wait()
                line.own[j, sl] = (
                    dot_nt(dgate[sl], ring[slot]) + dot_nt(dup[sl], ring[slot + 1])
                ).astype(bf16)

                @pl.when(j + 2 < n_tp)
                def _():
                    fetch(rows_of(wg_hbm, j + 2, part), slot).start()
                    fetch(rows_of(wu_hbm, j + 2, part), slot + 1).start()

                @pl.when((j + 2 >= n_tp) & (c == 0))
                def _():
                    fetch(rows_of(wd_hbm, slot, cut), slot).start()
                    fetch(rows_of(wd_hbm, slot + 1, cut), slot + 1).start()

                beside(n_cut + j, j, c * ticks + n_cut // 2)
                return carry

            lax.fori_loop(0, n_tp, hidden_back, 0)
            return carry

        lax.fori_loop(0, 2, row_half, 0)
        outs = load_list([(dgate, dgate_out), (dup, dup_out)], stores)
        done, used = 2 * ticks, (n_cut + n_tp) * lead

        def one(it, carry):
            line.pieces(used + (it - done) * pace, pace)
            grads.tick(it)
            return carry

        line_its = -(-(line.steps * row_chains - used) // pace)
        lax.fori_loop(done, max(done + line_its, grads.steps), one, 0)
        outs += line.ship(back_out, stores, 2, 0, rows)
        line.drain()
        grads.drain()
        for copy in outs:
            copy.wait()

    sem = pltpu.SemaphoreType.DMA
    return kernel_call(
        body, [down, grad, mlp_gain, gate, up, inner, hid_t, w_gate, w_up, w_down], "hhvhhhhhhh",
        [((rows, width), bf16), ((rows, wide), bf16), ((rows, wide), bf16), ((1, width), f32),
         ((rows, 1), f32)]
        + grads.out_shapes(widths),
        "hhhvv" + "v" * n_out,
        [
            pltpu.VMEM((rows, wide), bf16), pltpu.VMEM((rows, wide), bf16),
            pltpu.VMEM((rows, wide), bf16), pltpu.VMEM((width, rows), bf16),
            pltpu.VMEM((rows, width), bf16), pltpu.VMEM((width, rows), bf16),
            pltpu.VMEM((rows, wide), bf16), pltpu.VMEM((rows, wide), bf16),
            pltpu.VMEM((4, cut, width), bf16),
            sem((6,)), sem((4,)), sem((2 + n_tp,)),
        ] + line.scratch() + grads.scratch(),
        cid, "mlp_back",
    )


def last_sums(dqkv, w_query, w_key, w_value, ats, bs, jobs, widths, gains, cid):
    rows = dqkv.shape[0]
    width, local = w_query.shape
    n_ctx, n_seq = lax.axis_size("ctx"), lax.axis_size("seq")
    n_tp = lax.axis_size("tp")
    line = LineSum(n_tp, rows, width)
    grads = GradScatter(n_ctx, n_seq, width, jobs)
    small = GainSum(n_ctx, n_seq, gains.shape[0])
    na, nb, n_out = len(ats), len(bs), len(widths)
    n_line, n_grads = len(line.scratch()), len(grads.scratch())
    part = line.part

    def body(dqkv_ref, wq_ref, wk_ref, wv_ref, *refs):
        at_refs, b_refs = refs[:na], refs[na : na + nb]
        gain_ref, last_out = refs[na + nb], refs[na + nb + 1]
        refs = refs[na + nb + 2 :]
        grad_outs, gain_out, stores, scratch = refs[:n_out], refs[n_out], refs[n_out + 1], refs[n_out + 2 :]
        line.bind(scratch[:n_line])
        grads.bind(scratch[n_line : n_line + n_grads], at_refs, list(b_refs) + [dqkv_ref], grad_outs)
        small.bind(scratch[n_line + n_grads :], gain_ref, gain_out)
        bar = pltpu.get_barrier_semaphore()
        peers = line.greet(bar) + small.greet(bar)
        pl.semaphore_wait(bar, peers)
        small.start()

        def input_back(j, carry):
            rs = pl.ds(pl.multiple_of(j * part, part), part)
            line.own[j] = (
                dot_nt(dqkv_ref[:, :local], wq_ref[rs])
                + dot_nt(dqkv_ref[:, local : 2 * local], wk_ref[rs])
                + dot_nt(dqkv_ref[:, 2 * local :], wv_ref[rs])
            ).astype(bf16)

            @pl.when(lax.rem(j, 2) == 0)
            def _():
                grads.tick(j // 2)

            return carry

        lax.fori_loop(0, n_tp, input_back, 0)
        done = n_tp // 2

        def one(it, carry):
            grads.tick(it)
            line.pieces((it - done) * pace, pace)
            return carry

        line_steps = -(-line.steps * row_chains // pace)
        lax.fori_loop(done, max(done + line_steps, grads.steps), one, 0)
        small.finish()
        outs = line.ship(last_out, stores, 0, 0, rows)
        line.drain()
        grads.drain()
        for copy in outs:
            copy.wait()

    sem = pltpu.SemaphoreType.DMA
    return kernel_call(
        body, [dqkv, w_query, w_key, w_value] + list(ats) + list(bs) + [gains],
        "vvvv" + "v" * (na + nb + 1),
        [((rows, width), bf16)] + grads.out_shapes(widths) + [(gains.shape, f32)],
        "h" + "v" * (n_out + 1),
        [sem((n_tp,))] + line.scratch() + grads.scratch() + small.scratch(),
        cid, "last_sums",
    )


def row_tiles(body, args, out_shape, name):
    rows, width = out_shape
    tile = rows // 4

    def spec(arg):
        if arg.shape[0] == 1:
            return pl.BlockSpec((1, arg.shape[1]), lambda i: (0, 0))
        return pl.BlockSpec((tile, arg.shape[1]), lambda i: (i, 0))

    def whole(*refs):
        refs[-1][...] = body(*[ref[...].astype(f32) for ref in refs[:-1]])

    return pl.pallas_call(
        whole,
        grid=(4,),
        out_shape=jax.ShapeDtypeStruct(out_shape, f32),
        in_specs=[spec(arg) for arg in args],
        out_specs=pl.BlockSpec((tile, width), lambda i: (i, 0)),
        compiler_params=pltpu.CompilerParams(vmem_limit_bytes=32 * 2**20),
        name=name,
    )(*args)


def per_device(
    tokens,
    out_grad,
    group_order,
    w_query,
    w_key,
    w_value,
    query_gain,
    key_gain,
    w_output,
    attn_gain,
    w_gate,
    w_up,
    w_down,
    mlp_gain,
):
    inputs = tokens[0]
    upstream = out_grad[0]
    rows, width = inputs.shape
    heads, head_dim = query_gain.shape
    local = heads * head_dim
    wide = w_gate.shape[1]
    positions = key_positions(group_order[0], lax.axis_index("ctx") * rows, rows, rows // 2)
    angle_cos, angle_sin = rope_tables(positions, head_dim)
    qgain = query_gain.reshape(1, local)
    kgain = key_gain.reshape(1, local)
    (query_rot, keys, values, query_norm, key_norm, attn, tokens_t, scales, lse) = front(
        inputs, w_query, w_key, w_value, qgain, kgain, angle_cos, angle_sin, group_order, 1
    )
    proj, hidden_t, gate, up, inner, down, proj_scale = middle(
        attn, inputs, attn_gain[None], w_output, w_gate, w_up, w_down, 2
    )
    chunk_cols = 2 * lanes
    chunks = wide // chunk_cols
    thin = local // chunk_cols
    back, d_gate, d_up, d_mlp_gain, down_scale, grad_down, grad_gate = mlp_back(
        down, upstream, mlp_gain[None], gate, up, inner, hidden_t, w_gate, w_up, w_down,
        [
            dict(a=0, b=0, first=0, count=chunks, out=0, place=0, flip=True),
            dict(a=1, b=1, first=0, count=chunks, out=1, place=0, flip=False),
        ],
        [wide, wide],
        3,
    )
    d_qkv, d_proj_t, d_attn_gain, d_query_gain, d_key_gain = attention_back(
        back, upstream, proj, attn_gain[None], w_output, query_rot, keys, values, attn, lse,
        positions[None], group_order, query_norm, key_norm, scales, qgain, kgain, angle_cos,
        angle_sin, [], [], [], [], 4,
    )
    owners = lax.axis_size("ctx") * lax.axis_size("seq")
    gains = [d_attn_gain, d_mlp_gain, d_query_gain, d_key_gain]
    ends = [gain.shape[1] for gain in gains]
    ends = [sum(ends[: i + 1]) for i in range(4)]
    packed = jnp.concatenate(gains, axis=1).reshape(-1, lanes)
    last, grad_up, grad_qkv, grad_output, small = last_sums(
        d_qkv, w_query, w_key, w_value,
        [hidden_t, tokens_t, d_proj_t],
        [d_up, attn],
        [
            dict(a=0, b=0, first=0, count=chunks, out=0, place=0, flip=False),
            dict(a=2, b=1, first=0, count=thin, out=2, place=0, flip=True),
            dict(a=1, b=2, first=0, count=3 * thin, out=1, place=0, flip=False),
        ],
        [wide, 3 * local, local],
        packed,
        5,
    )
    small = small.reshape(-1)
    me = lax.axis_index("ctx") * lax.axis_size("seq") + lax.axis_index("seq")

    def my_part(start, end, lead):
        whole = small[start:end].reshape(lead, -1)
        size = whole.shape[1] // owners
        return lax.dynamic_slice_in_dim(whole, me * size, size, 1)

    g_attn = my_part(0, ends[0], 1)[0]
    g_mlp = my_part(ends[0], ends[1], 1)[0]
    g_query = my_part(ends[1], ends[2], heads)
    g_key = my_part(ends[2], ends[3], heads)
    grad_query, grad_key, grad_value = jnp.split(grad_qkv, 3, axis=1)
    block_out = row_tiles(
        lambda x, a, ra, ga, d, rd, gd: x + (a * ra) * ga + (d * rd) * gd,
        [inputs, proj, proj_scale, attn_gain[None], down, down_scale, mlp_gain[None]],
        inputs.shape, "block_out",
    )
    input_grad = row_tiles(
        lambda g, a, b: g + a + b, [upstream, back, last], inputs.shape, "input_grad"
    )
    return (
        block_out[None],
        input_grad[None],
        grad_query,
        grad_key,
        grad_value,
        g_query,
        g_key,
        grad_output,
        g_attn,
        grad_gate,
        grad_up,
        grad_down,
        g_mlp,
    )


def solution(mesh):
    return jax.shard_map(
        per_device,
        mesh=mesh,
        in_specs=(
            P("seq", "ctx", None),
            P("seq", "ctx", None),
            P("seq", None),
            P(None, "tp"),
            P(None, "tp"),
            P(None, "tp"),
            P("tp", None),
            P("tp", None),
            P("tp", None),
            P(),
            P(None, "tp"),
            P(None, "tp"),
            P("tp", None),
            P(),
        ),
        out_specs=(
            P("seq", "ctx", None),
            P("seq", "ctx", None),
            P(("ctx", "seq"), "tp"),
            P(("ctx", "seq"), "tp"),
            P(("ctx", "seq"), "tp"),
            P("tp", ("ctx", "seq")),
            P("tp", ("ctx", "seq")),
            P("tp", ("ctx", "seq")),
            P(("ctx", "seq")),
            P(("ctx", "seq"), "tp"),
            P(("ctx", "seq"), "tp"),
            P("tp", ("ctx", "seq")),
            P(("ctx", "seq")),
        ),
        check_vma=False,
    )
```

```python
import jax
import jax.numpy as jnp
from jax import lax
from jax.sharding import PartitionSpec as P
from jax.experimental import pallas as pl
from jax.experimental.pallas import tpu as pltpu

norm_eps = 1e-06
rope_base = 500000.0
masked_score = -1e30


def rope_tables(positions, head_dim):
    half = head_dim // 2
    channel = jnp.arange(head_dim, dtype=jnp.int32)
    rates = rope_base ** (-((channel % half).astype(jnp.float32) * 2.0 / head_dim))
    angle = positions.astype(jnp.float32)[:, None] * rates[None, :]
    return jnp.cos(angle), jnp.where(channel[None, :] < half, -jnp.sin(angle), jnp.sin(angle))


def key_positions(order, first_row, count, group):
    row_ids = first_row + jnp.arange(count, dtype=jnp.int32)
    slots = row_ids // group
    picks = slots[:, None] == jnp.arange(order.shape[0], dtype=jnp.int32)[None, :]
    return jnp.sum(jnp.where(picks, order[None, :], 0), axis=1) * group + row_ids % group


MESH = pl.DeviceIdType.MESH
bf16 = jnp.bfloat16
f32 = jnp.float32
lanes = 128
row_blocks = 16
row_chains = 8
pace = 6


def remote(src, dst, send, recv, where):
    return pltpu.make_async_remote_copy(
        src, dst, send, recv, device_id=where, device_id_type=MESH
    )


class LineSum:
    def __init__(self, n, rows, width, blocks=row_blocks):
        self.n, self.rows, self.width = n, rows, width
        self.part = width // n
        self.rc = rows // blocks
        self.total = blocks // row_chains * n
        self.steps = self.total + n - 1

    def scratch(self):
        shape = (self.n, self.rows, self.part)
        return (
            [pltpu.VMEM(shape, bf16)] * 4
            + [pltpu.SemaphoreType.DMA] * 2
            + [pltpu.SemaphoreType.DMA((row_chains, self.total))] * 2
        )

    def bind(self, refs):
        self.own, self.from_l, self.from_r, self.res = refs[:4]
        self.send_r, self.send_l, self.recv_l, self.recv_r = refs[4:]
        self.i = lax.axis_index("tp")
        self.has_l, self.has_r = self.i > 0, self.i < self.n - 1

    def greet(self, bar):
        @pl.when(self.has_l)
        def _():
            pl.semaphore_signal(bar, inc=1, device_id={"tp": self.i - 1}, device_id_type=MESH)

        @pl.when(self.has_r)
        def _():
            pl.semaphore_signal(bar, inc=1, device_id={"tp": self.i + 1}, device_id_type=MESH)

        return self.has_l.astype(jnp.int32) + self.has_r.astype(jnp.int32)

    def load(self, x_ref):
        for j in range(self.n):
            self.own[j] = x_ref[:, j * self.part : (j + 1) * self.part]

    def rows_of(self, g, p):
        block = (p // self.n) * row_chains + g
        return pl.ds(pl.multiple_of(block * self.rc, self.rc), self.rc)

    def right(self, src, dst, g, p, j):
        sl = self.rows_of(g, p)
        return remote(
            src.at[j, sl], dst.at[j, sl], self.send_r, self.recv_l.at[g, p],
            {"tp": self.i + 1},
        )

    def left(self, src, dst, g, q, j):
        sl = self.rows_of(g, q)
        return remote(
            src.at[j, sl], dst.at[j, sl], self.send_l, self.recv_r.at[g, q],
            {"tp": self.i - 1},
        )

    def wait_l(self, g, p, j):
        sl = self.rows_of(g, p)
        remote(
            self.own.at[j, sl], self.from_l.at[j, sl], self.send_r, self.recv_l.at[g, p],
            {"tp": self.i - 1},
        ).wait_recv()

    def wait_r(self, g, q, j):
        sl = self.rows_of(g, q)
        remote(
            self.own.at[j, sl], self.from_r.at[j, sl], self.send_l, self.recv_r.at[g, q],
            {"tp": self.i + 1},
        ).wait_recv()

    def step(self, t):
        self.pieces(t * row_chains, row_chains)

    def pieces(self, first, count):
        def one(v, carry):
            self.piece(first + v)
            return carry

        lax.fori_loop(0, count, one, 0)

    def piece(self, e):
        t = e // row_chains

        @pl.when(t < self.steps)
        def _():
            self.sub_step(t, lax.rem(e, row_chains))

    def sub_step(self, t, g):
        n, i, has_l, has_r = self.n, self.i, self.has_l, self.has_r
        own, from_l, from_r, res = self.own, self.from_l, self.from_r, self.res
        p = t - i
        q = t - (n - 1 - i)
        jr = n - 1 - lax.rem(p + n * self.total, n)
        jl = lax.rem(q + n * self.total, n)
        pv = (p >= 0) & (p < self.total)
        qv = (q >= 0) & (q < self.total)

        @pl.when(pv & has_l)
        def _():
            self.wait_l(g, p, jr)

        @pl.when(qv & has_r)
        def _():
            self.wait_r(g, q, jl)

        @pl.when(pv & (jr > i))
        def _():
            sl = self.rows_of(g, p)

            @pl.when(has_l)
            def _():
                own[jr, sl] = (own[jr, sl].astype(f32) + from_l[jr, sl].astype(f32)).astype(bf16)

            self.right(own, from_l, g, p, jr).start()

        @pl.when(qv & (jl < i))
        def _():
            sl = self.rows_of(g, q)

            @pl.when(has_r)
            def _():
                own[jl, sl] = (own[jl, sl].astype(f32) + from_r[jl, sl].astype(f32)).astype(bf16)

            self.left(own, from_r, g, q, jl).start()

        @pl.when(pv & (jr == i))
        def _():
            sl = self.rows_of(g, p)

            @pl.when(has_l & has_r)
            def _():
                res[i, sl] = (
                    own[i, sl].astype(f32) + from_l[i, sl].astype(f32) + from_r[i, sl].astype(f32)
                ).astype(bf16)

            @pl.when(jnp.logical_not(has_l))
            def _():
                res[i, sl] = (own[i, sl].astype(f32) + from_r[i, sl].astype(f32)).astype(bf16)

            @pl.when(jnp.logical_not(has_r))
            def _():
                res[i, sl] = (own[i, sl].astype(f32) + from_l[i, sl].astype(f32)).astype(bf16)

        @pl.when(pv & (jr <= i) & has_r)
        def _():
            self.right(res, res, g, p, jr).start()

        @pl.when(qv & (jl >= i) & has_l)
        def _():
            self.left(res, res, g, q, jl).start()

    def drain(self):
        @pl.when(self.has_r)
        def _():
            remote(
                self.own, self.from_l, self.send_r, self.recv_l.at[0, 0], {"tp": self.i + 1}
            ).wait_send()

        @pl.when(self.has_l)
        def _():
            remote(
                self.own, self.from_r, self.send_l, self.recv_r.at[0, 0], {"tp": self.i - 1}
            ).wait_send()

    def ship(self, out_ref, sems, base, start, count):
        return load_list(
            [
                (
                    self.res.at[j, pl.ds(start, count)],
                    out_ref.at[:, pl.ds(j * self.part, self.part)],
                )
                for j in range(self.n)
            ],
            sems, base,
        )


class GradScatter:
    def __init__(self, n_ctx, n_seq, width, jobs, orders=("xy", "yx")):
        self.nx, self.ny = n_ctx // 2, n_seq
        self.rows = width // (n_ctx * n_seq)
        self.jobs, self.orders = jobs, orders
        start = 0
        self.spans = []
        for job in jobs:
            self.spans.append((start, start + job["count"]))
            start += job["count"]
        self.total = start
        self.steps = start + 5

    def out_shapes(self, widths):
        flips = {job["out"] for job in self.jobs if job["flip"]}
        return [
            ((w, self.rows) if i in flips else (self.rows, w), f32) for i, w in enumerate(widths)
        ]

    def sizes(self, order):
        return (self.nx, self.ny) if order == "xy" else (self.ny, self.nx)

    def scratch(self):
        nx, ny, t = self.nx, self.ny, self.total
        tile = (self.rows, lanes)
        sem = pltpu.SemaphoreType.DMA
        out = [
            pltpu.VMEM((2, nx, ny, 2) + tile, bf16),
            pltpu.VMEM((2, nx, ny, 2) + tile, f32),
            pltpu.VMEM((t, nx, ny, 2) + tile, bf16),
            sem((2,)), sem((t,)),
        ]
        for order in self.orders:
            n1, n2 = self.sizes(order)
            out += [
                pltpu.VMEM((3, n1, n2) + tile, bf16),
                pltpu.VMEM((t, n1 - 1, n2) + tile, bf16),
                pltpu.VMEM((3, n2) + tile, bf16),
                pltpu.VMEM((t, n2 - 1) + tile, bf16),
                sem((3, n1 - 1)), sem((t, n1 - 1)), sem((3, n2 - 1)), sem((t, n2 - 1)),
            ]
        return out

    def bind(self, refs, at_refs, b_refs, out_refs):
        self.send0, self.keep, self.recv0, self.s0, self.d0 = refs[:5]
        self.half = [refs[5 + 8 * h : 13 + 8 * h] for h in range(2)]
        self.at_refs, self.b_refs, self.out_refs = at_refs, b_refs, out_refs
        ctx = lax.axis_index("ctx")
        self.mx, self.core, self.my = ctx // 2, lax.rem(ctx, 2), lax.axis_index("seq")

    def axis(self, name, d):
        if name == "x":
            to = lax.rem(self.mx + d, self.nx)
            return to, {"ctx": to * 2 + self.core}
        to = lax.rem(self.my + d, self.ny)
        return to, {"seq": to}

    def at_mate(self):
        return {"ctx": self.mx * 2 + 1 - self.core}

    def greet(self, bar):
        places = [self.at_mate()]
        places += [self.axis("x", d)[1] for d in range(1, self.nx)]
        places += [self.axis("y", d)[1] for d in range(1, self.ny)]
        for place in places:
            pl.semaphore_signal(bar, inc=1, device_id=place, device_id_type=MESH)
        return len(places)

    def c0(self, c):
        slot = lax.rem(c, 2)
        return remote(
            self.send0.at[slot], self.recv0.at[c], self.s0.at[slot], self.d0.at[c], self.at_mate()
        )

    def c1(self, h, c, d):
        p, r1, _, _, sent, done, _, _ = self.half[h]
        to, where = self.axis(self.orders[h][0], d)
        slot = lax.rem(c, 3)
        return remote(p.at[slot, to], r1.at[c, d - 1], sent.at[slot, d - 1], done.at[c, d - 1], where)

    def c2(self, h, c, d):
        _, _, q, r2, _, _, sent, done = self.half[h]
        to, where = self.axis(self.orders[h][1], d)
        slot = lax.rem(c, 3)
        return remote(q.at[slot, to], r2.at[c, d - 1], sent.at[slot, d - 1], done.at[c, d - 1], where)

    def make(self, c):
        slot = lax.rem(c, 2)
        nx, ny, r = self.nx, self.ny, self.rows

        @pl.when(c >= 2)
        def _():
            self.c0(c).wait_send()

        def products(at_ref, b_ref, col, parity, write):
            def tile(e, carry):
                x, y = e // ny, lax.rem(e, ny)
                row = pl.multiple_of(((x * 2 + parity) * ny + y) * r, r)
                acc = jnp.dot(
                    at_ref[pl.ds(row, r), :], b_ref[:, pl.ds(col, 2 * lanes)],
                    preferred_element_type=f32,
                )
                write(x, y, acc)
                return carry

            lax.fori_loop(0, nx * ny, tile, 0)

        def to_send(x, y, acc):
            self.send0[slot, x, y, 0] = acc[:, :lanes].astype(bf16)
            self.send0[slot, x, y, 1] = acc[:, lanes:].astype(bf16)

        def to_keep(x, y, acc):
            self.keep[slot, x, y, 0] = acc[:, :lanes]
            self.keep[slot, x, y, 1] = acc[:, lanes:]

        for job, (lo, hi) in zip(self.jobs, self.spans):

            @pl.when((c >= lo) & (c < hi))
            def _():
                at_ref, b_ref = self.at_refs[job["a"]], self.b_refs[job["b"]]
                col = pl.multiple_of((c - lo + job["first"]) * (2 * lanes), 2 * lanes)
                products(at_ref, b_ref, col, 1 - self.core, to_send)
                self.c0(c).start()
                products(at_ref, b_ref, col, self.core, to_keep)

    def pair(self, c):
        slot, two = lax.rem(c, 3), lax.rem(c, 2)

        @pl.when(c >= 3)
        def _():
            for h in range(2):
                for d in range(1, self.sizes(self.orders[h])[0]):
                    self.c1(h, c, d).wait_send()

        self.c0(c).wait_recv()
        for h, order in enumerate(self.orders):
            p = self.half[h][0]
            for x in range(self.nx):
                for y in range(self.ny):
                    spot = (x, y) if order == "xy" else (y, x)
                    p[(slot,) + spot] = (
                        self.keep[two, x, y, h] + self.recv0[c, x, y, h].astype(f32)
                    ).astype(bf16)
            for d in range(1, self.sizes(order)[0]):
                self.c1(h, c, d).start()

    def own(self, name):
        return self.mx if name == "x" else self.my

    def cross(self, c):
        slot = lax.rem(c, 3)

        @pl.when(c >= 3)
        def _():
            for h in range(2):
                for d in range(1, self.sizes(self.orders[h])[1]):
                    self.c2(h, c, d).wait_send()

        for h, order in enumerate(self.orders):
            n1, n2 = self.sizes(order)
            p, r1, q = self.half[h][:3]
            for d in range(1, n1):
                self.c1(h, c, d).wait_recv()
            for e in range(n2):
                acc = p[slot, self.own(order[0]), e].astype(f32)
                for d in range(1, n1):
                    acc = acc + r1[c, d - 1, e].astype(f32)
                q[slot, e] = acc.astype(bf16)
            for d in range(1, n2):
                self.c2(h, c, d).start()

    def finish(self, c):
        slot = lax.rem(c, 3)
        totals = []
        for h, order in enumerate(self.orders):
            n2 = self.sizes(order)[1]
            q, r2 = self.half[h][2:4]
            for d in range(1, n2):
                self.c2(h, c, d).wait_recv()
            acc = q[slot, self.own(order[1])].astype(f32)
            for d in range(1, n2):
                acc = acc + r2[c, d - 1].astype(f32)
            totals.append(acc)
        for job, (lo, hi) in zip(self.jobs, self.spans):

            @pl.when((c >= lo) & (c < hi))
            def _():
                out_ref = self.out_refs[job["out"]]
                col = pl.multiple_of((c - lo + job["place"]) * (2 * lanes), 2 * lanes)
                for h in range(2):
                    place = pl.ds(col + h * lanes, lanes)
                    if job["flip"]:
                        out_ref[place, :] = jnp.transpose(totals[h])
                    else:
                        out_ref[:, place] = totals[h]

    def tick(self, it):
        @pl.when((it >= 5) & (it < self.total + 5))
        def _():
            self.finish(it - 5)

        @pl.when((it >= 3) & (it < self.total + 3))
        def _():
            self.cross(it - 3)

        @pl.when((it >= 1) & (it < self.total + 1))
        def _():
            self.pair(it - 1)

        @pl.when(it < self.total)
        def _():
            self.make(it)

    def drain(self):
        for c in range(max(self.total - 2, 0), self.total):
            self.c0(c).wait_send()
        for c in range(max(self.total - 3, 0), self.total):
            for h, order in enumerate(self.orders):
                n1, n2 = self.sizes(order)
                for d in range(1, n1):
                    self.c1(h, c, d).wait_send()
                for d in range(1, n2):
                    self.c2(h, c, d).wait_send()


class GainSum:
    def __init__(self, n_ctx, n_seq, rows):
        self.ny, self.n, self.rows = n_seq, n_ctx * n_seq, rows

    def scratch(self):
        sem = pltpu.SemaphoreType.DMA
        return [pltpu.VMEM((self.n - 1, self.rows, lanes), f32), sem((self.n - 1,)), sem((self.n - 1,))]

    def bind(self, refs, in_ref, out_ref):
        self.got, self.sent, self.done = refs
        self.in_ref, self.out_ref = in_ref, out_ref
        self.me = lax.axis_index("ctx") * self.ny + lax.axis_index("seq")

    def place(self, d):
        to = lax.rem(self.me + d, self.n)
        return {"ctx": to // self.ny, "seq": lax.rem(to, self.ny)}

    def copy(self, d):
        return remote(
            self.in_ref, self.got.at[d - 1], self.sent.at[d - 1], self.done.at[d - 1], self.place(d)
        )

    def greet(self, bar):
        for d in range(1, self.n):
            pl.semaphore_signal(bar, inc=1, device_id=self.place(d), device_id_type=MESH)
        return self.n - 1

    def start(self):
        for d in range(1, self.n):
            self.copy(d).start()

    def finish(self):
        acc = self.in_ref[...]
        for d in range(1, self.n):
            self.copy(d).wait_recv()
            acc = acc + self.got[d - 1]
        self.out_ref[...] = acc
        for d in range(1, self.n):
            self.copy(d).wait_send()


def vmem_spec():
    return pl.BlockSpec(memory_space=pltpu.VMEM)


def comm_call(body, args, outs, scratch, cid, name, scalars=()):
    return pl.pallas_call(
        body,
        out_shape=outs,
        in_specs=[
            pl.BlockSpec(memory_space=pltpu.SMEM) if i in scalars else vmem_spec()
            for i in range(len(args))
        ],
        out_specs=[vmem_spec()] * len(outs),
        scratch_shapes=scratch,
        compiler_params=pltpu.CompilerParams(
            collective_id=cid, has_side_effects=True, vmem_limit_bytes=62 * 2**20
        ),
        name=name,
    )(*args)


class LineSmall:
    def __init__(self, n, rows):
        self.n, self.rows = n, rows

    def scratch(self):
        sem = pltpu.SemaphoreType.DMA
        return [
            pltpu.VMEM((8, self.rows), f32), pltpu.VMEM((self.n - 1, 8, self.rows), f32),
            sem((self.n - 1,)), sem((self.n - 1,)),
        ]

    def bind(self, refs):
        self.mine, self.got, self.sent, self.done = refs
        self.i = lax.axis_index("tp")

    def greet(self, bar):
        for d in range(1, self.n):
            pl.semaphore_signal(
                bar, inc=1, device_id={"tp": lax.rem(self.i + d, self.n)}, device_id_type=MESH
            )
        return self.n - 1

    def copy(self, d):
        return remote(
            self.mine, self.got.at[d - 1], self.sent.at[d - 1], self.done.at[d - 1],
            {"tp": lax.rem(self.i + d, self.n)},
        )

    def total(self, columns):
        self.mine[...] = jnp.transpose(columns)[:8]
        for d in range(1, self.n):
            self.copy(d).start()
        acc = self.mine[...]
        for d in range(1, self.n):
            self.copy(d).wait_recv()
            acc = acc + self.got[d - 1]
        for d in range(1, self.n):
            self.copy(d).wait_send()
        return jnp.transpose(jnp.concatenate([acc, jnp.zeros((lanes - 8, self.rows), f32)], axis=0))


def lane_pair(first, second, rows):
    lane = lax.broadcasted_iota(jnp.int32, (rows, lanes), 1)
    return jnp.where(lane == 0, first, 0.0) + jnp.where(lane == 1, second, 0.0)


def dot_nt(left, right):
    return lax.dot_general(left, right, (((1,), (1,)), ((), ())), preferred_element_type=f32)


def dot_tn(left, right):
    return lax.dot_general(left, right, (((0,), (0,)), ((), ())), preferred_element_type=f32)


def attention_back(
    back, grad, proj, attn_gain, w_output, query_rot, keys, values, attn, lse, pos_row, order,
    query_norm, key_norm, scales, qgain, kgain, cosine, sine, ats, bs, jobs, widths, cid,
):
    rows, width = back.shape
    local = w_output.shape[0]
    head_dim = lanes
    heads = local // head_dim
    count = keys.shape[0]
    nx, n_tp = lax.axis_size("ctx") // 2, lax.axis_size("tp")
    small = LineSmall(n_tp, rows)
    n_small = len(small.scratch())
    scale = head_dim ** (-0.5)
    tile = 64
    sub = rows // 2
    na, nb, n_out = len(ats), len(bs), len(widths)
    grads = None
    if jobs:
        grads = GradScatter(2 * nx, lax.axis_size("seq"), width, jobs, ("yx", "yx"))

    def body(
        back_ref, grad_ref, proj_ref, again_ref, w_ref, q_ref, k_ref, v_ref, attn_ref, lse_ref,
        prow_ref, order_ref, qn_ref, kn_ref, sc_ref, qg_ref, kg_ref, cos_ref, sin_ref, *rest,
    ):
        at_refs, b_refs, rest = rest[:na], rest[na : na + nb], rest[na + nb :]
        dqkv_ref, dprojt_ref, dagain_ref, dqg_ref, dkg_ref = rest[:5]
        grad_outs, rest = rest[5 : 5 + n_out], rest[5 + n_out :]
        (dproj, dout, columns, delta, dqs, dks, send0, keep, recv0, recv1, s0, d0, s1, d1) = rest[:14]
        small.bind(rest[14 : 14 + n_small])
        if jobs:
            grads.bind(rest[14 + n_small :], at_refs, b_refs, grad_outs)

        def tick(it):
            if jobs:
                grads.tick(it)

        ctx = lax.axis_index("ctx")
        mx, core = ctx // 2, lax.rem(ctx, 2)
        bar = pltpu.get_barrier_semaphore()
        mate = {"ctx": mx * 2 + 1 - core}
        if jobs:
            peers = small.greet(bar) + grads.greet(bar)
        else:
            peers = small.greet(bar) + nx
            pl.semaphore_signal(bar, inc=1, device_id=mate, device_id_type=MESH)
            for d in range(1, nx):
                pl.semaphore_signal(
                    bar, inc=1, device_id={"ctx": lax.rem(mx + d, nx) * 2 + core},
                    device_id_type=MESH,
                )
        pl.semaphore_wait(bar, peers)
        tick(jnp.int32(0))

        dagain_ref[...] = jnp.zeros_like(dagain_ref)

        def norm_rows(t, carry):
            sl = pl.ds(pl.multiple_of(t * tile, tile), tile)
            dres = grad_ref[sl].astype(f32) + back_ref[sl].astype(f32)
            out = proj_ref[sl].astype(f32)
            inv = lax.rsqrt(jnp.mean(out * out, axis=1, keepdims=True) + norm_eps)
            norm = out * inv
            dagain_ref[...] += jnp.sum(dres * norm, axis=0, keepdims=True)
            dnorm = dres * again_ref[...]
            dot = jnp.mean(dnorm * norm, axis=1, keepdims=True)
            dproj[sl] = (inv * (dnorm - norm * dot)).astype(bf16)
            return carry

        lax.fori_loop(0, rows // tile, norm_rows, 0)
        for h in range(local // sub):
            dout[:, h * sub : (h + 1) * sub] = dot_nt(
                dproj[...], w_ref[h * sub : (h + 1) * sub, :]
            ).astype(bf16)
        lane = lax.broadcasted_iota(jnp.int32, (rows, lanes), 1)
        acc = jnp.zeros((rows, lanes), f32)
        for h in range(heads):
            hs = slice(h * head_dim, (h + 1) * head_dim)
            row_sum = jnp.sum(
                dout[:, hs].astype(f32) * attn_ref[:, hs].astype(f32), axis=1, keepdims=True
            )
            acc = jnp.where(lane == h, row_sum, acc)
        columns[...] = acc
        delta[...] = jnp.transpose(columns[...])[:8]
        dqs[...] = jnp.zeros_like(dqs)

        def c0(h):
            slot = lax.rem(h, 2)
            return remote(send0.at[slot], recv0.at[h], s0.at[slot], d0.at[h], mate)

        def c1(h, d):
            to = lax.rem(mx + d, nx)
            return remote(
                recv0.at[h, to], recv1.at[h, d - 1], s1.at[h, d - 1], d1.at[h, d - 1],
                {"ctx": to * 2 + core},
            )

        def one_block(h, hs, x, owner, write):
            start = (x * 2 + owner) * rows
            for part in range(rows // sub):
                ks = pl.ds(pl.multiple_of(start + part * sub, sub), sub)
                key, value = k_ref[ks, hs], v_ref[ks, hs]
                query, dhead = q_ref[:, hs], dout[:, hs]
                score = dot_nt(key, query) * scale
                place = order_ref[0, (x * 2 + owner) * 2 + part] * sub
                seen = place + lax.broadcasted_iota(jnp.int32, (sub, rows), 0) <= prow_ref[...]
                share = jnp.where(seen, jnp.exp(score - lse_ref[pl.ds(h, 1), :]), 0.0)
                dshare = dot_nt(value, dhead)
                dscore = share * (dshare - delta[pl.ds(h, 1), :]) * scale
                high = dscore.astype(bf16)
                low = (dscore - high.astype(f32)).astype(bf16)
                dqs[:, hs] += dot_tn(high, key) + dot_tn(low, key)
                write(
                    x, slice(part * sub, (part + 1) * sub),
                    jnp.dot(high, query, preferred_element_type=f32)
                    + jnp.dot(low, query, preferred_element_type=f32),
                    jnp.dot(share.astype(bf16), dhead, preferred_element_type=f32),
                )

        def one_head(h):
            hs = pl.ds(pl.multiple_of(h * head_dim, head_dim), head_dim)
            slot = lax.rem(h, 2)

            def to_send(x, rs, dk, dv):
                send0[slot, x, rs, :lanes] = dk.astype(bf16)
                send0[slot, x, rs, lanes:] = dv.astype(bf16)

            def to_keep(x, rs, dk, dv):
                keep[slot, x, rs, :lanes] = dk.astype(bf16)
                keep[slot, x, rs, lanes:] = dv.astype(bf16)

            @pl.when(h >= 2)
            def _():
                c0(h).wait_send()

            def mates(e, carry):
                one_block(h, hs, lax.rem(mx + 1 + e, nx), 1 - core, to_send)
                return carry

            lax.fori_loop(0, nx, mates, 0)
            c0(h).start()
            tick(2 * h + 1)

            def owns(e, carry):
                one_block(h, hs, lax.rem(mx + 1 + e, nx), core, to_keep)
                return carry

            lax.fori_loop(0, nx, owns, 0)
            c0(h).wait_recv()

            def add(x, carry):
                recv0[h, x] = (keep[slot, x].astype(f32) + recv0[h, x].astype(f32)).astype(bf16)
                return carry

            lax.fori_loop(0, nx, add, 0)
            for d in range(1, nx):
                c1(h, d).start()
            tick(2 * h + 2)

        def heads_loop(h, carry):
            one_head(h)
            return carry

        lax.fori_loop(0, heads, heads_loop, 0)
        if jobs:

            def more(it, carry):
                grads.tick(it)
                return carry

            lax.fori_loop(2 * heads + 1, grads.steps, more, 0)

        dot_q = jnp.zeros((rows, 1), f32)
        for h in range(heads):
            hs = slice(h * head_dim, (h + 1) * head_dim)
            dq = dqs[:, hs]
            dq = dq * cos_ref[...] - pltpu.roll(dq, head_dim // 2, 1) * sin_ref[...]
            norm = qn_ref[:, hs]
            dqg_ref[:, hs] = jnp.sum(dq * norm, axis=0, keepdims=True)
            dq = dq * qg_ref[:, hs]
            dqs[:, hs] = dq
            dot_q = dot_q + jnp.sum(dq * norm, axis=1, keepdims=True)
        dprojt_ref[...] = jnp.transpose(dproj[...])
        dot_k = jnp.zeros((rows, 1), f32)
        for h in range(heads):
            hs = slice(h * head_dim, (h + 1) * head_dim)
            total = recv0[h, mx].astype(f32)
            for d in range(1, nx):
                c1(h, d).wait_recv()
                total = total + recv1[h, d - 1].astype(f32)
            dqkv_ref[:, 2 * local + h * head_dim : 2 * local + (h + 1) * head_dim] = total[
                :, lanes:
            ].astype(bf16)
            dk = total[:, :lanes]
            dk = dk * cos_ref[...] - pltpu.roll(dk, head_dim // 2, 1) * sin_ref[...]
            norm = kn_ref[:, hs]
            dkg_ref[:, hs] = jnp.sum(dk * norm, axis=0, keepdims=True)
            dk = dk * kg_ref[:, hs]
            dks[:, hs] = dk
            dot_k = dot_k + jnp.sum(dk * norm, axis=1, keepdims=True)
        dots = small.total(lane_pair(dot_q, dot_k, rows)) * (1.0 / width)
        for h in range(heads):
            hs = slice(h * head_dim, (h + 1) * head_dim)
            dqkv_ref[:, hs] = (
                sc_ref[:, 0:1] * (dqs[:, hs] - qn_ref[:, hs] * dots[:, 0:1])
            ).astype(bf16)
            dqkv_ref[:, local + h * head_dim : local + (h + 1) * head_dim] = (
                sc_ref[:, 1:2] * (dks[:, hs] - kn_ref[:, hs] * dots[:, 1:2])
            ).astype(bf16)
        for h in range(heads):
            if h >= heads - 2:
                c0(h).wait_send()
            for d in range(1, nx):
                c1(h, d).wait_send()
        if jobs:
            grads.drain()

    sem = pltpu.SemaphoreType.DMA
    pair = (rows, 2 * lanes)
    return comm_call(
        body,
        [back, grad, proj, attn_gain, w_output, query_rot, keys, values, attn, lse, pos_row,
         order, query_norm, key_norm, scales, qgain, kgain, cosine, sine] + ats + bs,
        [
            jax.ShapeDtypeStruct((rows, 3 * local), bf16),
            jax.ShapeDtypeStruct((width, rows), bf16),
            jax.ShapeDtypeStruct((1, width), f32),
            jax.ShapeDtypeStruct((1, local), f32),
            jax.ShapeDtypeStruct((1, local), f32),
        ] + [jax.ShapeDtypeStruct(*out) for out in (grads.out_shapes(widths) if jobs else [])],
        [
            pltpu.VMEM((rows, width), bf16), pltpu.VMEM((rows, local), bf16),
            pltpu.VMEM((rows, lanes), f32), pltpu.VMEM((8, rows), f32),
            pltpu.VMEM((rows, local), f32), pltpu.VMEM((rows, local), f32),
            pltpu.VMEM((2, nx) + pair, bf16), pltpu.VMEM((2, nx) + pair, bf16),
            pltpu.VMEM((heads, nx) + pair, bf16), pltpu.VMEM((heads, nx - 1) + pair, bf16),
            sem((2,)), sem((heads,)), sem((heads, nx - 1)), sem((heads, nx - 1)),
        ] + small.scratch() + (grads.scratch() if jobs else []),
        cid, "attention_back", {11},
    )


def front(tokens, w_query, w_key, w_value, qgain, kgain, cosine, sine, order, cid):
    rows, width = tokens.shape
    local = w_query.shape[1]
    head_dim = lanes
    heads = local // head_dim
    nx = lax.axis_size("ctx") // 2
    count = nx * 2 * rows
    n_tp = lax.axis_size("tp")
    small = LineSmall(n_tp, rows)
    n_small = len(small.scratch())
    scale = head_dim ** (-0.5)
    group = rows // 2

    def body(
        tok_hbm, wq_hbm, wk_hbm, wv_hbm, qg_ref, kg_ref, cos_ref, sin_ref, order_ref,
        qrot_out, key_out, value_out, qn_out, kn_out, attn_out, tokt_out, sc_out, lse_out,
        tok, tokt, w3, qn, kn, qrot, keys, values, peak, total, acc, attn, loads, stores,
        sx, dx, sm, dm, sf, df, *rest,
    ):
        small.bind(rest[:n_small])
        copies = [
            pltpu.make_async_copy(src, dst, loads.at[i])
            for i, (src, dst) in enumerate(
                [(tok_hbm, tok), (wv_hbm, w3.at[2]), (wq_hbm, w3.at[0]), (wk_hbm, w3.at[1])]
            )
        ]
        for copy in copies:
            copy.start()
        ctx = lax.axis_index("ctx")
        mx, core = ctx // 2, lax.rem(ctx, 2)
        mate = {"ctx": mx * 2 + 1 - core}

        def peer(d):
            return {"ctx": lax.rem(mx + d, nx) * 2 + core}

        bar = pltpu.get_barrier_semaphore()
        pl.semaphore_signal(bar, inc=1, device_id=mate, device_id_type=MESH)
        for d in range(1, nx):
            pl.semaphore_signal(bar, inc=1, device_id=peer(d), device_id_type=MESH)
        peers = small.greet(bar) + nx

        def at(x, owner):
            return pl.ds(pl.multiple_of((x * 2 + owner) * rows, rows), rows)

        mine = at(mx, core)
        side = local // 2
        boxes = [(keys, pl.ds(0, side)), (keys, pl.ds(side, side)), (values, pl.ds(0, local))]

        def move(t, rs, sent, done, where):
            box, cols = boxes[t]
            return remote(box.at[rs, cols], box.at[rs, cols], sent, done, where)

        def to_peer(t, d):
            return move(t, mine, sx.at[t, d - 1], dx.at[t, d - 1], peer(d))

        def from_peer(t, d):
            rs = at(lax.rem(mx + nx - d, nx), core)
            return move(t, rs, sx.at[t, d - 1], dx.at[t, d - 1], peer(d))

        def to_mate(t):
            return move(t, mine, sm.at[t], dm.at[t], mate)

        def from_mate(t):
            return move(t, at(mx, 1 - core), sm.at[t], dm.at[t], mate)

        def pass_on(t, d):
            rs = at(lax.rem(mx + nx - d, nx), core)
            return move(t, rs, sf.at[t, d - 1], df.at[t, d - 1], mate)

        def passed(t, d):
            rs = at(lax.rem(mx + nx - d, nx), 1 - core)
            return move(t, rs, sf.at[t, d - 1], df.at[t, d - 1], mate)

        def each_peer(act):
            def one(d, carry):
                act(d)
                return carry

            lax.fori_loop(1, nx, one, 0)

        copies[0].wait()
        copies[1].wait()
        values[mine] = jnp.dot(tok[...], w3[2], preferred_element_type=f32).astype(bf16)
        pl.semaphore_wait(bar, peers)
        each_peer(lambda d: to_peer(2, d).start())
        to_mate(2).start()
        copies[2].wait()
        qn[...] = jnp.dot(tok[...], w3[0], preferred_element_type=f32)
        copies[3].wait()
        kn[...] = jnp.dot(tok[...], w3[1], preferred_element_type=f32)

        def squares(ref):
            acc_sq = jnp.zeros((rows, 1), f32)
            for h in range(heads):
                part = ref[:, h * head_dim : (h + 1) * head_dim]
                acc_sq = acc_sq + jnp.sum(part * part, axis=1, keepdims=True)
            return acc_sq

        sums = small.total(lane_pair(squares(qn), squares(kn), rows))
        scales = lax.rsqrt(sums * (1.0 / width) + norm_eps)
        sc_out[...] = scales

        def rotated(ref, column, gain_ref, h):
            hs = slice(h * head_dim, (h + 1) * head_dim)
            norm = ref[:, hs] * sc_out[:, column : column + 1]
            ref[:, hs] = norm
            norm = norm * gain_ref[:, hs]
            return (
                norm * cos_ref[...] + pltpu.roll(norm, head_dim // 2, 1) * sin_ref[...]
            ).astype(bf16)

        for h in range(heads):
            keys[mine, h * head_dim : (h + 1) * head_dim] = rotated(kn, 1, kg_ref, h)
            if (h + 1) * head_dim in (side, local):
                t = (h + 1) * head_dim // side - 1
                each_peer(lambda d: to_peer(t, d).start())
                to_mate(t).start()
        for h in range(heads):
            qrot[:, h * head_dim : (h + 1) * head_dim] = rotated(qn, 0, qg_ref, h)
        peak[...] = jnp.full_like(peak, masked_score)
        total[...] = jnp.zeros_like(total)
        acc[...] = jnp.zeros_like(acc)

        def places(block, shape, axis):
            spot = lax.broadcasted_iota(jnp.int32, shape, axis)
            first, second = order_ref[0, block * 2], order_ref[0, block * 2 + 1]
            return jnp.where(spot < group, first * group + spot, (second - 1) * group + spot)

        def attend(x, owner, low, high):
            block = x * 2 + owner
            rs = at(x, owner)

            def one(h, carry):
                hs = pl.ds(pl.multiple_of(h * head_dim, head_dim), head_dim)
                score = dot_nt(qrot[:, hs], keys[rs, hs]) * scale
                seen = places(block, (1, rows), 1) <= places(ctx, (rows, 1), 0)
                old = peak[h]
                new = jnp.maximum(
                    old, jnp.max(jnp.where(seen, score, masked_score), axis=1, keepdims=True)
                )
                share = jnp.where(seen, jnp.exp(score - new), 0.0)
                fade = jnp.exp(old - new)
                peak[h] = new
                total[h] = total[h] * fade + jnp.sum(share, axis=1, keepdims=True)
                acc[:, hs] = acc[:, hs] * fade + jnp.dot(
                    share.astype(bf16), values[rs, hs], preferred_element_type=f32
                )
                return carry

            lax.fori_loop(low, high, one, 0)

        attend(mx, core, 0, heads)

        def hand_on(t, d):
            from_peer(t, d).wait_recv()
            pass_on(t, d).start()

        each_peer(lambda d: hand_on(2, d))
        for t in range(3):
            from_mate(t).wait_recv()
        attend(mx, 1 - core, 0, heads)
        tokt[...] = jnp.transpose(tok[...])

        def half_heads(t, carry):
            low, high = t * heads // 2, (t + 1) * heads // 2

            def near(d):
                for v in range(2):

                    @pl.when(t == v)
                    def _():
                        hand_on(v, d)

                attend(lax.rem(mx + nx - d, nx), core, low, high)

            def far(d):
                @pl.when(t == 0)
                def _():
                    passed(2, d).wait_recv()
                    passed(0, d).wait_recv()

                @pl.when(t == 1)
                def _():
                    passed(1, d).wait_recv()

                attend(lax.rem(mx + nx - d, nx), 1 - core, low, high)

            each_peer(near)
            each_peer(far)
            return carry

        lax.fori_loop(0, 2, half_heads, 0)

        lane = lax.broadcasted_iota(jnp.int32, (rows, lanes), 1)
        logs = jnp.zeros((rows, lanes), f32)
        for h in range(heads):
            hs = slice(h * head_dim, (h + 1) * head_dim)
            attn[:, hs] = (acc[:, hs] / total[h]).astype(bf16)
            logs = jnp.where(lane == h, peak[h] + jnp.log(total[h]), logs)
        lse_out[...] = jnp.transpose(logs)[:8]
        outs = [
            pltpu.make_async_copy(src, dst, stores.at[i])
            for i, (src, dst) in enumerate(
                [(qrot, qrot_out), (keys, key_out), (values, value_out), (qn, qn_out),
                 (kn, kn_out), (attn, attn_out), (tokt, tokt_out)]
            )
        ]
        for copy in outs:
            copy.start()
        for copy in outs:
            copy.wait()
        for t in range(3):
            to_mate(t).wait_send()

            def sent(d):
                to_peer(t, d).wait_send()
                pass_on(t, d).wait_send()

            each_peer(sent)

    sem = pltpu.SemaphoreType.DMA
    hbm = pl.BlockSpec(memory_space=pl.ANY)
    block = jax.ShapeDtypeStruct
    return pl.pallas_call(
        body,
        out_shape=[
            block((rows, local), bf16), block((count, local), bf16), block((count, local), bf16),
            block((rows, local), f32), block((rows, local), f32), block((rows, local), bf16),
            block((width, rows), bf16),
            block((rows, lanes), f32), block((8, rows), f32),
        ],
        in_specs=[hbm] * 4 + [vmem_spec()] * 4 + [pl.BlockSpec(memory_space=pltpu.SMEM)],
        out_specs=[hbm] * 7 + [vmem_spec()] * 2,
        scratch_shapes=[
            pltpu.VMEM((rows, width), bf16), pltpu.VMEM((width, rows), bf16),
            pltpu.VMEM((3, width, local), bf16),
            pltpu.VMEM((rows, local), f32),
            pltpu.VMEM((rows, local), f32), pltpu.VMEM((rows, local), bf16),
            pltpu.VMEM((count, local), bf16), pltpu.VMEM((count, local), bf16),
            pltpu.VMEM((heads, rows, 1), f32), pltpu.VMEM((heads, rows, 1), f32),
            pltpu.VMEM((rows, local), f32), pltpu.VMEM((rows, local), bf16),
            sem((4,)), sem((7,)),
            sem((3, nx - 1)), sem((3, nx - 1)), sem((3,)), sem((3,)),
            sem((3, nx - 1)), sem((3, nx - 1)),
        ] + small.scratch(),
        compiler_params=pltpu.CompilerParams(
            collective_id=cid, has_side_effects=True, vmem_limit_bytes=62 * 2**20
        ),
        name="front",
    )(tokens, w_query, w_key, w_value, qgain, kgain, cosine, sine, order)


def load_list(pairs, sems, base=0):
    copies = [
        pltpu.make_async_copy(src, dst, sems.at[base + i]) for i, (src, dst) in enumerate(pairs)
    ]
    for copy in copies:
        copy.start()
    return copies


def kernel_call(body, args, kinds, outs, out_kinds, scratch, cid, name):
    spec = {
        "v": vmem_spec(),
        "h": pl.BlockSpec(memory_space=pl.ANY),
        "s": pl.BlockSpec(memory_space=pltpu.SMEM),
    }
    return pl.pallas_call(
        body,
        out_shape=[jax.ShapeDtypeStruct(*out) for out in outs],
        in_specs=[spec[kind] for kind in kinds],
        out_specs=[spec[kind] for kind in out_kinds],
        scratch_shapes=scratch,
        compiler_params=pltpu.CompilerParams(
            collective_id=cid, has_side_effects=True, vmem_limit_bytes=62 * 2**20
        ),
        name=name,
    )(*args)


def middle(attn, tokens, attn_gain, w_output, w_gate, w_up, w_down, cid):
    rows, width = tokens.shape
    local, wide = w_output.shape[0], w_gate.shape[1]
    n_tp = lax.axis_size("tp")
    line = LineSum(n_tp, 2 * rows, width, 4 * row_chains)
    n_line = len(line.scratch())
    half = rows // 2
    tile = 64
    cut = 512
    n_cut = wide // cut
    part = line.part

    def body(
        attn_hbm, tok_hbm, again_ref, wo_hbm, wg_hbm, wu_hbm, wd_hbm,
        proj_out, hidt_out, gate_out, up_out, inner_out, down_out, inv_out,
        attn_v, tok, wo, hid, hidt, gate, up, inner, wg, wu, wd, first, loads, stores, *rest,
    ):
        line.bind(rest[:n_line])
        start = load_list([(attn_hbm, attn_v), (wo_hbm, wo), (tok_hbm, tok)], first)
        pairs = []
        for j in range(n_cut):
            cols = pl.ds(j * cut, cut)
            pairs += [(wg_hbm.at[:, cols], wg.at[j]), (wu_hbm.at[:, cols], wu.at[j])]
        for j in range(n_tp):
            cols = pl.ds(j * part, part)
            pairs += [(wd_hbm.at[:, cols], wd.at[j])]
        weights = load_list(pairs, loads)
        bar = pltpu.get_barrier_semaphore()
        peers = line.greet(bar)
        for copy in start:
            copy.wait()
        for j in range(n_tp):
            line.own[j, :rows] = jnp.dot(
                attn_v[...], wo[:, j * part : (j + 1) * part], preferred_element_type=f32
            ).astype(bf16)
        pl.semaphore_wait(bar, peers)

        def step(t, carry):
            line.step(t)

            @pl.when(t == 3 * n_tp + 1)
            def _():
                hidt[...] = jnp.transpose(hid[...])

            return carry

        def row_half(c, carry):
            base = pl.multiple_of(c * half, half)
            sl = pl.ds(base, half)
            lax.fori_loop(c * 2 * n_tp, c * n_tp + 2 * n_tp - 1, step, 0)

            def norm_rows(t, carry):
                rs = pl.ds(pl.multiple_of(base + t * tile, tile), tile)
                outs = [line.res[j, rs].astype(f32) for j in range(n_tp)]
                square = sum(jnp.sum(out * out, axis=1, keepdims=True) for out in outs)
                inv = lax.rsqrt(square * (1.0 / width) + norm_eps)
                inv_out[rs, :] = inv
                for j, out in enumerate(outs):
                    cols = slice(j * part, (j + 1) * part)
                    hid[rs, cols] = (
                        tok[rs, cols].astype(f32) + out * inv * again_ref[:, cols]
                    ).astype(bf16)
                return carry

            lax.fori_loop(0, half // tile, norm_rows, 0)
            for j in range(n_cut):
                cols = slice(j * cut, (j + 1) * cut)

                @pl.when(c == 0)
                def _():
                    weights[2 * j].wait()
                    weights[2 * j + 1].wait()

                g = jnp.dot(hid[sl], wg[j], preferred_element_type=f32)
                u = jnp.dot(hid[sl], wu[j], preferred_element_type=f32)
                gate[sl, cols] = g.astype(bf16)
                up[sl, cols] = u.astype(bf16)
                inner[sl, cols] = (g * jax.nn.sigmoid(g) * u).astype(bf16)
                low, high = j * row_chains // n_cut, (j + 1) * row_chains // n_cut
                line.pieces(((c + 2) * n_tp - 1) * row_chains + low, high - low)
            for j in range(n_tp):

                @pl.when(c == 0)
                def _():
                    weights[2 * n_cut + j].wait()

                line.own[j, pl.ds(rows + base, half)] = jnp.dot(
                    inner[sl], wd[j], preferred_element_type=f32
                ).astype(bf16)
            return carry

        lax.fori_loop(0, 2, row_half, 0)
        outs = load_list([(gate, gate_out), (up, up_out), (inner, inner_out)], stores)
        ready = line.ship(proj_out, stores, 4, 0, rows)
        lax.fori_loop(3 * n_tp, line.steps, step, 0)
        last = pltpu.make_async_copy(hidt, hidt_out, stores.at[3])
        last.start()
        ready = ready + line.ship(down_out, stores, 4 + n_tp, rows, rows)
        line.drain()
        for copy in outs + [last] + ready:
            copy.wait()

    sem = pltpu.SemaphoreType.DMA
    return kernel_call(
        body, [attn, tokens, attn_gain, w_output, w_gate, w_up, w_down], "hhvhhhh",
        [((rows, width), bf16), ((width, rows), bf16), ((rows, wide), bf16), ((rows, wide), bf16),
         ((rows, wide), bf16), ((rows, width), bf16), ((rows, 1), f32)],
        "hhhhhhv",
        [
            pltpu.VMEM((rows, local), bf16), pltpu.VMEM((rows, width), bf16),
            pltpu.VMEM((local, width), bf16),
            pltpu.VMEM((rows, width), bf16), pltpu.VMEM((width, rows), bf16),
            pltpu.VMEM((rows, wide), bf16), pltpu.VMEM((rows, wide), bf16),
            pltpu.VMEM((rows, wide), bf16),
            pltpu.VMEM((n_cut, width, cut), bf16), pltpu.VMEM((n_cut, width, cut), bf16),
            pltpu.VMEM((n_tp, wide, part), bf16),
            sem((3,)), sem((2 * n_cut + n_tp,)), sem((4 + 2 * n_tp,)),
        ] + line.scratch(),
        cid, "middle",
    )


def mlp_back(down, grad, mlp_gain, gate, up, inner, hid_t, w_gate, w_up, w_down, jobs, widths, cid):
    rows, width = down.shape
    wide = gate.shape[1]
    n_tp = lax.axis_size("tp")
    line = LineSum(n_tp, rows, width)
    grads = GradScatter(lax.axis_size("ctx"), lax.axis_size("seq"), width, jobs)
    n_line, n_grads, n_out = len(line.scratch()), len(grads.scratch()), len(widths)
    tile = 64
    cut = 512
    n_cut = wide // cut
    part = line.part
    lead = row_chains * n_tp // (n_cut + n_tp)
    ticks = n_cut // 2 + n_tp // 2

    def body(
        down_hbm, grad_hbm, mgain_ref, gate_hbm, up_hbm, inner_hbm, hidt_hbm, wg_hbm, wu_hbm, wd_hbm,
        back_out, dgate_out, dup_out, dgain_out, inv_out, *rest,
    ):
        grad_outs, rest = rest[:n_out], rest[n_out:]
        (gate_v, up_v, inner_v, hidt, ddown, ddownt, dgate, dup, ring, loads, wsem, stores) = rest[:12]
        line.bind(rest[12 : 12 + n_line])
        grads.bind(rest[12 + n_line :], [ddownt, hidt], [inner_v, dgate, dup], grad_outs)

        def fetch(src, index):
            return pltpu.make_async_copy(src, ring.at[index], wsem.at[index])

        def rows_of(ref, j, size):
            return ref.at[pl.ds(pl.multiple_of(j * size, size), size)]

        for j in range(4):
            fetch(rows_of(wd_hbm, j, cut), j).start()
        down_ref, grad_ref = dgate.at[:, pl.ds(0, width)], dup.at[:, pl.ds(0, width)]
        first = load_list([(down_hbm, down_ref), (grad_hbm, grad_ref)], loads, 4)
        early = load_list(
            [(inner_hbm, inner_v), (gate_hbm, gate_v), (up_hbm, up_v), (hidt_hbm, hidt)], loads
        )
        bar = pltpu.get_barrier_semaphore()
        peers = line.greet(bar) + grads.greet(bar)
        dgain_out[...] = jnp.zeros_like(dgain_out)
        for copy in first:
            copy.wait()

        def norm_rows(t, carry):
            sl = pl.ds(pl.multiple_of(t * tile, tile), tile)
            out = down_ref[sl].astype(f32)
            upstream = grad_ref[sl].astype(f32)
            inv = lax.rsqrt(jnp.mean(out * out, axis=1, keepdims=True) + norm_eps)
            norm = out * inv
            inv_out[sl, :] = inv
            dgain_out[...] += jnp.sum(upstream * norm, axis=0, keepdims=True)
            dnorm = upstream * mgain_ref[...]
            dot = jnp.mean(dnorm * norm, axis=1, keepdims=True)
            ddown[sl] = (inv * (dnorm - norm * dot)).astype(bf16)
            return carry

        lax.fori_loop(0, rows // tile, norm_rows, 0)
        ddownt[...] = jnp.transpose(ddown[...])
        for copy in early:
            copy.wait()
        pl.semaphore_wait(bar, peers)

        half = rows // 2

        def row_half(c, carry):
            sl = pl.ds(pl.multiple_of(c * half, half), half)

            def beside(i, j, first):
                @pl.when(c == 1)
                def _():
                    line.pieces(i * lead, lead)

                @pl.when(lax.rem(j, 2) == 1)
                def _():
                    grads.tick(first + j // 2)

            def inner_back(j, carry):
                fetch(rows_of(wd_hbm, j, cut), j).wait()
                cols = pl.ds(pl.multiple_of(j * cut, cut), cut)
                dmix = dot_nt(ddown[sl], ring[j])
                g, u = gate_v[sl, cols].astype(f32), up_v[sl, cols].astype(f32)
                sig = jax.nn.sigmoid(g)
                dgate[sl, cols] = (dmix * u * sig * (1.0 + g * (1.0 - sig))).astype(bf16)
                dup[sl, cols] = (dmix * (g * sig)).astype(bf16)

                @pl.when(lax.rem(j, 2) == 0)
                def _():
                    fetch(rows_of(wg_hbm, j // 2, part), j).start()

                @pl.when(lax.rem(j, 2) == 1)
                def _():
                    fetch(rows_of(wu_hbm, j // 2, part), j).start()

                beside(j, j, c * ticks)
                return carry

            lax.fori_loop(0, n_cut, inner_back, 0)

            def hidden_back(j, carry):
                slot = lax.rem(2 * j, 4)
                fetch(rows_of(wg_hbm, j, part), slot).wait()
                fetch(rows_of(wu_hbm, j, part), slot + 1).wait()
                line.own[j, sl] = (
                    dot_nt(dgate[sl], ring[slot]) + dot_nt(dup[sl], ring[slot + 1])
                ).astype(bf16)

                @pl.when(j + 2 < n_tp)
                def _():
                    fetch(rows_of(wg_hbm, j + 2, part), slot).start()
                    fetch(rows_of(wu_hbm, j + 2, part), slot + 1).start()

                @pl.when((j + 2 >= n_tp) & (c == 0))
                def _():
                    fetch(rows_of(wd_hbm, slot, cut), slot).start()
                    fetch(rows_of(wd_hbm, slot + 1, cut), slot + 1).start()

                beside(n_cut + j, j, c * ticks + n_cut // 2)
                return carry

            lax.fori_loop(0, n_tp, hidden_back, 0)
            return carry

        lax.fori_loop(0, 2, row_half, 0)
        outs = load_list([(dgate, dgate_out), (dup, dup_out)], stores)
        done, used = 2 * ticks, (n_cut + n_tp) * lead

        def one(it, carry):
            line.pieces(used + (it - done) * pace, pace)
            grads.tick(it)
            return carry

        line_its = -(-(line.steps * row_chains - used) // pace)
        lax.fori_loop(done, max(done + line_its, grads.steps), one, 0)
        outs += line.ship(back_out, stores, 2, 0, rows)
        line.drain()
        grads.drain()
        for copy in outs:
            copy.wait()

    sem = pltpu.SemaphoreType.DMA
    return kernel_call(
        body, [down, grad, mlp_gain, gate, up, inner, hid_t, w_gate, w_up, w_down], "hhvhhhhhhh",
        [((rows, width), bf16), ((rows, wide), bf16), ((rows, wide), bf16), ((1, width), f32),
         ((rows, 1), f32)]
        + grads.out_shapes(widths),
        "hhhvv" + "v" * n_out,
        [
            pltpu.VMEM((rows, wide), bf16), pltpu.VMEM((rows, wide), bf16),
            pltpu.VMEM((rows, wide), bf16), pltpu.VMEM((width, rows), bf16),
            pltpu.VMEM((rows, width), bf16), pltpu.VMEM((width, rows), bf16),
            pltpu.VMEM((rows, wide), bf16), pltpu.VMEM((rows, wide), bf16),
            pltpu.VMEM((4, cut, width), bf16),
            sem((6,)), sem((4,)), sem((2 + n_tp,)),
        ] + line.scratch() + grads.scratch(),
        cid, "mlp_back",
    )


def last_sums(dqkv, w_query, w_key, w_value, ats, bs, jobs, widths, gains, cid):
    rows = dqkv.shape[0]
    width, local = w_query.shape
    n_ctx, n_seq = lax.axis_size("ctx"), lax.axis_size("seq")
    n_tp = lax.axis_size("tp")
    line = LineSum(n_tp, rows, width)
    grads = GradScatter(n_ctx, n_seq, width, jobs)
    small = GainSum(n_ctx, n_seq, gains.shape[0])
    na, nb, n_out = len(ats), len(bs), len(widths)
    n_line, n_grads = len(line.scratch()), len(grads.scratch())
    part = line.part

    def body(dqkv_ref, wq_ref, wk_ref, wv_ref, *refs):
        at_refs, b_refs = refs[:na], refs[na : na + nb]
        gain_ref, last_out = refs[na + nb], refs[na + nb + 1]
        refs = refs[na + nb + 2 :]
        grad_outs, gain_out, stores, scratch = refs[:n_out], refs[n_out], refs[n_out + 1], refs[n_out + 2 :]
        line.bind(scratch[:n_line])
        grads.bind(scratch[n_line : n_line + n_grads], at_refs, list(b_refs) + [dqkv_ref], grad_outs)
        small.bind(scratch[n_line + n_grads :], gain_ref, gain_out)
        bar = pltpu.get_barrier_semaphore()
        peers = line.greet(bar) + small.greet(bar)
        pl.semaphore_wait(bar, peers)
        small.start()

        def input_back(j, carry):
            rs = pl.ds(pl.multiple_of(j * part, part), part)
            line.own[j] = (
                dot_nt(dqkv_ref[:, :local], wq_ref[rs])
                + dot_nt(dqkv_ref[:, local : 2 * local], wk_ref[rs])
                + dot_nt(dqkv_ref[:, 2 * local :], wv_ref[rs])
            ).astype(bf16)

            @pl.when(lax.rem(j, 2) == 0)
            def _():
                grads.tick(j // 2)

            return carry

        lax.fori_loop(0, n_tp, input_back, 0)
        done = n_tp // 2

        def one(it, carry):
            grads.tick(it)
            line.pieces((it - done) * pace, pace)
            return carry

        line_steps = -(-line.steps * row_chains // pace)
        lax.fori_loop(done, max(done + line_steps, grads.steps), one, 0)
        small.finish()
        outs = line.ship(last_out, stores, 0, 0, rows)
        line.drain()
        grads.drain()
        for copy in outs:
            copy.wait()

    sem = pltpu.SemaphoreType.DMA
    return kernel_call(
        body, [dqkv, w_query, w_key, w_value] + list(ats) + list(bs) + [gains],
        "vvvv" + "v" * (na + nb + 1),
        [((rows, width), bf16)] + grads.out_shapes(widths) + [(gains.shape, f32)],
        "h" + "v" * (n_out + 1),
        [sem((n_tp,))] + line.scratch() + grads.scratch() + small.scratch(),
        cid, "last_sums",
    )


def row_tiles(body, args, outs, name):
    count = 4

    def spec(shape):
        if shape[0] == 1:
            return pl.BlockSpec(shape, lambda i: (0, 0))
        return pl.BlockSpec((shape[0] // count, shape[1]), lambda i: (i, 0))

    def whole(*refs):
        body(refs[: len(args)], refs[len(args) :])

    return pl.pallas_call(
        whole,
        grid=(count,),
        out_shape=[jax.ShapeDtypeStruct(shape, f32) for shape in outs],
        in_specs=[spec(arg.shape) for arg in args],
        out_specs=[spec(shape) for shape in outs],
        compiler_params=pltpu.CompilerParams(vmem_limit_bytes=62 * 2**20),
        name=name,
    )(*args)


def block_tile(ins, outs):
    x, a, ra, ga, d, rd, gd = [ref[...].astype(f32) for ref in ins[:7]]
    outs[0][...] = x + (a * ra) * ga + (d * rd) * gd
    for src, dst in zip(ins[7:], outs[1:]):
        dst[...] = src[...]


def input_tile(ins, outs):
    outs[0][...] = ins[0][...].astype(f32) + ins[1][...].astype(f32) + ins[2][...].astype(f32)
    outs[1][...] = ins[3][...]
    outs[2][...] = ins[4][...]
    size = outs[3].shape[1]
    for i in range(3):
        outs[3 + i][...] = ins[5][:, i * size : (i + 1) * size]


def per_device(
    tokens,
    out_grad,
    group_order,
    w_query,
    w_key,
    w_value,
    query_gain,
    key_gain,
    w_output,
    attn_gain,
    w_gate,
    w_up,
    w_down,
    mlp_gain,
):
    inputs = tokens[0]
    upstream = out_grad[0]
    rows, width = inputs.shape
    heads, head_dim = query_gain.shape
    local = heads * head_dim
    wide = w_gate.shape[1]
    positions = key_positions(group_order[0], lax.axis_index("ctx") * rows, rows, rows // 2)
    angle_cos, angle_sin = rope_tables(positions, head_dim)
    qgain = query_gain.reshape(1, local)
    kgain = key_gain.reshape(1, local)
    (query_rot, keys, values, query_norm, key_norm, attn, tokens_t, scales, lse) = front(
        inputs, w_query, w_key, w_value, qgain, kgain, angle_cos, angle_sin, group_order, 1
    )
    proj, hidden_t, gate, up, inner, down, proj_scale = middle(
        attn, inputs, attn_gain[None], w_output, w_gate, w_up, w_down, 2
    )
    chunk_cols = 2 * lanes
    chunks = wide // chunk_cols
    thin = local // chunk_cols
    back, d_gate, d_up, d_mlp_gain, down_scale, grad_down, grad_gate = mlp_back(
        down, upstream, mlp_gain[None], gate, up, inner, hidden_t, w_gate, w_up, w_down,
        [
            dict(a=0, b=0, first=0, count=chunks, out=0, place=0, flip=True),
            dict(a=1, b=1, first=0, count=chunks, out=1, place=0, flip=False),
        ],
        [wide, wide],
        3,
    )
    d_qkv, d_proj_t, d_attn_gain, d_query_gain, d_key_gain = attention_back(
        back, upstream, proj, attn_gain[None], w_output, query_rot, keys, values, attn, lse,
        positions[None], group_order, query_norm, key_norm, scales, qgain, kgain, angle_cos,
        angle_sin, [], [], [], [], 4,
    )
    owners = lax.axis_size("ctx") * lax.axis_size("seq")
    gains = [d_attn_gain, d_mlp_gain, d_query_gain, d_key_gain]
    ends = [gain.shape[1] for gain in gains]
    ends = [sum(ends[: i + 1]) for i in range(4)]
    packed = jnp.concatenate(gains, axis=1).reshape(-1, lanes)
    last, grad_up, grad_qkv, grad_output, small = last_sums(
        d_qkv, w_query, w_key, w_value,
        [hidden_t, tokens_t, d_proj_t],
        [d_up, attn],
        [
            dict(a=0, b=0, first=0, count=chunks, out=0, place=0, flip=False),
            dict(a=2, b=1, first=0, count=thin, out=2, place=0, flip=True),
            dict(a=1, b=2, first=0, count=3 * thin, out=1, place=0, flip=False),
        ],
        [wide, 3 * local, local],
        packed,
        5,
    )
    small = small.reshape(-1)
    me = lax.axis_index("ctx") * lax.axis_size("seq") + lax.axis_index("seq")

    def my_part(start, end, lead):
        whole = small[start:end].reshape(lead, -1)
        size = whole.shape[1] // owners
        return lax.dynamic_slice_in_dim(whole, me * size, size, 1)

    g_attn = my_part(0, ends[0], 1)[0]
    g_mlp = my_part(ends[0], ends[1], 1)[0]
    g_query = my_part(ends[1], ends[2], heads)
    g_key = my_part(ends[2], ends[3], heads)
    block_out, grad_down, grad_gate = row_tiles(
        block_tile,
        [inputs, proj, proj_scale, attn_gain[None], down, down_scale, mlp_gain[None], grad_down,
         grad_gate],
        [inputs.shape, grad_down.shape, grad_gate.shape], "block_out",
    )
    own = grad_qkv.shape[0]
    input_grad, grad_up, grad_output, grad_query, grad_key, grad_value = row_tiles(
        input_tile, [upstream, back, last, grad_up, grad_output, grad_qkv],
        [inputs.shape, grad_up.shape, grad_output.shape] + [(own, local)] * 3, "input_grad",
    )
    return (
        block_out[None],
        input_grad[None],
        grad_query,
        grad_key,
        grad_value,
        g_query,
        g_key,
        grad_output,
        g_attn,
        grad_gate,
        grad_up,
        grad_down,
        g_mlp,
    )


def solution(mesh):
    return jax.shard_map(
        per_device,
        mesh=mesh,
        in_specs=(
            P("seq", "ctx", None),
            P("seq", "ctx", None),
            P("seq", None),
            P(None, "tp"),
            P(None, "tp"),
            P(None, "tp"),
            P("tp", None),
            P("tp", None),
            P("tp", None),
            P(),
            P(None, "tp"),
            P(None, "tp"),
            P("tp", None),
            P(),
        ),
        out_specs=(
            P("seq", "ctx", None),
            P("seq", "ctx", None),
            P(("ctx", "seq"), "tp"),
            P(("ctx", "seq"), "tp"),
            P(("ctx", "seq"), "tp"),
            P("tp", ("ctx", "seq")),
            P("tp", ("ctx", "seq")),
            P("tp", ("ctx", "seq")),
            P(("ctx", "seq")),
            P(("ctx", "seq"), "tp"),
            P(("ctx", "seq"), "tp"),
            P("tp", ("ctx", "seq")),
            P(("ctx", "seq")),
        ),
        check_vma=False,
    )
```

```python
import jax
import jax.numpy as jnp
from jax import lax
from jax.sharding import PartitionSpec as P
from jax.experimental import pallas as pl
from jax.experimental.pallas import tpu as pltpu

norm_eps = 1e-06
rope_base = 500000.0
masked_score = -1e30


def rope_tables(positions, head_dim):
    half = head_dim // 2
    channel = jnp.arange(head_dim, dtype=jnp.int32)
    rates = rope_base ** (-((channel % half).astype(jnp.float32) * 2.0 / head_dim))
    angle = positions.astype(jnp.float32)[:, None] * rates[None, :]
    return jnp.cos(angle), jnp.where(channel[None, :] < half, -jnp.sin(angle), jnp.sin(angle))


def key_positions(order, first_row, count, group):
    row_ids = first_row + jnp.arange(count, dtype=jnp.int32)
    slots = row_ids // group
    picks = slots[:, None] == jnp.arange(order.shape[0], dtype=jnp.int32)[None, :]
    return jnp.sum(jnp.where(picks, order[None, :], 0), axis=1) * group + row_ids % group


MESH = pl.DeviceIdType.MESH
bf16 = jnp.bfloat16
f32 = jnp.float32
lanes = 128
row_blocks = 16
row_chains = 8
pace = 6


def remote(src, dst, send, recv, where):
    return pltpu.make_async_remote_copy(
        src, dst, send, recv, device_id=where, device_id_type=MESH
    )


class LineSum:
    def __init__(self, n, rows, width, blocks=row_blocks):
        self.n, self.rows, self.width = n, rows, width
        self.part = width // n
        self.rc = rows // blocks
        self.total = blocks // row_chains * n
        self.steps = self.total + n - 1

    def scratch(self):
        shape = (self.n, self.rows, self.part)
        return (
            [pltpu.VMEM(shape, bf16)] * 4
            + [pltpu.SemaphoreType.DMA] * 2
            + [pltpu.SemaphoreType.DMA((row_chains, self.total))] * 2
        )

    def bind(self, refs):
        self.own, self.from_l, self.from_r, self.res = refs[:4]
        self.send_r, self.send_l, self.recv_l, self.recv_r = refs[4:]
        self.i = lax.axis_index("tp")
        self.has_l, self.has_r = self.i > 0, self.i < self.n - 1

    def greet(self, bar):
        @pl.when(self.has_l)
        def _():
            pl.semaphore_signal(bar, inc=1, device_id={"tp": self.i - 1}, device_id_type=MESH)

        @pl.when(self.has_r)
        def _():
            pl.semaphore_signal(bar, inc=1, device_id={"tp": self.i + 1}, device_id_type=MESH)

        return self.has_l.astype(jnp.int32) + self.has_r.astype(jnp.int32)

    def load(self, x_ref):
        for j in range(self.n):
            self.own[j] = x_ref[:, j * self.part : (j + 1) * self.part]

    def rows_of(self, g, p):
        block = (p // self.n) * row_chains + g
        return pl.ds(pl.multiple_of(block * self.rc, self.rc), self.rc)

    def right(self, src, dst, g, p, j):
        sl = self.rows_of(g, p)
        return remote(
            src.at[j, sl], dst.at[j, sl], self.send_r, self.recv_l.at[g, p],
            {"tp": self.i + 1},
        )

    def left(self, src, dst, g, q, j):
        sl = self.rows_of(g, q)
        return remote(
            src.at[j, sl], dst.at[j, sl], self.send_l, self.recv_r.at[g, q],
            {"tp": self.i - 1},
        )

    def wait_l(self, g, p, j):
        sl = self.rows_of(g, p)
        remote(
            self.own.at[j, sl], self.from_l.at[j, sl], self.send_r, self.recv_l.at[g, p],
            {"tp": self.i - 1},
        ).wait_recv()

    def wait_r(self, g, q, j):
        sl = self.rows_of(g, q)
        remote(
            self.own.at[j, sl], self.from_r.at[j, sl], self.send_l, self.recv_r.at[g, q],
            {"tp": self.i + 1},
        ).wait_recv()

    def step(self, t):
        self.pieces(t * row_chains, row_chains)

    def pieces(self, first, count):
        def one(v, carry):
            self.piece(first + v)
            return carry

        lax.fori_loop(0, count, one, 0)

    def piece(self, e):
        t = e // row_chains

        @pl.when(t < self.steps)
        def _():
            self.sub_step(t, lax.rem(e, row_chains))

    def sub_step(self, t, g):
        n, i, has_l, has_r = self.n, self.i, self.has_l, self.has_r
        own, from_l, from_r, res = self.own, self.from_l, self.from_r, self.res
        p = t - i
        q = t - (n - 1 - i)
        jr = n - 1 - lax.rem(p + n * self.total, n)
        jl = lax.rem(q + n * self.total, n)
        pv = (p >= 0) & (p < self.total)
        qv = (q >= 0) & (q < self.total)

        @pl.when(pv & has_l)
        def _():
            self.wait_l(g, p, jr)

        @pl.when(qv & has_r)
        def _():
            self.wait_r(g, q, jl)

        @pl.when(pv & (jr > i))
        def _():
            sl = self.rows_of(g, p)

            @pl.when(has_l)
            def _():
                own[jr, sl] = (own[jr, sl].astype(f32) + from_l[jr, sl].astype(f32)).astype(bf16)

            self.right(own, from_l, g, p, jr).start()

        @pl.when(qv & (jl < i))
        def _():
            sl = self.rows_of(g, q)

            @pl.when(has_r)
            def _():
                own[jl, sl] = (own[jl, sl].astype(f32) + from_r[jl, sl].astype(f32)).astype(bf16)

            self.left(own, from_r, g, q, jl).start()

        @pl.when(pv & (jr == i))
        def _():
            sl = self.rows_of(g, p)

            @pl.when(has_l & has_r)
            def _():
                res[i, sl] = (
                    own[i, sl].astype(f32) + from_l[i, sl].astype(f32) + from_r[i, sl].astype(f32)
                ).astype(bf16)

            @pl.when(jnp.logical_not(has_l))
            def _():
                res[i, sl] = (own[i, sl].astype(f32) + from_r[i, sl].astype(f32)).astype(bf16)

            @pl.when(jnp.logical_not(has_r))
            def _():
                res[i, sl] = (own[i, sl].astype(f32) + from_l[i, sl].astype(f32)).astype(bf16)

        @pl.when(pv & (jr <= i) & has_r)
        def _():
            self.right(res, res, g, p, jr).start()

        @pl.when(qv & (jl >= i) & has_l)
        def _():
            self.left(res, res, g, q, jl).start()

    def drain(self):
        @pl.when(self.has_r)
        def _():
            remote(
                self.own, self.from_l, self.send_r, self.recv_l.at[0, 0], {"tp": self.i + 1}
            ).wait_send()

        @pl.when(self.has_l)
        def _():
            remote(
                self.own, self.from_r, self.send_l, self.recv_r.at[0, 0], {"tp": self.i - 1}
            ).wait_send()

    def ship(self, out_ref, sems, base, start, count):
        return load_list(
            [
                (
                    self.res.at[j, pl.ds(start, count)],
                    out_ref.at[:, pl.ds(j * self.part, self.part)],
                )
                for j in range(self.n)
            ],
            sems, base,
        )


class GradScatter:
    def __init__(self, n_ctx, n_seq, width, jobs, orders=("xy", "yx")):
        self.nx, self.ny = n_ctx // 2, n_seq
        self.rows = width // (n_ctx * n_seq)
        self.jobs, self.orders = jobs, orders
        start = 0
        self.spans = []
        for job in jobs:
            self.spans.append((start, start + job["count"]))
            start += job["count"]
        self.total = start
        self.steps = start + 5

    def out_shapes(self, widths):
        flips = {job["out"] for job in self.jobs if job["flip"]}
        return [
            ((w, self.rows) if i in flips else (self.rows, w), f32) for i, w in enumerate(widths)
        ]

    def sizes(self, order):
        return (self.nx, self.ny) if order == "xy" else (self.ny, self.nx)

    def scratch(self):
        nx, ny, t = self.nx, self.ny, self.total
        tile = (self.rows, lanes)
        sem = pltpu.SemaphoreType.DMA
        out = [
            pltpu.VMEM((2, nx, ny, 2) + tile, bf16),
            pltpu.VMEM((2, nx, ny, 2) + tile, f32),
            pltpu.VMEM((t, nx, ny, 2) + tile, bf16),
            sem((2,)), sem((t,)),
        ]
        for order in self.orders:
            n1, n2 = self.sizes(order)
            out += [
                pltpu.VMEM((3, n1, n2) + tile, bf16),
                pltpu.VMEM((t, n1 - 1, n2) + tile, bf16),
                pltpu.VMEM((3, n2) + tile, bf16),
                pltpu.VMEM((t, n2 - 1) + tile, bf16),
                sem((3, n1 - 1)), sem((t, n1 - 1)), sem((3, n2 - 1)), sem((t, n2 - 1)),
            ]
        return out

    def bind(self, refs, at_refs, b_refs, out_refs):
        self.send0, self.keep, self.recv0, self.s0, self.d0 = refs[:5]
        self.half = [refs[5 + 8 * h : 13 + 8 * h] for h in range(2)]
        self.at_refs, self.b_refs, self.out_refs = at_refs, b_refs, out_refs
        ctx = lax.axis_index("ctx")
        self.mx, self.core, self.my = ctx // 2, lax.rem(ctx, 2), lax.axis_index("seq")

    def axis(self, name, d):
        if name == "x":
            to = lax.rem(self.mx + d, self.nx)
            return to, {"ctx": to * 2 + self.core}
        to = lax.rem(self.my + d, self.ny)
        return to, {"seq": to}

    def at_mate(self):
        return {"ctx": self.mx * 2 + 1 - self.core}

    def greet(self, bar):
        places = [self.at_mate()]
        places += [self.axis("x", d)[1] for d in range(1, self.nx)]
        places += [self.axis("y", d)[1] for d in range(1, self.ny)]
        for place in places:
            pl.semaphore_signal(bar, inc=1, device_id=place, device_id_type=MESH)
        return len(places)

    def c0(self, c):
        slot = lax.rem(c, 2)
        return remote(
            self.send0.at[slot], self.recv0.at[c], self.s0.at[slot], self.d0.at[c], self.at_mate()
        )

    def c1(self, h, c, d):
        p, r1, _, _, sent, done, _, _ = self.half[h]
        to, where = self.axis(self.orders[h][0], d)
        slot = lax.rem(c, 3)
        return remote(p.at[slot, to], r1.at[c, d - 1], sent.at[slot, d - 1], done.at[c, d - 1], where)

    def c2(self, h, c, d):
        _, _, q, r2, _, _, sent, done = self.half[h]
        to, where = self.axis(self.orders[h][1], d)
        slot = lax.rem(c, 3)
        return remote(q.at[slot, to], r2.at[c, d - 1], sent.at[slot, d - 1], done.at[c, d - 1], where)

    def make(self, c):
        slot = lax.rem(c, 2)
        nx, ny, r = self.nx, self.ny, self.rows

        @pl.when(c >= 2)
        def _():
            self.c0(c).wait_send()

        def products(at_ref, b_ref, col, parity, write):
            def tile(e, carry):
                x, y = e // ny, lax.rem(e, ny)
                row = pl.multiple_of(((x * 2 + parity) * ny + y) * r, r)
                acc = jnp.dot(
                    at_ref[pl.ds(row, r), :], b_ref[:, pl.ds(col, 2 * lanes)],
                    preferred_element_type=f32,
                )
                write(x, y, acc)
                return carry

            lax.fori_loop(0, nx * ny, tile, 0)

        def to_send(x, y, acc):
            self.send0[slot, x, y, 0] = acc[:, :lanes].astype(bf16)
            self.send0[slot, x, y, 1] = acc[:, lanes:].astype(bf16)

        def to_keep(x, y, acc):
            self.keep[slot, x, y, 0] = acc[:, :lanes]
            self.keep[slot, x, y, 1] = acc[:, lanes:]

        for job, (lo, hi) in zip(self.jobs, self.spans):

            @pl.when((c >= lo) & (c < hi))
            def _():
                at_ref, b_ref = self.at_refs[job["a"]], self.b_refs[job["b"]]
                col = pl.multiple_of((c - lo + job["first"]) * (2 * lanes), 2 * lanes)
                products(at_ref, b_ref, col, 1 - self.core, to_send)
                self.c0(c).start()
                products(at_ref, b_ref, col, self.core, to_keep)

    def pair(self, c):
        slot, two = lax.rem(c, 3), lax.rem(c, 2)

        @pl.when(c >= 3)
        def _():
            for h in range(2):
                for d in range(1, self.sizes(self.orders[h])[0]):
                    self.c1(h, c, d).wait_send()

        self.c0(c).wait_recv()
        for h, order in enumerate(self.orders):
            p = self.half[h][0]
            for x in range(self.nx):
                for y in range(self.ny):
                    spot = (x, y) if order == "xy" else (y, x)
                    p[(slot,) + spot] = (
                        self.keep[two, x, y, h] + self.recv0[c, x, y, h].astype(f32)
                    ).astype(bf16)
            for d in range(1, self.sizes(order)[0]):
                self.c1(h, c, d).start()

    def own(self, name):
        return self.mx if name == "x" else self.my

    def cross(self, c):
        slot = lax.rem(c, 3)

        @pl.when(c >= 3)
        def _():
            for h in range(2):
                for d in range(1, self.sizes(self.orders[h])[1]):
                    self.c2(h, c, d).wait_send()

        for h, order in enumerate(self.orders):
            n1, n2 = self.sizes(order)
            p, r1, q = self.half[h][:3]
            for d in range(1, n1):
                self.c1(h, c, d).wait_recv()
            for e in range(n2):
                acc = p[slot, self.own(order[0]), e].astype(f32)
                for d in range(1, n1):
                    acc = acc + r1[c, d - 1, e].astype(f32)
                q[slot, e] = acc.astype(bf16)
            for d in range(1, n2):
                self.c2(h, c, d).start()

    def finish(self, c):
        slot = lax.rem(c, 3)
        totals = []
        for h, order in enumerate(self.orders):
            n2 = self.sizes(order)[1]
            q, r2 = self.half[h][2:4]
            for d in range(1, n2):
                self.c2(h, c, d).wait_recv()
            acc = q[slot, self.own(order[1])].astype(f32)
            for d in range(1, n2):
                acc = acc + r2[c, d - 1].astype(f32)
            totals.append(acc)
        for job, (lo, hi) in zip(self.jobs, self.spans):

            @pl.when((c >= lo) & (c < hi))
            def _():
                out_ref = self.out_refs[job["out"]]
                col = pl.multiple_of((c - lo + job["place"]) * (2 * lanes), 2 * lanes)
                for h in range(2):
                    place = pl.ds(col + h * lanes, lanes)
                    if job["flip"]:
                        out_ref[place, :] = jnp.transpose(totals[h])
                    else:
                        out_ref[:, place] = totals[h]

    def tick(self, it):
        @pl.when((it >= 5) & (it < self.total + 5))
        def _():
            self.finish(it - 5)

        @pl.when((it >= 3) & (it < self.total + 3))
        def _():
            self.cross(it - 3)

        @pl.when((it >= 1) & (it < self.total + 1))
        def _():
            self.pair(it - 1)

        @pl.when(it < self.total)
        def _():
            self.make(it)

    def drain(self):
        for c in range(max(self.total - 2, 0), self.total):
            self.c0(c).wait_send()
        for c in range(max(self.total - 3, 0), self.total):
            for h, order in enumerate(self.orders):
                n1, n2 = self.sizes(order)
                for d in range(1, n1):
                    self.c1(h, c, d).wait_send()
                for d in range(1, n2):
                    self.c2(h, c, d).wait_send()


class GainSum:
    def __init__(self, n_ctx, n_seq, rows):
        self.ny, self.n, self.rows = n_seq, n_ctx * n_seq, rows

    def scratch(self):
        sem = pltpu.SemaphoreType.DMA
        return [pltpu.VMEM((self.n - 1, self.rows, lanes), f32), sem((self.n - 1,)), sem((self.n - 1,))]

    def bind(self, refs, in_ref, out_ref):
        self.got, self.sent, self.done = refs
        self.in_ref, self.out_ref = in_ref, out_ref
        self.me = lax.axis_index("ctx") * self.ny + lax.axis_index("seq")

    def place(self, d):
        to = lax.rem(self.me + d, self.n)
        return {"ctx": to // self.ny, "seq": lax.rem(to, self.ny)}

    def copy(self, d):
        return remote(
            self.in_ref, self.got.at[d - 1], self.sent.at[d - 1], self.done.at[d - 1], self.place(d)
        )

    def greet(self, bar):
        for d in range(1, self.n):
            pl.semaphore_signal(bar, inc=1, device_id=self.place(d), device_id_type=MESH)
        return self.n - 1

    def start(self):
        for d in range(1, self.n):
            self.copy(d).start()

    def finish(self):
        acc = self.in_ref[...]
        for d in range(1, self.n):
            self.copy(d).wait_recv()
            acc = acc + self.got[d - 1]
        self.out_ref[...] = acc
        for d in range(1, self.n):
            self.copy(d).wait_send()


def vmem_spec():
    return pl.BlockSpec(memory_space=pltpu.VMEM)


def comm_call(body, args, outs, scratch, cid, name, scalars=()):
    return pl.pallas_call(
        body,
        out_shape=outs,
        in_specs=[
            pl.BlockSpec(memory_space=pltpu.SMEM) if i in scalars else vmem_spec()
            for i in range(len(args))
        ],
        out_specs=[vmem_spec()] * len(outs),
        scratch_shapes=scratch,
        compiler_params=pltpu.CompilerParams(
            collective_id=cid, has_side_effects=True, vmem_limit_bytes=62 * 2**20
        ),
        name=name,
    )(*args)


class LineSmall:
    def __init__(self, n, rows):
        self.n, self.rows = n, rows

    def scratch(self):
        sem = pltpu.SemaphoreType.DMA
        return [
            pltpu.VMEM((8, self.rows), f32), pltpu.VMEM((self.n - 1, 8, self.rows), f32),
            sem((self.n - 1,)), sem((self.n - 1,)),
        ]

    def bind(self, refs):
        self.mine, self.got, self.sent, self.done = refs
        self.i = lax.axis_index("tp")

    def greet(self, bar):
        for d in range(1, self.n):
            pl.semaphore_signal(
                bar, inc=1, device_id={"tp": lax.rem(self.i + d, self.n)}, device_id_type=MESH
            )
        return self.n - 1

    def copy(self, d):
        return remote(
            self.mine, self.got.at[d - 1], self.sent.at[d - 1], self.done.at[d - 1],
            {"tp": lax.rem(self.i + d, self.n)},
        )

    def total(self, columns):
        self.mine[...] = jnp.transpose(columns)[:8]
        for d in range(1, self.n):
            self.copy(d).start()
        acc = self.mine[...]
        for d in range(1, self.n):
            self.copy(d).wait_recv()
            acc = acc + self.got[d - 1]
        for d in range(1, self.n):
            self.copy(d).wait_send()
        return jnp.transpose(jnp.concatenate([acc, jnp.zeros((lanes - 8, self.rows), f32)], axis=0))


def lane_pair(first, second, rows):
    lane = lax.broadcasted_iota(jnp.int32, (rows, lanes), 1)
    return jnp.where(lane == 0, first, 0.0) + jnp.where(lane == 1, second, 0.0)


def dot_nt(left, right):
    return lax.dot_general(left, right, (((1,), (1,)), ((), ())), preferred_element_type=f32)


def dot_tn(left, right):
    return lax.dot_general(left, right, (((0,), (0,)), ((), ())), preferred_element_type=f32)


def attention_back(
    back, grad, proj, attn_gain, w_output, query_rot, keys, values, attn, lse, pos_row, order,
    query_norm, key_norm, scales, qgain, kgain, cosine, sine, ats, bs, jobs, widths, cid,
):
    rows, width = back.shape
    local = w_output.shape[0]
    head_dim = lanes
    heads = local // head_dim
    count = keys.shape[0]
    nx, n_tp = lax.axis_size("ctx") // 2, lax.axis_size("tp")
    small = LineSmall(n_tp, rows)
    n_small = len(small.scratch())
    scale = head_dim ** (-0.5)
    tile = 64
    sub = rows // 2
    na, nb, n_out = len(ats), len(bs), len(widths)
    grads = None
    if jobs:
        grads = GradScatter(2 * nx, lax.axis_size("seq"), width, jobs, ("yx", "yx"))

    def body(
        back_ref, grad_ref, proj_ref, again_ref, w_ref, q_ref, k_ref, v_ref, attn_ref, lse_ref,
        prow_ref, order_ref, qn_ref, kn_ref, sc_ref, qg_ref, kg_ref, cos_ref, sin_ref, *rest,
    ):
        at_refs, b_refs, rest = rest[:na], rest[na : na + nb], rest[na + nb :]
        dqkv_ref, dprojt_ref, dagain_ref, dqg_ref, dkg_ref = rest[:5]
        grad_outs, rest = rest[5 : 5 + n_out], rest[5 + n_out :]
        (dproj, dout, columns, delta, dqs, dks, send0, keep, recv0, recv1, s0, d0, s1, d1) = rest[:14]
        small.bind(rest[14 : 14 + n_small])
        if jobs:
            grads.bind(rest[14 + n_small :], at_refs, b_refs, grad_outs)

        def tick(it):
            if jobs:
                grads.tick(it)

        ctx = lax.axis_index("ctx")
        mx, core = ctx // 2, lax.rem(ctx, 2)
        bar = pltpu.get_barrier_semaphore()
        mate = {"ctx": mx * 2 + 1 - core}
        if jobs:
            peers = small.greet(bar) + grads.greet(bar)
        else:
            peers = small.greet(bar) + nx
            pl.semaphore_signal(bar, inc=1, device_id=mate, device_id_type=MESH)
            for d in range(1, nx):
                pl.semaphore_signal(
                    bar, inc=1, device_id={"ctx": lax.rem(mx + d, nx) * 2 + core},
                    device_id_type=MESH,
                )
        pl.semaphore_wait(bar, peers)
        tick(jnp.int32(0))

        dagain_ref[...] = jnp.zeros_like(dagain_ref)

        def norm_rows(t, carry):
            sl = pl.ds(pl.multiple_of(t * tile, tile), tile)
            dres = grad_ref[sl].astype(f32) + back_ref[sl].astype(f32)
            out = proj_ref[sl].astype(f32)
            inv = lax.rsqrt(jnp.mean(out * out, axis=1, keepdims=True) + norm_eps)
            norm = out * inv
            dagain_ref[...] += jnp.sum(dres * norm, axis=0, keepdims=True)
            dnorm = dres * again_ref[...]
            dot = jnp.mean(dnorm * norm, axis=1, keepdims=True)
            dproj[sl] = (inv * (dnorm - norm * dot)).astype(bf16)
            return carry

        lax.fori_loop(0, rows // tile, norm_rows, 0)
        for h in range(local // sub):
            dout[:, h * sub : (h + 1) * sub] = dot_nt(
                dproj[...], w_ref[h * sub : (h + 1) * sub, :]
            ).astype(bf16)
        lane = lax.broadcasted_iota(jnp.int32, (rows, lanes), 1)
        acc = jnp.zeros((rows, lanes), f32)
        for h in range(heads):
            hs = slice(h * head_dim, (h + 1) * head_dim)
            row_sum = jnp.sum(
                dout[:, hs].astype(f32) * attn_ref[:, hs].astype(f32), axis=1, keepdims=True
            )
            acc = jnp.where(lane == h, row_sum, acc)
        columns[...] = acc
        delta[...] = jnp.transpose(columns[...])[:8]
        dqs[...] = jnp.zeros_like(dqs)

        def c0(h):
            slot = lax.rem(h, 2)
            return remote(send0.at[slot], recv0.at[h], s0.at[slot], d0.at[h], mate)

        def c1(h, d):
            to = lax.rem(mx + d, nx)
            return remote(
                recv0.at[h, to], recv1.at[h, d - 1], s1.at[h, d - 1], d1.at[h, d - 1],
                {"ctx": to * 2 + core},
            )

        def one_block(h, hs, x, owner, write):
            start = (x * 2 + owner) * rows

            def one_part(part, carry):
                ks = pl.ds(pl.multiple_of(start + part * sub, sub), sub)
                key, value = k_ref[ks, hs], v_ref[ks, hs]
                query, dhead = q_ref[:, hs], dout[:, hs]
                score = dot_nt(key, query) * scale
                place = order_ref[0, (x * 2 + owner) * 2 + part] * sub
                seen = place + lax.broadcasted_iota(jnp.int32, (sub, rows), 0) <= prow_ref[...]
                share = jnp.where(seen, jnp.exp(score - lse_ref[pl.ds(h, 1), :]), 0.0)
                dshare = dot_nt(value, dhead)
                dscore = share * (dshare - delta[pl.ds(h, 1), :]) * scale
                high = dscore.astype(bf16)
                low = (dscore - high.astype(f32)).astype(bf16)
                dqs[:, hs] += dot_tn(high, key) + dot_tn(low, key)
                write(
                    x, pl.ds(pl.multiple_of(part * sub, sub), sub),
                    jnp.dot(high, query, preferred_element_type=f32)
                    + jnp.dot(low, query, preferred_element_type=f32),
                    jnp.dot(share.astype(bf16), dhead, preferred_element_type=f32),
                )
                return carry

            lax.fori_loop(0, rows // sub, one_part, 0)

        def one_head(h):
            hs = pl.ds(pl.multiple_of(h * head_dim, head_dim), head_dim)
            slot = lax.rem(h, 2)

            def to_send(x, rs, dk, dv):
                send0[slot, x, rs, :lanes] = dk.astype(bf16)
                send0[slot, x, rs, lanes:] = dv.astype(bf16)

            def to_keep(x, rs, dk, dv):
                keep[slot, x, rs, :lanes] = dk.astype(bf16)
                keep[slot, x, rs, lanes:] = dv.astype(bf16)

            @pl.when(h >= 2)
            def _():
                c0(h).wait_send()

            def mates(e, carry):
                one_block(h, hs, lax.rem(mx + 1 + e, nx), 1 - core, to_send)
                return carry

            lax.fori_loop(0, nx, mates, 0)
            c0(h).start()
            tick(2 * h + 1)

            def owns(e, carry):
                one_block(h, hs, lax.rem(mx + 1 + e, nx), core, to_keep)
                return carry

            lax.fori_loop(0, nx, owns, 0)
            c0(h).wait_recv()

            def add(x, carry):
                recv0[h, x] = (keep[slot, x].astype(f32) + recv0[h, x].astype(f32)).astype(bf16)
                return carry

            lax.fori_loop(0, nx, add, 0)
            for d in range(1, nx):
                c1(h, d).start()
            tick(2 * h + 2)

        def heads_loop(h, carry):
            one_head(h)
            return carry

        lax.fori_loop(0, heads, heads_loop, 0)
        if jobs:

            def more(it, carry):
                grads.tick(it)
                return carry

            lax.fori_loop(2 * heads + 1, grads.steps, more, 0)

        dot_q = jnp.zeros((rows, 1), f32)
        for h in range(heads):
            hs = slice(h * head_dim, (h + 1) * head_dim)
            dq = dqs[:, hs]
            dq = dq * cos_ref[...] - pltpu.roll(dq, head_dim // 2, 1) * sin_ref[...]
            norm = qn_ref[:, hs]
            dqg_ref[:, hs] = jnp.sum(dq * norm, axis=0, keepdims=True)
            dq = dq * qg_ref[:, hs]
            dqs[:, hs] = dq
            dot_q = dot_q + jnp.sum(dq * norm, axis=1, keepdims=True)
        dprojt_ref[...] = jnp.transpose(dproj[...])
        dot_k = jnp.zeros((rows, 1), f32)
        for h in range(heads):
            hs = slice(h * head_dim, (h + 1) * head_dim)
            total = recv0[h, mx].astype(f32)
            for d in range(1, nx):
                c1(h, d).wait_recv()
                total = total + recv1[h, d - 1].astype(f32)
            dqkv_ref[:, 2 * local + h * head_dim : 2 * local + (h + 1) * head_dim] = total[
                :, lanes:
            ].astype(bf16)
            dk = total[:, :lanes]
            dk = dk * cos_ref[...] - pltpu.roll(dk, head_dim // 2, 1) * sin_ref[...]
            norm = kn_ref[:, hs]
            dkg_ref[:, hs] = jnp.sum(dk * norm, axis=0, keepdims=True)
            dk = dk * kg_ref[:, hs]
            dks[:, hs] = dk
            dot_k = dot_k + jnp.sum(dk * norm, axis=1, keepdims=True)
        dots = small.total(lane_pair(dot_q, dot_k, rows)) * (1.0 / width)
        for h in range(heads):
            hs = slice(h * head_dim, (h + 1) * head_dim)
            dqkv_ref[:, hs] = (
                sc_ref[:, 0:1] * (dqs[:, hs] - qn_ref[:, hs] * dots[:, 0:1])
            ).astype(bf16)
            dqkv_ref[:, local + h * head_dim : local + (h + 1) * head_dim] = (
                sc_ref[:, 1:2] * (dks[:, hs] - kn_ref[:, hs] * dots[:, 1:2])
            ).astype(bf16)
        for h in range(heads):
            if h >= heads - 2:
                c0(h).wait_send()
            for d in range(1, nx):
                c1(h, d).wait_send()
        if jobs:
            grads.drain()

    sem = pltpu.SemaphoreType.DMA
    pair = (rows, 2 * lanes)
    return comm_call(
        body,
        [back, grad, proj, attn_gain, w_output, query_rot, keys, values, attn, lse, pos_row,
         order, query_norm, key_norm, scales, qgain, kgain, cosine, sine] + ats + bs,
        [
            jax.ShapeDtypeStruct((rows, 3 * local), bf16),
            jax.ShapeDtypeStruct((width, rows), bf16),
            jax.ShapeDtypeStruct((1, width), f32),
            jax.ShapeDtypeStruct((1, local), f32),
            jax.ShapeDtypeStruct((1, local), f32),
        ] + [jax.ShapeDtypeStruct(*out) for out in (grads.out_shapes(widths) if jobs else [])],
        [
            pltpu.VMEM((rows, width), bf16), pltpu.VMEM((rows, local), bf16),
            pltpu.VMEM((rows, lanes), f32), pltpu.VMEM((8, rows), f32),
            pltpu.VMEM((rows, local), f32), pltpu.VMEM((rows, local), f32),
            pltpu.VMEM((2, nx) + pair, bf16), pltpu.VMEM((2, nx) + pair, bf16),
            pltpu.VMEM((heads, nx) + pair, bf16), pltpu.VMEM((heads, nx - 1) + pair, bf16),
            sem((2,)), sem((heads,)), sem((heads, nx - 1)), sem((heads, nx - 1)),
        ] + small.scratch() + (grads.scratch() if jobs else []),
        cid, "attention_back", {11},
    )


def front(tokens, w_query, w_key, w_value, qgain, kgain, cosine, sine, order, cid):
    rows, width = tokens.shape
    local = w_query.shape[1]
    head_dim = lanes
    heads = local // head_dim
    nx = lax.axis_size("ctx") // 2
    count = nx * 2 * rows
    n_tp = lax.axis_size("tp")
    small = LineSmall(n_tp, rows)
    n_small = len(small.scratch())
    scale = head_dim ** (-0.5)
    group = rows // 2

    def body(
        tok_hbm, wq_hbm, wk_hbm, wv_hbm, qg_ref, kg_ref, cos_ref, sin_ref, order_ref,
        qrot_out, key_out, value_out, qn_out, kn_out, attn_out, tokt_out, sc_out, lse_out,
        tok, tokt, w3, qn, kn, qrot, keys, values, peak, total, acc, attn, loads, stores,
        sx, dx, sm, dm, sf, df, *rest,
    ):
        small.bind(rest[:n_small])
        copies = [
            pltpu.make_async_copy(src, dst, loads.at[i])
            for i, (src, dst) in enumerate(
                [(tok_hbm, tok), (wv_hbm, w3.at[2]), (wq_hbm, w3.at[0]), (wk_hbm, w3.at[1])]
            )
        ]
        for copy in copies:
            copy.start()
        ctx = lax.axis_index("ctx")
        mx, core = ctx // 2, lax.rem(ctx, 2)
        mate = {"ctx": mx * 2 + 1 - core}

        def peer(d):
            return {"ctx": lax.rem(mx + d, nx) * 2 + core}

        bar = pltpu.get_barrier_semaphore()
        pl.semaphore_signal(bar, inc=1, device_id=mate, device_id_type=MESH)
        for d in range(1, nx):
            pl.semaphore_signal(bar, inc=1, device_id=peer(d), device_id_type=MESH)
        peers = small.greet(bar) + nx

        def at(x, owner):
            return pl.ds(pl.multiple_of((x * 2 + owner) * rows, rows), rows)

        mine = at(mx, core)
        side = local // 2
        boxes = [(keys, pl.ds(0, side)), (keys, pl.ds(side, side)), (values, pl.ds(0, local))]

        def move(t, rs, sent, done, where):
            box, cols = boxes[t]
            return remote(box.at[rs, cols], box.at[rs, cols], sent, done, where)

        def to_peer(t, d):
            return move(t, mine, sx.at[t, d - 1], dx.at[t, d - 1], peer(d))

        def from_peer(t, d):
            rs = at(lax.rem(mx + nx - d, nx), core)
            return move(t, rs, sx.at[t, d - 1], dx.at[t, d - 1], peer(d))

        def to_mate(t):
            return move(t, mine, sm.at[t], dm.at[t], mate)

        def from_mate(t):
            return move(t, at(mx, 1 - core), sm.at[t], dm.at[t], mate)

        def pass_on(t, d):
            rs = at(lax.rem(mx + nx - d, nx), core)
            return move(t, rs, sf.at[t, d - 1], df.at[t, d - 1], mate)

        def passed(t, d):
            rs = at(lax.rem(mx + nx - d, nx), 1 - core)
            return move(t, rs, sf.at[t, d - 1], df.at[t, d - 1], mate)

        def each_peer(act):
            def one(d, carry):
                act(d)
                return carry

            lax.fori_loop(1, nx, one, 0)

        copies[0].wait()
        copies[1].wait()
        values[mine] = jnp.dot(tok[...], w3[2], preferred_element_type=f32).astype(bf16)
        pl.semaphore_wait(bar, peers)
        each_peer(lambda d: to_peer(2, d).start())
        to_mate(2).start()
        copies[2].wait()
        qn[...] = jnp.dot(tok[...], w3[0], preferred_element_type=f32)
        copies[3].wait()
        kn[...] = jnp.dot(tok[...], w3[1], preferred_element_type=f32)

        def squares(ref):
            acc_sq = jnp.zeros((rows, 1), f32)
            for h in range(heads):
                part = ref[:, h * head_dim : (h + 1) * head_dim]
                acc_sq = acc_sq + jnp.sum(part * part, axis=1, keepdims=True)
            return acc_sq

        sums = small.total(lane_pair(squares(qn), squares(kn), rows))
        scales = lax.rsqrt(sums * (1.0 / width) + norm_eps)
        sc_out[...] = scales

        def rotated(ref, column, gain_ref, h):
            hs = slice(h * head_dim, (h + 1) * head_dim)
            norm = ref[:, hs] * sc_out[:, column : column + 1]
            ref[:, hs] = norm
            norm = norm * gain_ref[:, hs]
            return (
                norm * cos_ref[...] + pltpu.roll(norm, head_dim // 2, 1) * sin_ref[...]
            ).astype(bf16)

        for h in range(heads):
            keys[mine, h * head_dim : (h + 1) * head_dim] = rotated(kn, 1, kg_ref, h)
            if (h + 1) * head_dim in (side, local):
                t = (h + 1) * head_dim // side - 1
                each_peer(lambda d: to_peer(t, d).start())
                to_mate(t).start()
        for h in range(heads):
            qrot[:, h * head_dim : (h + 1) * head_dim] = rotated(qn, 0, qg_ref, h)
        peak[...] = jnp.full_like(peak, masked_score)
        total[...] = jnp.zeros_like(total)
        acc[...] = jnp.zeros_like(acc)

        def places(block, shape, axis):
            spot = lax.broadcasted_iota(jnp.int32, shape, axis)
            first, second = order_ref[0, block * 2], order_ref[0, block * 2 + 1]
            return jnp.where(spot < group, first * group + spot, (second - 1) * group + spot)

        def attend(x, owner, low, high):
            block = x * 2 + owner
            rs = at(x, owner)

            def one(h, carry):
                hs = pl.ds(pl.multiple_of(h * head_dim, head_dim), head_dim)
                score = dot_nt(qrot[:, hs], keys[rs, hs]) * scale
                seen = places(block, (1, rows), 1) <= places(ctx, (rows, 1), 0)
                old = peak[h]
                new = jnp.maximum(
                    old, jnp.max(jnp.where(seen, score, masked_score), axis=1, keepdims=True)
                )
                share = jnp.where(seen, jnp.exp(score - new), 0.0)
                fade = jnp.exp(old - new)
                peak[h] = new
                total[h] = total[h] * fade + jnp.sum(share, axis=1, keepdims=True)
                acc[:, hs] = acc[:, hs] * fade + jnp.dot(
                    share.astype(bf16), values[rs, hs], preferred_element_type=f32
                )
                return carry

            lax.fori_loop(low, high, one, 0)

        attend(mx, core, 0, heads)

        def hand_on(t, d):
            from_peer(t, d).wait_recv()
            pass_on(t, d).start()

        each_peer(lambda d: hand_on(2, d))
        for t in range(3):
            from_mate(t).wait_recv()
        attend(mx, 1 - core, 0, heads)
        tokt[...] = jnp.transpose(tok[...])

        def half_heads(t, carry):
            low, high = t * heads // 2, (t + 1) * heads // 2

            def near(d):
                for v in range(2):

                    @pl.when(t == v)
                    def _():
                        hand_on(v, d)

                attend(lax.rem(mx + nx - d, nx), core, low, high)

            def far(d):
                @pl.when(t == 0)
                def _():
                    passed(2, d).wait_recv()
                    passed(0, d).wait_recv()

                @pl.when(t == 1)
                def _():
                    passed(1, d).wait_recv()

                attend(lax.rem(mx + nx - d, nx), 1 - core, low, high)

            each_peer(near)
            each_peer(far)
            return carry

        lax.fori_loop(0, 2, half_heads, 0)

        lane = lax.broadcasted_iota(jnp.int32, (rows, lanes), 1)
        logs = jnp.zeros((rows, lanes), f32)
        for h in range(heads):
            hs = slice(h * head_dim, (h + 1) * head_dim)
            attn[:, hs] = (acc[:, hs] / total[h]).astype(bf16)
            logs = jnp.where(lane == h, peak[h] + jnp.log(total[h]), logs)
        lse_out[...] = jnp.transpose(logs)[:8]
        outs = [
            pltpu.make_async_copy(src, dst, stores.at[i])
            for i, (src, dst) in enumerate(
                [(qrot, qrot_out), (keys, key_out), (values, value_out), (qn, qn_out),
                 (kn, kn_out), (attn, attn_out), (tokt, tokt_out)]
            )
        ]
        for copy in outs:
            copy.start()
        for copy in outs:
            copy.wait()
        for t in range(3):
            to_mate(t).wait_send()

            def sent(d):
                to_peer(t, d).wait_send()
                pass_on(t, d).wait_send()

            each_peer(sent)

    sem = pltpu.SemaphoreType.DMA
    hbm = pl.BlockSpec(memory_space=pl.ANY)
    block = jax.ShapeDtypeStruct
    return pl.pallas_call(
        body,
        out_shape=[
            block((rows, local), bf16), block((count, local), bf16), block((count, local), bf16),
            block((rows, local), f32), block((rows, local), f32), block((rows, local), bf16),
            block((width, rows), bf16),
            block((rows, lanes), f32), block((8, rows), f32),
        ],
        in_specs=[hbm] * 4 + [vmem_spec()] * 4 + [pl.BlockSpec(memory_space=pltpu.SMEM)],
        out_specs=[hbm] * 7 + [vmem_spec()] * 2,
        scratch_shapes=[
            pltpu.VMEM((rows, width), bf16), pltpu.VMEM((width, rows), bf16),
            pltpu.VMEM((3, width, local), bf16),
            pltpu.VMEM((rows, local), f32),
            pltpu.VMEM((rows, local), f32), pltpu.VMEM((rows, local), bf16),
            pltpu.VMEM((count, local), bf16), pltpu.VMEM((count, local), bf16),
            pltpu.VMEM((heads, rows, 1), f32), pltpu.VMEM((heads, rows, 1), f32),
            pltpu.VMEM((rows, local), f32), pltpu.VMEM((rows, local), bf16),
            sem((4,)), sem((7,)),
            sem((3, nx - 1)), sem((3, nx - 1)), sem((3,)), sem((3,)),
            sem((3, nx - 1)), sem((3, nx - 1)),
        ] + small.scratch(),
        compiler_params=pltpu.CompilerParams(
            collective_id=cid, has_side_effects=True, vmem_limit_bytes=62 * 2**20
        ),
        name="front",
    )(tokens, w_query, w_key, w_value, qgain, kgain, cosine, sine, order)


def load_list(pairs, sems, base=0):
    copies = [
        pltpu.make_async_copy(src, dst, sems.at[base + i]) for i, (src, dst) in enumerate(pairs)
    ]
    for copy in copies:
        copy.start()
    return copies


def kernel_call(body, args, kinds, outs, out_kinds, scratch, cid, name):
    spec = {
        "v": vmem_spec(),
        "h": pl.BlockSpec(memory_space=pl.ANY),
        "s": pl.BlockSpec(memory_space=pltpu.SMEM),
    }
    return pl.pallas_call(
        body,
        out_shape=[jax.ShapeDtypeStruct(*out) for out in outs],
        in_specs=[spec[kind] for kind in kinds],
        out_specs=[spec[kind] for kind in out_kinds],
        scratch_shapes=scratch,
        compiler_params=pltpu.CompilerParams(
            collective_id=cid, has_side_effects=True, vmem_limit_bytes=62 * 2**20
        ),
        name=name,
    )(*args)


def middle(attn, tokens, attn_gain, w_output, w_gate, w_up, w_down, cid):
    rows, width = tokens.shape
    local, wide = w_output.shape[0], w_gate.shape[1]
    n_tp = lax.axis_size("tp")
    line = LineSum(n_tp, 2 * rows, width, 4 * row_chains)
    n_line = len(line.scratch())
    half = rows // 2
    tile = 64
    cut = 512
    n_cut = wide // cut
    part = line.part

    def body(
        attn_hbm, tok_hbm, again_ref, wo_hbm, wg_hbm, wu_hbm, wd_hbm,
        proj_out, hidt_out, gate_out, up_out, inner_out, down_out, inv_out,
        attn_v, tok, wo, hid, hidt, gate, up, inner, wg, wu, wd, first, loads, stores, *rest,
    ):
        line.bind(rest[:n_line])
        start = load_list([(attn_hbm, attn_v), (wo_hbm, wo), (tok_hbm, tok)], first)

        def load(src, dst, j, size, spot):
            cols = pl.ds(pl.multiple_of(j * size, size), size)
            return pltpu.make_async_copy(src.at[:, cols], dst.at[j], loads.at[spot])

        def gate_load(j):
            return load(wg_hbm, wg, j, cut, 2 * j)

        def up_load(j):
            return load(wu_hbm, wu, j, cut, 2 * j + 1)

        def down_load(j):
            return load(wd_hbm, wd, j, part, 2 * n_cut + j)

        for j in range(n_cut):
            gate_load(j).start()
            up_load(j).start()
        for j in range(n_tp):
            down_load(j).start()
        bar = pltpu.get_barrier_semaphore()
        peers = line.greet(bar)
        for copy in start:
            copy.wait()

        def project(j, carry):
            cols = pl.ds(pl.multiple_of(j * part, part), part)
            line.own[j, :rows] = jnp.dot(
                attn_v[...], wo[:, cols], preferred_element_type=f32
            ).astype(bf16)
            return carry

        lax.fori_loop(0, n_tp, project, 0)
        pl.semaphore_wait(bar, peers)

        def step(t, carry):
            line.step(t)

            @pl.when(t == 3 * n_tp + 1)
            def _():
                hidt[...] = jnp.transpose(hid[...])

            return carry

        def row_half(c, carry):
            base = pl.multiple_of(c * half, half)
            sl = pl.ds(base, half)
            lax.fori_loop(c * 2 * n_tp, c * n_tp + 2 * n_tp - 1, step, 0)

            def norm_rows(t, carry):
                rs = pl.ds(pl.multiple_of(base + t * tile, tile), tile)
                outs = [line.res[j, rs].astype(f32) for j in range(n_tp)]
                square = sum(jnp.sum(out * out, axis=1, keepdims=True) for out in outs)
                inv = lax.rsqrt(square * (1.0 / width) + norm_eps)
                inv_out[rs, :] = inv
                for j, out in enumerate(outs):
                    cols = slice(j * part, (j + 1) * part)
                    hid[rs, cols] = (
                        tok[rs, cols].astype(f32) + out * inv * again_ref[:, cols]
                    ).astype(bf16)
                return carry

            lax.fori_loop(0, half // tile, norm_rows, 0)
            per = row_chains // n_cut

            def widen(j, carry):
                cols = pl.ds(pl.multiple_of(j * cut, cut), cut)

                @pl.when(c == 0)
                def _():
                    gate_load(j).wait()
                    up_load(j).wait()

                g = jnp.dot(hid[sl], wg[j], preferred_element_type=f32)
                u = jnp.dot(hid[sl], wu[j], preferred_element_type=f32)
                gate[sl, cols] = g.astype(bf16)
                up[sl, cols] = u.astype(bf16)
                inner[sl, cols] = (g * jax.nn.sigmoid(g) * u).astype(bf16)
                line.pieces(((c + 2) * n_tp - 1) * row_chains + j * per, per)
                return carry

            lax.fori_loop(0, n_cut, widen, 0)
            line.pieces(((c + 2) * n_tp - 1) * row_chains + n_cut * per, row_chains - n_cut * per)

            def narrow(j, carry):
                @pl.when(c == 0)
                def _():
                    down_load(j).wait()

                line.own[j, pl.ds(rows + base, half)] = jnp.dot(
                    inner[sl], wd[j], preferred_element_type=f32
                ).astype(bf16)
                return carry

            lax.fori_loop(0, n_tp, narrow, 0)
            return carry

        lax.fori_loop(0, 2, row_half, 0)
        outs = load_list([(gate, gate_out), (up, up_out), (inner, inner_out)], stores)
        ready = line.ship(proj_out, stores, 4, 0, rows)
        lax.fori_loop(3 * n_tp, line.steps, step, 0)
        last = pltpu.make_async_copy(hidt, hidt_out, stores.at[3])
        last.start()
        ready = ready + line.ship(down_out, stores, 4 + n_tp, rows, rows)
        line.drain()
        for copy in outs + [last] + ready:
            copy.wait()

    sem = pltpu.SemaphoreType.DMA
    return kernel_call(
        body, [attn, tokens, attn_gain, w_output, w_gate, w_up, w_down], "hhvhhhh",
        [((rows, width), bf16), ((width, rows), bf16), ((rows, wide), bf16), ((rows, wide), bf16),
         ((rows, wide), bf16), ((rows, width), bf16), ((rows, 1), f32)],
        "hhhhhhv",
        [
            pltpu.VMEM((rows, local), bf16), pltpu.VMEM((rows, width), bf16),
            pltpu.VMEM((local, width), bf16),
            pltpu.VMEM((rows, width), bf16), pltpu.VMEM((width, rows), bf16),
            pltpu.VMEM((rows, wide), bf16), pltpu.VMEM((rows, wide), bf16),
            pltpu.VMEM((rows, wide), bf16),
            pltpu.VMEM((n_cut, width, cut), bf16), pltpu.VMEM((n_cut, width, cut), bf16),
            pltpu.VMEM((n_tp, wide, part), bf16),
            sem((3,)), sem((2 * n_cut + n_tp,)), sem((4 + 2 * n_tp,)),
        ] + line.scratch(),
        cid, "middle",
    )


def mlp_back(down, grad, mlp_gain, gate, up, inner, hid_t, w_gate, w_up, w_down, jobs, widths, cid):
    rows, width = down.shape
    wide = gate.shape[1]
    n_tp = lax.axis_size("tp")
    line = LineSum(n_tp, rows, width)
    grads = GradScatter(lax.axis_size("ctx"), lax.axis_size("seq"), width, jobs)
    n_line, n_grads, n_out = len(line.scratch()), len(grads.scratch()), len(widths)
    tile = 64
    cut = 512
    n_cut = wide // cut
    part = line.part
    lead = row_chains * n_tp // (n_cut + n_tp)
    ticks = n_cut // 2 + n_tp // 2

    def body(
        down_hbm, grad_hbm, mgain_ref, gate_hbm, up_hbm, inner_hbm, hidt_hbm, wg_hbm, wu_hbm, wd_hbm,
        back_out, dgate_out, dup_out, dgain_out, inv_out, *rest,
    ):
        grad_outs, rest = rest[:n_out], rest[n_out:]
        (gate_v, up_v, inner_v, hidt, ddown, ddownt, dgate, dup, ring, loads, wsem, stores) = rest[:12]
        line.bind(rest[12 : 12 + n_line])
        grads.bind(rest[12 + n_line :], [ddownt, hidt], [inner_v, dgate, dup], grad_outs)

        def fetch(src, index):
            return pltpu.make_async_copy(src, ring.at[index], wsem.at[index])

        def rows_of(ref, j, size):
            return ref.at[pl.ds(pl.multiple_of(j * size, size), size)]

        for j in range(4):
            fetch(rows_of(wd_hbm, j, cut), j).start()
        down_ref, grad_ref = dgate.at[:, pl.ds(0, width)], dup.at[:, pl.ds(0, width)]
        first = load_list([(down_hbm, down_ref), (grad_hbm, grad_ref)], loads, 4)
        early = load_list(
            [(inner_hbm, inner_v), (gate_hbm, gate_v), (up_hbm, up_v), (hidt_hbm, hidt)], loads
        )
        bar = pltpu.get_barrier_semaphore()
        peers = line.greet(bar) + grads.greet(bar)
        dgain_out[...] = jnp.zeros_like(dgain_out)
        for copy in first:
            copy.wait()

        def norm_rows(t, carry):
            sl = pl.ds(pl.multiple_of(t * tile, tile), tile)
            out = down_ref[sl].astype(f32)
            upstream = grad_ref[sl].astype(f32)
            inv = lax.rsqrt(jnp.mean(out * out, axis=1, keepdims=True) + norm_eps)
            norm = out * inv
            inv_out[sl, :] = inv
            dgain_out[...] += jnp.sum(upstream * norm, axis=0, keepdims=True)
            dnorm = upstream * mgain_ref[...]
            dot = jnp.mean(dnorm * norm, axis=1, keepdims=True)
            ddown[sl] = (inv * (dnorm - norm * dot)).astype(bf16)
            return carry

        lax.fori_loop(0, rows // tile, norm_rows, 0)
        ddownt[...] = jnp.transpose(ddown[...])
        for copy in early:
            copy.wait()
        pl.semaphore_wait(bar, peers)

        half = rows // 2

        def row_half(c, carry):
            sl = pl.ds(pl.multiple_of(c * half, half), half)

            def beside(i, j, first):
                @pl.when(c == 1)
                def _():
                    line.pieces(i * lead, lead)

                @pl.when(lax.rem(j, 2) == 1)
                def _():
                    grads.tick(first + j // 2)

            def inner_back(j, carry):
                fetch(rows_of(wd_hbm, j, cut), j).wait()
                cols = pl.ds(pl.multiple_of(j * cut, cut), cut)
                dmix = dot_nt(ddown[sl], ring[j])
                g, u = gate_v[sl, cols].astype(f32), up_v[sl, cols].astype(f32)
                sig = jax.nn.sigmoid(g)
                dgate[sl, cols] = (dmix * u * sig * (1.0 + g * (1.0 - sig))).astype(bf16)
                dup[sl, cols] = (dmix * (g * sig)).astype(bf16)

                @pl.when(lax.rem(j, 2) == 0)
                def _():
                    fetch(rows_of(wg_hbm, j // 2, part), j).start()

                @pl.when(lax.rem(j, 2) == 1)
                def _():
                    fetch(rows_of(wu_hbm, j // 2, part), j).start()

                beside(j, j, c * ticks)
                return carry

            lax.fori_loop(0, n_cut, inner_back, 0)

            def hidden_back(j, carry):
                slot = lax.rem(2 * j, 4)
                fetch(rows_of(wg_hbm, j, part), slot).wait()
                fetch(rows_of(wu_hbm, j, part), slot + 1).wait()
                line.own[j, sl] = (
                    dot_nt(dgate[sl], ring[slot]) + dot_nt(dup[sl], ring[slot + 1])
                ).astype(bf16)

                @pl.when(j + 2 < n_tp)
                def _():
                    fetch(rows_of(wg_hbm, j + 2, part), slot).start()
                    fetch(rows_of(wu_hbm, j + 2, part), slot + 1).start()

                @pl.when((j + 2 >= n_tp) & (c == 0))
                def _():
                    fetch(rows_of(wd_hbm, slot, cut), slot).start()
                    fetch(rows_of(wd_hbm, slot + 1, cut), slot + 1).start()

                beside(n_cut + j, j, c * ticks + n_cut // 2)
                return carry

            lax.fori_loop(0, n_tp, hidden_back, 0)
            return carry

        lax.fori_loop(0, 2, row_half, 0)
        outs = load_list([(dgate, dgate_out), (dup, dup_out)], stores)
        done, used = 2 * ticks, (n_cut + n_tp) * lead

        def one(it, carry):
            line.pieces(used + (it - done) * pace, pace)
            grads.tick(it)
            return carry

        line_its = -(-(line.steps * row_chains - used) // pace)
        lax.fori_loop(done, max(done + line_its, grads.steps), one, 0)
        outs += line.ship(back_out, stores, 2, 0, rows)
        line.drain()
        grads.drain()
        for copy in outs:
            copy.wait()

    sem = pltpu.SemaphoreType.DMA
    return kernel_call(
        body, [down, grad, mlp_gain, gate, up, inner, hid_t, w_gate, w_up, w_down], "hhvhhhhhhh",
        [((rows, width), bf16), ((rows, wide), bf16), ((rows, wide), bf16), ((1, width), f32),
         ((rows, 1), f32)]
        + grads.out_shapes(widths),
        "hhhvv" + "v" * n_out,
        [
            pltpu.VMEM((rows, wide), bf16), pltpu.VMEM((rows, wide), bf16),
            pltpu.VMEM((rows, wide), bf16), pltpu.VMEM((width, rows), bf16),
            pltpu.VMEM((rows, width), bf16), pltpu.VMEM((width, rows), bf16),
            pltpu.VMEM((rows, wide), bf16), pltpu.VMEM((rows, wide), bf16),
            pltpu.VMEM((4, cut, width), bf16),
            sem((6,)), sem((4,)), sem((2 + n_tp,)),
        ] + line.scratch() + grads.scratch(),
        cid, "mlp_back",
    )


def last_sums(dqkv, w_query, w_key, w_value, ats, bs, jobs, widths, gains, cid):
    rows = dqkv.shape[0]
    width, local = w_query.shape
    n_ctx, n_seq = lax.axis_size("ctx"), lax.axis_size("seq")
    n_tp = lax.axis_size("tp")
    line = LineSum(n_tp, rows, width)
    grads = GradScatter(n_ctx, n_seq, width, jobs)
    small = GainSum(n_ctx, n_seq, gains.shape[0])
    na, nb, n_out = len(ats), len(bs), len(widths)
    n_line, n_grads = len(line.scratch()), len(grads.scratch())
    part = line.part

    def body(dqkv_ref, wq_ref, wk_ref, wv_ref, *refs):
        at_refs, b_refs = refs[:na], refs[na : na + nb]
        gain_ref, last_out = refs[na + nb], refs[na + nb + 1]
        refs = refs[na + nb + 2 :]
        grad_outs, gain_out, stores, scratch = refs[:n_out], refs[n_out], refs[n_out + 1], refs[n_out + 2 :]
        line.bind(scratch[:n_line])
        grads.bind(scratch[n_line : n_line + n_grads], at_refs, list(b_refs) + [dqkv_ref], grad_outs)
        small.bind(scratch[n_line + n_grads :], gain_ref, gain_out)
        bar = pltpu.get_barrier_semaphore()
        peers = line.greet(bar) + small.greet(bar)
        pl.semaphore_wait(bar, peers)
        small.start()

        def input_back(j, carry):
            rs = pl.ds(pl.multiple_of(j * part, part), part)
            line.own[j] = (
                dot_nt(dqkv_ref[:, :local], wq_ref[rs])
                + dot_nt(dqkv_ref[:, local : 2 * local], wk_ref[rs])
                + dot_nt(dqkv_ref[:, 2 * local :], wv_ref[rs])
            ).astype(bf16)

            @pl.when(lax.rem(j, 2) == 0)
            def _():
                grads.tick(j // 2)

            return carry

        lax.fori_loop(0, n_tp, input_back, 0)
        done = n_tp // 2

        def one(it, carry):
            grads.tick(it)
            line.pieces((it - done) * pace, pace)
            return carry

        line_steps = -(-line.steps * row_chains // pace)
        lax.fori_loop(done, max(done + line_steps, grads.steps), one, 0)
        small.finish()
        outs = line.ship(last_out, stores, 0, 0, rows)
        line.drain()
        grads.drain()
        for copy in outs:
            copy.wait()

    sem = pltpu.SemaphoreType.DMA
    return kernel_call(
        body, [dqkv, w_query, w_key, w_value] + list(ats) + list(bs) + [gains],
        "vvvv" + "v" * (na + nb + 1),
        [((rows, width), bf16)] + grads.out_shapes(widths) + [(gains.shape, f32)],
        "h" + "v" * (n_out + 1),
        [sem((n_tp,))] + line.scratch() + grads.scratch() + small.scratch(),
        cid, "last_sums",
    )


def row_tiles(body, args, outs, name):
    count = 8

    def spec(shape):
        if shape[0] == 1:
            return pl.BlockSpec(shape, lambda i: (0, 0))
        return pl.BlockSpec((shape[0] // count, shape[1]), lambda i: (i, 0))

    def whole(*refs):
        body(refs[: len(args)], refs[len(args) :])

    return pl.pallas_call(
        whole,
        grid=(count,),
        out_shape=[jax.ShapeDtypeStruct(shape, f32) for shape in outs],
        in_specs=[spec(arg.shape) for arg in args],
        out_specs=[spec(shape) for shape in outs],
        compiler_params=pltpu.CompilerParams(vmem_limit_bytes=62 * 2**20),
        name=name,
    )(*args)


def block_tile(ins, outs):
    x, a, ra, ga, d, rd, gd = [ref[...].astype(f32) for ref in ins[:7]]
    outs[0][...] = x + (a * ra) * ga + (d * rd) * gd
    for src, dst in zip(ins[7:], outs[1:]):
        dst[...] = src[...]


def input_tile(ins, outs):
    outs[0][...] = ins[0][...].astype(f32) + ins[1][...].astype(f32) + ins[2][...].astype(f32)
    outs[1][...] = ins[3][...]
    outs[2][...] = ins[4][...]
    size = outs[3].shape[1]
    for i in range(3):
        outs[3 + i][...] = ins[5][:, i * size : (i + 1) * size]


def per_device(
    tokens,
    out_grad,
    group_order,
    w_query,
    w_key,
    w_value,
    query_gain,
    key_gain,
    w_output,
    attn_gain,
    w_gate,
    w_up,
    w_down,
    mlp_gain,
):
    inputs = tokens[0]
    upstream = out_grad[0]
    rows, width = inputs.shape
    heads, head_dim = query_gain.shape
    local = heads * head_dim
    wide = w_gate.shape[1]
    positions = key_positions(group_order[0], lax.axis_index("ctx") * rows, rows, rows // 2)
    angle_cos, angle_sin = rope_tables(positions, head_dim)
    qgain = query_gain.reshape(1, local)
    kgain = key_gain.reshape(1, local)
    (query_rot, keys, values, query_norm, key_norm, attn, tokens_t, scales, lse) = front(
        inputs, w_query, w_key, w_value, qgain, kgain, angle_cos, angle_sin, group_order, 1
    )
    proj, hidden_t, gate, up, inner, down, proj_scale = middle(
        attn, inputs, attn_gain[None], w_output, w_gate, w_up, w_down, 2
    )
    chunk_cols = 2 * lanes
    chunks = wide // chunk_cols
    thin = local // chunk_cols
    back, d_gate, d_up, d_mlp_gain, down_scale, grad_down, grad_gate = mlp_back(
        down, upstream, mlp_gain[None], gate, up, inner, hidden_t, w_gate, w_up, w_down,
        [
            dict(a=0, b=0, first=0, count=chunks, out=0, place=0, flip=True),
            dict(a=1, b=1, first=0, count=chunks, out=1, place=0, flip=False),
        ],
        [wide, wide],
        3,
    )
    d_qkv, d_proj_t, d_attn_gain, d_query_gain, d_key_gain = attention_back(
        back, upstream, proj, attn_gain[None], w_output, query_rot, keys, values, attn, lse,
        positions[None], group_order, query_norm, key_norm, scales, qgain, kgain, angle_cos,
        angle_sin, [], [], [], [], 4,
    )
    owners = lax.axis_size("ctx") * lax.axis_size("seq")
    gains = [d_attn_gain, d_mlp_gain, d_query_gain, d_key_gain]
    ends = [gain.shape[1] for gain in gains]
    ends = [sum(ends[: i + 1]) for i in range(4)]
    packed = jnp.concatenate(gains, axis=1).reshape(-1, lanes)
    last, grad_up, grad_qkv, grad_output, small = last_sums(
        d_qkv, w_query, w_key, w_value,
        [hidden_t, tokens_t, d_proj_t],
        [d_up, attn],
        [
            dict(a=0, b=0, first=0, count=chunks, out=0, place=0, flip=False),
            dict(a=2, b=1, first=0, count=thin, out=2, place=0, flip=True),
            dict(a=1, b=2, first=0, count=3 * thin, out=1, place=0, flip=False),
        ],
        [wide, 3 * local, local],
        packed,
        5,
    )
    small = small.reshape(-1)
    me = lax.axis_index("ctx") * lax.axis_size("seq") + lax.axis_index("seq")

    def my_part(start, end, lead):
        whole = small[start:end].reshape(lead, -1)
        size = whole.shape[1] // owners
        return lax.dynamic_slice_in_dim(whole, me * size, size, 1)

    g_attn = my_part(0, ends[0], 1)[0]
    g_mlp = my_part(ends[0], ends[1], 1)[0]
    g_query = my_part(ends[1], ends[2], heads)
    g_key = my_part(ends[2], ends[3], heads)
    block_out, grad_down, grad_gate = row_tiles(
        block_tile,
        [inputs, proj, proj_scale, attn_gain[None], down, down_scale, mlp_gain[None], grad_down,
         grad_gate],
        [inputs.shape, grad_down.shape, grad_gate.shape], "block_out",
    )
    own = grad_qkv.shape[0]
    input_grad, grad_up, grad_output, grad_query, grad_key, grad_value = row_tiles(
        input_tile, [upstream, back, last, grad_up, grad_output, grad_qkv],
        [inputs.shape, grad_up.shape, grad_output.shape] + [(own, local)] * 3, "input_grad",
    )
    return (
        block_out[None],
        input_grad[None],
        grad_query,
        grad_key,
        grad_value,
        g_query,
        g_key,
        grad_output,
        g_attn,
        grad_gate,
        grad_up,
        grad_down,
        g_mlp,
    )


def solution(mesh):
    return jax.shard_map(
        per_device,
        mesh=mesh,
        in_specs=(
            P("seq", "ctx", None),
            P("seq", "ctx", None),
            P("seq", None),
            P(None, "tp"),
            P(None, "tp"),
            P(None, "tp"),
            P("tp", None),
            P("tp", None),
            P("tp", None),
            P(),
            P(None, "tp"),
            P(None, "tp"),
            P("tp", None),
            P(),
        ),
        out_specs=(
            P("seq", "ctx", None),
            P("seq", "ctx", None),
            P(("ctx", "seq"), "tp"),
            P(("ctx", "seq"), "tp"),
            P(("ctx", "seq"), "tp"),
            P("tp", ("ctx", "seq")),
            P("tp", ("ctx", "seq")),
            P("tp", ("ctx", "seq")),
            P(("ctx", "seq")),
            P(("ctx", "seq"), "tp"),
            P(("ctx", "seq"), "tp"),
            P("tp", ("ctx", "seq")),
            P(("ctx", "seq")),
        ),
        check_vma=False,
    )
```

```python
import jax
import jax.numpy as jnp
from jax import lax
from jax.sharding import PartitionSpec as P
from jax.experimental import pallas as pl
from jax.experimental.pallas import tpu as pltpu

norm_eps = 1e-06
rope_base = 500000.0
masked_score = -1e30


def rope_tables(positions, head_dim):
    half = head_dim // 2
    channel = jnp.arange(head_dim, dtype=jnp.int32)
    rates = rope_base ** (-((channel % half).astype(jnp.float32) * 2.0 / head_dim))
    angle = positions.astype(jnp.float32)[:, None] * rates[None, :]
    return jnp.cos(angle), jnp.where(channel[None, :] < half, -jnp.sin(angle), jnp.sin(angle))


def key_positions(order, first_row, count, group):
    row_ids = first_row + jnp.arange(count, dtype=jnp.int32)
    slots = row_ids // group
    picks = slots[:, None] == jnp.arange(order.shape[0], dtype=jnp.int32)[None, :]
    return jnp.sum(jnp.where(picks, order[None, :], 0), axis=1) * group + row_ids % group


MESH = pl.DeviceIdType.MESH
bf16 = jnp.bfloat16
f32 = jnp.float32
lanes = 128
row_blocks = 16
row_chains = 8
pace = 6


def remote(src, dst, send, recv, where):
    return pltpu.make_async_remote_copy(
        src, dst, send, recv, device_id=where, device_id_type=MESH
    )


class LineSum:
    def __init__(self, n, rows, width, blocks=row_blocks):
        self.n, self.rows, self.width = n, rows, width
        self.part = width // n
        self.rc = rows // blocks
        self.total = blocks // row_chains * n
        self.steps = self.total + n - 1

    def scratch(self):
        shape = (self.n, self.rows, self.part)
        return (
            [pltpu.VMEM(shape, bf16)] * 4
            + [pltpu.SemaphoreType.DMA] * 2
            + [pltpu.SemaphoreType.DMA((row_chains, self.total))] * 2
        )

    def bind(self, refs):
        self.own, self.from_l, self.from_r, self.res = refs[:4]
        self.send_r, self.send_l, self.recv_l, self.recv_r = refs[4:]
        self.i = lax.axis_index("tp")
        self.has_l, self.has_r = self.i > 0, self.i < self.n - 1

    def greet(self, bar):
        @pl.when(self.has_l)
        def _():
            pl.semaphore_signal(bar, inc=1, device_id={"tp": self.i - 1}, device_id_type=MESH)

        @pl.when(self.has_r)
        def _():
            pl.semaphore_signal(bar, inc=1, device_id={"tp": self.i + 1}, device_id_type=MESH)

        return self.has_l.astype(jnp.int32) + self.has_r.astype(jnp.int32)

    def load(self, x_ref):
        for j in range(self.n):
            self.own[j] = x_ref[:, j * self.part : (j + 1) * self.part]

    def rows_of(self, g, p):
        block = (p // self.n) * row_chains + g
        return pl.ds(pl.multiple_of(block * self.rc, self.rc), self.rc)

    def right(self, src, dst, g, p, j):
        sl = self.rows_of(g, p)
        return remote(
            src.at[j, sl], dst.at[j, sl], self.send_r, self.recv_l.at[g, p],
            {"tp": self.i + 1},
        )

    def left(self, src, dst, g, q, j):
        sl = self.rows_of(g, q)
        return remote(
            src.at[j, sl], dst.at[j, sl], self.send_l, self.recv_r.at[g, q],
            {"tp": self.i - 1},
        )

    def wait_l(self, g, p, j):
        sl = self.rows_of(g, p)
        remote(
            self.own.at[j, sl], self.from_l.at[j, sl], self.send_r, self.recv_l.at[g, p],
            {"tp": self.i - 1},
        ).wait_recv()

    def wait_r(self, g, q, j):
        sl = self.rows_of(g, q)
        remote(
            self.own.at[j, sl], self.from_r.at[j, sl], self.send_l, self.recv_r.at[g, q],
            {"tp": self.i + 1},
        ).wait_recv()

    def step(self, t):
        self.pieces(t * row_chains, row_chains)

    def pieces(self, first, count):
        def one(v, carry):
            self.piece(first + v)
            return carry

        lax.fori_loop(0, count, one, 0)

    def piece(self, e):
        t = e // row_chains

        @pl.when(t < self.steps)
        def _():
            self.sub_step(t, lax.rem(e, row_chains))

    def sub_step(self, t, g):
        n, i, has_l, has_r = self.n, self.i, self.has_l, self.has_r
        own, from_l, from_r, res = self.own, self.from_l, self.from_r, self.res
        p = t - i
        q = t - (n - 1 - i)
        jr = n - 1 - lax.rem(p + n * self.total, n)
        jl = lax.rem(q + n * self.total, n)
        pv = (p >= 0) & (p < self.total)
        qv = (q >= 0) & (q < self.total)

        @pl.when(pv & has_l)
        def _():
            self.wait_l(g, p, jr)

        @pl.when(qv & has_r)
        def _():
            self.wait_r(g, q, jl)

        @pl.when(pv & (jr > i))
        def _():
            sl = self.rows_of(g, p)

            @pl.when(has_l)
            def _():
                own[jr, sl] = (own[jr, sl].astype(f32) + from_l[jr, sl].astype(f32)).astype(bf16)

            self.right(own, from_l, g, p, jr).start()

        @pl.when(qv & (jl < i))
        def _():
            sl = self.rows_of(g, q)

            @pl.when(has_r)
            def _():
                own[jl, sl] = (own[jl, sl].astype(f32) + from_r[jl, sl].astype(f32)).astype(bf16)

            self.left(own, from_r, g, q, jl).start()

        @pl.when(pv & (jr == i))
        def _():
            sl = self.rows_of(g, p)

            @pl.when(has_l & has_r)
            def _():
                res[i, sl] = (
                    own[i, sl].astype(f32) + from_l[i, sl].astype(f32) + from_r[i, sl].astype(f32)
                ).astype(bf16)

            @pl.when(jnp.logical_not(has_l))
            def _():
                res[i, sl] = (own[i, sl].astype(f32) + from_r[i, sl].astype(f32)).astype(bf16)

            @pl.when(jnp.logical_not(has_r))
            def _():
                res[i, sl] = (own[i, sl].astype(f32) + from_l[i, sl].astype(f32)).astype(bf16)

        @pl.when(pv & (jr <= i) & has_r)
        def _():
            self.right(res, res, g, p, jr).start()

        @pl.when(qv & (jl >= i) & has_l)
        def _():
            self.left(res, res, g, q, jl).start()

    def drain(self):
        @pl.when(self.has_r)
        def _():
            remote(
                self.own, self.from_l, self.send_r, self.recv_l.at[0, 0], {"tp": self.i + 1}
            ).wait_send()

        @pl.when(self.has_l)
        def _():
            remote(
                self.own, self.from_r, self.send_l, self.recv_r.at[0, 0], {"tp": self.i - 1}
            ).wait_send()

    def ship(self, out_ref, sems, base, start, count):
        return load_list(
            [
                (
                    self.res.at[j, pl.ds(start, count)],
                    out_ref.at[:, pl.ds(j * self.part, self.part)],
                )
                for j in range(self.n)
            ],
            sems, base,
        )


class GradScatter:
    def __init__(self, n_ctx, n_seq, width, jobs, orders=("xy", "yx")):
        self.nx, self.ny = n_ctx // 2, n_seq
        self.rows = width // (n_ctx * n_seq)
        self.jobs, self.orders = jobs, orders
        start = 0
        self.spans = []
        for job in jobs:
            self.spans.append((start, start + job["count"]))
            start += job["count"]
        self.total = start
        self.steps = start + 5

    def out_shapes(self, widths):
        flips = {job["out"] for job in self.jobs if job["flip"]}
        return [
            ((w, self.rows) if i in flips else (self.rows, w), f32) for i, w in enumerate(widths)
        ]

    def sizes(self, order):
        return (self.nx, self.ny) if order == "xy" else (self.ny, self.nx)

    def scratch(self):
        nx, ny, t = self.nx, self.ny, self.total
        tile = (self.rows, lanes)
        sem = pltpu.SemaphoreType.DMA
        out = [
            pltpu.VMEM((2, nx, ny, 2) + tile, bf16),
            pltpu.VMEM((2, nx, ny, 2) + tile, f32),
            pltpu.VMEM((t, nx, ny, 2) + tile, bf16),
            sem((2,)), sem((t,)),
        ]
        for order in self.orders:
            n1, n2 = self.sizes(order)
            out += [
                pltpu.VMEM((3, n1, n2) + tile, bf16),
                pltpu.VMEM((t, n1 - 1, n2) + tile, bf16),
                pltpu.VMEM((3, n2) + tile, bf16),
                pltpu.VMEM((t, n2 - 1) + tile, bf16),
                sem((3, n1 - 1)), sem((t, n1 - 1)), sem((3, n2 - 1)), sem((t, n2 - 1)),
            ]
        return out

    def bind(self, refs, at_refs, b_refs, out_refs):
        self.send0, self.keep, self.recv0, self.s0, self.d0 = refs[:5]
        self.half = [refs[5 + 8 * h : 13 + 8 * h] for h in range(2)]
        self.at_refs, self.b_refs, self.out_refs = at_refs, b_refs, out_refs
        ctx = lax.axis_index("ctx")
        self.mx, self.core, self.my = ctx // 2, lax.rem(ctx, 2), lax.axis_index("seq")

    def axis(self, name, d):
        if name == "x":
            to = lax.rem(self.mx + d, self.nx)
            return to, {"ctx": to * 2 + self.core}
        to = lax.rem(self.my + d, self.ny)
        return to, {"seq": to}

    def at_mate(self):
        return {"ctx": self.mx * 2 + 1 - self.core}

    def greet(self, bar):
        places = [self.at_mate()]
        places += [self.axis("x", d)[1] for d in range(1, self.nx)]
        places += [self.axis("y", d)[1] for d in range(1, self.ny)]
        for place in places:
            pl.semaphore_signal(bar, inc=1, device_id=place, device_id_type=MESH)
        return len(places)

    def c0(self, c):
        slot = lax.rem(c, 2)
        return remote(
            self.send0.at[slot], self.recv0.at[c], self.s0.at[slot], self.d0.at[c], self.at_mate()
        )

    def c1(self, h, c, d):
        p, r1, _, _, sent, done, _, _ = self.half[h]
        to, where = self.axis(self.orders[h][0], d)
        slot = lax.rem(c, 3)
        return remote(p.at[slot, to], r1.at[c, d - 1], sent.at[slot, d - 1], done.at[c, d - 1], where)

    def c2(self, h, c, d):
        _, _, q, r2, _, _, sent, done = self.half[h]
        to, where = self.axis(self.orders[h][1], d)
        slot = lax.rem(c, 3)
        return remote(q.at[slot, to], r2.at[c, d - 1], sent.at[slot, d - 1], done.at[c, d - 1], where)

    def make(self, c):
        slot = lax.rem(c, 2)
        nx, ny, r = self.nx, self.ny, self.rows

        @pl.when(c >= 2)
        def _():
            self.c0(c).wait_send()

        def products(at_ref, b_ref, col, parity, write):
            def tile(e, carry):
                x, y = e // ny, lax.rem(e, ny)
                row = pl.multiple_of(((x * 2 + parity) * ny + y) * r, r)
                acc = jnp.dot(
                    at_ref[pl.ds(row, r), :], b_ref[:, pl.ds(col, 2 * lanes)],
                    preferred_element_type=f32,
                )
                write(x, y, acc)
                return carry

            lax.fori_loop(0, nx * ny, tile, 0)

        def to_send(x, y, acc):
            self.send0[slot, x, y, 0] = acc[:, :lanes].astype(bf16)
            self.send0[slot, x, y, 1] = acc[:, lanes:].astype(bf16)

        def to_keep(x, y, acc):
            self.keep[slot, x, y, 0] = acc[:, :lanes]
            self.keep[slot, x, y, 1] = acc[:, lanes:]

        for job, (lo, hi) in zip(self.jobs, self.spans):

            @pl.when((c >= lo) & (c < hi))
            def _():
                at_ref, b_ref = self.at_refs[job["a"]], self.b_refs[job["b"]]
                col = pl.multiple_of((c - lo + job["first"]) * (2 * lanes), 2 * lanes)
                products(at_ref, b_ref, col, 1 - self.core, to_send)
                self.c0(c).start()
                products(at_ref, b_ref, col, self.core, to_keep)

    def pair(self, c):
        slot, two = lax.rem(c, 3), lax.rem(c, 2)

        @pl.when(c >= 3)
        def _():
            for h in range(2):
                for d in range(1, self.sizes(self.orders[h])[0]):
                    self.c1(h, c, d).wait_send()

        self.c0(c).wait_recv()
        for h, order in enumerate(self.orders):
            p = self.half[h][0]
            for x in range(self.nx):
                for y in range(self.ny):
                    spot = (x, y) if order == "xy" else (y, x)
                    p[(slot,) + spot] = (
                        self.keep[two, x, y, h] + self.recv0[c, x, y, h].astype(f32)
                    ).astype(bf16)
            for d in range(1, self.sizes(order)[0]):
                self.c1(h, c, d).start()

    def own(self, name):
        return self.mx if name == "x" else self.my

    def cross(self, c):
        slot = lax.rem(c, 3)

        @pl.when(c >= 3)
        def _():
            for h in range(2):
                for d in range(1, self.sizes(self.orders[h])[1]):
                    self.c2(h, c, d).wait_send()

        for h, order in enumerate(self.orders):
            n1, n2 = self.sizes(order)
            p, r1, q = self.half[h][:3]
            for d in range(1, n1):
                self.c1(h, c, d).wait_recv()
            for e in range(n2):
                acc = p[slot, self.own(order[0]), e].astype(f32)
                for d in range(1, n1):
                    acc = acc + r1[c, d - 1, e].astype(f32)
                q[slot, e] = acc.astype(bf16)
            for d in range(1, n2):
                self.c2(h, c, d).start()

    def finish(self, c):
        slot = lax.rem(c, 3)
        totals = []
        for h, order in enumerate(self.orders):
            n2 = self.sizes(order)[1]
            q, r2 = self.half[h][2:4]
            for d in range(1, n2):
                self.c2(h, c, d).wait_recv()
            acc = q[slot, self.own(order[1])].astype(f32)
            for d in range(1, n2):
                acc = acc + r2[c, d - 1].astype(f32)
            totals.append(acc)
        for job, (lo, hi) in zip(self.jobs, self.spans):

            @pl.when((c >= lo) & (c < hi))
            def _():
                out_ref = self.out_refs[job["out"]]
                col = pl.multiple_of((c - lo + job["place"]) * (2 * lanes), 2 * lanes)
                for h in range(2):
                    place = pl.ds(col + h * lanes, lanes)
                    if job["flip"]:
                        out_ref[place, :] = jnp.transpose(totals[h])
                    else:
                        out_ref[:, place] = totals[h]

    def tick(self, it):
        @pl.when((it >= 5) & (it < self.total + 5))
        def _():
            self.finish(it - 5)

        @pl.when((it >= 3) & (it < self.total + 3))
        def _():
            self.cross(it - 3)

        @pl.when((it >= 1) & (it < self.total + 1))
        def _():
            self.pair(it - 1)

        @pl.when(it < self.total)
        def _():
            self.make(it)

    def drain(self):
        for c in range(max(self.total - 2, 0), self.total):
            self.c0(c).wait_send()
        for c in range(max(self.total - 3, 0), self.total):
            for h, order in enumerate(self.orders):
                n1, n2 = self.sizes(order)
                for d in range(1, n1):
                    self.c1(h, c, d).wait_send()
                for d in range(1, n2):
                    self.c2(h, c, d).wait_send()


class GainSum:
    def __init__(self, n_ctx, n_seq, rows):
        self.ny, self.n, self.rows = n_seq, n_ctx * n_seq, rows

    def scratch(self):
        sem = pltpu.SemaphoreType.DMA
        return [pltpu.VMEM((self.n - 1, self.rows, lanes), f32), sem((self.n - 1,)), sem((self.n - 1,))]

    def bind(self, refs, in_ref, out_ref):
        self.got, self.sent, self.done = refs
        self.in_ref, self.out_ref = in_ref, out_ref
        self.me = lax.axis_index("ctx") * self.ny + lax.axis_index("seq")

    def place(self, d):
        to = lax.rem(self.me + d, self.n)
        return {"ctx": to // self.ny, "seq": lax.rem(to, self.ny)}

    def copy(self, d):
        return remote(
            self.in_ref, self.got.at[d - 1], self.sent.at[d - 1], self.done.at[d - 1], self.place(d)
        )

    def greet(self, bar):
        for d in range(1, self.n):
            pl.semaphore_signal(bar, inc=1, device_id=self.place(d), device_id_type=MESH)
        return self.n - 1

    def start(self):
        for d in range(1, self.n):
            self.copy(d).start()

    def finish(self):
        acc = self.in_ref[...]
        for d in range(1, self.n):
            self.copy(d).wait_recv()
            acc = acc + self.got[d - 1]
        self.out_ref[...] = acc
        for d in range(1, self.n):
            self.copy(d).wait_send()


def vmem_spec():
    return pl.BlockSpec(memory_space=pltpu.VMEM)


def comm_call(body, args, outs, scratch, cid, name, scalars=()):
    return pl.pallas_call(
        body,
        out_shape=outs,
        in_specs=[
            pl.BlockSpec(memory_space=pltpu.SMEM) if i in scalars else vmem_spec()
            for i in range(len(args))
        ],
        out_specs=[vmem_spec()] * len(outs),
        scratch_shapes=scratch,
        compiler_params=pltpu.CompilerParams(
            collective_id=cid, has_side_effects=True, vmem_limit_bytes=62 * 2**20
        ),
        name=name,
    )(*args)


class LineSmall:
    def __init__(self, n, rows):
        self.n, self.rows = n, rows

    def scratch(self):
        sem = pltpu.SemaphoreType.DMA
        return [
            pltpu.VMEM((8, self.rows), f32), pltpu.VMEM((self.n - 1, 8, self.rows), f32),
            sem((self.n - 1,)), sem((self.n - 1,)),
        ]

    def bind(self, refs):
        self.mine, self.got, self.sent, self.done = refs
        self.i = lax.axis_index("tp")

    def greet(self, bar):
        for d in range(1, self.n):
            pl.semaphore_signal(
                bar, inc=1, device_id={"tp": lax.rem(self.i + d, self.n)}, device_id_type=MESH
            )
        return self.n - 1

    def copy(self, d):
        return remote(
            self.mine, self.got.at[d - 1], self.sent.at[d - 1], self.done.at[d - 1],
            {"tp": lax.rem(self.i + d, self.n)},
        )

    def total(self, columns):
        self.mine[...] = jnp.transpose(columns)[:8]
        for d in range(1, self.n):
            self.copy(d).start()
        acc = self.mine[...]
        for d in range(1, self.n):
            self.copy(d).wait_recv()
            acc = acc + self.got[d - 1]
        for d in range(1, self.n):
            self.copy(d).wait_send()
        return jnp.transpose(jnp.concatenate([acc, jnp.zeros((lanes - 8, self.rows), f32)], axis=0))


def lane_pair(first, second, rows):
    lane = lax.broadcasted_iota(jnp.int32, (rows, lanes), 1)
    return jnp.where(lane == 0, first, 0.0) + jnp.where(lane == 1, second, 0.0)


def dot_nt(left, right):
    return lax.dot_general(left, right, (((1,), (1,)), ((), ())), preferred_element_type=f32)


def dot_tn(left, right):
    return lax.dot_general(left, right, (((0,), (0,)), ((), ())), preferred_element_type=f32)


def attention_back(
    back, grad, proj, attn_gain, w_output, query_rot, keys, values, attn, lse, pos_row, order,
    query_norm, key_norm, scales, qgain, kgain, cosine, sine, ats, bs, jobs, widths, cid,
):
    rows, width = back.shape
    local = w_output.shape[0]
    head_dim = lanes
    heads = local // head_dim
    count = keys.shape[0]
    nx, n_tp = lax.axis_size("ctx") // 2, lax.axis_size("tp")
    small = LineSmall(n_tp, rows)
    n_small = len(small.scratch())
    scale = head_dim ** (-0.5)
    tile = 64
    sub = rows // 2
    na, nb, n_out = len(ats), len(bs), len(widths)
    grads = None
    if jobs:
        grads = GradScatter(2 * nx, lax.axis_size("seq"), width, jobs, ("yx", "yx"))

    def body(
        back_ref, grad_ref, proj_ref, again_ref, w_ref, q_ref, k_ref, v_ref, attn_ref, lse_ref,
        prow_ref, order_ref, qn_ref, kn_ref, sc_ref, qg_ref, kg_ref, cos_ref, sin_ref, *rest,
    ):
        at_refs, b_refs, rest = rest[:na], rest[na : na + nb], rest[na + nb :]
        dqkv_ref, dprojt_ref, dagain_ref, dqg_ref, dkg_ref = rest[:5]
        grad_outs, rest = rest[5 : 5 + n_out], rest[5 + n_out :]
        (dproj, dout, columns, delta, dqs, dks, send0, keep, recv0, recv1, s0, d0, s1, d1) = rest[:14]
        small.bind(rest[14 : 14 + n_small])
        if jobs:
            grads.bind(rest[14 + n_small :], at_refs, b_refs, grad_outs)

        def tick(it):
            if jobs:
                grads.tick(it)

        ctx = lax.axis_index("ctx")
        mx, core = ctx // 2, lax.rem(ctx, 2)
        bar = pltpu.get_barrier_semaphore()
        mate = {"ctx": mx * 2 + 1 - core}
        if jobs:
            peers = small.greet(bar) + grads.greet(bar)
        else:
            peers = small.greet(bar) + nx
            pl.semaphore_signal(bar, inc=1, device_id=mate, device_id_type=MESH)
            for d in range(1, nx):
                pl.semaphore_signal(
                    bar, inc=1, device_id={"ctx": lax.rem(mx + d, nx) * 2 + core},
                    device_id_type=MESH,
                )
        pl.semaphore_wait(bar, peers)
        tick(jnp.int32(0))

        dagain_ref[...] = jnp.zeros_like(dagain_ref)

        def norm_rows(t, carry):
            sl = pl.ds(pl.multiple_of(t * tile, tile), tile)
            dres = grad_ref[sl].astype(f32) + back_ref[sl].astype(f32)
            out = proj_ref[sl].astype(f32)
            inv = lax.rsqrt(jnp.mean(out * out, axis=1, keepdims=True) + norm_eps)
            norm = out * inv
            dagain_ref[...] += jnp.sum(dres * norm, axis=0, keepdims=True)
            dnorm = dres * again_ref[...]
            dot = jnp.mean(dnorm * norm, axis=1, keepdims=True)
            dproj[sl] = (inv * (dnorm - norm * dot)).astype(bf16)
            return carry

        lax.fori_loop(0, rows // tile, norm_rows, 0)
        for h in range(local // sub):
            dout[:, h * sub : (h + 1) * sub] = dot_nt(
                dproj[...], w_ref[h * sub : (h + 1) * sub, :]
            ).astype(bf16)
        lane = lax.broadcasted_iota(jnp.int32, (rows, lanes), 1)
        acc = jnp.zeros((rows, lanes), f32)
        for h in range(heads):
            hs = slice(h * head_dim, (h + 1) * head_dim)
            row_sum = jnp.sum(
                dout[:, hs].astype(f32) * attn_ref[:, hs].astype(f32), axis=1, keepdims=True
            )
            acc = jnp.where(lane == h, row_sum, acc)
        columns[...] = acc
        delta[...] = jnp.transpose(columns[...])[:8]
        dqs[...] = jnp.zeros_like(dqs)

        def c0(h):
            slot = lax.rem(h, 2)
            return remote(send0.at[slot], recv0.at[h], s0.at[slot], d0.at[h], mate)

        def c1(h, d):
            to = lax.rem(mx + d, nx)
            return remote(
                recv0.at[h, to], recv1.at[h, d - 1], s1.at[h, d - 1], d1.at[h, d - 1],
                {"ctx": to * 2 + core},
            )

        def one_block(h, hs, x, owner, write):
            start = (x * 2 + owner) * rows
            for part in range(rows // sub):
                ks = pl.ds(pl.multiple_of(start + part * sub, sub), sub)
                key, value = k_ref[ks, hs], v_ref[ks, hs]
                query, dhead = q_ref[:, hs], dout[:, hs]
                score = dot_nt(key, query) * scale
                place = order_ref[0, (x * 2 + owner) * 2 + part] * sub
                seen = place + lax.broadcasted_iota(jnp.int32, (sub, rows), 0) <= prow_ref[...]
                share = jnp.where(seen, jnp.exp(score - lse_ref[pl.ds(h, 1), :]), 0.0)
                dshare = dot_nt(value, dhead)
                dscore = share * (dshare - delta[pl.ds(h, 1), :]) * scale
                high = dscore.astype(bf16)
                low = (dscore - high.astype(f32)).astype(bf16)
                dqs[:, hs] += dot_tn(high, key) + dot_tn(low, key)
                write(
                    x, slice(part * sub, (part + 1) * sub),
                    jnp.dot(high, query, preferred_element_type=f32)
                    + jnp.dot(low, query, preferred_element_type=f32),
                    jnp.dot(share.astype(bf16), dhead, preferred_element_type=f32),
                )

        def one_head(h):
            hs = pl.ds(pl.multiple_of(h * head_dim, head_dim), head_dim)
            slot = lax.rem(h, 2)

            def to_send(x, rs, dk, dv):
                send0[slot, x, rs, :lanes] = dk.astype(bf16)
                send0[slot, x, rs, lanes:] = dv.astype(bf16)

            def to_keep(x, rs, dk, dv):
                keep[slot, x, rs, :lanes] = dk.astype(bf16)
                keep[slot, x, rs, lanes:] = dv.astype(bf16)

            @pl.when(h >= 2)
            def _():
                c0(h).wait_send()

            def mates(e, carry):
                one_block(h, hs, lax.rem(mx + 1 + e, nx), 1 - core, to_send)
                return carry

            lax.fori_loop(0, nx, mates, 0)
            c0(h).start()
            tick(2 * h + 1)

            def owns(e, carry):
                one_block(h, hs, lax.rem(mx + 1 + e, nx), core, to_keep)
                return carry

            lax.fori_loop(0, nx, owns, 0)
            c0(h).wait_recv()

            def add(x, carry):
                recv0[h, x] = (keep[slot, x].astype(f32) + recv0[h, x].astype(f32)).astype(bf16)
                return carry

            lax.fori_loop(0, nx, add, 0)
            for d in range(1, nx):
                c1(h, d).start()
            tick(2 * h + 2)

        def heads_loop(h, carry):
            one_head(h)
            return carry

        lax.fori_loop(0, heads, heads_loop, 0)
        if jobs:

            def more(it, carry):
                grads.tick(it)
                return carry

            lax.fori_loop(2 * heads + 1, grads.steps, more, 0)

        dot_q = jnp.zeros((rows, 1), f32)
        for h in range(heads):
            hs = slice(h * head_dim, (h + 1) * head_dim)
            dq = dqs[:, hs]
            dq = dq * cos_ref[...] - pltpu.roll(dq, head_dim // 2, 1) * sin_ref[...]
            norm = qn_ref[:, hs]
            dqg_ref[:, hs] = jnp.sum(dq * norm, axis=0, keepdims=True)
            dq = dq * qg_ref[:, hs]
            dqs[:, hs] = dq
            dot_q = dot_q + jnp.sum(dq * norm, axis=1, keepdims=True)
        dprojt_ref[...] = jnp.transpose(dproj[...])
        dot_k = jnp.zeros((rows, 1), f32)
        for h in range(heads):
            hs = slice(h * head_dim, (h + 1) * head_dim)
            total = recv0[h, mx].astype(f32)
            for d in range(1, nx):
                c1(h, d).wait_recv()
                total = total + recv1[h, d - 1].astype(f32)
            dqkv_ref[:, 2 * local + h * head_dim : 2 * local + (h + 1) * head_dim] = total[
                :, lanes:
            ].astype(bf16)
            dk = total[:, :lanes]
            dk = dk * cos_ref[...] - pltpu.roll(dk, head_dim // 2, 1) * sin_ref[...]
            norm = kn_ref[:, hs]
            dkg_ref[:, hs] = jnp.sum(dk * norm, axis=0, keepdims=True)
            dk = dk * kg_ref[:, hs]
            dks[:, hs] = dk
            dot_k = dot_k + jnp.sum(dk * norm, axis=1, keepdims=True)
        dots = small.total(lane_pair(dot_q, dot_k, rows)) * (1.0 / width)
        for h in range(heads):
            hs = slice(h * head_dim, (h + 1) * head_dim)
            dqkv_ref[:, hs] = (
                sc_ref[:, 0:1] * (dqs[:, hs] - qn_ref[:, hs] * dots[:, 0:1])
            ).astype(bf16)
            dqkv_ref[:, local + h * head_dim : local + (h + 1) * head_dim] = (
                sc_ref[:, 1:2] * (dks[:, hs] - kn_ref[:, hs] * dots[:, 1:2])
            ).astype(bf16)
        for h in range(heads):
            if h >= heads - 2:
                c0(h).wait_send()
            for d in range(1, nx):
                c1(h, d).wait_send()
        if jobs:
            grads.drain()

    sem = pltpu.SemaphoreType.DMA
    pair = (rows, 2 * lanes)
    return comm_call(
        body,
        [back, grad, proj, attn_gain, w_output, query_rot, keys, values, attn, lse, pos_row,
         order, query_norm, key_norm, scales, qgain, kgain, cosine, sine] + ats + bs,
        [
            jax.ShapeDtypeStruct((rows, 3 * local), bf16),
            jax.ShapeDtypeStruct((width, rows), bf16),
            jax.ShapeDtypeStruct((1, width), f32),
            jax.ShapeDtypeStruct((1, local), f32),
            jax.ShapeDtypeStruct((1, local), f32),
        ] + [jax.ShapeDtypeStruct(*out) for out in (grads.out_shapes(widths) if jobs else [])],
        [
            pltpu.VMEM((rows, width), bf16), pltpu.VMEM((rows, local), bf16),
            pltpu.VMEM((rows, lanes), f32), pltpu.VMEM((8, rows), f32),
            pltpu.VMEM((rows, local), f32), pltpu.VMEM((rows, local), f32),
            pltpu.VMEM((2, nx) + pair, bf16), pltpu.VMEM((2, nx) + pair, bf16),
            pltpu.VMEM((heads, nx) + pair, bf16), pltpu.VMEM((heads, nx - 1) + pair, bf16),
            sem((2,)), sem((heads,)), sem((heads, nx - 1)), sem((heads, nx - 1)),
        ] + small.scratch() + (grads.scratch() if jobs else []),
        cid, "attention_back", {11},
    )


def front(tokens, w_query, w_key, w_value, qgain, kgain, cosine, sine, order, cid):
    rows, width = tokens.shape
    local = w_query.shape[1]
    head_dim = lanes
    heads = local // head_dim
    nx = lax.axis_size("ctx") // 2
    count = nx * 2 * rows
    n_tp = lax.axis_size("tp")
    small = LineSmall(n_tp, rows)
    n_small = len(small.scratch())
    scale = head_dim ** (-0.5)
    group = rows // 2

    def body(
        tok_hbm, wq_hbm, wk_hbm, wv_hbm, qg_ref, kg_ref, cos_ref, sin_ref, order_ref,
        qrot_out, key_out, value_out, qn_out, kn_out, attn_out, tokt_out, sc_out, lse_out,
        tok, tokt, w3, qn, kn, qrot, keys, values, peak, total, acc, attn, loads, stores,
        sx, dx, sm, dm, sf, df, *rest,
    ):
        small.bind(rest[:n_small])
        copies = [
            pltpu.make_async_copy(src, dst, loads.at[i])
            for i, (src, dst) in enumerate(
                [(tok_hbm, tok), (wv_hbm, w3.at[2]), (wq_hbm, w3.at[0]), (wk_hbm, w3.at[1])]
            )
        ]
        for copy in copies:
            copy.start()
        ctx = lax.axis_index("ctx")
        mx, core = ctx // 2, lax.rem(ctx, 2)
        mate = {"ctx": mx * 2 + 1 - core}

        def peer(d):
            return {"ctx": lax.rem(mx + d, nx) * 2 + core}

        bar = pltpu.get_barrier_semaphore()
        pl.semaphore_signal(bar, inc=1, device_id=mate, device_id_type=MESH)
        for d in range(1, nx):
            pl.semaphore_signal(bar, inc=1, device_id=peer(d), device_id_type=MESH)
        peers = small.greet(bar) + nx

        def at(x, owner):
            return pl.ds(pl.multiple_of((x * 2 + owner) * rows, rows), rows)

        mine = at(mx, core)
        side = local // 2
        boxes = [(keys, pl.ds(0, side)), (keys, pl.ds(side, side)), (values, pl.ds(0, local))]

        def move(t, rs, sent, done, where):
            box, cols = boxes[t]
            return remote(box.at[rs, cols], box.at[rs, cols], sent, done, where)

        def to_peer(t, d):
            return move(t, mine, sx.at[t, d - 1], dx.at[t, d - 1], peer(d))

        def from_peer(t, d):
            rs = at(lax.rem(mx + nx - d, nx), core)
            return move(t, rs, sx.at[t, d - 1], dx.at[t, d - 1], peer(d))

        def to_mate(t):
            return move(t, mine, sm.at[t], dm.at[t], mate)

        def from_mate(t):
            return move(t, at(mx, 1 - core), sm.at[t], dm.at[t], mate)

        def pass_on(t, d):
            rs = at(lax.rem(mx + nx - d, nx), core)
            return move(t, rs, sf.at[t, d - 1], df.at[t, d - 1], mate)

        def passed(t, d):
            rs = at(lax.rem(mx + nx - d, nx), 1 - core)
            return move(t, rs, sf.at[t, d - 1], df.at[t, d - 1], mate)

        def each_peer(act):
            def one(d, carry):
                act(d)
                return carry

            lax.fori_loop(1, nx, one, 0)

        copies[0].wait()
        copies[1].wait()
        values[mine] = jnp.dot(tok[...], w3[2], preferred_element_type=f32).astype(bf16)
        pl.semaphore_wait(bar, peers)
        each_peer(lambda d: to_peer(2, d).start())
        to_mate(2).start()
        copies[2].wait()
        qn[...] = jnp.dot(tok[...], w3[0], preferred_element_type=f32)
        copies[3].wait()
        kn[...] = jnp.dot(tok[...], w3[1], preferred_element_type=f32)

        def squares(ref):
            acc_sq = jnp.zeros((rows, 1), f32)
            for h in range(heads):
                part = ref[:, h * head_dim : (h + 1) * head_dim]
                acc_sq = acc_sq + jnp.sum(part * part, axis=1, keepdims=True)
            return acc_sq

        sums = small.total(lane_pair(squares(qn), squares(kn), rows))
        scales = lax.rsqrt(sums * (1.0 / width) + norm_eps)
        sc_out[...] = scales

        def rotated(ref, column, gain_ref, h):
            hs = slice(h * head_dim, (h + 1) * head_dim)
            norm = ref[:, hs] * sc_out[:, column : column + 1]
            ref[:, hs] = norm
            norm = norm * gain_ref[:, hs]
            return (
                norm * cos_ref[...] + pltpu.roll(norm, head_dim // 2, 1) * sin_ref[...]
            ).astype(bf16)

        for h in range(heads):
            keys[mine, h * head_dim : (h + 1) * head_dim] = rotated(kn, 1, kg_ref, h)
            if (h + 1) * head_dim in (side, local):
                t = (h + 1) * head_dim // side - 1
                each_peer(lambda d: to_peer(t, d).start())
                to_mate(t).start()
        for h in range(heads):
            qrot[:, h * head_dim : (h + 1) * head_dim] = rotated(qn, 0, qg_ref, h)
        peak[...] = jnp.full_like(peak, masked_score)
        total[...] = jnp.zeros_like(total)
        acc[...] = jnp.zeros_like(acc)

        def places(block, shape, axis):
            spot = lax.broadcasted_iota(jnp.int32, shape, axis)
            first, second = order_ref[0, block * 2], order_ref[0, block * 2 + 1]
            return jnp.where(spot < group, first * group + spot, (second - 1) * group + spot)

        def attend(x, owner, low, high):
            block = x * 2 + owner
            rs = at(x, owner)

            def one(h, carry):
                hs = pl.ds(pl.multiple_of(h * head_dim, head_dim), head_dim)
                score = dot_nt(qrot[:, hs], keys[rs, hs]) * scale
                seen = places(block, (1, rows), 1) <= places(ctx, (rows, 1), 0)
                old = peak[h]
                new = jnp.maximum(
                    old, jnp.max(jnp.where(seen, score, masked_score), axis=1, keepdims=True)
                )
                share = jnp.where(seen, jnp.exp(score - new), 0.0)
                fade = jnp.exp(old - new)
                peak[h] = new
                total[h] = total[h] * fade + jnp.sum(share, axis=1, keepdims=True)
                acc[:, hs] = acc[:, hs] * fade + jnp.dot(
                    share.astype(bf16), values[rs, hs], preferred_element_type=f32
                )
                return carry

            lax.fori_loop(low, high, one, 0)

        attend(mx, core, 0, heads)

        def hand_on(t, d):
            from_peer(t, d).wait_recv()
            pass_on(t, d).start()

        each_peer(lambda d: hand_on(2, d))
        for t in range(3):
            from_mate(t).wait_recv()
        attend(mx, 1 - core, 0, heads)
        tokt[...] = jnp.transpose(tok[...])

        def half_heads(t, carry):
            low, high = t * heads // 2, (t + 1) * heads // 2

            def near(d):
                for v in range(2):

                    @pl.when(t == v)
                    def _():
                        hand_on(v, d)

                attend(lax.rem(mx + nx - d, nx), core, low, high)

            def far(d):
                @pl.when(t == 0)
                def _():
                    passed(2, d).wait_recv()
                    passed(0, d).wait_recv()

                @pl.when(t == 1)
                def _():
                    passed(1, d).wait_recv()

                attend(lax.rem(mx + nx - d, nx), 1 - core, low, high)

            each_peer(near)
            each_peer(far)
            return carry

        lax.fori_loop(0, 2, half_heads, 0)

        lane = lax.broadcasted_iota(jnp.int32, (rows, lanes), 1)
        logs = jnp.zeros((rows, lanes), f32)
        for h in range(heads):
            hs = slice(h * head_dim, (h + 1) * head_dim)
            attn[:, hs] = (acc[:, hs] / total[h]).astype(bf16)
            logs = jnp.where(lane == h, peak[h] + jnp.log(total[h]), logs)
        lse_out[...] = jnp.transpose(logs)[:8]
        outs = [
            pltpu.make_async_copy(src, dst, stores.at[i])
            for i, (src, dst) in enumerate(
                [(qrot, qrot_out), (keys, key_out), (values, value_out), (qn, qn_out),
                 (kn, kn_out), (attn, attn_out), (tokt, tokt_out)]
            )
        ]
        for copy in outs:
            copy.start()
        for copy in outs:
            copy.wait()
        for t in range(3):
            to_mate(t).wait_send()

            def sent(d):
                to_peer(t, d).wait_send()
                pass_on(t, d).wait_send()

            each_peer(sent)

    sem = pltpu.SemaphoreType.DMA
    hbm = pl.BlockSpec(memory_space=pl.ANY)
    block = jax.ShapeDtypeStruct
    return pl.pallas_call(
        body,
        out_shape=[
            block((rows, local), bf16), block((count, local), bf16), block((count, local), bf16),
            block((rows, local), f32), block((rows, local), f32), block((rows, local), bf16),
            block((width, rows), bf16),
            block((rows, lanes), f32), block((8, rows), f32),
        ],
        in_specs=[hbm] * 4 + [vmem_spec()] * 4 + [pl.BlockSpec(memory_space=pltpu.SMEM)],
        out_specs=[hbm] * 7 + [vmem_spec()] * 2,
        scratch_shapes=[
            pltpu.VMEM((rows, width), bf16), pltpu.VMEM((width, rows), bf16),
            pltpu.VMEM((3, width, local), bf16),
            pltpu.VMEM((rows, local), f32),
            pltpu.VMEM((rows, local), f32), pltpu.VMEM((rows, local), bf16),
            pltpu.VMEM((count, local), bf16), pltpu.VMEM((count, local), bf16),
            pltpu.VMEM((heads, rows, 1), f32), pltpu.VMEM((heads, rows, 1), f32),
            pltpu.VMEM((rows, local), f32), pltpu.VMEM((rows, local), bf16),
            sem((4,)), sem((7,)),
            sem((3, nx - 1)), sem((3, nx - 1)), sem((3,)), sem((3,)),
            sem((3, nx - 1)), sem((3, nx - 1)),
        ] + small.scratch(),
        compiler_params=pltpu.CompilerParams(
            collective_id=cid, has_side_effects=True, vmem_limit_bytes=62 * 2**20
        ),
        name="front",
    )(tokens, w_query, w_key, w_value, qgain, kgain, cosine, sine, order)


def load_list(pairs, sems, base=0):
    copies = [
        pltpu.make_async_copy(src, dst, sems.at[base + i]) for i, (src, dst) in enumerate(pairs)
    ]
    for copy in copies:
        copy.start()
    return copies


def kernel_call(body, args, kinds, outs, out_kinds, scratch, cid, name):
    spec = {
        "v": vmem_spec(),
        "h": pl.BlockSpec(memory_space=pl.ANY),
        "s": pl.BlockSpec(memory_space=pltpu.SMEM),
    }
    return pl.pallas_call(
        body,
        out_shape=[jax.ShapeDtypeStruct(*out) for out in outs],
        in_specs=[spec[kind] for kind in kinds],
        out_specs=[spec[kind] for kind in out_kinds],
        scratch_shapes=scratch,
        compiler_params=pltpu.CompilerParams(
            collective_id=cid, has_side_effects=True, vmem_limit_bytes=62 * 2**20
        ),
        name=name,
    )(*args)


def middle(attn, tokens, attn_gain, w_output, w_gate, w_up, w_down, cid):
    rows, width = tokens.shape
    local, wide = w_output.shape[0], w_gate.shape[1]
    n_tp = lax.axis_size("tp")
    line = LineSum(n_tp, 2 * rows, width, 4 * row_chains)
    n_line = len(line.scratch())
    half = rows // 2
    tile = 64
    cut = 512
    n_cut = wide // cut
    part = line.part

    def body(
        attn_hbm, tok_hbm, again_ref, wo_hbm, wg_hbm, wu_hbm, wd_hbm,
        proj_out, hidt_out, gate_out, up_out, inner_out, down_out, inv_out,
        attn_v, tok, wo, hid, hidt, gate, up, inner, wg, wu, wd, first, loads, stores, *rest,
    ):
        line.bind(rest[:n_line])
        start = load_list([(attn_hbm, attn_v), (wo_hbm, wo), (tok_hbm, tok)], first)

        def load(src, dst, j, size, spot):
            cols = pl.ds(pl.multiple_of(j * size, size), size)
            return pltpu.make_async_copy(src.at[:, cols], dst.at[j], loads.at[spot])

        def gate_load(j):
            return load(wg_hbm, wg, j, cut, 2 * j)

        def up_load(j):
            return load(wu_hbm, wu, j, cut, 2 * j + 1)

        def down_load(j):
            return load(wd_hbm, wd, j, part, 2 * n_cut + j)

        for j in range(n_cut):
            gate_load(j).start()
            up_load(j).start()
        for j in range(n_tp):
            down_load(j).start()
        bar = pltpu.get_barrier_semaphore()
        peers = line.greet(bar)
        for copy in start:
            copy.wait()

        def project(j, carry):
            cols = pl.ds(pl.multiple_of(j * part, part), part)
            line.own[j, :rows] = jnp.dot(
                attn_v[...], wo[:, cols], preferred_element_type=f32
            ).astype(bf16)
            return carry

        lax.fori_loop(0, n_tp, project, 0)
        pl.semaphore_wait(bar, peers)

        def step(t, carry):
            line.step(t)

            @pl.when(t == 3 * n_tp + 1)
            def _():
                hidt[...] = jnp.transpose(hid[...])

            return carry

        def row_half(c, carry):
            base = pl.multiple_of(c * half, half)
            sl = pl.ds(base, half)
            lax.fori_loop(c * 2 * n_tp, c * n_tp + 2 * n_tp - 1, step, 0)

            def norm_rows(t, carry):
                rs = pl.ds(pl.multiple_of(base + t * tile, tile), tile)
                outs = [line.res[j, rs].astype(f32) for j in range(n_tp)]
                square = sum(jnp.sum(out * out, axis=1, keepdims=True) for out in outs)
                inv = lax.rsqrt(square * (1.0 / width) + norm_eps)
                inv_out[rs, :] = inv
                for j, out in enumerate(outs):
                    cols = slice(j * part, (j + 1) * part)
                    hid[rs, cols] = (
                        tok[rs, cols].astype(f32) + out * inv * again_ref[:, cols]
                    ).astype(bf16)
                return carry

            lax.fori_loop(0, half // tile, norm_rows, 0)
            per = row_chains // n_cut

            def widen(j, carry):
                cols = pl.ds(pl.multiple_of(j * cut, cut), cut)

                @pl.when(c == 0)
                def _():
                    gate_load(j).wait()
                    up_load(j).wait()

                g = jnp.dot(hid[sl], wg[j], preferred_element_type=f32)
                u = jnp.dot(hid[sl], wu[j], preferred_element_type=f32)
                gate[sl, cols] = g.astype(bf16)
                up[sl, cols] = u.astype(bf16)
                inner[sl, cols] = (g * jax.nn.sigmoid(g) * u).astype(bf16)
                line.pieces(((c + 2) * n_tp - 1) * row_chains + j * per, per)
                return carry

            lax.fori_loop(0, n_cut, widen, 0)
            line.pieces(((c + 2) * n_tp - 1) * row_chains + n_cut * per, row_chains - n_cut * per)

            def narrow(j, carry):
                @pl.when(c == 0)
                def _():
                    down_load(j).wait()

                line.own[j, pl.ds(rows + base, half)] = jnp.dot(
                    inner[sl], wd[j], preferred_element_type=f32
                ).astype(bf16)
                return carry

            lax.fori_loop(0, n_tp, narrow, 0)
            return carry

        lax.fori_loop(0, 2, row_half, 0)
        outs = load_list([(gate, gate_out), (up, up_out), (inner, inner_out)], stores)
        ready = line.ship(proj_out, stores, 4, 0, rows)
        lax.fori_loop(3 * n_tp, line.steps, step, 0)
        last = pltpu.make_async_copy(hidt, hidt_out, stores.at[3])
        last.start()
        ready = ready + line.ship(down_out, stores, 4 + n_tp, rows, rows)
        line.drain()
        for copy in outs + [last] + ready:
            copy.wait()

    sem = pltpu.SemaphoreType.DMA
    return kernel_call(
        body, [attn, tokens, attn_gain, w_output, w_gate, w_up, w_down], "hhvhhhh",
        [((rows, width), bf16), ((width, rows), bf16), ((rows, wide), bf16), ((rows, wide), bf16),
         ((rows, wide), bf16), ((rows, width), bf16), ((rows, 1), f32)],
        "hhhhhhv",
        [
            pltpu.VMEM((rows, local), bf16), pltpu.VMEM((rows, width), bf16),
            pltpu.VMEM((local, width), bf16),
            pltpu.VMEM((rows, width), bf16), pltpu.VMEM((width, rows), bf16),
            pltpu.VMEM((rows, wide), bf16), pltpu.VMEM((rows, wide), bf16),
            pltpu.VMEM((rows, wide), bf16),
            pltpu.VMEM((n_cut, width, cut), bf16), pltpu.VMEM((n_cut, width, cut), bf16),
            pltpu.VMEM((n_tp, wide, part), bf16),
            sem((3,)), sem((2 * n_cut + n_tp,)), sem((4 + 2 * n_tp,)),
        ] + line.scratch(),
        cid, "middle",
    )


def mlp_back(down, grad, mlp_gain, gate, up, inner, hid_t, w_gate, w_up, w_down, jobs, widths, cid):
    rows, width = down.shape
    wide = gate.shape[1]
    n_tp = lax.axis_size("tp")
    line = LineSum(n_tp, rows, width)
    grads = GradScatter(lax.axis_size("ctx"), lax.axis_size("seq"), width, jobs)
    n_line, n_grads, n_out = len(line.scratch()), len(grads.scratch()), len(widths)
    tile = 64
    cut = 512
    n_cut = wide // cut
    part = line.part
    lead = row_chains * n_tp // (n_cut + n_tp)
    ticks = n_cut // 2 + n_tp // 2

    def body(
        down_hbm, grad_hbm, mgain_ref, gate_hbm, up_hbm, inner_hbm, hidt_hbm, wg_hbm, wu_hbm, wd_hbm,
        back_out, dgate_out, dup_out, dgain_out, inv_out, *rest,
    ):
        grad_outs, rest = rest[:n_out], rest[n_out:]
        (gate_v, up_v, inner_v, hidt, ddown, ddownt, dgate, dup, ring, loads, wsem, stores) = rest[:12]
        line.bind(rest[12 : 12 + n_line])
        grads.bind(rest[12 + n_line :], [ddownt, hidt], [inner_v, dgate, dup], grad_outs)

        def fetch(src, index):
            return pltpu.make_async_copy(src, ring.at[index], wsem.at[index])

        def rows_of(ref, j, size):
            return ref.at[pl.ds(pl.multiple_of(j * size, size), size)]

        for j in range(4):
            fetch(rows_of(wd_hbm, j, cut), j).start()
        down_ref, grad_ref = dgate.at[:, pl.ds(0, width)], dup.at[:, pl.ds(0, width)]
        first = load_list([(down_hbm, down_ref), (grad_hbm, grad_ref)], loads, 4)
        early = load_list(
            [(inner_hbm, inner_v), (gate_hbm, gate_v), (up_hbm, up_v), (hidt_hbm, hidt)], loads
        )
        bar = pltpu.get_barrier_semaphore()
        peers = line.greet(bar) + grads.greet(bar)
        dgain_out[...] = jnp.zeros_like(dgain_out)
        for copy in first:
            copy.wait()

        def norm_rows(t, carry):
            sl = pl.ds(pl.multiple_of(t * tile, tile), tile)
            out = down_ref[sl].astype(f32)
            upstream = grad_ref[sl].astype(f32)
            inv = lax.rsqrt(jnp.mean(out * out, axis=1, keepdims=True) + norm_eps)
            norm = out * inv
            inv_out[sl, :] = inv
            dgain_out[...] += jnp.sum(upstream * norm, axis=0, keepdims=True)
            dnorm = upstream * mgain_ref[...]
            dot = jnp.mean(dnorm * norm, axis=1, keepdims=True)
            ddown[sl] = (inv * (dnorm - norm * dot)).astype(bf16)
            return carry

        lax.fori_loop(0, rows // tile, norm_rows, 0)
        ddownt[...] = jnp.transpose(ddown[...])
        for copy in early:
            copy.wait()
        pl.semaphore_wait(bar, peers)

        half = rows // 2

        def row_half(c, carry):
            sl = pl.ds(pl.multiple_of(c * half, half), half)

            def beside(i, j, first):
                @pl.when(c == 1)
                def _():
                    line.pieces(i * lead, lead)

                @pl.when(lax.rem(j, 2) == 1)
                def _():
                    grads.tick(first + j // 2)

            def inner_back(j, carry):
                fetch(rows_of(wd_hbm, j, cut), j).wait()
                cols = pl.ds(pl.multiple_of(j * cut, cut), cut)
                dmix = dot_nt(ddown[sl], ring[j])
                g, u = gate_v[sl, cols].astype(f32), up_v[sl, cols].astype(f32)
                sig = jax.nn.sigmoid(g)
                dgate[sl, cols] = (dmix * u * sig * (1.0 + g * (1.0 - sig))).astype(bf16)
                dup[sl, cols] = (dmix * (g * sig)).astype(bf16)

                @pl.when(lax.rem(j, 2) == 0)
                def _():
                    fetch(rows_of(wg_hbm, j // 2, part), j).start()

                @pl.when(lax.rem(j, 2) == 1)
                def _():
                    fetch(rows_of(wu_hbm, j // 2, part), j).start()

                beside(j, j, c * ticks)
                return carry

            lax.fori_loop(0, n_cut, inner_back, 0)

            def hidden_back(j, carry):
                slot = lax.rem(2 * j, 4)
                fetch(rows_of(wg_hbm, j, part), slot).wait()
                fetch(rows_of(wu_hbm, j, part), slot + 1).wait()
                line.own[j, sl] = (
                    dot_nt(dgate[sl], ring[slot]) + dot_nt(dup[sl], ring[slot + 1])
                ).astype(bf16)

                @pl.when(j + 2 < n_tp)
                def _():
                    fetch(rows_of(wg_hbm, j + 2, part), slot).start()
                    fetch(rows_of(wu_hbm, j + 2, part), slot + 1).start()

                @pl.when((j + 2 >= n_tp) & (c == 0))
                def _():
                    fetch(rows_of(wd_hbm, slot, cut), slot).start()
                    fetch(rows_of(wd_hbm, slot + 1, cut), slot + 1).start()

                beside(n_cut + j, j, c * ticks + n_cut // 2)
                return carry

            lax.fori_loop(0, n_tp, hidden_back, 0)
            return carry

        lax.fori_loop(0, 2, row_half, 0)
        outs = load_list([(dgate, dgate_out), (dup, dup_out)], stores)
        done, used = 2 * ticks, (n_cut + n_tp) * lead

        def one(it, carry):
            line.pieces(used + (it - done) * pace, pace)
            grads.tick(it)
            return carry

        line_its = -(-(line.steps * row_chains - used) // pace)
        lax.fori_loop(done, max(done + line_its, grads.steps), one, 0)
        outs += line.ship(back_out, stores, 2, 0, rows)
        line.drain()
        grads.drain()
        for copy in outs:
            copy.wait()

    sem = pltpu.SemaphoreType.DMA
    return kernel_call(
        body, [down, grad, mlp_gain, gate, up, inner, hid_t, w_gate, w_up, w_down], "hhvhhhhhhh",
        [((rows, width), bf16), ((rows, wide), bf16), ((rows, wide), bf16), ((1, width), f32),
         ((rows, 1), f32)]
        + grads.out_shapes(widths),
        "hhhvv" + "v" * n_out,
        [
            pltpu.VMEM((rows, wide), bf16), pltpu.VMEM((rows, wide), bf16),
            pltpu.VMEM((rows, wide), bf16), pltpu.VMEM((width, rows), bf16),
            pltpu.VMEM((rows, width), bf16), pltpu.VMEM((width, rows), bf16),
            pltpu.VMEM((rows, wide), bf16), pltpu.VMEM((rows, wide), bf16),
            pltpu.VMEM((4, cut, width), bf16),
            sem((6,)), sem((4,)), sem((2 + n_tp,)),
        ] + line.scratch() + grads.scratch(),
        cid, "mlp_back",
    )


def last_sums(dqkv, w_query, w_key, w_value, ats, bs, jobs, widths, gains, cid):
    rows = dqkv.shape[0]
    width, local = w_query.shape
    n_ctx, n_seq = lax.axis_size("ctx"), lax.axis_size("seq")
    n_tp = lax.axis_size("tp")
    line = LineSum(n_tp, rows, width)
    grads = GradScatter(n_ctx, n_seq, width, jobs)
    small = GainSum(n_ctx, n_seq, gains.shape[0])
    na, nb, n_out = len(ats), len(bs), len(widths)
    n_line, n_grads = len(line.scratch()), len(grads.scratch())
    part = line.part

    def body(dqkv_ref, wq_ref, wk_ref, wv_ref, *refs):
        at_refs, b_refs = refs[:na], refs[na : na + nb]
        gain_ref, last_out = refs[na + nb], refs[na + nb + 1]
        refs = refs[na + nb + 2 :]
        grad_outs, gain_out, stores, scratch = refs[:n_out], refs[n_out], refs[n_out + 1], refs[n_out + 2 :]
        line.bind(scratch[:n_line])
        grads.bind(scratch[n_line : n_line + n_grads], at_refs, list(b_refs) + [dqkv_ref], grad_outs)
        small.bind(scratch[n_line + n_grads :], gain_ref, gain_out)
        bar = pltpu.get_barrier_semaphore()
        peers = line.greet(bar) + small.greet(bar)
        pl.semaphore_wait(bar, peers)
        small.start()

        def input_back(j, carry):
            rs = pl.ds(pl.multiple_of(j * part, part), part)
            line.own[j] = (
                dot_nt(dqkv_ref[:, :local], wq_ref[rs])
                + dot_nt(dqkv_ref[:, local : 2 * local], wk_ref[rs])
                + dot_nt(dqkv_ref[:, 2 * local :], wv_ref[rs])
            ).astype(bf16)

            @pl.when(lax.rem(j, 2) == 0)
            def _():
                grads.tick(j // 2)

            return carry

        lax.fori_loop(0, n_tp, input_back, 0)
        done = n_tp // 2

        def one(it, carry):
            grads.tick(it)
            line.pieces((it - done) * pace, pace)
            return carry

        line_steps = -(-line.steps * row_chains // pace)
        lax.fori_loop(done, max(done + line_steps, grads.steps), one, 0)
        small.finish()
        outs = line.ship(last_out, stores, 0, 0, rows)
        line.drain()
        grads.drain()
        for copy in outs:
            copy.wait()

    sem = pltpu.SemaphoreType.DMA
    return kernel_call(
        body, [dqkv, w_query, w_key, w_value] + list(ats) + list(bs) + [gains],
        "vvvv" + "v" * (na + nb + 1),
        [((rows, width), bf16)] + grads.out_shapes(widths) + [(gains.shape, f32)],
        "h" + "v" * (n_out + 1),
        [sem((n_tp,))] + line.scratch() + grads.scratch() + small.scratch(),
        cid, "last_sums",
    )


def row_tiles(body, args, outs, name):
    count = 4

    def spec(shape):
        if shape[0] == 1:
            return pl.BlockSpec(shape, lambda i: (0, 0))
        return pl.BlockSpec((shape[0] // count, shape[1]), lambda i: (i, 0))

    def whole(*refs):
        body(refs[: len(args)], refs[len(args) :])

    return pl.pallas_call(
        whole,
        grid=(count,),
        out_shape=[jax.ShapeDtypeStruct(shape, f32) for shape in outs],
        in_specs=[spec(arg.shape) for arg in args],
        out_specs=[spec(shape) for shape in outs],
        compiler_params=pltpu.CompilerParams(vmem_limit_bytes=62 * 2**20),
        name=name,
    )(*args)


def block_tile(ins, outs):
    x, a, ra, ga, d, rd, gd = [ref[...].astype(f32) for ref in ins[:7]]
    outs[0][...] = x + (a * ra) * ga + (d * rd) * gd
    for src, dst in zip(ins[7:], outs[1:]):
        dst[...] = src[...]


def input_tile(ins, outs):
    outs[0][...] = ins[0][...].astype(f32) + ins[1][...].astype(f32) + ins[2][...].astype(f32)
    outs[1][...] = ins[3][...]
    outs[2][...] = ins[4][...]
    size = outs[3].shape[1]
    for i in range(3):
        outs[3 + i][...] = ins[5][:, i * size : (i + 1) * size]


def per_device(
    tokens,
    out_grad,
    group_order,
    w_query,
    w_key,
    w_value,
    query_gain,
    key_gain,
    w_output,
    attn_gain,
    w_gate,
    w_up,
    w_down,
    mlp_gain,
):
    inputs = tokens[0]
    upstream = out_grad[0]
    rows, width = inputs.shape
    heads, head_dim = query_gain.shape
    local = heads * head_dim
    wide = w_gate.shape[1]
    positions = key_positions(group_order[0], lax.axis_index("ctx") * rows, rows, rows // 2)
    angle_cos, angle_sin = rope_tables(positions, head_dim)
    qgain = query_gain.reshape(1, local)
    kgain = key_gain.reshape(1, local)
    (query_rot, keys, values, query_norm, key_norm, attn, tokens_t, scales, lse) = front(
        inputs, w_query, w_key, w_value, qgain, kgain, angle_cos, angle_sin, group_order, 1
    )
    proj, hidden_t, gate, up, inner, down, proj_scale = middle(
        attn, inputs, attn_gain[None], w_output, w_gate, w_up, w_down, 2
    )
    chunk_cols = 2 * lanes
    chunks = wide // chunk_cols
    thin = local // chunk_cols
    back, d_gate, d_up, d_mlp_gain, down_scale, grad_down, grad_gate = mlp_back(
        down, upstream, mlp_gain[None], gate, up, inner, hidden_t, w_gate, w_up, w_down,
        [
            dict(a=0, b=0, first=0, count=chunks, out=0, place=0, flip=True),
            dict(a=1, b=1, first=0, count=chunks, out=1, place=0, flip=False),
        ],
        [wide, wide],
        3,
    )
    d_qkv, d_proj_t, d_attn_gain, d_query_gain, d_key_gain = attention_back(
        back, upstream, proj, attn_gain[None], w_output, query_rot, keys, values, attn, lse,
        positions[None], group_order, query_norm, key_norm, scales, qgain, kgain, angle_cos,
        angle_sin, [], [], [], [], 4,
    )
    owners = lax.axis_size("ctx") * lax.axis_size("seq")
    gains = [d_attn_gain, d_mlp_gain, d_query_gain, d_key_gain]
    ends = [gain.shape[1] for gain in gains]
    ends = [sum(ends[: i + 1]) for i in range(4)]
    packed = jnp.concatenate(gains, axis=1).reshape(-1, lanes)
    last, grad_up, grad_qkv, grad_output, small = last_sums(
        d_qkv, w_query, w_key, w_value,
        [hidden_t, tokens_t, d_proj_t],
        [d_up, attn],
        [
            dict(a=0, b=0, first=0, count=chunks, out=0, place=0, flip=False),
            dict(a=2, b=1, first=0, count=thin, out=2, place=0, flip=True),
            dict(a=1, b=2, first=0, count=3 * thin, out=1, place=0, flip=False),
        ],
        [wide, 3 * local, local],
        packed,
        5,
    )
    small = small.reshape(-1)
    me = lax.axis_index("ctx") * lax.axis_size("seq") + lax.axis_index("seq")

    def my_part(start, end, lead):
        whole = small[start:end].reshape(lead, -1)
        size = whole.shape[1] // owners
        return lax.dynamic_slice_in_dim(whole, me * size, size, 1)

    g_attn = my_part(0, ends[0], 1)[0]
    g_mlp = my_part(ends[0], ends[1], 1)[0]
    g_query = my_part(ends[1], ends[2], heads)
    g_key = my_part(ends[2], ends[3], heads)
    block_out, grad_down, grad_gate = row_tiles(
        block_tile,
        [inputs, proj, proj_scale, attn_gain[None], down, down_scale, mlp_gain[None], grad_down,
         grad_gate],
        [inputs.shape, grad_down.shape, grad_gate.shape], "block_out",
    )
    own = grad_qkv.shape[0]
    input_grad, grad_up, grad_output, grad_query, grad_key, grad_value = row_tiles(
        input_tile, [upstream, back, last, grad_up, grad_output, grad_qkv],
        [inputs.shape, grad_up.shape, grad_output.shape] + [(own, local)] * 3, "input_grad",
    )
    return (
        block_out[None],
        input_grad[None],
        grad_query,
        grad_key,
        grad_value,
        g_query,
        g_key,
        grad_output,
        g_attn,
        grad_gate,
        grad_up,
        grad_down,
        g_mlp,
    )


def solution(mesh):
    return jax.shard_map(
        per_device,
        mesh=mesh,
        in_specs=(
            P("seq", "ctx", None),
            P("seq", "ctx", None),
            P("seq", None),
            P(None, "tp"),
            P(None, "tp"),
            P(None, "tp"),
            P("tp", None),
            P("tp", None),
            P("tp", None),
            P(),
            P(None, "tp"),
            P(None, "tp"),
            P("tp", None),
            P(),
        ),
        out_specs=(
            P("seq", "ctx", None),
            P("seq", "ctx", None),
            P(("ctx", "seq"), "tp"),
            P(("ctx", "seq"), "tp"),
            P(("ctx", "seq"), "tp"),
            P("tp", ("ctx", "seq")),
            P("tp", ("ctx", "seq")),
            P("tp", ("ctx", "seq")),
            P(("ctx", "seq")),
            P(("ctx", "seq"), "tp"),
            P(("ctx", "seq"), "tp"),
            P("tp", ("ctx", "seq")),
            P(("ctx", "seq")),
        ),
        check_vma=False,
    )
```

```python
import jax
import jax.numpy as jnp
from jax import lax
from jax.sharding import PartitionSpec as P
from jax.experimental import pallas as pl
from jax.experimental.pallas import tpu as pltpu

norm_eps = 1e-06
rope_base = 500000.0
masked_score = -1e30


def rope_tables(positions, head_dim):
    half = head_dim // 2
    channel = jnp.arange(head_dim, dtype=jnp.int32)
    rates = rope_base ** (-((channel % half).astype(jnp.float32) * 2.0 / head_dim))
    angle = positions.astype(jnp.float32)[:, None] * rates[None, :]
    return jnp.cos(angle), jnp.where(channel[None, :] < half, -jnp.sin(angle), jnp.sin(angle))


def key_positions(order, first_row, count, group):
    row_ids = first_row + jnp.arange(count, dtype=jnp.int32)
    slots = row_ids // group
    picks = slots[:, None] == jnp.arange(order.shape[0], dtype=jnp.int32)[None, :]
    return jnp.sum(jnp.where(picks, order[None, :], 0), axis=1) * group + row_ids % group


MESH = pl.DeviceIdType.MESH
bf16 = jnp.bfloat16
f32 = jnp.float32
lanes = 128
row_blocks = 16
row_chains = 8
pace = 6


def remote(src, dst, send, recv, where):
    return pltpu.make_async_remote_copy(
        src, dst, send, recv, device_id=where, device_id_type=MESH
    )


class LineSum:
    def __init__(self, n, rows, width, blocks=row_blocks):
        self.n, self.rows, self.width = n, rows, width
        self.part = width // n
        self.rc = rows // blocks
        self.total = blocks // row_chains * n
        self.steps = self.total + n - 1

    def scratch(self):
        shape = (self.n, self.rows, self.part)
        return (
            [pltpu.VMEM(shape, bf16)] * 4
            + [pltpu.SemaphoreType.DMA] * 2
            + [pltpu.SemaphoreType.DMA((row_chains, self.total))] * 2
        )

    def bind(self, refs):
        self.own, self.from_l, self.from_r, self.res = refs[:4]
        self.send_r, self.send_l, self.recv_l, self.recv_r = refs[4:]
        self.i = lax.axis_index("tp")
        self.has_l, self.has_r = self.i > 0, self.i < self.n - 1

    def greet(self, bar):
        @pl.when(self.has_l)
        def _():
            pl.semaphore_signal(bar, inc=1, device_id={"tp": self.i - 1}, device_id_type=MESH)

        @pl.when(self.has_r)
        def _():
            pl.semaphore_signal(bar, inc=1, device_id={"tp": self.i + 1}, device_id_type=MESH)

        return self.has_l.astype(jnp.int32) + self.has_r.astype(jnp.int32)

    def load(self, x_ref):
        for j in range(self.n):
            self.own[j] = x_ref[:, j * self.part : (j + 1) * self.part]

    def rows_of(self, g, p):
        block = (p // self.n) * row_chains + g
        return pl.ds(pl.multiple_of(block * self.rc, self.rc), self.rc)

    def right(self, src, dst, g, p, j):
        sl = self.rows_of(g, p)
        return remote(
            src.at[j, sl], dst.at[j, sl], self.send_r, self.recv_l.at[g, p],
            {"tp": self.i + 1},
        )

    def left(self, src, dst, g, q, j):
        sl = self.rows_of(g, q)
        return remote(
            src.at[j, sl], dst.at[j, sl], self.send_l, self.recv_r.at[g, q],
            {"tp": self.i - 1},
        )

    def wait_l(self, g, p, j):
        sl = self.rows_of(g, p)
        remote(
            self.own.at[j, sl], self.from_l.at[j, sl], self.send_r, self.recv_l.at[g, p],
            {"tp": self.i - 1},
        ).wait_recv()

    def wait_r(self, g, q, j):
        sl = self.rows_of(g, q)
        remote(
            self.own.at[j, sl], self.from_r.at[j, sl], self.send_l, self.recv_r.at[g, q],
            {"tp": self.i + 1},
        ).wait_recv()

    def step(self, t):
        self.pieces(t * row_chains, row_chains)

    def pieces(self, first, count):
        def one(v, carry):
            self.piece(first + v)
            return carry

        lax.fori_loop(0, count, one, 0)

    def piece(self, e):
        t = e // row_chains

        @pl.when(t < self.steps)
        def _():
            self.sub_step(t, lax.rem(e, row_chains))

    def sub_step(self, t, g):
        n, i, has_l, has_r = self.n, self.i, self.has_l, self.has_r
        own, from_l, from_r, res = self.own, self.from_l, self.from_r, self.res
        p = t - i
        q = t - (n - 1 - i)
        jr = n - 1 - lax.rem(p + n * self.total, n)
        jl = lax.rem(q + n * self.total, n)
        pv = (p >= 0) & (p < self.total)
        qv = (q >= 0) & (q < self.total)

        @pl.when(pv & has_l)
        def _():
            self.wait_l(g, p, jr)

        @pl.when(qv & has_r)
        def _():
            self.wait_r(g, q, jl)

        @pl.when(pv & (jr > i))
        def _():
            sl = self.rows_of(g, p)

            @pl.when(has_l)
            def _():
                own[jr, sl] = (own[jr, sl].astype(f32) + from_l[jr, sl].astype(f32)).astype(bf16)

            self.right(own, from_l, g, p, jr).start()

        @pl.when(qv & (jl < i))
        def _():
            sl = self.rows_of(g, q)

            @pl.when(has_r)
            def _():
                own[jl, sl] = (own[jl, sl].astype(f32) + from_r[jl, sl].astype(f32)).astype(bf16)

            self.left(own, from_r, g, q, jl).start()

        @pl.when(pv & (jr == i))
        def _():
            sl = self.rows_of(g, p)

            @pl.when(has_l & has_r)
            def _():
                res[i, sl] = (
                    own[i, sl].astype(f32) + from_l[i, sl].astype(f32) + from_r[i, sl].astype(f32)
                ).astype(bf16)

            @pl.when(jnp.logical_not(has_l))
            def _():
                res[i, sl] = (own[i, sl].astype(f32) + from_r[i, sl].astype(f32)).astype(bf16)

            @pl.when(jnp.logical_not(has_r))
            def _():
                res[i, sl] = (own[i, sl].astype(f32) + from_l[i, sl].astype(f32)).astype(bf16)

        @pl.when(pv & (jr <= i) & has_r)
        def _():
            self.right(res, res, g, p, jr).start()

        @pl.when(qv & (jl >= i) & has_l)
        def _():
            self.left(res, res, g, q, jl).start()

    def drain(self):
        @pl.when(self.has_r)
        def _():
            remote(
                self.own, self.from_l, self.send_r, self.recv_l.at[0, 0], {"tp": self.i + 1}
            ).wait_send()

        @pl.when(self.has_l)
        def _():
            remote(
                self.own, self.from_r, self.send_l, self.recv_r.at[0, 0], {"tp": self.i - 1}
            ).wait_send()

    def ship(self, out_ref, sems, base, start, count):
        return load_list(
            [
                (
                    self.res.at[j, pl.ds(start, count)],
                    out_ref.at[:, pl.ds(j * self.part, self.part)],
                )
                for j in range(self.n)
            ],
            sems, base,
        )


class GradScatter:
    def __init__(self, n_ctx, n_seq, width, jobs, orders=("xy", "yx")):
        self.nx, self.ny = n_ctx // 2, n_seq
        self.rows = width // (n_ctx * n_seq)
        self.jobs, self.orders = jobs, orders
        start = 0
        self.spans = []
        for job in jobs:
            self.spans.append((start, start + job["count"]))
            start += job["count"]
        self.total = start
        self.steps = start + 5

    def out_shapes(self, widths):
        flips = {job["out"] for job in self.jobs if job["flip"]}
        return [
            ((w, self.rows) if i in flips else (self.rows, w), f32) for i, w in enumerate(widths)
        ]

    def sizes(self, order):
        return (self.nx, self.ny) if order == "xy" else (self.ny, self.nx)

    def scratch(self):
        nx, ny, t = self.nx, self.ny, self.total
        tile = (self.rows, lanes)
        sem = pltpu.SemaphoreType.DMA
        out = [
            pltpu.VMEM((2, nx, ny, 2) + tile, bf16),
            pltpu.VMEM((2, nx, ny, 2) + tile, f32),
            pltpu.VMEM((t, nx, ny, 2) + tile, bf16),
            sem((2,)), sem((t,)),
        ]
        for order in self.orders:
            n1, n2 = self.sizes(order)
            out += [
                pltpu.VMEM((3, n1, n2) + tile, bf16),
                pltpu.VMEM((t, n1 - 1, n2) + tile, bf16),
                pltpu.VMEM((3, n2) + tile, bf16),
                pltpu.VMEM((t, n2 - 1) + tile, bf16),
                sem((3, n1 - 1)), sem((t, n1 - 1)), sem((3, n2 - 1)), sem((t, n2 - 1)),
            ]
        return out

    def bind(self, refs, at_refs, b_refs, out_refs):
        self.send0, self.keep, self.recv0, self.s0, self.d0 = refs[:5]
        self.half = [refs[5 + 8 * h : 13 + 8 * h] for h in range(2)]
        self.at_refs, self.b_refs, self.out_refs = at_refs, b_refs, out_refs
        ctx = lax.axis_index("ctx")
        self.mx, self.core, self.my = ctx // 2, lax.rem(ctx, 2), lax.axis_index("seq")

    def axis(self, name, d):
        if name == "x":
            to = lax.rem(self.mx + d, self.nx)
            return to, {"ctx": to * 2 + self.core}
        to = lax.rem(self.my + d, self.ny)
        return to, {"seq": to}

    def at_mate(self):
        return {"ctx": self.mx * 2 + 1 - self.core}

    def greet(self, bar):
        places = [self.at_mate()]
        places += [self.axis("x", d)[1] for d in range(1, self.nx)]
        places += [self.axis("y", d)[1] for d in range(1, self.ny)]
        for place in places:
            pl.semaphore_signal(bar, inc=1, device_id=place, device_id_type=MESH)
        return len(places)

    def c0(self, c):
        slot = lax.rem(c, 2)
        return remote(
            self.send0.at[slot], self.recv0.at[c], self.s0.at[slot], self.d0.at[c], self.at_mate()
        )

    def c1(self, h, c, d):
        p, r1, _, _, sent, done, _, _ = self.half[h]
        to, where = self.axis(self.orders[h][0], d)
        slot = lax.rem(c, 3)
        return remote(p.at[slot, to], r1.at[c, d - 1], sent.at[slot, d - 1], done.at[c, d - 1], where)

    def c2(self, h, c, d):
        _, _, q, r2, _, _, sent, done = self.half[h]
        to, where = self.axis(self.orders[h][1], d)
        slot = lax.rem(c, 3)
        return remote(q.at[slot, to], r2.at[c, d - 1], sent.at[slot, d - 1], done.at[c, d - 1], where)

    def make(self, c):
        slot = lax.rem(c, 2)
        nx, ny, r = self.nx, self.ny, self.rows

        @pl.when(c >= 2)
        def _():
            self.c0(c).wait_send()

        def products(at_ref, b_ref, col, parity, write):
            def tile(e, carry):
                x, y = e // ny, lax.rem(e, ny)
                row = pl.multiple_of(((x * 2 + parity) * ny + y) * r, r)
                acc = jnp.dot(
                    at_ref[pl.ds(row, r), :], b_ref[:, pl.ds(col, 2 * lanes)],
                    preferred_element_type=f32,
                )
                write(x, y, acc)
                return carry

            lax.fori_loop(0, nx * ny, tile, 0)

        def to_send(x, y, acc):
            self.send0[slot, x, y, 0] = acc[:, :lanes].astype(bf16)
            self.send0[slot, x, y, 1] = acc[:, lanes:].astype(bf16)

        def to_keep(x, y, acc):
            self.keep[slot, x, y, 0] = acc[:, :lanes]
            self.keep[slot, x, y, 1] = acc[:, lanes:]

        for job, (lo, hi) in zip(self.jobs, self.spans):

            @pl.when((c >= lo) & (c < hi))
            def _():
                at_ref, b_ref = self.at_refs[job["a"]], self.b_refs[job["b"]]
                col = pl.multiple_of((c - lo + job["first"]) * (2 * lanes), 2 * lanes)
                products(at_ref, b_ref, col, 1 - self.core, to_send)
                self.c0(c).start()
                products(at_ref, b_ref, col, self.core, to_keep)

    def pair(self, c):
        slot, two = lax.rem(c, 3), lax.rem(c, 2)

        @pl.when(c >= 3)
        def _():
            for h in range(2):
                for d in range(1, self.sizes(self.orders[h])[0]):
                    self.c1(h, c, d).wait_send()

        self.c0(c).wait_recv()
        for h, order in enumerate(self.orders):
            p = self.half[h][0]
            for x in range(self.nx):
                for y in range(self.ny):
                    spot = (x, y) if order == "xy" else (y, x)
                    p[(slot,) + spot] = (
                        self.keep[two, x, y, h] + self.recv0[c, x, y, h].astype(f32)
                    ).astype(bf16)
            for d in range(1, self.sizes(order)[0]):
                self.c1(h, c, d).start()

    def own(self, name):
        return self.mx if name == "x" else self.my

    def cross(self, c):
        slot = lax.rem(c, 3)

        @pl.when(c >= 3)
        def _():
            for h in range(2):
                for d in range(1, self.sizes(self.orders[h])[1]):
                    self.c2(h, c, d).wait_send()

        for h, order in enumerate(self.orders):
            n1, n2 = self.sizes(order)
            p, r1, q = self.half[h][:3]
            for d in range(1, n1):
                self.c1(h, c, d).wait_recv()
            for e in range(n2):
                acc = p[slot, self.own(order[0]), e].astype(f32)
                for d in range(1, n1):
                    acc = acc + r1[c, d - 1, e].astype(f32)
                q[slot, e] = acc.astype(bf16)
            for d in range(1, n2):
                self.c2(h, c, d).start()

    def finish(self, c):
        slot = lax.rem(c, 3)
        totals = []
        for h, order in enumerate(self.orders):
            n2 = self.sizes(order)[1]
            q, r2 = self.half[h][2:4]
            for d in range(1, n2):
                self.c2(h, c, d).wait_recv()
            acc = q[slot, self.own(order[1])].astype(f32)
            for d in range(1, n2):
                acc = acc + r2[c, d - 1].astype(f32)
            totals.append(acc)
        for job, (lo, hi) in zip(self.jobs, self.spans):

            @pl.when((c >= lo) & (c < hi))
            def _():
                out_ref = self.out_refs[job["out"]]
                col = pl.multiple_of((c - lo + job["place"]) * (2 * lanes), 2 * lanes)
                for h in range(2):
                    place = pl.ds(col + h * lanes, lanes)
                    if job["flip"]:
                        out_ref[place, :] = jnp.transpose(totals[h])
                    else:
                        out_ref[:, place] = totals[h]

    def tick(self, it):
        @pl.when((it >= 5) & (it < self.total + 5))
        def _():
            self.finish(it - 5)

        @pl.when((it >= 3) & (it < self.total + 3))
        def _():
            self.cross(it - 3)

        @pl.when((it >= 1) & (it < self.total + 1))
        def _():
            self.pair(it - 1)

        @pl.when(it < self.total)
        def _():
            self.make(it)

    def drain(self):
        for c in range(max(self.total - 2, 0), self.total):
            self.c0(c).wait_send()
        for c in range(max(self.total - 3, 0), self.total):
            for h, order in enumerate(self.orders):
                n1, n2 = self.sizes(order)
                for d in range(1, n1):
                    self.c1(h, c, d).wait_send()
                for d in range(1, n2):
                    self.c2(h, c, d).wait_send()


class GainSum:
    def __init__(self, n_ctx, n_seq, rows):
        self.ny, self.n, self.rows = n_seq, n_ctx * n_seq, rows

    def scratch(self):
        sem = pltpu.SemaphoreType.DMA
        return [pltpu.VMEM((self.n - 1, self.rows, lanes), f32), sem((self.n - 1,)), sem((self.n - 1,))]

    def bind(self, refs, in_ref, out_ref):
        self.got, self.sent, self.done = refs
        self.in_ref, self.out_ref = in_ref, out_ref
        self.me = lax.axis_index("ctx") * self.ny + lax.axis_index("seq")

    def place(self, d):
        to = lax.rem(self.me + d, self.n)
        return {"ctx": to // self.ny, "seq": lax.rem(to, self.ny)}

    def copy(self, d):
        return remote(
            self.in_ref, self.got.at[d - 1], self.sent.at[d - 1], self.done.at[d - 1], self.place(d)
        )

    def greet(self, bar):
        for d in range(1, self.n):
            pl.semaphore_signal(bar, inc=1, device_id=self.place(d), device_id_type=MESH)
        return self.n - 1

    def start(self):
        for d in range(1, self.n):
            self.copy(d).start()

    def finish(self):
        acc = self.in_ref[...]
        for d in range(1, self.n):
            self.copy(d).wait_recv()
            acc = acc + self.got[d - 1]
        self.out_ref[...] = acc
        for d in range(1, self.n):
            self.copy(d).wait_send()


def vmem_spec():
    return pl.BlockSpec(memory_space=pltpu.VMEM)


def comm_call(body, args, outs, scratch, cid, name, scalars=()):
    return pl.pallas_call(
        body,
        out_shape=outs,
        in_specs=[
            pl.BlockSpec(memory_space=pltpu.SMEM) if i in scalars else vmem_spec()
            for i in range(len(args))
        ],
        out_specs=[vmem_spec()] * len(outs),
        scratch_shapes=scratch,
        compiler_params=pltpu.CompilerParams(
            collective_id=cid, has_side_effects=True, vmem_limit_bytes=62 * 2**20
        ),
        name=name,
    )(*args)


class LineSmall:
    def __init__(self, n, rows):
        self.n, self.rows = n, rows

    def scratch(self):
        sem = pltpu.SemaphoreType.DMA
        return [
            pltpu.VMEM((8, self.rows), f32), pltpu.VMEM((self.n - 1, 8, self.rows), f32),
            sem((self.n - 1,)), sem((self.n - 1,)),
        ]

    def bind(self, refs):
        self.mine, self.got, self.sent, self.done = refs
        self.i = lax.axis_index("tp")

    def greet(self, bar):
        for d in range(1, self.n):
            pl.semaphore_signal(
                bar, inc=1, device_id={"tp": lax.rem(self.i + d, self.n)}, device_id_type=MESH
            )
        return self.n - 1

    def copy(self, d):
        return remote(
            self.mine, self.got.at[d - 1], self.sent.at[d - 1], self.done.at[d - 1],
            {"tp": lax.rem(self.i + d, self.n)},
        )

    def total(self, columns, meanwhile=lambda: None):
        self.mine[...] = jnp.transpose(columns)[:8]
        for d in range(1, self.n):
            self.copy(d).start()
        meanwhile()
        acc = self.mine[...]
        for d in range(1, self.n):
            self.copy(d).wait_recv()
            acc = acc + self.got[d - 1]
        for d in range(1, self.n):
            self.copy(d).wait_send()
        return jnp.transpose(jnp.concatenate([acc, jnp.zeros((lanes - 8, self.rows), f32)], axis=0))


def lane_pair(first, second, rows):
    lane = lax.broadcasted_iota(jnp.int32, (rows, lanes), 1)
    return jnp.where(lane == 0, first, 0.0) + jnp.where(lane == 1, second, 0.0)


def dot_nt(left, right):
    return lax.dot_general(left, right, (((1,), (1,)), ((), ())), preferred_element_type=f32)


def dot_tn(left, right):
    return lax.dot_general(left, right, (((0,), (0,)), ((), ())), preferred_element_type=f32)


def attention_back(
    back, grad, proj, attn_gain, w_output, query_rot, keys, values, attn, lse, pos_row, order,
    query_norm, key_norm, scales, qgain, kgain, cosine, sine, ats, bs, jobs, widths, cid,
):
    rows, width = back.shape
    local = w_output.shape[0]
    head_dim = lanes
    heads = local // head_dim
    count = keys.shape[0]
    nx, n_tp = lax.axis_size("ctx") // 2, lax.axis_size("tp")
    small = LineSmall(n_tp, rows)
    n_small = len(small.scratch())
    scale = head_dim ** (-0.5)
    tile = 64
    sub = rows // 2
    na, nb, n_out = len(ats), len(bs), len(widths)
    grads = None
    if jobs:
        grads = GradScatter(2 * nx, lax.axis_size("seq"), width, jobs, ("yx", "yx"))

    def body(
        back_ref, grad_ref, proj_ref, again_ref, w_ref, q_ref, k_ref, v_ref, attn_ref, lse_ref,
        prow_ref, order_ref, qn_ref, kn_ref, sc_ref, qg_ref, kg_ref, cos_ref, sin_ref, *rest,
    ):
        at_refs, b_refs, rest = rest[:na], rest[na : na + nb], rest[na + nb :]
        dqkv_ref, dprojt_ref, dagain_ref, dqg_ref, dkg_ref = rest[:5]
        grad_outs, rest = rest[5 : 5 + n_out], rest[5 + n_out :]
        (dproj, dout, columns, delta, dqs, dks, send0, keep, recv0, recv1, s0, d0, s1, d1) = rest[:14]
        small.bind(rest[14 : 14 + n_small])
        if jobs:
            grads.bind(rest[14 + n_small :], at_refs, b_refs, grad_outs)

        def tick(it):
            if jobs:
                grads.tick(it)

        ctx = lax.axis_index("ctx")
        mx, core = ctx // 2, lax.rem(ctx, 2)
        bar = pltpu.get_barrier_semaphore()
        mate = {"ctx": mx * 2 + 1 - core}
        if jobs:
            peers = small.greet(bar) + grads.greet(bar)
        else:
            peers = small.greet(bar) + nx
            pl.semaphore_signal(bar, inc=1, device_id=mate, device_id_type=MESH)
            for d in range(1, nx):
                pl.semaphore_signal(
                    bar, inc=1, device_id={"ctx": lax.rem(mx + d, nx) * 2 + core},
                    device_id_type=MESH,
                )
        pl.semaphore_wait(bar, peers)
        tick(jnp.int32(0))

        dagain_ref[...] = jnp.zeros_like(dagain_ref)

        def norm_rows(t, carry):
            sl = pl.ds(pl.multiple_of(t * tile, tile), tile)
            dres = grad_ref[sl].astype(f32) + back_ref[sl].astype(f32)
            out = proj_ref[sl].astype(f32)
            inv = lax.rsqrt(jnp.mean(out * out, axis=1, keepdims=True) + norm_eps)
            norm = out * inv
            dagain_ref[...] += jnp.sum(dres * norm, axis=0, keepdims=True)
            dnorm = dres * again_ref[...]
            dot = jnp.mean(dnorm * norm, axis=1, keepdims=True)
            dproj[sl] = (inv * (dnorm - norm * dot)).astype(bf16)
            return carry

        lax.fori_loop(0, rows // tile, norm_rows, 0)
        for h in range(local // sub):
            dout[:, h * sub : (h + 1) * sub] = dot_nt(
                dproj[...], w_ref[h * sub : (h + 1) * sub, :]
            ).astype(bf16)
        lane = lax.broadcasted_iota(jnp.int32, (rows, lanes), 1)
        acc = jnp.zeros((rows, lanes), f32)
        for h in range(heads):
            hs = slice(h * head_dim, (h + 1) * head_dim)
            row_sum = jnp.sum(
                dout[:, hs].astype(f32) * attn_ref[:, hs].astype(f32), axis=1, keepdims=True
            )
            acc = jnp.where(lane == h, row_sum, acc)
        columns[...] = acc
        delta[...] = jnp.transpose(columns[...])[:8]
        dqs[...] = jnp.zeros_like(dqs)

        def c0(h):
            slot = lax.rem(h, 2)
            return remote(send0.at[slot], recv0.at[h], s0.at[slot], d0.at[h], mate)

        def c1(h, d):
            to = lax.rem(mx + d, nx)
            return remote(
                recv0.at[h, to], recv1.at[h, d - 1], s1.at[h, d - 1], d1.at[h, d - 1],
                {"ctx": to * 2 + core},
            )

        def one_block(h, hs, x, owner, write):
            start = (x * 2 + owner) * rows
            for part in range(rows // sub):
                ks = pl.ds(pl.multiple_of(start + part * sub, sub), sub)
                key, value = k_ref[ks, hs], v_ref[ks, hs]
                query, dhead = q_ref[:, hs], dout[:, hs]
                score = dot_nt(key, query) * scale
                place = order_ref[0, (x * 2 + owner) * 2 + part] * sub
                seen = place + lax.broadcasted_iota(jnp.int32, (sub, rows), 0) <= prow_ref[...]
                share = jnp.where(seen, jnp.exp(score - lse_ref[pl.ds(h, 1), :]), 0.0)
                dshare = dot_nt(value, dhead)
                dscore = share * (dshare - delta[pl.ds(h, 1), :]) * scale
                high = dscore.astype(bf16)
                low = (dscore - high.astype(f32)).astype(bf16)
                dqs[:, hs] += dot_tn(high, key) + dot_tn(low, key)
                write(
                    x, slice(part * sub, (part + 1) * sub),
                    jnp.dot(high, query, preferred_element_type=f32)
                    + jnp.dot(low, query, preferred_element_type=f32),
                    jnp.dot(share.astype(bf16), dhead, preferred_element_type=f32),
                )

        def one_head(h):
            hs = pl.ds(pl.multiple_of(h * head_dim, head_dim), head_dim)
            slot = lax.rem(h, 2)

            def to_send(x, rs, dk, dv):
                send0[slot, x, rs, :lanes] = dk.astype(bf16)
                send0[slot, x, rs, lanes:] = dv.astype(bf16)

            def to_keep(x, rs, dk, dv):
                keep[slot, x, rs, :lanes] = dk.astype(bf16)
                keep[slot, x, rs, lanes:] = dv.astype(bf16)

            @pl.when(h >= 2)
            def _():
                c0(h).wait_send()

            def mates(e, carry):
                one_block(h, hs, lax.rem(mx + 1 + e, nx), 1 - core, to_send)
                return carry

            lax.fori_loop(0, nx, mates, 0)
            c0(h).start()
            tick(2 * h + 1)

            def owns(e, carry):
                one_block(h, hs, lax.rem(mx + 1 + e, nx), core, to_keep)
                return carry

            lax.fori_loop(0, nx, owns, 0)
            c0(h).wait_recv()

            def add(x, carry):
                recv0[h, x] = (keep[slot, x].astype(f32) + recv0[h, x].astype(f32)).astype(bf16)
                return carry

            lax.fori_loop(0, nx, add, 0)
            for d in range(1, nx):
                c1(h, d).start()
            tick(2 * h + 2)

        def heads_loop(h, carry):
            one_head(h)
            return carry

        lax.fori_loop(0, heads, heads_loop, 0)
        if jobs:

            def more(it, carry):
                grads.tick(it)
                return carry

            lax.fori_loop(2 * heads + 1, grads.steps, more, 0)

        dot_q = jnp.zeros((rows, 1), f32)
        for h in range(heads):
            hs = slice(h * head_dim, (h + 1) * head_dim)
            dq = dqs[:, hs]
            dq = dq * cos_ref[...] - pltpu.roll(dq, head_dim // 2, 1) * sin_ref[...]
            norm = qn_ref[:, hs]
            dqg_ref[:, hs] = jnp.sum(dq * norm, axis=0, keepdims=True)
            dq = dq * qg_ref[:, hs]
            dqs[:, hs] = dq
            dot_q = dot_q + jnp.sum(dq * norm, axis=1, keepdims=True)
        dprojt_ref[...] = jnp.transpose(dproj[...])
        dot_k = jnp.zeros((rows, 1), f32)
        for h in range(heads):
            hs = slice(h * head_dim, (h + 1) * head_dim)
            total = recv0[h, mx].astype(f32)
            for d in range(1, nx):
                c1(h, d).wait_recv()
                total = total + recv1[h, d - 1].astype(f32)
            dqkv_ref[:, 2 * local + h * head_dim : 2 * local + (h + 1) * head_dim] = total[
                :, lanes:
            ].astype(bf16)
            dk = total[:, :lanes]
            dk = dk * cos_ref[...] - pltpu.roll(dk, head_dim // 2, 1) * sin_ref[...]
            norm = kn_ref[:, hs]
            dkg_ref[:, hs] = jnp.sum(dk * norm, axis=0, keepdims=True)
            dk = dk * kg_ref[:, hs]
            dks[:, hs] = dk
            dot_k = dot_k + jnp.sum(dk * norm, axis=1, keepdims=True)
        dots = small.total(lane_pair(dot_q, dot_k, rows)) * (1.0 / width)
        for h in range(heads):
            hs = slice(h * head_dim, (h + 1) * head_dim)
            dqkv_ref[:, hs] = (
                sc_ref[:, 0:1] * (dqs[:, hs] - qn_ref[:, hs] * dots[:, 0:1])
            ).astype(bf16)
            dqkv_ref[:, local + h * head_dim : local + (h + 1) * head_dim] = (
                sc_ref[:, 1:2] * (dks[:, hs] - kn_ref[:, hs] * dots[:, 1:2])
            ).astype(bf16)
        for h in range(heads):
            if h >= heads - 2:
                c0(h).wait_send()
            for d in range(1, nx):
                c1(h, d).wait_send()
        if jobs:
            grads.drain()

    sem = pltpu.SemaphoreType.DMA
    pair = (rows, 2 * lanes)
    return comm_call(
        body,
        [back, grad, proj, attn_gain, w_output, query_rot, keys, values, attn, lse, pos_row,
         order, query_norm, key_norm, scales, qgain, kgain, cosine, sine] + ats + bs,
        [
            jax.ShapeDtypeStruct((rows, 3 * local), bf16),
            jax.ShapeDtypeStruct((width, rows), bf16),
            jax.ShapeDtypeStruct((1, width), f32),
            jax.ShapeDtypeStruct((1, local), f32),
            jax.ShapeDtypeStruct((1, local), f32),
        ] + [jax.ShapeDtypeStruct(*out) for out in (grads.out_shapes(widths) if jobs else [])],
        [
            pltpu.VMEM((rows, width), bf16), pltpu.VMEM((rows, local), bf16),
            pltpu.VMEM((rows, lanes), f32), pltpu.VMEM((8, rows), f32),
            pltpu.VMEM((rows, local), f32), pltpu.VMEM((rows, local), f32),
            pltpu.VMEM((2, nx) + pair, bf16), pltpu.VMEM((2, nx) + pair, bf16),
            pltpu.VMEM((heads, nx) + pair, bf16), pltpu.VMEM((heads, nx - 1) + pair, bf16),
            sem((2,)), sem((heads,)), sem((heads, nx - 1)), sem((heads, nx - 1)),
        ] + small.scratch() + (grads.scratch() if jobs else []),
        cid, "attention_back", {11},
    )


def front(tokens, w_query, w_key, w_value, qgain, kgain, cosine, sine, order, cid):
    rows, width = tokens.shape
    local = w_query.shape[1]
    head_dim = lanes
    heads = local // head_dim
    nx = lax.axis_size("ctx") // 2
    count = nx * 2 * rows
    n_tp = lax.axis_size("tp")
    small = LineSmall(n_tp, rows)
    n_small = len(small.scratch())
    scale = head_dim ** (-0.5)
    group = rows // 2

    def body(
        tok_hbm, wq_hbm, wk_hbm, wv_hbm, qg_ref, kg_ref, cos_ref, sin_ref, order_ref,
        qrot_out, key_out, value_out, qn_out, kn_out, attn_out, tokt_out, sc_out, lse_out,
        tok, tokt, w3, qn, kn, qrot, keys, values, peak, total, acc, attn, loads, stores,
        sx, dx, sm, dm, sf, df, *rest,
    ):
        small.bind(rest[:n_small])
        copies = [
            pltpu.make_async_copy(src, dst, loads.at[i])
            for i, (src, dst) in enumerate(
                [(tok_hbm, tok), (wv_hbm, w3.at[2]), (wq_hbm, w3.at[0]), (wk_hbm, w3.at[1])]
            )
        ]
        for copy in copies:
            copy.start()
        ctx = lax.axis_index("ctx")
        mx, core = ctx // 2, lax.rem(ctx, 2)
        mate = {"ctx": mx * 2 + 1 - core}

        def peer(d):
            return {"ctx": lax.rem(mx + d, nx) * 2 + core}

        bar = pltpu.get_barrier_semaphore()
        pl.semaphore_signal(bar, inc=1, device_id=mate, device_id_type=MESH)
        for d in range(1, nx):
            pl.semaphore_signal(bar, inc=1, device_id=peer(d), device_id_type=MESH)
        peers = small.greet(bar) + nx

        def at(x, owner):
            return pl.ds(pl.multiple_of((x * 2 + owner) * rows, rows), rows)

        mine = at(mx, core)
        side = local // 2
        boxes = [(keys, pl.ds(0, side)), (keys, pl.ds(side, side)), (values, pl.ds(0, local))]

        def move(t, rs, sent, done, where):
            box, cols = boxes[t]
            return remote(box.at[rs, cols], box.at[rs, cols], sent, done, where)

        def to_peer(t, d):
            return move(t, mine, sx.at[t, d - 1], dx.at[t, d - 1], peer(d))

        def from_peer(t, d):
            rs = at(lax.rem(mx + nx - d, nx), core)
            return move(t, rs, sx.at[t, d - 1], dx.at[t, d - 1], peer(d))

        def to_mate(t):
            return move(t, mine, sm.at[t], dm.at[t], mate)

        def from_mate(t):
            return move(t, at(mx, 1 - core), sm.at[t], dm.at[t], mate)

        def pass_on(t, d):
            rs = at(lax.rem(mx + nx - d, nx), core)
            return move(t, rs, sf.at[t, d - 1], df.at[t, d - 1], mate)

        def passed(t, d):
            rs = at(lax.rem(mx + nx - d, nx), 1 - core)
            return move(t, rs, sf.at[t, d - 1], df.at[t, d - 1], mate)

        def each_peer(act):
            def one(d, carry):
                act(d)
                return carry

            lax.fori_loop(1, nx, one, 0)

        copies[0].wait()
        copies[1].wait()
        values[mine] = jnp.dot(tok[...], w3[2], preferred_element_type=f32).astype(bf16)
        pl.semaphore_wait(bar, peers)
        each_peer(lambda d: to_peer(2, d).start())
        to_mate(2).start()
        copies[2].wait()
        qn[...] = jnp.dot(tok[...], w3[0], preferred_element_type=f32)
        copies[3].wait()
        kn[...] = jnp.dot(tok[...], w3[1], preferred_element_type=f32)

        def squares(ref):
            acc_sq = jnp.zeros((rows, 1), f32)
            for h in range(heads):
                part = ref[:, h * head_dim : (h + 1) * head_dim]
                acc_sq = acc_sq + jnp.sum(part * part, axis=1, keepdims=True)
            return acc_sq

        def transpose_tokens():
            tokt[...] = jnp.transpose(tok[...])

        sums = small.total(lane_pair(squares(qn), squares(kn), rows), transpose_tokens)
        scales = lax.rsqrt(sums * (1.0 / width) + norm_eps)
        sc_out[...] = scales

        def rotated(ref, column, gain_ref, h):
            hs = slice(h * head_dim, (h + 1) * head_dim)
            norm = ref[:, hs] * sc_out[:, column : column + 1]
            ref[:, hs] = norm
            norm = norm * gain_ref[:, hs]
            return (
                norm * cos_ref[...] + pltpu.roll(norm, head_dim // 2, 1) * sin_ref[...]
            ).astype(bf16)

        for h in range(heads):
            keys[mine, h * head_dim : (h + 1) * head_dim] = rotated(kn, 1, kg_ref, h)
            if (h + 1) * head_dim in (side, local):
                t = (h + 1) * head_dim // side - 1
                each_peer(lambda d: to_peer(t, d).start())
                to_mate(t).start()
        for h in range(heads):
            qrot[:, h * head_dim : (h + 1) * head_dim] = rotated(qn, 0, qg_ref, h)
        peak[...] = jnp.full_like(peak, masked_score)
        total[...] = jnp.zeros_like(total)
        acc[...] = jnp.zeros_like(acc)

        def places(block, shape, axis):
            spot = lax.broadcasted_iota(jnp.int32, shape, axis)
            first, second = order_ref[0, block * 2], order_ref[0, block * 2 + 1]
            return jnp.where(spot < group, first * group + spot, (second - 1) * group + spot)

        def attend(x, owner, low, high):
            block = x * 2 + owner
            rs = at(x, owner)

            def one(h, carry):
                hs = pl.ds(pl.multiple_of(h * head_dim, head_dim), head_dim)
                score = dot_nt(qrot[:, hs], keys[rs, hs]) * scale
                seen = places(block, (1, rows), 1) <= places(ctx, (rows, 1), 0)
                old = peak[h]
                new = jnp.maximum(
                    old, jnp.max(jnp.where(seen, score, masked_score), axis=1, keepdims=True)
                )
                share = jnp.where(seen, jnp.exp(score - new), 0.0)
                fade = jnp.exp(old - new)
                peak[h] = new
                total[h] = total[h] * fade + jnp.sum(share, axis=1, keepdims=True)
                acc[:, hs] = acc[:, hs] * fade + jnp.dot(
                    share.astype(bf16), values[rs, hs], preferred_element_type=f32
                )
                return carry

            lax.fori_loop(low, high, one, 0)

        attend(mx, core, 0, heads)

        def hand_on(t, d):
            from_peer(t, d).wait_recv()
            pass_on(t, d).start()

        each_peer(lambda d: hand_on(2, d))
        for t in range(3):
            from_mate(t).wait_recv()
        attend(mx, 1 - core, 0, heads)

        def half_heads(t, carry):
            low, high = t * heads // 2, (t + 1) * heads // 2

            def near(d):
                for v in range(2):

                    @pl.when(t == v)
                    def _():
                        hand_on(v, d)

                attend(lax.rem(mx + nx - d, nx), core, low, high)

            def far(d):
                @pl.when(t == 0)
                def _():
                    passed(2, d).wait_recv()
                    passed(0, d).wait_recv()

                @pl.when(t == 1)
                def _():
                    passed(1, d).wait_recv()

                attend(lax.rem(mx + nx - d, nx), 1 - core, low, high)

            each_peer(near)
            each_peer(far)
            return carry

        lax.fori_loop(0, 2, half_heads, 0)

        lane = lax.broadcasted_iota(jnp.int32, (rows, lanes), 1)
        logs = jnp.zeros((rows, lanes), f32)
        for h in range(heads):
            hs = slice(h * head_dim, (h + 1) * head_dim)
            attn[:, hs] = (acc[:, hs] / total[h]).astype(bf16)
            logs = jnp.where(lane == h, peak[h] + jnp.log(total[h]), logs)
        lse_out[...] = jnp.transpose(logs)[:8]
        outs = [
            pltpu.make_async_copy(src, dst, stores.at[i])
            for i, (src, dst) in enumerate(
                [(qrot, qrot_out), (keys, key_out), (values, value_out), (qn, qn_out),
                 (kn, kn_out), (attn, attn_out), (tokt, tokt_out)]
            )
        ]
        for copy in outs:
            copy.start()
        for copy in outs:
            copy.wait()
        for t in range(3):
            to_mate(t).wait_send()

            def sent(d):
                to_peer(t, d).wait_send()
                pass_on(t, d).wait_send()

            each_peer(sent)

    sem = pltpu.SemaphoreType.DMA
    hbm = pl.BlockSpec(memory_space=pl.ANY)
    block = jax.ShapeDtypeStruct
    return pl.pallas_call(
        body,
        out_shape=[
            block((rows, local), bf16), block((count, local), bf16), block((count, local), bf16),
            block((rows, local), f32), block((rows, local), f32), block((rows, local), bf16),
            block((width, rows), bf16),
            block((rows, lanes), f32), block((8, rows), f32),
        ],
        in_specs=[hbm] * 4 + [vmem_spec()] * 4 + [pl.BlockSpec(memory_space=pltpu.SMEM)],
        out_specs=[hbm] * 7 + [vmem_spec()] * 2,
        scratch_shapes=[
            pltpu.VMEM((rows, width), bf16), pltpu.VMEM((width, rows), bf16),
            pltpu.VMEM((3, width, local), bf16),
            pltpu.VMEM((rows, local), f32),
            pltpu.VMEM((rows, local), f32), pltpu.VMEM((rows, local), bf16),
            pltpu.VMEM((count, local), bf16), pltpu.VMEM((count, local), bf16),
            pltpu.VMEM((heads, rows, 1), f32), pltpu.VMEM((heads, rows, 1), f32),
            pltpu.VMEM((rows, local), f32), pltpu.VMEM((rows, local), bf16),
            sem((4,)), sem((7,)),
            sem((3, nx - 1)), sem((3, nx - 1)), sem((3,)), sem((3,)),
            sem((3, nx - 1)), sem((3, nx - 1)),
        ] + small.scratch(),
        compiler_params=pltpu.CompilerParams(
            collective_id=cid, has_side_effects=True, vmem_limit_bytes=62 * 2**20
        ),
        name="front",
    )(tokens, w_query, w_key, w_value, qgain, kgain, cosine, sine, order)


def load_list(pairs, sems, base=0):
    copies = [
        pltpu.make_async_copy(src, dst, sems.at[base + i]) for i, (src, dst) in enumerate(pairs)
    ]
    for copy in copies:
        copy.start()
    return copies


def kernel_call(body, args, kinds, outs, out_kinds, scratch, cid, name):
    spec = {
        "v": vmem_spec(),
        "h": pl.BlockSpec(memory_space=pl.ANY),
        "s": pl.BlockSpec(memory_space=pltpu.SMEM),
    }
    return pl.pallas_call(
        body,
        out_shape=[jax.ShapeDtypeStruct(*out) for out in outs],
        in_specs=[spec[kind] for kind in kinds],
        out_specs=[spec[kind] for kind in out_kinds],
        scratch_shapes=scratch,
        compiler_params=pltpu.CompilerParams(
            collective_id=cid, has_side_effects=True, vmem_limit_bytes=62 * 2**20
        ),
        name=name,
    )(*args)


def middle(attn, tokens, attn_gain, w_output, w_gate, w_up, w_down, cid):
    rows, width = tokens.shape
    local, wide = w_output.shape[0], w_gate.shape[1]
    n_tp = lax.axis_size("tp")
    line = LineSum(n_tp, 2 * rows, width, 4 * row_chains)
    n_line = len(line.scratch())
    half = rows // 2
    tile = 64
    cut = 512
    n_cut = wide // cut
    part = line.part

    def body(
        attn_hbm, tok_hbm, again_ref, wo_hbm, wg_hbm, wu_hbm, wd_hbm,
        proj_out, hidt_out, gate_out, up_out, inner_out, down_out, inv_out,
        attn_v, tok, wo, hid, hidt, gate, up, inner, wg, wu, wd, first, loads, stores, *rest,
    ):
        line.bind(rest[:n_line])
        start = load_list([(attn_hbm, attn_v), (wo_hbm, wo), (tok_hbm, tok)], first)

        def load(src, dst, j, size, spot):
            cols = pl.ds(pl.multiple_of(j * size, size), size)
            return pltpu.make_async_copy(src.at[:, cols], dst.at[j], loads.at[spot])

        def gate_load(j):
            return load(wg_hbm, wg, j, cut, 2 * j)

        def up_load(j):
            return load(wu_hbm, wu, j, cut, 2 * j + 1)

        def down_load(j):
            return load(wd_hbm, wd, j, part, 2 * n_cut + j)

        for j in range(n_cut):
            gate_load(j).start()
            up_load(j).start()
        for j in range(n_tp):
            down_load(j).start()
        bar = pltpu.get_barrier_semaphore()
        peers = line.greet(bar)
        for copy in start:
            copy.wait()

        def project(j, carry):
            cols = pl.ds(pl.multiple_of(j * part, part), part)
            line.own[j, :rows] = jnp.dot(
                attn_v[...], wo[:, cols], preferred_element_type=f32
            ).astype(bf16)
            return carry

        lax.fori_loop(0, n_tp, project, 0)
        pl.semaphore_wait(bar, peers)

        def step(t, carry):
            line.step(t)

            @pl.when(t == 3 * n_tp + 1)
            def _():
                hidt[...] = jnp.transpose(hid[...])

            return carry

        def row_half(c, carry):
            base = pl.multiple_of(c * half, half)
            sl = pl.ds(base, half)
            lax.fori_loop(c * 2 * n_tp, c * n_tp + 2 * n_tp - 1, step, 0)

            def norm_rows(t, carry):
                rs = pl.ds(pl.multiple_of(base + t * tile, tile), tile)
                outs = [line.res[j, rs].astype(f32) for j in range(n_tp)]
                square = sum(jnp.sum(out * out, axis=1, keepdims=True) for out in outs)
                inv = lax.rsqrt(square * (1.0 / width) + norm_eps)
                inv_out[rs, :] = inv
                for j, out in enumerate(outs):
                    cols = slice(j * part, (j + 1) * part)
                    hid[rs, cols] = (
                        tok[rs, cols].astype(f32) + out * inv * again_ref[:, cols]
                    ).astype(bf16)
                return carry

            lax.fori_loop(0, half // tile, norm_rows, 0)
            per = row_chains // n_cut

            def widen(j, carry):
                cols = pl.ds(pl.multiple_of(j * cut, cut), cut)

                @pl.when(c == 0)
                def _():
                    gate_load(j).wait()
                    up_load(j).wait()

                g = jnp.dot(hid[sl], wg[j], preferred_element_type=f32)
                u = jnp.dot(hid[sl], wu[j], preferred_element_type=f32)
                gate[sl, cols] = g.astype(bf16)
                up[sl, cols] = u.astype(bf16)
                inner[sl, cols] = (g * jax.nn.sigmoid(g) * u).astype(bf16)
                line.pieces(((c + 2) * n_tp - 1) * row_chains + j * per, per)
                return carry

            lax.fori_loop(0, n_cut, widen, 0)
            line.pieces(((c + 2) * n_tp - 1) * row_chains + n_cut * per, row_chains - n_cut * per)

            def narrow(j, carry):
                @pl.when(c == 0)
                def _():
                    down_load(j).wait()

                line.own[j, pl.ds(rows + base, half)] = jnp.dot(
                    inner[sl], wd[j], preferred_element_type=f32
                ).astype(bf16)
                return carry

            lax.fori_loop(0, n_tp, narrow, 0)
            return carry

        lax.fori_loop(0, 2, row_half, 0)
        outs = load_list([(gate, gate_out), (up, up_out), (inner, inner_out)], stores)
        ready = line.ship(proj_out, stores, 4, 0, rows)
        lax.fori_loop(3 * n_tp, line.steps, step, 0)
        last = pltpu.make_async_copy(hidt, hidt_out, stores.at[3])
        last.start()
        ready = ready + line.ship(down_out, stores, 4 + n_tp, rows, rows)
        line.drain()
        for copy in outs + [last] + ready:
            copy.wait()

    sem = pltpu.SemaphoreType.DMA
    return kernel_call(
        body, [attn, tokens, attn_gain, w_output, w_gate, w_up, w_down], "hhvhhhh",
        [((rows, width), bf16), ((width, rows), bf16), ((rows, wide), bf16), ((rows, wide), bf16),
         ((rows, wide), bf16), ((rows, width), bf16), ((rows, 1), f32)],
        "hhhhhhv",
        [
            pltpu.VMEM((rows, local), bf16), pltpu.VMEM((rows, width), bf16),
            pltpu.VMEM((local, width), bf16),
            pltpu.VMEM((rows, width), bf16), pltpu.VMEM((width, rows), bf16),
            pltpu.VMEM((rows, wide), bf16), pltpu.VMEM((rows, wide), bf16),
            pltpu.VMEM((rows, wide), bf16),
            pltpu.VMEM((n_cut, width, cut), bf16), pltpu.VMEM((n_cut, width, cut), bf16),
            pltpu.VMEM((n_tp, wide, part), bf16),
            sem((3,)), sem((2 * n_cut + n_tp,)), sem((4 + 2 * n_tp,)),
        ] + line.scratch(),
        cid, "middle",
    )


def mlp_back(down, grad, mlp_gain, gate, up, inner, hid_t, w_gate, w_up, w_down, jobs, widths, cid):
    rows, width = down.shape
    wide = gate.shape[1]
    n_tp = lax.axis_size("tp")
    line = LineSum(n_tp, rows, width)
    grads = GradScatter(lax.axis_size("ctx"), lax.axis_size("seq"), width, jobs)
    n_line, n_grads, n_out = len(line.scratch()), len(grads.scratch()), len(widths)
    tile = 64
    cut = 512
    n_cut = wide // cut
    part = line.part
    lead = row_chains * n_tp // (n_cut + n_tp)
    ticks = n_cut // 2 + n_tp // 2

    def body(
        down_hbm, grad_hbm, mgain_ref, gate_hbm, up_hbm, inner_hbm, hidt_hbm, wg_hbm, wu_hbm, wd_hbm,
        back_out, dgate_out, dup_out, dgain_out, inv_out, *rest,
    ):
        grad_outs, rest = rest[:n_out], rest[n_out:]
        (gate_v, up_v, inner_v, hidt, ddown, ddownt, dgate, dup, ring, loads, wsem, stores) = rest[:12]
        line.bind(rest[12 : 12 + n_line])
        grads.bind(rest[12 + n_line :], [ddownt, hidt], [inner_v, dgate, dup], grad_outs)

        def fetch(src, index):
            return pltpu.make_async_copy(src, ring.at[index], wsem.at[index])

        def rows_of(ref, j, size):
            return ref.at[pl.ds(pl.multiple_of(j * size, size), size)]

        for j in range(4):
            fetch(rows_of(wd_hbm, j, cut), j).start()
        down_ref, grad_ref = dgate.at[:, pl.ds(0, width)], dup.at[:, pl.ds(0, width)]
        first = load_list([(down_hbm, down_ref), (grad_hbm, grad_ref)], loads, 4)
        early = load_list(
            [(inner_hbm, inner_v), (gate_hbm, gate_v), (up_hbm, up_v), (hidt_hbm, hidt)], loads
        )
        bar = pltpu.get_barrier_semaphore()
        peers = line.greet(bar) + grads.greet(bar)
        dgain_out[...] = jnp.zeros_like(dgain_out)
        for copy in first:
            copy.wait()

        def norm_rows(t, carry):
            sl = pl.ds(pl.multiple_of(t * tile, tile), tile)
            out = down_ref[sl].astype(f32)
            upstream = grad_ref[sl].astype(f32)
            inv = lax.rsqrt(jnp.mean(out * out, axis=1, keepdims=True) + norm_eps)
            norm = out * inv
            inv_out[sl, :] = inv
            dgain_out[...] += jnp.sum(upstream * norm, axis=0, keepdims=True)
            dnorm = upstream * mgain_ref[...]
            dot = jnp.mean(dnorm * norm, axis=1, keepdims=True)
            ddown[sl] = (inv * (dnorm - norm * dot)).astype(bf16)
            return carry

        lax.fori_loop(0, rows // tile, norm_rows, 0)
        ddownt[...] = jnp.transpose(ddown[...])
        for copy in early:
            copy.wait()
        pl.semaphore_wait(bar, peers)

        half = rows // 2

        def row_half(c, carry):
            sl = pl.ds(pl.multiple_of(c * half, half), half)

            def beside(i, j, first):
                @pl.when(c == 1)
                def _():
                    line.pieces(i * lead, lead)

                @pl.when(lax.rem(j, 2) == 1)
                def _():
                    grads.tick(first + j // 2)

            def inner_back(j, carry):
                fetch(rows_of(wd_hbm, j, cut), j).wait()
                cols = pl.ds(pl.multiple_of(j * cut, cut), cut)
                dmix = dot_nt(ddown[sl], ring[j])
                g, u = gate_v[sl, cols].astype(f32), up_v[sl, cols].astype(f32)
                sig = jax.nn.sigmoid(g)
                dgate[sl, cols] = (dmix * u * sig * (1.0 + g * (1.0 - sig))).astype(bf16)
                dup[sl, cols] = (dmix * (g * sig)).astype(bf16)

                @pl.when(lax.rem(j, 2) == 0)
                def _():
                    fetch(rows_of(wg_hbm, j // 2, part), j).start()

                @pl.when(lax.rem(j, 2) == 1)
                def _():
                    fetch(rows_of(wu_hbm, j // 2, part), j).start()

                beside(j, j, c * ticks)
                return carry

            lax.fori_loop(0, n_cut, inner_back, 0)

            def hidden_back(j, carry):
                slot = lax.rem(2 * j, 4)
                fetch(rows_of(wg_hbm, j, part), slot).wait()
                fetch(rows_of(wu_hbm, j, part), slot + 1).wait()
                line.own[j, sl] = (
                    dot_nt(dgate[sl], ring[slot]) + dot_nt(dup[sl], ring[slot + 1])
                ).astype(bf16)

                @pl.when(j + 2 < n_tp)
                def _():
                    fetch(rows_of(wg_hbm, j + 2, part), slot).start()
                    fetch(rows_of(wu_hbm, j + 2, part), slot + 1).start()

                @pl.when((j + 2 >= n_tp) & (c == 0))
                def _():
                    fetch(rows_of(wd_hbm, slot, cut), slot).start()
                    fetch(rows_of(wd_hbm, slot + 1, cut), slot + 1).start()

                beside(n_cut + j, j, c * ticks + n_cut // 2)
                return carry

            lax.fori_loop(0, n_tp, hidden_back, 0)
            return carry

        lax.fori_loop(0, 2, row_half, 0)
        outs = load_list([(dgate, dgate_out), (dup, dup_out)], stores)
        done, used = 2 * ticks, (n_cut + n_tp) * lead

        def one(it, carry):
            line.pieces(used + (it - done) * pace, pace)
            grads.tick(it)
            return carry

        line_its = -(-(line.steps * row_chains - used) // pace)
        lax.fori_loop(done, max(done + line_its, grads.steps), one, 0)
        outs += line.ship(back_out, stores, 2, 0, rows)
        line.drain()
        grads.drain()
        for copy in outs:
            copy.wait()

    sem = pltpu.SemaphoreType.DMA
    return kernel_call(
        body, [down, grad, mlp_gain, gate, up, inner, hid_t, w_gate, w_up, w_down], "hhvhhhhhhh",
        [((rows, width), bf16), ((rows, wide), bf16), ((rows, wide), bf16), ((1, width), f32),
         ((rows, 1), f32)]
        + grads.out_shapes(widths),
        "hhhvv" + "v" * n_out,
        [
            pltpu.VMEM((rows, wide), bf16), pltpu.VMEM((rows, wide), bf16),
            pltpu.VMEM((rows, wide), bf16), pltpu.VMEM((width, rows), bf16),
            pltpu.VMEM((rows, width), bf16), pltpu.VMEM((width, rows), bf16),
            pltpu.VMEM((rows, wide), bf16), pltpu.VMEM((rows, wide), bf16),
            pltpu.VMEM((4, cut, width), bf16),
            sem((6,)), sem((4,)), sem((2 + n_tp,)),
        ] + line.scratch() + grads.scratch(),
        cid, "mlp_back",
    )


def last_sums(dqkv, w_query, w_key, w_value, ats, bs, jobs, widths, gains, cid):
    rows = dqkv.shape[0]
    width, local = w_query.shape
    n_ctx, n_seq = lax.axis_size("ctx"), lax.axis_size("seq")
    n_tp = lax.axis_size("tp")
    line = LineSum(n_tp, rows, width)
    grads = GradScatter(n_ctx, n_seq, width, jobs)
    small = GainSum(n_ctx, n_seq, gains.shape[0])
    na, nb, n_out = len(ats), len(bs), len(widths)
    n_line, n_grads = len(line.scratch()), len(grads.scratch())
    part = line.part

    def body(dqkv_ref, wq_ref, wk_ref, wv_ref, *refs):
        at_refs, b_refs = refs[:na], refs[na : na + nb]
        gain_ref, last_out = refs[na + nb], refs[na + nb + 1]
        refs = refs[na + nb + 2 :]
        grad_outs, gain_out, stores, scratch = refs[:n_out], refs[n_out], refs[n_out + 1], refs[n_out + 2 :]
        line.bind(scratch[:n_line])
        grads.bind(scratch[n_line : n_line + n_grads], at_refs, list(b_refs) + [dqkv_ref], grad_outs)
        small.bind(scratch[n_line + n_grads :], gain_ref, gain_out)
        bar = pltpu.get_barrier_semaphore()
        peers = line.greet(bar) + small.greet(bar)
        pl.semaphore_wait(bar, peers)
        small.start()

        def input_back(j, carry):
            rs = pl.ds(pl.multiple_of(j * part, part), part)
            line.own[j] = (
                dot_nt(dqkv_ref[:, :local], wq_ref[rs])
                + dot_nt(dqkv_ref[:, local : 2 * local], wk_ref[rs])
                + dot_nt(dqkv_ref[:, 2 * local :], wv_ref[rs])
            ).astype(bf16)

            @pl.when(lax.rem(j, 2) == 0)
            def _():
                grads.tick(j // 2)

            return carry

        lax.fori_loop(0, n_tp, input_back, 0)
        done = n_tp // 2

        def one(it, carry):
            grads.tick(it)
            line.pieces((it - done) * pace, pace)
            return carry

        line_steps = -(-line.steps * row_chains // pace)
        lax.fori_loop(done, max(done + line_steps, grads.steps), one, 0)
        small.finish()
        outs = line.ship(last_out, stores, 0, 0, rows)
        line.drain()
        grads.drain()
        for copy in outs:
            copy.wait()

    sem = pltpu.SemaphoreType.DMA
    return kernel_call(
        body, [dqkv, w_query, w_key, w_value] + list(ats) + list(bs) + [gains],
        "vvvv" + "v" * (na + nb + 1),
        [((rows, width), bf16)] + grads.out_shapes(widths) + [(gains.shape, f32)],
        "h" + "v" * (n_out + 1),
        [sem((n_tp,))] + line.scratch() + grads.scratch() + small.scratch(),
        cid, "last_sums",
    )


def row_tiles(body, args, outs, name):
    count = 4

    def spec(shape):
        if shape[0] == 1:
            return pl.BlockSpec(shape, lambda i: (0, 0))
        return pl.BlockSpec((shape[0] // count, shape[1]), lambda i: (i, 0))

    def whole(*refs):
        body(refs[: len(args)], refs[len(args) :])

    return pl.pallas_call(
        whole,
        grid=(count,),
        out_shape=[jax.ShapeDtypeStruct(shape, f32) for shape in outs],
        in_specs=[spec(arg.shape) for arg in args],
        out_specs=[spec(shape) for shape in outs],
        compiler_params=pltpu.CompilerParams(vmem_limit_bytes=62 * 2**20),
        name=name,
    )(*args)


def block_tile(ins, outs):
    x, a, ra, ga, d, rd, gd = [ref[...].astype(f32) for ref in ins[:7]]
    outs[0][...] = x + (a * ra) * ga + (d * rd) * gd
    for src, dst in zip(ins[7:], outs[1:]):
        dst[...] = src[...]


def input_tile(ins, outs):
    outs[0][...] = ins[0][...].astype(f32) + ins[1][...].astype(f32) + ins[2][...].astype(f32)
    outs[1][...] = ins[3][...]
    outs[2][...] = ins[4][...]
    size = outs[3].shape[1]
    for i in range(3):
        outs[3 + i][...] = ins[5][:, i * size : (i + 1) * size]


def per_device(
    tokens,
    out_grad,
    group_order,
    w_query,
    w_key,
    w_value,
    query_gain,
    key_gain,
    w_output,
    attn_gain,
    w_gate,
    w_up,
    w_down,
    mlp_gain,
):
    inputs = tokens[0]
    upstream = out_grad[0]
    rows, width = inputs.shape
    heads, head_dim = query_gain.shape
    local = heads * head_dim
    wide = w_gate.shape[1]
    positions = key_positions(group_order[0], lax.axis_index("ctx") * rows, rows, rows // 2)
    angle_cos, angle_sin = rope_tables(positions, head_dim)
    qgain = query_gain.reshape(1, local)
    kgain = key_gain.reshape(1, local)
    (query_rot, keys, values, query_norm, key_norm, attn, tokens_t, scales, lse) = front(
        inputs, w_query, w_key, w_value, qgain, kgain, angle_cos, angle_sin, group_order, 1
    )
    proj, hidden_t, gate, up, inner, down, proj_scale = middle(
        attn, inputs, attn_gain[None], w_output, w_gate, w_up, w_down, 2
    )
    chunk_cols = 2 * lanes
    chunks = wide // chunk_cols
    thin = local // chunk_cols
    back, d_gate, d_up, d_mlp_gain, down_scale, grad_down, grad_gate = mlp_back(
        down, upstream, mlp_gain[None], gate, up, inner, hidden_t, w_gate, w_up, w_down,
        [
            dict(a=0, b=0, first=0, count=chunks, out=0, place=0, flip=True),
            dict(a=1, b=1, first=0, count=chunks, out=1, place=0, flip=False),
        ],
        [wide, wide],
        3,
    )
    d_qkv, d_proj_t, d_attn_gain, d_query_gain, d_key_gain = attention_back(
        back, upstream, proj, attn_gain[None], w_output, query_rot, keys, values, attn, lse,
        positions[None], group_order, query_norm, key_norm, scales, qgain, kgain, angle_cos,
        angle_sin, [], [], [], [], 4,
    )
    owners = lax.axis_size("ctx") * lax.axis_size("seq")
    gains = [d_attn_gain, d_mlp_gain, d_query_gain, d_key_gain]
    ends = [gain.shape[1] for gain in gains]
    ends = [sum(ends[: i + 1]) for i in range(4)]
    packed = jnp.concatenate(gains, axis=1).reshape(-1, lanes)
    last, grad_up, grad_qkv, grad_output, small = last_sums(
        d_qkv, w_query, w_key, w_value,
        [hidden_t, tokens_t, d_proj_t],
        [d_up, attn],
        [
            dict(a=0, b=0, first=0, count=chunks, out=0, place=0, flip=False),
            dict(a=2, b=1, first=0, count=thin, out=2, place=0, flip=True),
            dict(a=1, b=2, first=0, count=3 * thin, out=1, place=0, flip=False),
        ],
        [wide, 3 * local, local],
        packed,
        5,
    )
    small = small.reshape(-1)
    me = lax.axis_index("ctx") * lax.axis_size("seq") + lax.axis_index("seq")

    def my_part(start, end, lead):
        whole = small[start:end].reshape(lead, -1)
        size = whole.shape[1] // owners
        return lax.dynamic_slice_in_dim(whole, me * size, size, 1)

    g_attn = my_part(0, ends[0], 1)[0]
    g_mlp = my_part(ends[0], ends[1], 1)[0]
    g_query = my_part(ends[1], ends[2], heads)
    g_key = my_part(ends[2], ends[3], heads)
    block_out, grad_down, grad_gate = row_tiles(
        block_tile,
        [inputs, proj, proj_scale, attn_gain[None], down, down_scale, mlp_gain[None], grad_down,
         grad_gate],
        [inputs.shape, grad_down.shape, grad_gate.shape], "block_out",
    )
    own = grad_qkv.shape[0]
    input_grad, grad_up, grad_output, grad_query, grad_key, grad_value = row_tiles(
        input_tile, [upstream, back, last, grad_up, grad_output, grad_qkv],
        [inputs.shape, grad_up.shape, grad_output.shape] + [(own, local)] * 3, "input_grad",
    )
    return (
        block_out[None],
        input_grad[None],
        grad_query,
        grad_key,
        grad_value,
        g_query,
        g_key,
        grad_output,
        g_attn,
        grad_gate,
        grad_up,
        grad_down,
        g_mlp,
    )


def solution(mesh):
    return jax.shard_map(
        per_device,
        mesh=mesh,
        in_specs=(
            P("seq", "ctx", None),
            P("seq", "ctx", None),
            P("seq", None),
            P(None, "tp"),
            P(None, "tp"),
            P(None, "tp"),
            P("tp", None),
            P("tp", None),
            P("tp", None),
            P(),
            P(None, "tp"),
            P(None, "tp"),
            P("tp", None),
            P(),
        ),
        out_specs=(
            P("seq", "ctx", None),
            P("seq", "ctx", None),
            P(("ctx", "seq"), "tp"),
            P(("ctx", "seq"), "tp"),
            P(("ctx", "seq"), "tp"),
            P("tp", ("ctx", "seq")),
            P("tp", ("ctx", "seq")),
            P("tp", ("ctx", "seq")),
            P(("ctx", "seq")),
            P(("ctx", "seq"), "tp"),
            P(("ctx", "seq"), "tp"),
            P("tp", ("ctx", "seq")),
            P(("ctx", "seq")),
        ),
        check_vma=False,
    )
```
